32 devices in a mesh: fsdp: 32 (over z, y, x, core).
Axes of the slice: x: 2, y: 2, z: 4, core: 2. Of those that a mesh axis runs over, the one named last changes fastest.
Arguments:
- tokens: bfloat16 [2, 128, 128, 1536], P(None, 'fsdp'), may hold values from -6 to 6
- in_weight: bfloat16 [1536, 6448], P('fsdp'), may hold values from -0.15625 to 0.15625
- conv_weight: bfloat16 [3328, 4], P('fsdp'), may hold values from -3 to 3
- conv_bias: bfloat16 [3328], P('fsdp'), may hold values from -3 to 3
- dt_bias: float32 [48], replicated, may hold values from -6.5 to -4.5
- a_log: float32 [48], replicated, may hold values from 0 to 2.8
- skip_d: float32 [48], replicated, may hold values from 0.5 to 1.5
- norm_scale: bfloat16 [1536], P('fsdp'), may hold values from 0.5 to 1.5
- gate_scale: bfloat16 [3072], P('fsdp'), may hold values from 0.5 to 1.5
- out_weight: bfloat16 [3072, 1536], P('fsdp'), may hold values from -0.109375 to 0.109375
- grad_out: bfloat16 [2, 128, 128, 1536], P(None, 'fsdp'), may hold values from -6 to 6
Outputs:
- output: bfloat16 [2, 128, 128, 1536], P(None, 'fsdp')
- d_tokens: float32 [2, 128, 128, 1536], P(None, 'fsdp')
- d_in_weight: float32 [1536, 6448], P('fsdp')
- d_conv_weight: float32 [3328, 4], P('fsdp')
- d_conv_bias: float32 [3328], P('fsdp')
- d_dt_bias: float32 [48], replicated
- d_a_log: float32 [48], replicated
- d_skip_d: float32 [48], replicated
- d_norm_scale: float32 [1536], P('fsdp')
- d_gate_scale: float32 [3072], P('fsdp')
- d_out_weight: float32 [3072, 1536], P('fsdp')
The draws below stay inside these ranges and needn't reach their ends.
All inputs are finite; a program needn't handle non-finite values.
Results may differ from the reference program's by a relative error of at most 0.0093.
Values may be sent and summed in bfloat16 or wider, within the bound.
A program may use at most 320 MiB of HBM per device.

```python
import jax
import jax.numpy as jnp
from jax import lax

D = 1536
H = 48
KW = 4
L = 128
MB = 2
SEQ_MB = 4
DI = 3072
CONVCH = 3328
E = 6448
BATCH = 128


def shard_levels(own_key, dims, pieces, low, top_value):
    loudness = 1.0
    for position, parts in pieces:
        draws = jax.random.uniform(jax.random.fold_in(jax.random.fold_in(own_key, 6), position), (parts,), jnp.float32, low / len(pieces), top_value / len(pieces))
        loudness = loudness * jnp.repeat(jnp.exp(draws), dims[position] // parts).reshape((-1,) + (1,) * (len(dims) - 1 - position))
    return loudness


def bell_draw(rng, dims, scale, bound, shards=(), held_as=jnp.bfloat16):
    loudness = shard_levels(rng, dims, shards, -0.22, 0.18) if shards else 1.0
    entries = jax.random.normal(rng, dims, jnp.float32) * scale * loudness
    return jnp.minimum(jnp.maximum(entries, -bound), bound).astype(held_as)


def setup_inputs(seed: int = 0) -> dict:
    arg_keys = jax.random.split(jax.random.key(seed), 12)
    return {
        "tokens": bell_draw(arg_keys[0], (MB, BATCH, L, D), 1.0, 6.0, ((1, 32),)),
        "in_weight": bell_draw(arg_keys[1], (D, E), D ** -0.5, 0.15625, ((0, 32),)),
        "conv_weight": bell_draw(arg_keys[2], (CONVCH, KW), KW ** -0.5, 3.0, ((0, 32),)),
        "conv_bias": bell_draw(arg_keys[3], (CONVCH,), 0.5, 3.0, ((0, 32),)),
        "dt_bias": jnp.clip(jax.random.uniform(arg_keys[4], (H,), jnp.float32, -6.5, -4.5), -6.5, -4.5),
        "a_log": jnp.clip(jax.random.uniform(arg_keys[5], (H,), jnp.float32, 0.0, 2.8), 0.0, 2.8),
        "skip_d": jnp.clip(jax.random.uniform(arg_keys[6], (H,), jnp.float32, 0.5, 1.5), 0.5, 1.5),
        "norm_scale": jnp.clip(1.0 + 0.1 * jax.random.normal(arg_keys[7], (D,), jnp.float32), 0.5, 1.5).astype(jnp.bfloat16),
        "gate_scale": jnp.clip(1.0 + 0.1 * jax.random.normal(arg_keys[8], (DI,), jnp.float32), 0.5, 1.5).astype(jnp.bfloat16),
        "out_weight": bell_draw(arg_keys[9], (DI, D), DI ** -0.5, 0.109375, ((0, 32),)),
        "grad_out": bell_draw(arg_keys[10], (MB, BATCH, L, D), 1.0, 6.0, ((1, 32),)),
    }


epsilon = 1e-05

def batched(form, left, right):
    return jnp.einsum(form, left.astype(jnp.float32), right.astype(jnp.float32))

def silu_grad(value):
    sigma = jax.nn.sigmoid(value)
    return sigma * (1.0 + value * (1.0 - sigma))

def layer_forward(block, weights, params):
    in_weight, conv_weight, conv_bias, norm_scale, gate_scale, out_weight = weights
    dt_bias, a_log, skip_d = params
    seq_count, seq_length, width = block.shape
    inner_width = out_weight.shape[0]
    head_count = a_log.shape[0]
    head_dim = inner_width // head_count
    channels = conv_weight.shape[0]
    state_width = (channels - inner_width) // 2
    kernel_width = conv_weight.shape[1]
    row_count = seq_count * seq_length
    u_full = block.astype(jnp.float32)
    rstd_in = lax.rsqrt(lax.optimization_barrier(jnp.mean(u_full * u_full, axis=-1, keepdims=True)) + epsilon)
    u_hat = u_full * rstd_in
    normed = (u_hat * norm_scale.astype(jnp.float32)).astype(jnp.bfloat16).reshape(row_count, width)
    projected = jnp.dot(normed, in_weight, preferred_element_type=jnp.float32).astype(jnp.bfloat16)
    gate_in = projected[:, :inner_width].astype(jnp.float32).reshape(seq_count, seq_length, inner_width)
    conv_in = projected[:, inner_width:inner_width + channels].reshape(seq_count, seq_length, channels)
    dt_raw = projected[:, inner_width + channels:].astype(jnp.float32).reshape(seq_count, seq_length, head_count)
    conv_pad = jnp.pad(conv_in, ((0, 0), (kernel_width - 1, 0), (0, 0))).astype(jnp.float32)
    taps = conv_weight.astype(jnp.float32)
    conv_out = jnp.zeros((seq_count, seq_length, channels), jnp.float32) + conv_bias.astype(jnp.float32)
    for offset in range(kernel_width):
        conv_out = conv_out + conv_pad[:, offset:offset + seq_length, :] * taps[:, offset]
    active = jax.nn.silu(conv_out).astype(jnp.bfloat16)
    x_heads = active[..., :inner_width].reshape(seq_count, seq_length, head_count, head_dim)
    b_mat = active[..., inner_width:inner_width + state_width]
    c_mat = active[..., inner_width + state_width:]
    dt_pre = dt_raw + dt_bias
    step_size = jax.nn.softplus(dt_pre)
    decay_rate = -jnp.exp(a_log)
    step_heads = jnp.transpose(step_size, (0, 2, 1))
    log_decay = jnp.cumsum(step_heads * decay_rate[:, None], axis=-1)
    causal = jnp.arange(seq_length)[:, None] >= jnp.arange(seq_length)[None, :]
    spread = log_decay[..., :, None] - log_decay[..., None, :]
    decay = jnp.where(causal, jnp.exp(jnp.minimum(spread, 0.0)), 0.0)
    scores = batched('sln,smn->slm', c_mat, b_mat)
    mixing = (scores[:, None] * decay * step_heads[:, :, None, :]).astype(jnp.bfloat16)
    ssd = batched('shtr,srhp->sthp', mixing, x_heads) + skip_d[:, None] * x_heads.astype(jnp.float32)
    ssd = ssd.reshape(seq_count, seq_length, inner_width)
    gate_act = jax.nn.silu(gate_in)
    gated = ssd * gate_act
    rstd_gate = lax.rsqrt(lax.optimization_barrier(jnp.mean(gated * gated, axis=-1, keepdims=True)) + epsilon)
    gated_hat = gated * rstd_gate
    mixed = (gated_hat * gate_scale.astype(jnp.float32)).astype(jnp.bfloat16).reshape(row_count, inner_width)
    branch = jnp.dot(mixed, out_weight, preferred_element_type=jnp.float32)
    output = (u_full.reshape(row_count, width) + branch).astype(jnp.bfloat16).reshape(seq_count, seq_length, width)
    saved = (u_hat, rstd_in, normed, gate_in, conv_pad, conv_out, x_heads, b_mat, c_mat, dt_pre, step_heads, decay_rate, decay, scores, mixing, ssd, gate_act, gated_hat, rstd_gate, mixed)
    return (output, saved)

def layer_backward(grad_block, saved, weights, params):
    in_weight, conv_weight, conv_bias, norm_scale, gate_scale, out_weight = weights
    dt_bias, a_log, skip_d = params
    u_hat, rstd_in, normed, gate_in, conv_pad, conv_out, x_heads, b_mat, c_mat, dt_pre, step_heads, decay_rate, decay, scores, mixing, ssd, gate_act, gated_hat, rstd_gate, mixed = saved
    seq_count, seq_length, width = grad_block.shape
    inner_width = out_weight.shape[0]
    head_count = a_log.shape[0]
    head_dim = inner_width // head_count
    kernel_width = conv_weight.shape[1]
    row_count = seq_count * seq_length
    grad_rows = grad_block.reshape(row_count, width)
    d_out_weight = jnp.dot(mixed.T, grad_rows, preferred_element_type=jnp.float32)
    d_mixed = jnp.dot(grad_rows, out_weight.T, preferred_element_type=jnp.float32).reshape(seq_count, seq_length, inner_width)
    d_gate_scale = lax.optimization_barrier(jnp.sum(d_mixed * gated_hat, axis=(0, 1)))
    d_hat = d_mixed * gate_scale.astype(jnp.float32)
    d_gated = rstd_gate * (d_hat - gated_hat * lax.optimization_barrier(jnp.mean(d_hat * gated_hat, axis=-1, keepdims=True)))
    d_ssd = d_gated * gate_act
    d_gate_in = d_gated * ssd * silu_grad(gate_in)
    d_ssd_heads = d_ssd.reshape(seq_count, seq_length, head_count, head_dim)
    d_ssd_low = d_ssd_heads.astype(jnp.bfloat16)
    d_skip = lax.optimization_barrier(jnp.sum(d_ssd_heads * x_heads.astype(jnp.float32), axis=(0, 1, 3)))
    d_x_heads = batched('shtr,sthp->srhp', mixing, d_ssd_low) + skip_d[:, None] * d_ssd_heads
    d_mixing = batched('sthp,srhp->shtr', d_ssd_low, x_heads)
    path = d_mixing * decay
    d_scores = lax.optimization_barrier(jnp.sum(path * step_heads[:, :, None, :], axis=1)).astype(jnp.bfloat16)
    through = path * scores[:, None]
    weighted = through * step_heads[:, :, None, :]
    d_log = lax.optimization_barrier(jnp.sum(weighted, axis=3)) - lax.optimization_barrier(jnp.sum(weighted, axis=2))
    d_steps = lax.cumsum(d_log, axis=2, reverse=True)
    d_step_heads = lax.optimization_barrier(jnp.sum(through, axis=2)) + d_steps * decay_rate[:, None]
    d_a_log = lax.optimization_barrier(jnp.sum(d_steps * step_heads, axis=(0, 2))) * decay_rate
    d_dt_raw = jnp.transpose(d_step_heads, (0, 2, 1)) * jax.nn.sigmoid(dt_pre)
    d_dt_bias = lax.optimization_barrier(jnp.sum(d_dt_raw, axis=(0, 1)))
    d_c_mat = batched('slm,smn->sln', d_scores, b_mat)
    d_b_mat = batched('slm,sln->smn', d_scores, c_mat)
    d_active = jnp.concatenate([d_x_heads.reshape(seq_count, seq_length, inner_width), d_b_mat, d_c_mat], axis=-1)
    d_conv_out = d_active * silu_grad(conv_out)
    d_conv_bias = lax.optimization_barrier(jnp.sum(d_conv_out, axis=(0, 1)))
    taps = conv_weight.astype(jnp.float32)
    d_conv_weight = jnp.stack([lax.optimization_barrier(jnp.sum(d_conv_out * conv_pad[:, offset:offset + seq_length, :], axis=(0, 1))) for offset in range(kernel_width)], axis=1)
    d_pad = jnp.pad(d_conv_out, ((0, 0), (0, kernel_width - 1), (0, 0)))
    d_conv_in = jnp.zeros_like(d_conv_out)
    for offset in range(kernel_width):
        begin = kernel_width - 1 - offset
        d_conv_in = d_conv_in + taps[:, offset] * d_pad[:, begin:begin + seq_length, :]
    d_projected = jnp.concatenate([d_gate_in, d_conv_in, d_dt_raw], axis=-1).astype(jnp.bfloat16).reshape(row_count, -1)
    d_in_weight = jnp.dot(normed.T, d_projected, preferred_element_type=jnp.float32)
    d_normed = jnp.dot(d_projected, in_weight.T, preferred_element_type=jnp.float32).reshape(seq_count, seq_length, width)
    d_norm_scale = lax.optimization_barrier(jnp.sum(d_normed * u_hat, axis=(0, 1)))
    d_uhat = d_normed * norm_scale.astype(jnp.float32)
    d_input = grad_block.astype(jnp.float32) + rstd_in * (d_uhat - u_hat * lax.optimization_barrier(jnp.mean(d_uhat * u_hat, axis=-1, keepdims=True)))
    grads = (d_in_weight, d_conv_weight, d_conv_bias, d_norm_scale, d_gate_scale, d_out_weight)
    return (d_input, grads, (d_dt_bias, d_a_log, d_skip))

def reference(tokens, in_weight, conv_weight, conv_bias, dt_bias, a_log, skip_d, norm_scale, gate_scale, out_weight, grad_out):
    block_count = MB * BATCH // SEQ_MB
    token_blocks = tokens.reshape(block_count, SEQ_MB, L, D)
    grad_blocks = grad_out.reshape(block_count, SEQ_MB, L, D)
    weights = (in_weight, conv_weight, conv_bias, norm_scale, gate_scale, out_weight)
    params = (dt_bias, a_log, skip_d)
    totals = tuple((jnp.zeros(w.shape, jnp.float32) for w in weights))
    head_totals = tuple((jnp.zeros(p.shape, jnp.float32) for p in params))

    def advance(carry, pair):
        grad_sums, head_sums = carry
        output, saved = layer_forward(pair[0], weights, params)
        d_input, grads, head_grads = layer_backward(pair[1], saved, weights, params)
        grad_sums = jax.tree.map(jnp.add, grad_sums, grads)
        head_sums = jax.tree.map(jnp.add, head_sums, head_grads)
        return ((grad_sums, head_sums), (output, d_input))
    (totals, head_totals), (outputs, d_inputs) = lax.scan(advance, (totals, head_totals), (token_blocks, grad_blocks))
    return (outputs.reshape(MB, BATCH, L, D), d_inputs.reshape(MB, BATCH, L, D), totals[0], totals[1], totals[2], head_totals[0], head_totals[1], head_totals[2], totals[3], totals[4], totals[5])
```

```python
import functools

import jax
import jax.numpy as jnp
from jax import lax
from jax.experimental import pallas as pl
from jax.experimental.pallas import tpu as pltpu
from jax.sharding import PartitionSpec as P

epsilon = 1e-05
LOG2E = 1.4426950408889634
BIG = 3.0e38
LANES = 128
FRONT = 8
f32 = jnp.float32
bf16 = jnp.bfloat16
UNROLL_F = 2
UNROLL_B = 2


def sigmoid(v):
    return 0.5 * jnp.tanh(0.5 * v) + 0.5


def sum8(v):
    rows, lanes = v.shape
    return jnp.sum(v.reshape(rows // 8, 8, lanes), axis=0)


def iotas(rows, lanes):
    return (
        lax.broadcasted_iota(jnp.int32, (rows, lanes), 0),
        lax.broadcasted_iota(jnp.int32, (rows, lanes), 1),
    )


def step_stage(dims, proj, hpar, dtp):
    T, DI, C, H = dims["T"], dims["DI"], dims["C"], dims["H"]
    dtp[...] = jnp.zeros_like(dtp)
    dtp[:, 0:H] = proj[:, DI + C : DI + C + H].astype(f32)
    v = dtp[...] + hpar[0:1, :]
    e = jnp.exp(-jnp.abs(v))
    step = jnp.maximum(v, 0.0) + jnp.log1p(e)
    row, col = iotas(T, T)
    tri = (row >= col).astype(f32)
    ld = jnp.dot(
        tri, step * (hpar[1:2, :] * LOG2E), precision=lax.Precision.HIGHEST,
        preferred_element_type=f32,
    )
    return v, e, step, ld, ld - jnp.log2(step)


def conv_tile(dims, proj, cpar, pad, c0):
    T, DI, KW = dims["T"], dims["DI"], dims["KW"]
    lanes = pl.ds(c0, LANES)
    cin = proj[:, pl.ds(DI + c0, LANES)].astype(f32)
    pad[FRONT : FRONT + T, :] = cin
    out = cpar[KW : KW + 1, lanes] + cin * cpar[KW - 1 : KW, lanes]
    for k in range(KW - 1):
        out = out + pad[FRONT - KW + 1 + k : FRONT - KW + 1 + k + T, :] * cpar[k : k + 1, lanes]
    return out


def stack_heads(dims, v):
    T, HD = dims["T"], dims["HD"]
    _, lane = iotas(T, LANES)
    zero = jnp.zeros_like(v)
    return jnp.concatenate(
        [jnp.where(lane // HD == a, v, zero) for a in range(LANES // HD)], axis=0
    )


def mix_forward(dims, proj, cpar, hpar, dpar, mixed, ssd, rstd,
                pad, gated, colb, rowb, mask, scores, acc, dtp):
    T, DI, H, HD, ST = dims["T"], dims["DI"], dims["H"], dims["HD"], dims["ST"]
    HP = LANES // HD
    tiles = DI // LANES
    pad[:, 0:FRONT, :] = jnp.zeros((pad.shape[0], FRONT, LANES), f32)
    _, _, _, ld, ld2 = step_stage(dims, proj, hpar, dtp)
    row, col = iotas(T, T)
    mask[...] = jnp.where(col <= row, BIG, -BIG)
    rowb[...] = ld2.T
    for h in range(H):
        colb[h] = jnp.broadcast_to(ld[:, h : h + 1], (T, LANES))
    bc = []
    for a in range(2):
        conv = conv_tile(dims, proj, cpar, pad.at[a], DI + a * ST)
        bc.append((conv * sigmoid(conv)).astype(bf16))
    scores[...] = lax.dot_general(
        bc[1], bc[0], (((1,), (1,)), ((), ())), preferred_element_type=f32
    )
    acc[...] = jnp.zeros_like(acc)

    def tile(j, u):
        c0 = pl.multiple_of(j * LANES, LANES)
        lanes = pl.ds(c0, LANES)
        conv = conv_tile(dims, proj, cpar, pad.at[u], c0)
        x = (conv * sigmoid(conv)).astype(bf16)
        mix = []
        for a in range(HP):
            h = j * HP + a
            expo = jnp.minimum(colb[h] - rowb[pl.ds(h, 1), :], mask[...])
            mix.append((jnp.exp2(expo) * scores[...]).astype(bf16))
        core = jnp.dot(
            jnp.concatenate(mix, axis=1), stack_heads(dims, x), preferred_element_type=f32
        )
        out = core + dpar[1:2, lanes] * x.astype(f32)
        ssd[:, lanes] = out
        gate = proj[:, lanes].astype(f32)
        g = out * (gate * sigmoid(gate))
        gated[:, lanes] = g
        return g * g

    def body(j, _):
        total = tile(j * UNROLL_F, 0)
        for u in range(1, UNROLL_F):
            total = total + tile(j * UNROLL_F + u, u)
        acc[...] += total
        return 0

    lax.fori_loop(0, tiles // UNROLL_F, body, 0)
    r = lax.rsqrt(jnp.sum(acc[...], axis=1, keepdims=True) * (1.0 / DI) + epsilon)
    rb = jnp.broadcast_to(r, (T, LANES))
    rstd[...] = rb

    def finish(j, _):
        lanes = pl.ds(pl.multiple_of(j * LANES, LANES), LANES)
        mixed[:, lanes] = (gated[:, lanes] * rb * dpar[0:1, lanes]).astype(bf16)
        return 0

    lax.fori_loop(0, tiles, finish, 0)


def mix_backward(dims, proj, dmixed, ssd, rstd, cpar, hpar, dpar, dproj, cacc, dacc, hacc,
                 pad, dpad, colb, rowb, mask, scores, acc, dtp, dscores, dlog, csum, bcs):
    T, DI, C, H, HD, ST, KW = (dims[k] for k in ("T", "DI", "C", "H", "HD", "ST", "KW"))
    HP = LANES // HD
    tiles = DI // LANES

    @pl.when(pl.program_id(0) == 0)
    def _():
        cacc[...] = jnp.zeros_like(cacc)
        dacc[...] = jnp.zeros_like(dacc)
        hacc[...] = jnp.zeros_like(hacc)

    pad[:, 0:FRONT, :] = jnp.zeros((pad.shape[0], FRONT, LANES), f32)
    dpad[:, T:, :] = jnp.zeros((dpad.shape[0], FRONT, LANES), f32)
    v, e, step, ld, ld2 = step_stage(dims, proj, hpar, dtp)
    row, col = iotas(T, T)
    mask[...] = jnp.where(row <= col, BIG, -BIG)
    rowb[...] = ld.T
    for h in range(H):
        colb[h] = jnp.broadcast_to(ld2[:, h : h + 1], (T, LANES))
    for a in range(2):
        conv = conv_tile(dims, proj, cpar, pad.at[a], DI + a * ST)
        bcs[a] = (conv * sigmoid(conv)).astype(bf16)
    scores[...] = lax.dot_general(
        bcs[0], bcs[1], (((1,), (1,)), ((), ())), preferred_element_type=f32
    )
    acc[...] = jnp.zeros_like(acc)
    dscores[...] = jnp.zeros_like(dscores)
    dlog[...] = jnp.zeros_like(dlog)
    csum[...] = jnp.zeros_like(csum)
    rb = rstd[...]

    def first(j, _):
        lanes = pl.ds(pl.multiple_of(j * LANES, LANES), LANES)
        gate = proj[:, lanes].astype(f32)
        p = dmixed[:, lanes] * (ssd[:, lanes] * (gate * sigmoid(gate)))
        acc[...] += p * dpar[0:1, lanes]
        dacc[0:8, lanes] += sum8(p * rb)
        return 0

    lax.fori_loop(0, tiles, first, 0)
    mean = jnp.sum(acc[...], axis=1, keepdims=True) * (1.0 / DI)
    mb = jnp.broadcast_to(mean, (T, LANES)) * rb * rb * rb
    acc[...] = mb

    def conv_back(c0, dact, conv, sig, u):
        lanes = pl.ds(c0, LANES)
        dconv = dact * (sig * (1.0 + conv * (1.0 - sig)))
        dpad[u, 0:T, :] = dconv
        dcin = dconv * cpar[KW - 1 : KW, lanes]
        for k in range(KW - 1):
            dcin = dcin + dpad[u, KW - 1 - k : KW - 1 - k + T, :] * cpar[k : k + 1, lanes]
        dproj[:, pl.ds(DI + c0, LANES)] = dcin.astype(bf16)
        for k in range(KW):
            start = FRONT - KW + 1 + k
            cacc[8 * k : 8 * k + 8, lanes] += sum8(dconv * pad[u, start : start + T, :])
        cacc[8 * KW : 8 * KW + 8, lanes] += sum8(dconv)

    def tile(j, u):
        c0 = pl.multiple_of(j * LANES, LANES)
        lanes = pl.ds(c0, LANES)
        conv = conv_tile(dims, proj, cpar, pad.at[u], c0)
        sig = sigmoid(conv)
        x = (conv * sig).astype(bf16)
        xf = x.astype(f32)
        gate = proj[:, lanes].astype(f32)
        gs = sigmoid(gate)
        act = gate * gs
        out = ssd[:, lanes]
        r = rstd[...]
        dgated = r * (dmixed[:, lanes] * dpar[0:1, lanes]) - (out * act) * acc[...]
        dssd = dgated * act
        dproj[:, lanes] = (dgated * out * (gs * (1.0 + gate * (1.0 - gs)))).astype(bf16)
        low = dssd.astype(bf16)
        dacc[8:16, lanes] += sum8(dssd * xf)
        lows = stack_heads(dims, low)
        dmix = lax.dot_general(
            x, lows, (((1,), (1,)), ((), ())), preferred_element_type=f32
        )
        mix = []
        part = None
        for a in range(HP):
            h = j * HP + a
            decay = jnp.exp2(jnp.minimum(rowb[pl.ds(h, 1), :] - colb[h], mask[...]))
            mix.append((decay * scores[...]).astype(bf16))
            term = dmix[:, a * T : (a + 1) * T] * decay
            part = term if part is None else part + term
        core = jnp.dot(jnp.concatenate(mix, axis=1), lows, preferred_element_type=f32)
        skip = dpar[1:2, lanes]
        from_cols = xf * core
        diff = low.astype(f32) * (out - skip * xf) - from_cols
        prow, pcol = iotas(LANES, LANES)
        place = (pcol == j * HP + prow // HD).astype(bf16)
        place = jnp.concatenate([place, place], axis=0)

        def by_head(w):
            hi = w.astype(bf16)
            lo = (w - hi.astype(f32)).astype(bf16)
            return jnp.dot(
                jnp.concatenate([hi, lo], axis=1), place, preferred_element_type=f32
            )

        conv_back(c0, core + skip * dssd, conv, sig, u)
        return part, by_head(diff), by_head(from_cols)

    def body(j, _):
        sums = tile(j * UNROLL_B, 0)
        for u in range(1, UNROLL_B):
            sums = tuple(p + q for p, q in zip(sums, tile(j * UNROLL_B + u, u)))
        dscores[...] += sums[0]
        dlog[...] += sums[1]
        csum[...] += sums[2]
        return 0

    lax.fori_loop(0, tiles // UNROLL_B, body, 0)
    ds = dscores[...].astype(bf16)
    dst = dscores[...].T.astype(bf16)
    dact = (
        jnp.dot(ds, bcs[1], preferred_element_type=f32),
        jnp.dot(dst, bcs[0], preferred_element_type=f32),
    )
    for a in range(2):
        conv = conv_tile(dims, proj, cpar, pad.at[a], DI + a * ST)
        conv_back(DI + a * ST, dact[a], conv, sigmoid(conv), a)
    dsteps = jnp.dot(
        (row <= col).astype(f32), dlog[...], precision=lax.Precision.HIGHEST,
        preferred_element_type=f32,
    )
    sg = jnp.where(v >= 0.0, 1.0, e) / (1.0 + e)
    ratio = jnp.where(step > 1e-30, sg / jnp.maximum(step, 1e-30), 1.0)
    ddt = csum[...] * ratio + dsteps * hpar[1:2, :] * sg
    dproj[:, DI + C : DI + C + H] = ddt[:, 0:H].astype(bf16)
    hacc[0:8, :] += sum8(ddt)
    hacc[8:16, :] += sum8(dsteps * step)


def run_forward(dims, proj, cpar, hpar, dpar):
    T, DI, C, H, KW = dims["T"], dims["DI"], dims["C"], dims["H"], dims["KW"]
    R, E = proj.shape
    rows = lambda w: pl.BlockSpec((T, w), lambda i: (i, 0))
    whole = lambda a: pl.BlockSpec(a.shape, lambda i: (0, 0))
    return pl.pallas_call(
        functools.partial(mix_forward, dims),
        grid=(R // T,),
        in_specs=[rows(E), whole(cpar), whole(hpar), whole(dpar)],
        out_specs=[rows(DI), rows(DI), rows(LANES)],
        out_shape=[
            jax.ShapeDtypeStruct((R, DI), bf16),
            jax.ShapeDtypeStruct((R, DI), f32),
            jax.ShapeDtypeStruct((R, LANES), f32),
        ],
        scratch_shapes=[
            pltpu.VMEM((max(2, UNROLL_F), FRONT + T, LANES), f32),
            pltpu.VMEM((T, DI), f32),
            pltpu.VMEM((H, T, LANES), f32),
            pltpu.VMEM((LANES, T), f32),
            pltpu.VMEM((T, T), f32),
            pltpu.VMEM((T, T), f32),
            pltpu.VMEM((T, LANES), f32),
            pltpu.VMEM((T, LANES), f32),
        ],
        compiler_params=pltpu.CompilerParams(vmem_limit_bytes=48 << 20),
        cost_estimate=pl.CostEstimate(
            flops=4 * R * DI * T, bytes_accessed=R * (2 * E + 6 * DI), transcendentals=R * H * T
        ),
        name="mix_forward",
    )(proj, cpar, hpar, dpar)


def run_backward(dims, proj, dmixed, ssd, rstd, cpar, hpar, dpar):
    T, DI, C, H, KW, ST = (dims[k] for k in ("T", "DI", "C", "H", "KW", "ST"))
    R, E = proj.shape
    rows = lambda w: pl.BlockSpec((T, w), lambda i: (i, 0))
    whole = lambda s: pl.BlockSpec(s, lambda i: (0, 0))
    sums = [(8 * (KW + 1), C), (16, DI), (16, LANES)]
    return pl.pallas_call(
        functools.partial(mix_backward, dims),
        grid=(R // T,),
        in_specs=[rows(E), rows(DI), rows(DI), rows(LANES)]
        + [whole(a.shape) for a in (cpar, hpar, dpar)],
        out_specs=[rows(E)] + [whole(s) for s in sums],
        out_shape=[jax.ShapeDtypeStruct((R, E), bf16)]
        + [jax.ShapeDtypeStruct(s, f32) for s in sums],
        scratch_shapes=[
            pltpu.VMEM((max(2, UNROLL_B), FRONT + T, LANES), f32),
            pltpu.VMEM((max(2, UNROLL_B), FRONT + T, LANES), f32),
            pltpu.VMEM((H, T, LANES), f32),
            pltpu.VMEM((LANES, T), f32),
            pltpu.VMEM((T, T), f32),
            pltpu.VMEM((T, T), f32),
            pltpu.VMEM((T, LANES), f32),
            pltpu.VMEM((T, LANES), f32),
            pltpu.VMEM((T, T), f32),
            pltpu.VMEM((T, LANES), f32),
            pltpu.VMEM((T, LANES), f32),
            pltpu.VMEM((2, T, ST), bf16),
        ],
        compiler_params=pltpu.CompilerParams(vmem_limit_bytes=56 << 20),
        cost_estimate=pl.CostEstimate(
            flops=8 * R * DI * T, bytes_accessed=R * (4 * E + 8 * DI), transcendentals=R * H * T
        ),
        name="mix_backward",
    )(proj, dmixed, ssd, rstd, cpar, hpar, dpar)


def local(axis, n, tokens, in_weight, conv_weight, conv_bias, dt_bias, a_log, skip_d,
          norm_scale, gate_scale, out_weight, grad_out):
    MB, S, T, D = tokens.shape
    R = MB * S * T
    E = in_weight.shape[1]
    H = a_log.shape[0]
    DI = out_weight.shape[0] * n
    C = conv_weight.shape[0] * n
    KW = conv_weight.shape[1]
    HD = DI // H
    ST = (C - DI) // 2
    dims = dict(T=T, DI=DI, C=C, H=H, HD=HD, ST=ST, KW=KW)
    assert LANES % HD == 0 and ST == LANES and DI % (LANES * 2) == 0 and T % 16 == 0

    small = jnp.concatenate(
        [conv_weight.reshape(-1), conv_bias, norm_scale, gate_scale]
    )
    smalls = lax.all_gather(small, axis, axis=0)
    c1, c2, c3 = C // n * KW, C // n * (KW + 1), C // n * (KW + 1) + D // n
    conv_w = smalls[:, :c1].reshape(C, KW).astype(f32)
    conv_b = smalls[:, c1:c2].reshape(C).astype(f32)
    norm_s = smalls[:, c2:c3].reshape(1, D).astype(f32)
    gate_s = smalls[:, c3:].reshape(DI).astype(f32)
    in_full = lax.all_gather(in_weight, axis, axis=0, tiled=True)
    out_full = lax.all_gather(out_weight, axis, axis=0, tiled=True)

    u = tokens.reshape(R, D).astype(f32)
    rstd_in = lax.rsqrt(jnp.mean(u * u, axis=-1, keepdims=True) + epsilon)
    normed = (u * rstd_in * norm_s).astype(bf16)
    proj = jnp.dot(normed, in_full, preferred_element_type=f32).astype(bf16)
    rate = -jnp.exp(a_log)
    cpar = jnp.concatenate([conv_w.T, conv_b[None], jnp.zeros((8 - KW - 1, C), f32)], axis=0)
    hpar = jnp.zeros((8, LANES), f32).at[0, :H].set(dt_bias).at[1, :H].set(rate)
    dpar = jnp.concatenate(
        [gate_s[None], jnp.repeat(skip_d, HD)[None], jnp.zeros((6, DI), f32)], axis=0
    )
    mixed, ssd, rstd = run_forward(dims, proj, cpar, hpar, dpar)
    grad_rows = grad_out.reshape(R, D)
    output = (u + jnp.dot(mixed, out_full, preferred_element_type=f32)).astype(bf16)
    d_out_w = lax.dot_general(
        mixed, grad_rows, (((0,), (0,)), ((), ())), preferred_element_type=f32
    ).astype(bf16)
    d_out_w = lax.psum_scatter(d_out_w, axis, scatter_dimension=0, tiled=True)
    d_mixed = lax.dot_general(
        grad_rows, out_full, (((1,), (1,)), ((), ())), preferred_element_type=f32
    )
    dproj, cacc, dacc, hacc = run_backward(dims, proj, d_mixed, ssd, rstd, cpar, hpar, dpar)
    d_in_w = lax.dot_general(
        normed, dproj, (((0,), (0,)), ((), ())), preferred_element_type=f32
    ).astype(bf16)
    d_in_w = lax.psum_scatter(d_in_w, axis, scatter_dimension=0, tiled=True)
    d_normed = lax.dot_general(
        dproj, in_full, (((1,), (1,)), ((), ())), preferred_element_type=f32
    )
    u_hat = u * rstd_in
    d_norm_scale = jnp.sum(d_normed * u_hat, axis=0)
    d_uhat = d_normed * norm_s
    d_tokens = grad_rows.astype(f32) + rstd_in * (
        d_uhat - u_hat * jnp.mean(d_uhat * u_hat, axis=-1, keepdims=True)
    )
    csums = cacc.reshape(KW + 1, 8, C).sum(axis=1)
    dsums = dacc.reshape(2, 8, DI).sum(axis=1)
    hsums = hacc.reshape(2, 8, LANES).sum(axis=1)
    d_skip = dsums[1].reshape(H, HD).sum(axis=1)
    heads = lax.psum(
        jnp.concatenate([hsums[0, :H], hsums[1, :H] * rate, d_skip]), axis
    )
    grads = jnp.concatenate(
        [
            csums[:KW].T.reshape(n, -1),
            csums[KW].reshape(n, -1),
            d_norm_scale.reshape(n, -1),
            dsums[0].reshape(n, -1),
        ],
        axis=1,
    )
    grads = lax.psum_scatter(grads, axis, scatter_dimension=0, tiled=True)[0]
    return (
        output.reshape(tokens.shape),
        d_tokens.reshape(tokens.shape),
        d_in_w.astype(f32),
        grads[:c1].reshape(C // n, KW),
        grads[c1:c2],
        heads[:H],
        heads[H : 2 * H],
        heads[2 * H :],
        grads[c2:c3],
        grads[c3:],
        d_out_w.astype(f32),
    )


def solution(mesh):
    axis = mesh.axis_names[0]
    n = mesh.shape[axis]
    rows, flat, batch = P(axis, None), P(axis), P(None, axis, None, None)
    return jax.shard_map(
        functools.partial(local, axis, n),
        mesh=mesh,
        in_specs=(batch, rows, rows, flat, P(), P(), P(), flat, flat, rows, batch),
        out_specs=(batch, batch, rows, rows, flat, P(), P(), P(), flat, flat, rows),
        check_vma=False,
    )
```

```python
import functools
import math

import jax
import jax.numpy as jnp
from jax import lax
from jax.experimental import pallas as pl
from jax.experimental.pallas import tpu as pltpu
from jax.sharding import PartitionSpec as P

epsilon = 1e-05
LOG2E = 1.4426950408889634
BIG = 3.0e38
LANES = 128
FRONT = 8
f32 = jnp.float32
bf16 = jnp.bfloat16
UNROLL_F = 2
UNROLL_B = 2


def sigmoid(v):
    return 0.5 * jnp.tanh(0.5 * v) + 0.5


def sum8(v):
    rows, lanes = v.shape
    return jnp.sum(v.reshape(rows // 8, 8, lanes), axis=0)


def iotas(rows, lanes):
    return (
        lax.broadcasted_iota(jnp.int32, (rows, lanes), 0),
        lax.broadcasted_iota(jnp.int32, (rows, lanes), 1),
    )


def step_stage(dims, proj, hpar, dtp):
    T, DI, C, H = dims["T"], dims["DI"], dims["C"], dims["H"]
    dtp[...] = jnp.zeros_like(dtp)
    dtp[:, 0:H] = proj[:, DI + C : DI + C + H].astype(f32)
    v = dtp[...] + hpar[0:1, :]
    e = jnp.exp(-jnp.abs(v))
    step = jnp.maximum(v, 0.0) + jnp.log1p(e)
    row, col = iotas(T, T)
    tri = (row >= col).astype(f32)
    ld = jnp.dot(
        tri, step * (hpar[1:2, :] * LOG2E), precision=lax.Precision.HIGHEST,
        preferred_element_type=f32,
    )
    return v, e, step, ld, ld - jnp.log2(step)


def conv_tile(dims, proj, cpar, pad, c0):
    T, DI, KW = dims["T"], dims["DI"], dims["KW"]
    lanes = pl.ds(c0, LANES)
    cin = proj[:, pl.ds(DI + c0, LANES)].astype(f32)
    pad[FRONT : FRONT + T, :] = cin
    out = cpar[KW : KW + 1, lanes] + cin * cpar[KW - 1 : KW, lanes]
    for k in range(KW - 1):
        out = out + pad[FRONT - KW + 1 + k : FRONT - KW + 1 + k + T, :] * cpar[k : k + 1, lanes]
    return out


def stack_heads(dims, v):
    T, HD = dims["T"], dims["HD"]
    _, lane = iotas(T, LANES)
    zero = jnp.zeros_like(v)
    return jnp.concatenate(
        [jnp.where(lane // HD == a, v, zero) for a in range(LANES // HD)], axis=0
    )


def mix_forward(dims, proj, cpar, hpar, dpar, mixed, ssd, rstd,
                pad, gated, colb, rowb, mask, scores, acc, dtp):
    T, DI, H, HD, ST = dims["T"], dims["DI"], dims["H"], dims["HD"], dims["ST"]
    HP = LANES // HD
    tiles = DI // LANES
    pad[:, 0:FRONT, :] = jnp.zeros((pad.shape[0], FRONT, LANES), f32)
    _, _, _, ld, ld2 = step_stage(dims, proj, hpar, dtp)
    row, col = iotas(T, T)
    mask[...] = jnp.where(col <= row, BIG, -BIG)
    rowb[...] = ld2.T
    for h in range(H):
        colb[h] = jnp.broadcast_to(ld[:, h : h + 1], (T, LANES))
    bc = []
    for a in range(2):
        conv = conv_tile(dims, proj, cpar, pad.at[a], DI + a * ST)
        bc.append((conv * sigmoid(conv)).astype(bf16))
    scores[...] = lax.dot_general(
        bc[1], bc[0], (((1,), (1,)), ((), ())), preferred_element_type=f32
    )
    acc[...] = jnp.zeros_like(acc)

    def tile(j, u):
        c0 = pl.multiple_of(j * LANES, LANES)
        lanes = pl.ds(c0, LANES)
        conv = conv_tile(dims, proj, cpar, pad.at[u], c0)
        x = (conv * sigmoid(conv)).astype(bf16)
        mix = []
        for a in range(HP):
            h = j * HP + a
            expo = jnp.minimum(colb[h] - rowb[pl.ds(h, 1), :], mask[...])
            mix.append((jnp.exp2(expo) * scores[...]).astype(bf16))
        core = jnp.dot(
            jnp.concatenate(mix, axis=1), stack_heads(dims, x), preferred_element_type=f32
        )
        out = core + dpar[0:1, lanes] * x.astype(f32)
        ssd[:, lanes] = out
        gate = proj[:, lanes].astype(f32)
        g = out * (gate * sigmoid(gate))
        gated[:, lanes] = g
        return g * g

    def body(j, _):
        total = tile(j * UNROLL_F, 0)
        for u in range(1, UNROLL_F):
            total = total + tile(j * UNROLL_F + u, u)
        acc[...] += total
        return 0

    lax.fori_loop(0, tiles // UNROLL_F, body, 0)
    r = lax.rsqrt(jnp.sum(acc[...], axis=1, keepdims=True) * (1.0 / DI) + epsilon)
    rb = jnp.broadcast_to(r, (T, LANES))
    rstd[...] = rb

    def finish(j, _):
        lanes = pl.ds(pl.multiple_of(j * LANES, LANES), LANES)
        mixed[:, lanes] = (gated[:, lanes] * rb * dpar[1:2, lanes]).astype(bf16)
        return 0

    lax.fori_loop(0, tiles, finish, 0)


def mix_backward(dims, steps, proj, dmixed, ssd, rstd, cpar, hpar, dpar, dproj, small,
                 cacc, dacc, hacc, pad, dpad, colb, rowb, mask, scores, acc, dtp, dscores, dlog, csum, bcs):
    T, DI, C, H, HD, ST, KW = (dims[k] for k in ("T", "DI", "C", "H", "HD", "ST", "KW"))
    HP = LANES // HD
    tiles = DI // LANES

    @pl.when(pl.program_id(0) == 0)
    def _():
        cacc[...] = jnp.zeros_like(cacc)
        dacc[...] = jnp.zeros_like(dacc)
        hacc[...] = jnp.zeros_like(hacc)

    pad[:, 0:FRONT, :] = jnp.zeros((pad.shape[0], FRONT, LANES), f32)
    dpad[:, T:, :] = jnp.zeros((dpad.shape[0], FRONT, LANES), f32)
    v, e, step, ld, ld2 = step_stage(dims, proj, hpar, dtp)
    row, col = iotas(T, T)
    mask[...] = jnp.where(row <= col, BIG, -BIG)
    rowb[...] = ld.T
    for h in range(H):
        colb[h] = jnp.broadcast_to(ld2[:, h : h + 1], (T, LANES))
    for a in range(2):
        conv = conv_tile(dims, proj, cpar, pad.at[a], DI + a * ST)
        bcs[a] = (conv * sigmoid(conv)).astype(bf16)
    scores[...] = lax.dot_general(
        bcs[0], bcs[1], (((1,), (1,)), ((), ())), preferred_element_type=f32
    )
    acc[...] = jnp.zeros_like(acc)
    dscores[...] = jnp.zeros_like(dscores)
    dlog[...] = jnp.zeros_like(dlog)
    csum[...] = jnp.zeros_like(csum)
    rb = rstd[...]

    def first(j, _):
        lanes = pl.ds(pl.multiple_of(j * LANES, LANES), LANES)
        gate = proj[:, lanes].astype(f32)
        p = dmixed[:, lanes] * (ssd[:, lanes] * (gate * sigmoid(gate)))
        acc[...] += p * dpar[1:2, lanes]
        dacc[8:16, lanes] += sum8(p * rb)
        return 0

    lax.fori_loop(0, tiles, first, 0)
    mean = jnp.sum(acc[...], axis=1, keepdims=True) * (1.0 / DI)
    mb = jnp.broadcast_to(mean, (T, LANES)) * rb * rb * rb
    acc[...] = mb

    def conv_back(c0, dact, conv, sig, u):
        lanes = pl.ds(c0, LANES)
        dconv = dact * (sig * (1.0 + conv * (1.0 - sig)))
        dpad[u, 0:T, :] = dconv
        dcin = dconv * cpar[KW - 1 : KW, lanes]
        for k in range(KW - 1):
            dcin = dcin + dpad[u, KW - 1 - k : KW - 1 - k + T, :] * cpar[k : k + 1, lanes]
        dproj[:, pl.ds(DI + c0, LANES)] = dcin.astype(bf16)
        for k in range(KW):
            start = FRONT - KW + 1 + k
            cacc[8 * k : 8 * k + 8, lanes] += sum8(dconv * pad[u, start : start + T, :])
        cacc[8 * KW : 8 * KW + 8, lanes] += sum8(dconv)

    def tile(j, u):
        c0 = pl.multiple_of(j * LANES, LANES)
        lanes = pl.ds(c0, LANES)
        conv = conv_tile(dims, proj, cpar, pad.at[u], c0)
        sig = sigmoid(conv)
        x = (conv * sig).astype(bf16)
        xf = x.astype(f32)
        gate = proj[:, lanes].astype(f32)
        gs = sigmoid(gate)
        act = gate * gs
        out = ssd[:, lanes]
        r = rstd[...]
        dgated = r * (dmixed[:, lanes] * dpar[1:2, lanes]) - (out * act) * acc[...]
        dssd = dgated * act
        dproj[:, lanes] = (dgated * out * (gs * (1.0 + gate * (1.0 - gs)))).astype(bf16)
        low = dssd.astype(bf16)
        dacc[0:8, lanes] += sum8(dssd * xf)
        lows = stack_heads(dims, low)
        dmix = lax.dot_general(
            x, lows, (((1,), (1,)), ((), ())), preferred_element_type=f32
        )
        mix = []
        part = None
        for a in range(HP):
            h = j * HP + a
            decay = jnp.exp2(jnp.minimum(rowb[pl.ds(h, 1), :] - colb[h], mask[...]))
            mix.append((decay * scores[...]).astype(bf16))
            term = dmix[:, a * T : (a + 1) * T] * decay
            part = term if part is None else part + term
        core = jnp.dot(jnp.concatenate(mix, axis=1), lows, preferred_element_type=f32)
        skip = dpar[0:1, lanes]
        from_cols = xf * core
        diff = low.astype(f32) * (out - skip * xf) - from_cols
        prow, pcol = iotas(LANES, LANES)
        place = (pcol == j * HP + prow // HD).astype(bf16)
        place = jnp.concatenate([place, place], axis=0)

        def by_head(w):
            hi = w.astype(bf16)
            lo = (w - hi.astype(f32)).astype(bf16)
            return jnp.dot(
                jnp.concatenate([hi, lo], axis=1), place, preferred_element_type=f32
            )

        conv_back(c0, core + skip * dssd, conv, sig, u)
        return part, by_head(diff), by_head(from_cols)

    def body(j, _):
        sums = tile(j * UNROLL_B, 0)
        for u in range(1, UNROLL_B):
            sums = tuple(p + q for p, q in zip(sums, tile(j * UNROLL_B + u, u)))
        dscores[...] += sums[0]
        dlog[...] += sums[1]
        csum[...] += sums[2]
        return 0

    lax.fori_loop(0, tiles // UNROLL_B, body, 0)
    ds = dscores[...].astype(bf16)
    dst = dscores[...].T.astype(bf16)
    dact = (
        jnp.dot(ds, bcs[1], preferred_element_type=f32),
        jnp.dot(dst, bcs[0], preferred_element_type=f32),
    )
    for a in range(2):
        conv = conv_tile(dims, proj, cpar, pad.at[a], DI + a * ST)
        conv_back(DI + a * ST, dact[a], conv, sigmoid(conv), a)
    dsteps = jnp.dot(
        (row <= col).astype(f32), dlog[...], precision=lax.Precision.HIGHEST,
        preferred_element_type=f32,
    )
    sg = jnp.where(v >= 0.0, 1.0, e) / (1.0 + e)
    ratio = jnp.where(step > 1e-30, sg / jnp.maximum(step, 1e-30), 1.0)
    ddt = csum[...] * ratio + dsteps * hpar[1:2, :] * sg
    tail = dproj.shape[1] - DI - C
    if tail > H:
        dproj[:, DI + C :] = jnp.concatenate(
            [ddt[:, 0:H].astype(bf16), jnp.zeros((T, tail - H), bf16)], axis=1
        )
    else:
        dproj[:, DI + C :] = ddt[:, 0:H].astype(bf16)
    hacc[0:8, :] += sum8(ddt)
    hacc[8:16, :] += sum8(dsteps * step)

    @pl.when(pl.program_id(0) == steps - 1)
    def _():
        small[...] = jnp.zeros_like(small)
        for k in range(KW + 1):
            small[k : k + 1, :] = jnp.sum(cacc[8 * k : 8 * k + 8, :], axis=0, keepdims=True)
        for k in range(2):
            small[KW + 1 + k : KW + 2 + k, 0:DI] = jnp.sum(
                dacc[8 * k : 8 * k + 8, :], axis=0, keepdims=True
            )
            small[KW + 3 : KW + 4, k * LANES : (k + 1) * LANES] = jnp.sum(
                hacc[8 * k : 8 * k + 8, :], axis=0, keepdims=True
            )


def run_forward(dims, proj, cpar, hpar, dpar):
    T, DI, C, H, KW = dims["T"], dims["DI"], dims["C"], dims["H"], dims["KW"]
    R, E = proj.shape
    rows = lambda w: pl.BlockSpec((T, w), lambda i: (i, 0))
    whole = lambda a: pl.BlockSpec(a.shape, lambda i: (0, 0))
    return pl.pallas_call(
        functools.partial(mix_forward, dims),
        grid=(R // T,),
        in_specs=[rows(E), whole(cpar), whole(hpar), whole(dpar)],
        out_specs=[rows(DI), rows(DI), rows(LANES)],
        out_shape=[
            jax.ShapeDtypeStruct((R, DI), bf16),
            jax.ShapeDtypeStruct((R, DI), f32),
            jax.ShapeDtypeStruct((R, LANES), f32),
        ],
        scratch_shapes=[
            pltpu.VMEM((max(2, UNROLL_F), FRONT + T, LANES), f32),
            pltpu.VMEM((T, DI), f32),
            pltpu.VMEM((H, T, LANES), f32),
            pltpu.VMEM((LANES, T), f32),
            pltpu.VMEM((T, T), f32),
            pltpu.VMEM((T, T), f32),
            pltpu.VMEM((T, LANES), f32),
            pltpu.VMEM((T, LANES), f32),
        ],
        compiler_params=pltpu.CompilerParams(vmem_limit_bytes=48 << 20),
        cost_estimate=pl.CostEstimate(
            flops=4 * R * DI * T, bytes_accessed=R * (2 * E + 6 * DI), transcendentals=R * H * T
        ),
        name="mix_forward",
    )(proj, cpar, hpar, dpar)


def run_backward(dims, EP, proj, dmixed, ssd, rstd, cpar, hpar, dpar):
    T, DI, C, H, KW, ST = (dims[k] for k in ("T", "DI", "C", "H", "KW", "ST"))
    R, E = proj.shape
    rows = lambda w: pl.BlockSpec((T, w), lambda i: (i, 0))
    whole = lambda s: pl.BlockSpec(s, lambda i: (0, 0))
    assert KW + 4 <= 8
    sums = [(8 * (KW + 1), C), (16, DI), (16, LANES)]
    return pl.pallas_call(
        functools.partial(mix_backward, dims, R // T),
        grid=(R // T,),
        in_specs=[rows(E), rows(DI), rows(DI), rows(LANES)]
        + [whole(a.shape) for a in (cpar, hpar, dpar)],
        out_specs=[rows(EP), whole((8, C))],
        out_shape=[
            jax.ShapeDtypeStruct((R, EP), bf16),
            jax.ShapeDtypeStruct((8, C), f32),
        ],
        scratch_shapes=[pltpu.VMEM(s, f32) for s in sums]
        + [
            pltpu.VMEM((max(2, UNROLL_B), FRONT + T, LANES), f32),
            pltpu.VMEM((max(2, UNROLL_B), FRONT + T, LANES), f32),
            pltpu.VMEM((H, T, LANES), f32),
            pltpu.VMEM((LANES, T), f32),
            pltpu.VMEM((T, T), f32),
            pltpu.VMEM((T, T), f32),
            pltpu.VMEM((T, LANES), f32),
            pltpu.VMEM((T, LANES), f32),
            pltpu.VMEM((T, T), f32),
            pltpu.VMEM((T, LANES), f32),
            pltpu.VMEM((T, LANES), f32),
            pltpu.VMEM((2, T, ST), bf16),
        ],
        compiler_params=pltpu.CompilerParams(vmem_limit_bytes=56 << 20),
        cost_estimate=pl.CostEstimate(
            flops=8 * R * DI * T, bytes_accessed=R * (4 * E + 8 * DI), transcendentals=R * H * T
        ),
        name="mix_backward",
    )(proj, dmixed, ssd, rstd, cpar, hpar, dpar)


MESH = pl.DeviceIdType.MESH
CHUNK = 512
VMEM = 67043328


def geometry(n):
    chips = n // 2
    A0 = 4 if chips % 4 == 0 else 1
    A = math.isqrt(chips // A0)
    return (A0, A) if n % 2 == 0 and A > 1 and A0 * A * A == chips else None


class Place:
    def __init__(self, axis, A0, A):
        me = lax.axis_index(axis)
        self.A0, self.A = A0, A
        self.c = lax.rem(me, 2)
        chip = lax.div(me, 2)
        self.a2 = lax.rem(chip, A)
        self.a1 = lax.rem(lax.div(chip, A), A)
        self.a0 = lax.div(chip, A * A)
        c = self.c
        self.f = self.a1 + c * (self.a2 - self.a1)
        self.s = self.a2 + c * (self.a1 - self.a2)
        self.sf = A + c * (1 - A)
        self.ss = 1 + c * (A - 1)

    def pos(self, f, s):
        return f * self.sf + s * self.ss

    def device(self, a0, f, s, c):
        return ((a0 * self.A * self.A + self.pos(f, s)) * 2 + c,)

    def line(self, q):
        return lax.rem(self.a0 + q + self.A0, self.A0)

    def first(self, q):
        return lax.rem(self.f + q + self.A, self.A)

    def second(self, q):
        return lax.rem(self.s + q + self.A, self.A)

    def partner(self):
        return self.device(self.a0, self.f, self.s, 1 - self.c)

    def peers(self):
        out = [self.partner()]
        out += [self.device(self.line(q), self.f, self.s, self.c) for q in range(1, self.A0)]
        out += [self.device(self.a0, self.first(q), self.s, self.c) for q in range(1, self.A)]
        out += [self.device(self.a0, self.f, self.second(q), self.c) for q in range(1, self.A)]
        return out

    def barrier(self):
        sem = pltpu.get_barrier_semaphore()
        peers = self.peers()
        for peer in peers:
            pl.semaphore_signal(sem, inc=1, device_id=peer, device_id_type=MESH)
        pl.semaphore_wait(sem, len(peers))


def send(src, dst, ssem, rsem, device):
    return pltpu.make_async_remote_copy(
        src_ref=src, dst_ref=dst, send_sem=ssem, recv_sem=rsem,
        device_id=device, device_id_type=MESH,
    )


class Gather:
    def __init__(self, at, K, wl, buf, ssem, rsem, lsem):
        self.at, self.K, self.wl, self.buf = at, K, wl, buf
        self.ssem, self.rsem, self.lsem = ssem, rsem, lsem

    @staticmethod
    def sems(A0, A):
        return (A0 - 1) + (A - 1) + (A - 1) * A + 1

    def local(self, j):
        at = self.at
        return pltpu.make_async_copy(
            self.wl.at[j], self.buf.at[j, at.a0, at.pos(at.f, at.s), at.c],
            self.lsem.at[lax.rem(j, 2)],
        )

    def copies(self, stage, j, sending):
        at, buf = self.at, self.buf
        A0, A = at.A0, at.A
        par = lax.rem(j, 2)
        out = []

        def add(k, src, dst, device):
            out.append(send(src, dst, self.ssem.at[par, k], self.rsem.at[j, k], device))

        if stage == 0:
            for q in range(1, A0):
                a = at.a0 if sending else at.line(-q)
                add(q - 1, self.wl.at[j], buf.at[j, a, at.pos(at.f, at.s), at.c],
                    at.device(at.line(q), at.f, at.s, at.c))
        elif stage == 1:
            for q in range(1, A):
                f = at.f if sending else at.first(-q)
                ref = buf.at[j, :, at.pos(f, at.s), at.c]
                add(A0 - 1 + q - 1, ref, ref, at.device(at.a0, at.first(q), at.s, at.c))
        elif stage == 2:
            for q in range(1, A):
                s = at.s if sending else at.second(-q)
                for o in range(A):
                    ref = buf.at[j, :, at.pos(o, s), at.c]
                    add(A0 - 1 + A - 1 + (q - 1) * A + o, ref, ref,
                        at.device(at.a0, at.f, at.second(q), at.c))
        else:
            ref = buf.at[j, :, :, at.c if sending else 1 - at.c]
            add(A0 - 1 + (A - 1) * (A + 1), ref, ref, at.partner())
        return out

    def step(self, i):
        for stage in range(5):
            j = i - stage

            @pl.when((j >= 0) & (j < self.K))
            def _(stage=stage, j=j):
                if stage > 0:
                    for cp in self.copies(stage - 1, j, False):
                        cp.wait_recv()
                if stage < 4:

                    @pl.when(j >= 2)
                    def _():
                        for cp in self.copies(stage, j - 2, True):
                            cp.wait_send()

                    if stage == 1:
                        self.local(j).wait()
                    for cp in self.copies(stage, j, True):
                        cp.start()
                    if stage == 0:
                        self.local(j).start()

    def drain(self):
        for j in range(max(0, self.K - 2), self.K):
            for stage in range(4):
                for cp in self.copies(stage, jnp.int32(j), True):
                    cp.wait_send()


class Reduce:
    def __init__(self, at, K, refs):
        self.at, self.K = at, K
        (self.own0, self.own1, self.own2, self.own3, self.s0, self.s1, self.s2, self.s3,
         self.r0, self.r1, self.r2, self.r3, self.ssem, self.rsem) = refs

    @staticmethod
    def sems(A0, A):
        return 1 + (A - 1) + (A - 1) + (A0 - 1)

    @staticmethod
    def scratch(K, A0, A, r, w):
        N = A0 * A * A
        NS = Reduce.sems(A0, A)
        return [
            pltpu.VMEM((2, N, r, w), f32),
            pltpu.VMEM((2, A0 * A, r, w), f32),
            pltpu.VMEM((2, A0, r, w), f32),
            pltpu.VMEM((2, r, w), f32),
            pltpu.VMEM((2, N, r, w), bf16),
            pltpu.VMEM((2, A - 1, A0 * A, r, w), bf16),
            pltpu.VMEM((2, A - 1, A0, r, w), bf16),
            pltpu.VMEM((2, A0 - 1, r, w), bf16),
            pltpu.VMEM((K, N, r, w), bf16),
            pltpu.VMEM((K, A - 1, A0 * A, r, w), bf16),
            pltpu.VMEM((K, A - 1, A0, r, w), bf16),
            pltpu.VMEM((K, A0 - 1, r, w), bf16),
            pltpu.SemaphoreType.DMA((2, NS)),
            pltpu.SemaphoreType.DMA((K, NS)),
        ]

    def copies(self, stage, j):
        at = self.at
        A0, A = at.A0, at.A
        par = lax.rem(j, 2)

        def make(k, src, dst, device):
            return send(src, dst, self.ssem.at[par, k], self.rsem.at[j, k], device)

        if stage == 0:
            return [make(0, self.s0.at[par], self.r0.at[j], at.partner())]
        if stage == 1:
            return [
                make(q, self.s1.at[par, q - 1], self.r1.at[j, q - 1],
                     at.device(at.a0, at.f, at.second(q), at.c))
                for q in range(1, A)
            ]
        if stage == 2:
            return [
                make(A - 1 + q, self.s2.at[par, q - 1], self.r2.at[j, q - 1],
                     at.device(at.a0, at.first(q), at.s, at.c))
                for q in range(1, A)
            ]
        return [
            make(2 * (A - 1) + q, self.s3.at[par, q - 1], self.r3.at[j, q - 1],
                 at.device(at.line(q), at.f, at.s, at.c))
            for q in range(1, A0)
        ]

    def free(self, stage, j):
        @pl.when(j >= 2)
        def _():
            for cp in self.copies(stage, j - 2):
                cp.wait_send()

    def start(self, stage, j):
        for cp in self.copies(stage, j):
            cp.start()

    def arrive(self, stage, j):
        for cp in self.copies(stage, j):
            cp.wait_recv()

    def step(self, i, finish):
        at = self.at
        A0, A = at.A0, at.A

        def stage1(j):
            par = lax.rem(j, 2)
            self.arrive(0, j)
            self.free(1, j)

            def line(a, _):
                for o in range(A):
                    for q in range(A):
                        b = a * A * A + at.pos(o, at.second(q))
                        v = self.own0[par, b] + self.r0[j, b].astype(f32)
                        if q == 0:
                            self.own1[par, a * A + o] = v
                        else:
                            self.s1[par, q - 1, a * A + o] = v.astype(bf16)
                return 0

            lax.fori_loop(0, A0, line, 0)
            self.start(1, j)

        def stage2(j):
            par = lax.rem(j, 2)
            self.arrive(1, j)
            self.free(2, j)

            def line(a, _):
                for q in range(A):
                    b = a * A + at.first(q)
                    v = self.own1[par, b]
                    for p in range(A - 1):
                        v = v + self.r1[j, p, b].astype(f32)
                    if q == 0:
                        self.own2[par, a] = v
                    else:
                        self.s2[par, q - 1, a] = v.astype(bf16)
                return 0

            lax.fori_loop(0, A0, line, 0)
            self.start(2, j)

        def stage3(j):
            par = lax.rem(j, 2)
            self.arrive(2, j)
            self.free(3, j)
            for q in range(A0):
                a = at.line(q)
                v = self.own2[par, a]
                for p in range(A - 1):
                    v = v + self.r2[j, p, a].astype(f32)
                if q == 0:
                    self.own3[par] = v
                else:
                    self.s3[par, q - 1] = v.astype(bf16)
            self.start(3, j)

        def stage4(j):
            self.arrive(3, j)
            v = self.own3[lax.rem(j, 2)]
            for p in range(A0 - 1):
                v = v + self.r3[j, p].astype(f32)
            finish(j, v)

        for k, stage in ((1, stage1), (2, stage2), (3, stage3), (4, stage4)):
            j = i - k

            @pl.when((j >= 0) & (j < self.K))
            def _(j=j, stage=stage):
                stage(j)

    def drain(self):
        for j in range(max(0, self.K - 2), self.K):
            for stage in range(4):
                for cp in self.copies(stage, jnp.int32(j)):
                    cp.wait_send()


class SumAll:
    def __init__(self, at, refs):
        self.at = at
        self.hold, self.land, self.ssem, self.rsem = refs

    @staticmethod
    def scratch(A0, A, shape):
        slots = 2 + A + A + A0
        return [
            pltpu.VMEM((4,) + shape, f32),
            pltpu.VMEM((slots,) + shape, f32),
            pltpu.SemaphoreType.DMA((slots,)),
            pltpu.SemaphoreType.DMA((slots,)),
        ]

    def group(self, stage):
        at = self.at
        A0, A = at.A0, at.A
        chip = at.a0 * A * A + at.a1 * A + at.a2
        if stage == 0:
            return 0, 2, at.c, 1, chip * 2
        if stage == 1:
            return 2, A, at.a2, 2, (chip - at.a2) * 2 + at.c
        if stage == 2:
            return 2 + A, A, at.a1, 2 * A, (chip - at.a1 * A) * 2 + at.c
        return 2 + 2 * A, A0, at.a0, 2 * A * A, (chip - at.a0 * A * A) * 2 + at.c

    def copies(self, stage, sending):
        base, size, mine, stride, origin = self.group(stage)
        out = []
        for q in range(1, size):
            to = lax.rem(mine + q, size)
            slot = mine if sending else lax.rem(mine - q + size, size)
            out.append(
                send(self.hold.at[stage], self.land.at[base + slot], self.ssem.at[base + q],
                     self.rsem.at[base + q], (origin + to * stride,))
            )
        return out

    def start(self, stage, value):
        base, _, mine, _, _ = self.group(stage)
        self.hold[stage] = value
        self.land[base + mine] = value
        for cp in self.copies(stage, True):
            cp.start()

    def finish(self, stage):
        base, size, _, _, _ = self.group(stage)
        for cp in self.copies(stage, False):
            cp.wait_recv()
        for cp in self.copies(stage, True):
            cp.wait_send()
        total = self.land[base]
        for k in range(1, size):
            total = total + self.land[base + k]
        return total


def gather_project(axis, geom, K, tok, wl, proj, wfull, uT, scale, buf, uh, ssem, rsem, lsem):
    A0, A = geom
    at = Place(axis, A0, A)
    i = pl.program_id(0)
    R, D = tok.shape
    w = wl.shape[2]

    @pl.when(i == 0)
    def _():
        at.barrier()

    net = Gather(at, K, wl, buf, ssem, rsem, lsem)
    net.step(i)

    @pl.when(i == 4)
    def _():
        last = buf[0].reshape(D, w)[:, w - LANES :].astype(f32).T
        scale[...] = jnp.broadcast_to(last[LANES - 1 :, :], scale.shape)

        def norm(k, _):
            rows = pl.ds(pl.multiple_of(k * LANES, LANES), LANES)
            u = tok[rows, :].astype(f32)
            r = lax.rsqrt(jnp.mean(u * u, axis=-1, keepdims=True) + epsilon)
            v = u * r * scale[0:1, :]
            uh[rows, :] = v.astype(bf16)
            uT[:, rows] = v.T.astype(bf16)
            return 0

        lax.fori_loop(0, R // LANES, norm, 0)

    @pl.when(i >= 4)
    def _():
        wfull[...] = buf[i - 4].reshape(D, w)
        M = 256

        def rows(k, _):
            at_ = pl.ds(pl.multiple_of(k * M, M), M)
            proj[at_, :] = jnp.dot(
                uh[at_, :], wfull[...], preferred_element_type=f32
            ).astype(bf16)
            return 0

        lax.fori_loop(0, R // M, rows, 0)

    @pl.when(i == K + 3)
    def _():
        net.drain()


def run_gather(axis, geom, tok, wl, E):
    A0, A = geom
    R, D = tok.shape
    K, r, w = wl.shape
    NS = Gather.sems(A0, A)
    late = lambda i: (0, lax.rem(jnp.maximum(i - 4, 0) + K - 1, K))
    once = dict(pipeline_mode=pl.Buffered(1))
    return pl.pallas_call(
        functools.partial(gather_project, axis, geom, K),
        grid=(K + 4,),
        in_specs=[
            pl.BlockSpec((R, D), lambda i: (0, 0), **once),
            pl.BlockSpec((K, r, w), lambda i: (0, 0, 0), **once),
        ],
        out_specs=[
            pl.BlockSpec((R, w), late),
            pl.BlockSpec((D, w), late),
            pl.BlockSpec((D, R), lambda i: (0, 0), **once),
            pl.BlockSpec((8, D), lambda i: (0, 0), **once),
        ],
        out_shape=[
            jax.ShapeDtypeStruct((R, E), bf16),
            jax.ShapeDtypeStruct((D, K * w), bf16),
            jax.ShapeDtypeStruct((D, R), bf16),
            jax.ShapeDtypeStruct((8, D), f32),
        ],
        scratch_shapes=[
            pltpu.VMEM((K, A0, A * A, 2, r, w), bf16),
            pltpu.VMEM((R, D), bf16),
            pltpu.SemaphoreType.DMA((2, NS)),
            pltpu.SemaphoreType.DMA((K, NS)),
            pltpu.SemaphoreType.DMA((2,)),
        ],
        compiler_params=pltpu.CompilerParams(
            collective_id=1, has_side_effects=True, vmem_limit_bytes=VMEM
        ),
        cost_estimate=pl.CostEstimate(
            flops=2 * R * D * E, bytes_accessed=2 * D * E * 40, transcendentals=0
        ),
        name="gather_project",
    )(tok, wl)


def reduce_in(axis, geom, K, E, uT, dproj, wfull, wl, scale, tok, go, small,
              dw, dns, dtok, sums, own, *refs):
    A0, A = geom
    at = Place(axis, A0, A)
    i = pl.program_id(0)
    R, D = tok.shape
    N, _, r, _ = uT.shape
    w = dproj.shape[1]
    net = Reduce(at, K, refs[:14])
    total = SumAll(at, refs[14:18])

    @pl.when(i == 0)
    def _():
        at.barrier()
        total.start(0, small[...])
        own[0] = uT[:, at.c].reshape(N * r, R)
        own[1] = uT[:, 1 - at.c].reshape(N * r, R)
        dns[...] = jnp.zeros_like(dns)

    for stage in range(1, 4):

        @pl.when(i == stage)
        def _(stage=stage):
            total.start(stage, total.finish(stage - 1))

    @pl.when(i == 4)
    def _():
        sums[...] = total.finish(3)

    @pl.when(i < K)
    def _():
        par = lax.rem(i, 2)
        net.free(0, i)
        d = dproj[...]
        net.s0[par] = (
            jnp.dot(own[1], d, preferred_element_type=f32).astype(bf16).reshape(N, r, w)
        )
        net.start(0, i)
        net.own0[par] = jnp.dot(own[0], d, preferred_element_type=f32).reshape(N, r, w)
        M = 256

        def rows(k, _):
            at_ = pl.ds(pl.multiple_of(k * M, M), M)
            part = lax.dot_general(
                dproj[at_, :], wfull[...], (((1,), (1,)), ((), ())), preferred_element_type=f32
            )

            @pl.when(i == 0)
            def _():
                dtok[at_, :] = part

            @pl.when(i > 0)
            def _():
                dtok[at_, :] += part

            return 0

        lax.fori_loop(0, R // M, rows, 0)

    def finish(j, v):
        dw[...] = v
        _, col = iotas(r, w)
        p = jnp.where(col < E - j * w, v * wl[:, pl.ds(0, w)].astype(f32), 0.0)
        part = p[:, 0:LANES]
        for k in range(1, w // LANES):
            part = part + p[:, k * LANES : (k + 1) * LANES]
        dns[...] += part

    net.step(i, finish)

    @pl.when((i >= K) & (i < K + 4))
    def _():
        M = R // 4

        def tail(k, _):
            at_ = pl.ds(pl.multiple_of((i - K) * M + k * 64, 64), 64)
            u = tok[at_, :].astype(f32)
            rs = lax.rsqrt(jnp.mean(u * u, axis=-1, keepdims=True) + epsilon)
            u = u * rs
            d = dtok[at_, :] * scale[0:1, :]
            m = jnp.mean(d * u, axis=-1, keepdims=True)
            dtok[at_, :] = go[at_, :].astype(f32) + rs * (d - u * m)
            return 0

        lax.fori_loop(0, M // 64, tail, 0)

    @pl.when(i == K + 3)
    def _():
        net.drain()


def run_reduce_in(axis, geom, uT, dproj, wfull, wl, scale, tok, go, small):
    A0, A = geom
    R, D = tok.shape
    r, E = wl.shape
    w = CHUNK
    K = dproj.shape[1] // w
    N = A0 * A * A
    once = dict(pipeline_mode=pl.Buffered(1))
    late = lambda i: (0, jnp.clip(i - 4, 0, K - 1))
    early = lambda i: (0, jnp.minimum(i, K - 1))
    whole = lambda i: (0, 0)
    return pl.pallas_call(
        functools.partial(reduce_in, axis, geom, K, E),
        grid=(K + 4,),
        in_specs=[
            pl.BlockSpec((N, 2, r, R), lambda i: (0, 0, 0, 0), **once),
            pl.BlockSpec((R, w), early),
            pl.BlockSpec((D, w), early),
            pl.BlockSpec((r, w), late),
            pl.BlockSpec((8, D), whole, **once),
            pl.BlockSpec((R, D), whole, **once),
            pl.BlockSpec((R, D), whole, **once),
            pl.BlockSpec(small.shape, whole, **once),
        ],
        out_specs=[
            pl.BlockSpec((r, w), late),
            pl.BlockSpec((r, LANES), whole, **once),
            pl.BlockSpec((R, D), whole, **once),
            pl.BlockSpec(small.shape, whole, **once),
        ],
        out_shape=[
            jax.ShapeDtypeStruct((r, E), f32),
            jax.ShapeDtypeStruct((r, LANES), f32),
            jax.ShapeDtypeStruct((R, D), f32),
            jax.ShapeDtypeStruct(small.shape, f32),
        ],
        scratch_shapes=[pltpu.VMEM((2, N * r, R), bf16)]
        + Reduce.scratch(K, A0, A, r, w)
        + SumAll.scratch(A0, A, small.shape),
        compiler_params=pltpu.CompilerParams(
            collective_id=2, has_side_effects=True, vmem_limit_bytes=VMEM
        ),
        cost_estimate=pl.CostEstimate(
            flops=4 * R * D * E, bytes_accessed=2 * D * E * 40, transcendentals=0
        ),
        name="reduce_in",
    )(uT.reshape(N, 2, r, R), dproj, wfull, wl, scale, tok, go, small)


def local(axis, n, tokens, in_weight, conv_weight, conv_bias, dt_bias, a_log, skip_d,
          norm_scale, gate_scale, out_weight, grad_out):
    MB, S, T, D = tokens.shape
    R = MB * S * T
    r, E = in_weight.shape
    H = a_log.shape[0]
    DI = out_weight.shape[0] * n
    Cn, KW = conv_weight.shape
    C = Cn * n
    HD = DI // H
    ST = (C - DI) // 2
    dims = dict(T=T, DI=DI, C=C, H=H, HD=HD, ST=ST, KW=KW)
    assert LANES % HD == 0 and ST == LANES and DI % (LANES * 2) == 0 and T % 16 == 0
    geom = geometry(n)
    w = CHUNK
    K = -(-E // w)
    EP = K * w
    Gn = DI // n
    own = (
        geom is not None and r % 16 == 0 and EP - LANES >= E and max(Cn, Gn) < LANES
        and KW + 2 <= r
    )
    me = lax.axis_index(axis)

    ns = norm_scale.astype(f32)
    tok = tokens.reshape(R, D)
    go = grad_out.reshape(R, D)
    out_full = lax.all_gather(out_weight, axis, axis=0, tiled=True)
    if own:
        rows = [conv_weight.T, conv_bias[None], gate_scale[None]]
        pads = jnp.concatenate(
            [jnp.pad(v, ((0, 0), (0, LANES - 1 - v.shape[1]))) for v in rows]
            + [jnp.zeros((r - KW - 2, LANES - 1), bf16)],
            axis=0,
        )
        wl = jnp.concatenate(
            [in_weight, jnp.zeros((r, EP - LANES - E), bf16), pads, norm_scale[:, None]], axis=1
        )
        wl = jnp.roll(wl.reshape(r, K, w).transpose(1, 0, 2), 1, axis=0)
        proj, wfull, uT, scale = run_gather(axis, geom, tok, wl, E)
        got = wfull.reshape(n, r, EP)[:, : KW + 2, EP - LANES :]
        conv, gate = got[:, : KW + 1, :Cn], got[:, KW + 1, :Gn]
    else:
        EP = E
        wfull = lax.all_gather(in_weight, axis, axis=0, tiled=True)
        conv = lax.all_gather(jnp.concatenate([conv_weight.T, conv_bias[None]]), axis, axis=0)
        gate = lax.all_gather(gate_scale, axis, axis=0)
        scale = lax.all_gather(norm_scale, axis, axis=0).reshape(1, D).astype(f32)
        u = tok.astype(f32)
        rs = lax.rsqrt(jnp.mean(u * u, axis=-1, keepdims=True) + epsilon)
        uh = (u * rs * scale).astype(bf16)
        proj = jnp.dot(uh, wfull, preferred_element_type=f32).astype(bf16)
    conv = conv.transpose(1, 0, 2).reshape(KW + 1, C).astype(f32)

    rate = -jnp.exp(a_log)
    cpar = jnp.concatenate([conv, jnp.zeros((8 - KW - 1, C), f32)], axis=0)
    hpar = jnp.zeros((8, LANES), f32).at[0, :H].set(dt_bias).at[1, :H].set(rate)
    dpar = jnp.concatenate(
        [jnp.repeat(skip_d, HD)[None], gate.reshape(1, DI).astype(f32), jnp.zeros((6, DI), f32)]
    )
    mixed, ssd, rstd = run_forward(dims, proj, cpar, hpar, dpar)
    output = (tok.astype(f32) + jnp.dot(mixed, out_full, preferred_element_type=f32)).astype(bf16)
    g_out = lax.dot_general(
        mixed, go, (((0,), (0,)), ((), ())), preferred_element_type=f32
    ).astype(bf16)
    g_out = lax.psum_scatter(g_out, axis, scatter_dimension=0, tiled=True)
    d_mixed = lax.dot_general(go, out_full, (((1,), (1,)), ((), ())), preferred_element_type=f32)
    dproj, small = run_backward(dims, EP, proj, d_mixed, ssd, rstd, cpar, hpar, dpar)
    if own:
        dw, dns, dtok, sums = run_reduce_in(
            axis, geom, uT, dproj, wfull, in_weight, scale, tok, go, small
        )
    else:
        g_in = lax.dot_general(
            uh, dproj, (((0,), (0,)), ((), ())), preferred_element_type=f32
        ).astype(bf16)
        dw = lax.psum_scatter(g_in, axis, scatter_dimension=0, tiled=True).astype(f32)
        dns = dw * in_weight.astype(f32)
        d = lax.dot_general(dproj, wfull, (((1,), (1,)), ((), ())), preferred_element_type=f32)
        u, d = u * rs, d * scale
        dtok = go.astype(f32) + rs * (d - u * jnp.mean(d * u, axis=-1, keepdims=True))
        sums = lax.psum(small, axis)
    dconv = lax.dynamic_slice(sums, (0, me * Cn), (KW + 1, Cn))
    heads = sums[KW + 3]
    return (
        output.reshape(tokens.shape),
        dtok.reshape(tokens.shape),
        dw,
        dconv[:KW].T,
        dconv[KW],
        heads[:H],
        heads[LANES : LANES + H] * rate,
        sums[KW + 1, :DI].reshape(H, HD).sum(axis=1),
        dns.sum(axis=1) / ns,
        lax.dynamic_slice(sums[KW + 2], (me * Gn,), (Gn,)),
        g_out.astype(f32),
    )


def solution(mesh):
    axis = mesh.axis_names[0]
    n = mesh.shape[axis]
    rows, flat, batch = P(axis, None), P(axis), P(None, axis, None, None)
    return jax.shard_map(
        functools.partial(local, axis, n),
        mesh=mesh,
        in_specs=(batch, rows, rows, flat, P(), P(), P(), flat, flat, rows, batch),
        out_specs=(batch, batch, rows, rows, flat, P(), P(), P(), flat, flat, rows),
        check_vma=False,
    )
```

```python
import functools
import math

import jax
import jax.numpy as jnp
from jax import lax
from jax.experimental import pallas as pl
from jax.experimental.pallas import tpu as pltpu
from jax.sharding import PartitionSpec as P

epsilon = 1e-05
LOG2E = 1.4426950408889634
BIG = 3.0e38
LANES = 128
FRONT = 8
f32 = jnp.float32
bf16 = jnp.bfloat16
UNROLL_F = 2
UNROLL_B = 2


def sigmoid(v):
    return 0.5 * jnp.tanh(0.5 * v) + 0.5


def sum8(v):
    rows, lanes = v.shape
    return jnp.sum(v.reshape(rows // 8, 8, lanes), axis=0)


def iotas(rows, lanes):
    return (
        lax.broadcasted_iota(jnp.int32, (rows, lanes), 0),
        lax.broadcasted_iota(jnp.int32, (rows, lanes), 1),
    )


def step_stage(dims, proj, hpar, dtp):
    T, DI, C, H = dims["T"], dims["DI"], dims["C"], dims["H"]
    dtp[...] = jnp.zeros_like(dtp)
    dtp[:, 0:H] = proj[:, DI + C : DI + C + H].astype(f32)
    v = dtp[...] + hpar[0:1, :]
    e = jnp.exp(-jnp.abs(v))
    step = jnp.maximum(v, 0.0) + jnp.log1p(e)
    row, col = iotas(T, T)
    tri = (row >= col).astype(f32)
    ld = jnp.dot(
        tri, step * (hpar[1:2, :] * LOG2E), precision=lax.Precision.HIGHEST,
        preferred_element_type=f32,
    )
    return v, e, step, ld, ld - jnp.log2(step)


def conv_tile(dims, proj, cpar, pad, c0):
    T, DI, KW = dims["T"], dims["DI"], dims["KW"]
    lanes = pl.ds(c0, LANES)
    cin = proj[:, pl.ds(DI + c0, LANES)].astype(f32)
    pad[FRONT : FRONT + T, :] = cin
    out = cpar[KW : KW + 1, lanes] + cin * cpar[KW - 1 : KW, lanes]
    for k in range(KW - 1):
        out = out + pad[FRONT - KW + 1 + k : FRONT - KW + 1 + k + T, :] * cpar[k : k + 1, lanes]
    return out


def stack_heads(dims, v):
    T, HD = dims["T"], dims["HD"]
    _, lane = iotas(T, LANES)
    zero = jnp.zeros_like(v)
    return jnp.concatenate(
        [jnp.where(lane // HD == a, v, zero) for a in range(LANES // HD)], axis=0
    )


MESH = pl.DeviceIdType.MESH
CHUNK = 512
VMEM = 67043328


def geometry(n):
    chips = n // 2
    A0 = 4 if chips % 4 == 0 else 1
    A = math.isqrt(chips // A0)
    return (A0, A) if n % 2 == 0 and A > 1 and A0 * A * A == chips else None


class Place:
    def __init__(self, axis, A0, A):
        me = lax.axis_index(axis)
        self.A0, self.A = A0, A
        self.c = lax.rem(me, 2)
        chip = lax.div(me, 2)
        self.a2 = lax.rem(chip, A)
        self.a1 = lax.rem(lax.div(chip, A), A)
        self.a0 = lax.div(chip, A * A)
        c = self.c
        self.f = self.a1 + c * (self.a2 - self.a1)
        self.s = self.a2 + c * (self.a1 - self.a2)
        self.sf = A + c * (1 - A)
        self.ss = 1 + c * (A - 1)

    def pos(self, f, s):
        return f * self.sf + s * self.ss

    def device(self, a0, f, s, c):
        return ((a0 * self.A * self.A + self.pos(f, s)) * 2 + c,)

    def line(self, q):
        return lax.rem(self.a0 + q + self.A0, self.A0)

    def first(self, q):
        return lax.rem(self.f + q + self.A, self.A)

    def second(self, q):
        return lax.rem(self.s + q + self.A, self.A)

    def partner(self):
        return self.device(self.a0, self.f, self.s, 1 - self.c)

    def peers(self):
        out = [self.partner()]
        out += [self.device(self.line(q), self.f, self.s, self.c) for q in range(1, self.A0)]
        out += [self.device(self.a0, self.first(q), self.s, self.c) for q in range(1, self.A)]
        out += [self.device(self.a0, self.f, self.second(q), self.c) for q in range(1, self.A)]
        return out

    def barrier(self):
        sem = pltpu.get_barrier_semaphore()
        peers = self.peers()
        for peer in peers:
            pl.semaphore_signal(sem, inc=1, device_id=peer, device_id_type=MESH)
        pl.semaphore_wait(sem, len(peers))


def columns(j, w):
    return pl.ds(pl.multiple_of(j * w, w), w)


def send(src, dst, ssem, rsem, device):
    return pltpu.make_async_remote_copy(
        src_ref=src, dst_ref=dst, send_sem=ssem, recv_sem=rsem,
        device_id=device, device_id_type=MESH,
    )


class Gather:
    def __init__(self, at, K, mine, whole, ssem, rsem, lsem):
        self.at, self.K, self.mine, self.whole = at, K, mine, whole
        self.ssem, self.rsem, self.lsem = ssem, rsem, lsem

    @staticmethod
    def scratch(K, A0, A):
        NS = (A0 - 1) + (A - 1) + (A - 1) * A + 1
        return [
            pltpu.SemaphoreType.DMA((2, NS)),
            pltpu.SemaphoreType.DMA((K, NS)),
            pltpu.SemaphoreType.DMA((2,)),
        ]

    def local(self, j):
        at = self.at
        return pltpu.make_async_copy(
            self.mine(j), self.whole(j, at.a0, at.pos(at.f, at.s), at.c),
            self.lsem.at[lax.rem(j, 2)],
        )

    def copies(self, stage, j, sending):
        at, whole = self.at, self.whole
        A0, A = at.A0, at.A
        par = lax.rem(j, 2)
        every = slice(None)
        out = []

        def add(k, src, dst, device):
            out.append(send(src, dst, self.ssem.at[par, k], self.rsem.at[j, k], device))

        if stage == 0:
            for q in range(1, A0):
                a = at.a0 if sending else at.line(-q)
                add(q - 1, self.mine(j), whole(j, a, at.pos(at.f, at.s), at.c),
                    at.device(at.line(q), at.f, at.s, at.c))
        elif stage == 1:
            for q in range(1, A):
                f = at.f if sending else at.first(-q)
                ref = whole(j, every, at.pos(f, at.s), at.c)
                add(A0 - 1 + q - 1, ref, ref, at.device(at.a0, at.first(q), at.s, at.c))
        elif stage == 2:
            for q in range(1, A):
                s = at.s if sending else at.second(-q)
                for o in range(A):
                    ref = whole(j, every, at.pos(o, s), at.c)
                    add(A0 - 1 + A - 1 + (q - 1) * A + o, ref, ref,
                        at.device(at.a0, at.f, at.second(q), at.c))
        else:
            ref = whole(j, every, every, at.c if sending else 1 - at.c)
            add(A0 - 1 + (A - 1) * (A + 1), ref, ref, at.partner())
        return out

    def step(self, i):
        for stage in range(5):
            j = i - stage

            @pl.when((j >= 0) & (j < self.K))
            def _(stage=stage, j=j):
                if stage > 0:
                    for cp in self.copies(stage - 1, j, False):
                        cp.wait_recv()
                if stage < 4:

                    @pl.when(j >= 2)
                    def _():
                        for cp in self.copies(stage, j - 2, True):
                            cp.wait_send()

                    if stage == 1:
                        self.local(j).wait()
                    for cp in self.copies(stage, j, True):
                        cp.start()
                    if stage == 0:
                        self.local(j).start()

    def drain(self):
        for j in range(max(0, self.K - 2), self.K):
            for stage in range(4):
                for cp in self.copies(stage, jnp.int32(j), True):
                    cp.wait_send()


class Reduce:
    def __init__(self, at, K, refs):
        self.at, self.K = at, K
        (self.own0, self.own1, self.own2, self.own3, self.s0, self.s1, self.s2, self.s3,
         self.r0, self.r1, self.r2, self.r3, self.ssem, self.rsem) = refs

    @staticmethod
    def sems(A0, A):
        return 1 + (A - 1) + (A - 1) + (A0 - 1)

    @staticmethod
    def scratch(K, A0, A, r, w):
        N = A0 * A * A
        NS = Reduce.sems(A0, A)
        return [
            pltpu.VMEM((2, N, r, w), f32),
            pltpu.VMEM((2, A0 * A, r, w), f32),
            pltpu.VMEM((2, A0, r, w), f32),
            pltpu.VMEM((2, r, w), f32),
            pltpu.VMEM((2, N, r, w), bf16),
            pltpu.VMEM((2, A - 1, A0 * A, r, w), bf16),
            pltpu.VMEM((2, A - 1, A0, r, w), bf16),
            pltpu.VMEM((2, A0 - 1, r, w), bf16),
            pltpu.VMEM((K, N, r, w), bf16),
            pltpu.VMEM((K, A - 1, A0 * A, r, w), bf16),
            pltpu.VMEM((K, A - 1, A0, r, w), bf16),
            pltpu.VMEM((K, A0 - 1, r, w), bf16),
            pltpu.SemaphoreType.DMA((2, NS)),
            pltpu.SemaphoreType.DMA((K, NS)),
        ]

    def copies(self, stage, j):
        at = self.at
        A0, A = at.A0, at.A
        par = lax.rem(j, 2)

        def make(k, src, dst, device):
            return send(src, dst, self.ssem.at[par, k], self.rsem.at[j, k], device)

        if stage == 0:
            return [make(0, self.s0.at[par], self.r0.at[j], at.partner())]
        if stage == 1:
            return [
                make(q, self.s1.at[par, q - 1], self.r1.at[j, q - 1],
                     at.device(at.a0, at.f, at.second(q), at.c))
                for q in range(1, A)
            ]
        if stage == 2:
            return [
                make(A - 1 + q, self.s2.at[par, q - 1], self.r2.at[j, q - 1],
                     at.device(at.a0, at.first(q), at.s, at.c))
                for q in range(1, A)
            ]
        return [
            make(2 * (A - 1) + q, self.s3.at[par, q - 1], self.r3.at[j, q - 1],
                 at.device(at.line(q), at.f, at.s, at.c))
            for q in range(1, A0)
        ]

    def free(self, stage, j):
        @pl.when(j >= 2)
        def _():
            for cp in self.copies(stage, j - 2):
                cp.wait_send()

    def start(self, stage, j):
        for cp in self.copies(stage, j):
            cp.start()

    def arrive(self, stage, j):
        for cp in self.copies(stage, j):
            cp.wait_recv()

    def begin(self, j, own, right):
        N, r, w = self.own0.shape[1:]
        par = lax.rem(j, 2)
        self.free(0, j)
        self.s0[par] = (
            jnp.dot(own[1], right, preferred_element_type=f32).astype(bf16).reshape(N, r, w)
        )
        self.start(0, j)
        self.own0[par] = jnp.dot(own[0], right, preferred_element_type=f32).reshape(N, r, w)

    def step(self, i, finish):
        at = self.at
        A0, A = at.A0, at.A

        def stage1(j):
            par = lax.rem(j, 2)
            self.arrive(0, j)
            self.free(1, j)

            def line(a, _):
                for o in range(A):
                    for q in range(A):
                        b = a * A * A + at.pos(o, at.second(q))
                        v = self.own0[par, b] + self.r0[j, b].astype(f32)
                        if q == 0:
                            self.own1[par, a * A + o] = v
                        else:
                            self.s1[par, q - 1, a * A + o] = v.astype(bf16)
                return 0

            lax.fori_loop(0, A0, line, 0)
            self.start(1, j)

        def stage2(j):
            par = lax.rem(j, 2)
            self.arrive(1, j)
            self.free(2, j)

            def line(a, _):
                for q in range(A):
                    b = a * A + at.first(q)
                    v = self.own1[par, b]
                    for p in range(A - 1):
                        v = v + self.r1[j, p, b].astype(f32)
                    if q == 0:
                        self.own2[par, a] = v
                    else:
                        self.s2[par, q - 1, a] = v.astype(bf16)
                return 0

            lax.fori_loop(0, A0, line, 0)
            self.start(2, j)

        def stage3(j):
            par = lax.rem(j, 2)
            self.arrive(2, j)
            self.free(3, j)
            for q in range(A0):
                a = at.line(q)
                v = self.own2[par, a]
                for p in range(A - 1):
                    v = v + self.r2[j, p, a].astype(f32)
                if q == 0:
                    self.own3[par] = v
                else:
                    self.s3[par, q - 1] = v.astype(bf16)
            self.start(3, j)

        def stage4(j):
            self.arrive(3, j)
            v = self.own3[lax.rem(j, 2)]
            for p in range(A0 - 1):
                v = v + self.r3[j, p].astype(f32)
            finish(j, v)

        for k, stage in ((1, stage1), (2, stage2), (3, stage3), (4, stage4)):
            j = i - k

            @pl.when((j >= 0) & (j < self.K))
            def _(j=j, stage=stage):
                stage(j)

    def drain(self):
        for j in range(max(0, self.K - 2), self.K):
            for stage in range(4):
                for cp in self.copies(stage, jnp.int32(j)):
                    cp.wait_send()


class SumAll:
    def __init__(self, at, refs):
        self.at = at
        self.hold, self.land, self.ssem, self.rsem = refs

    @staticmethod
    def scratch(A0, A, shape):
        slots = 2 + A + A + A0
        return [
            pltpu.VMEM((4,) + shape, f32),
            pltpu.VMEM((slots,) + shape, f32),
            pltpu.SemaphoreType.DMA((slots,)),
            pltpu.SemaphoreType.DMA((slots,)),
        ]

    def group(self, stage):
        at = self.at
        A0, A = at.A0, at.A
        chip = at.a0 * A * A + at.a1 * A + at.a2
        if stage == 0:
            return 0, 2, at.c, 1, chip * 2
        if stage == 1:
            return 2, A, at.a2, 2, (chip - at.a2) * 2 + at.c
        if stage == 2:
            return 2 + A, A, at.a1, 2 * A, (chip - at.a1 * A) * 2 + at.c
        return 2 + 2 * A, A0, at.a0, 2 * A * A, (chip - at.a0 * A * A) * 2 + at.c

    def copies(self, stage, sending):
        base, size, mine, stride, origin = self.group(stage)
        out = []
        for q in range(1, size):
            to = lax.rem(mine + q, size)
            slot = mine if sending else lax.rem(mine - q + size, size)
            out.append(
                send(self.hold.at[stage], self.land.at[base + slot], self.ssem.at[base + q],
                     self.rsem.at[base + q], (origin + to * stride,))
            )
        return out

    def start(self, stage, value):
        base, _, mine, _, _ = self.group(stage)
        self.hold[stage] = value
        self.land[base + mine] = value
        for cp in self.copies(stage, True):
            cp.start()

    def finish(self, stage):
        base, size, _, _, _ = self.group(stage)
        for cp in self.copies(stage, False):
            cp.wait_recv()
        for cp in self.copies(stage, True):
            cp.wait_send()
        total = self.land[base]
        for k in range(1, size):
            total = total + self.land[base + k]
        return total


def mix_forward(dims, net_of, proj, cpar, hpar, dpar, *refs):
    if net_of is None:
        mixed, ssd, rstd, *refs = refs
        between = lambda half: None
    else:
        wl, mixed, ssd, rstd, wfull, *refs = refs
        net = net_of(wl, wfull, refs[8:])
        i = pl.program_id(0)

        @pl.when(i == 0)
        def _():
            net.at.barrier()

        between = lambda half: net.step(2 * i + half)
    pad, gated, colb, rowb, mask, scores, acc, dtp = refs[:8]
    between(0)
    T, DI, H, HD, ST = dims["T"], dims["DI"], dims["H"], dims["HD"], dims["ST"]
    HP = LANES // HD
    tiles = DI // LANES
    pad[:, 0:FRONT, :] = jnp.zeros((pad.shape[0], FRONT, LANES), f32)
    _, _, _, ld, ld2 = step_stage(dims, proj, hpar, dtp)
    row, col = iotas(T, T)
    mask[...] = jnp.where(col <= row, BIG, -BIG)
    rowb[...] = ld2.T
    for h in range(H):
        colb[h] = jnp.broadcast_to(ld[:, h : h + 1], (T, LANES))
    bc = []
    for a in range(2):
        conv = conv_tile(dims, proj, cpar, pad.at[a], DI + a * ST)
        bc.append((conv * sigmoid(conv)).astype(bf16))
    scores[...] = lax.dot_general(
        bc[1], bc[0], (((1,), (1,)), ((), ())), preferred_element_type=f32
    )
    acc[...] = jnp.zeros_like(acc)

    def tile(j, u):
        c0 = pl.multiple_of(j * LANES, LANES)
        lanes = pl.ds(c0, LANES)
        conv = conv_tile(dims, proj, cpar, pad.at[u], c0)
        x = (conv * sigmoid(conv)).astype(bf16)
        mix = []
        for a in range(HP):
            h = j * HP + a
            expo = jnp.minimum(colb[h] - rowb[pl.ds(h, 1), :], mask[...])
            mix.append((jnp.exp2(expo) * scores[...]).astype(bf16))
        core = jnp.dot(
            jnp.concatenate(mix, axis=1), stack_heads(dims, x), preferred_element_type=f32
        )
        out = core + dpar[0:1, lanes] * x.astype(f32)
        ssd[:, lanes] = out
        gate = proj[:, lanes].astype(f32)
        g = out * (gate * sigmoid(gate))
        gated[:, lanes] = g
        return g * g

    def body(j, _):
        total = tile(j * UNROLL_F, 0)
        for u in range(1, UNROLL_F):
            total = total + tile(j * UNROLL_F + u, u)
        acc[...] += total
        return 0

    trips = tiles // UNROLL_F
    lax.fori_loop(0, trips // 2, body, 0)
    between(1)
    lax.fori_loop(trips // 2, trips, body, 0)
    r = lax.rsqrt(jnp.sum(acc[...], axis=1, keepdims=True) * (1.0 / DI) + epsilon)
    rb = jnp.broadcast_to(r, (T, LANES))
    rstd[...] = rb

    def finish(j, _):
        lanes = pl.ds(pl.multiple_of(j * LANES, LANES), LANES)
        mixed[lanes, :] = (gated[:, lanes] * rb * dpar[1:2, lanes]).T.astype(bf16)
        return 0

    lax.fori_loop(0, tiles, finish, 0)
    if net_of is not None:

        @pl.when(i == pl.num_programs(0) - 1)
        def _():
            net.drain()


def mix_backward(dims, steps, net_of, proj, dmixed, ssd, rstd, cpar, hpar, dpar, *refs):
    if net_of is None:
        dproj, small, *refs = refs
        between = lambda half: None
    else:
        mT, go, dproj, small, dow, *refs = refs
        net, own = net_of(refs[15:])
        N, _, r, R = mT.shape
        w = net.own3.shape[2]
        i = pl.program_id(0)

        @pl.when(i == 0)
        def _():
            net.at.barrier()
            own[0] = mT[:, net.at.c].reshape(N * r, R)
            own[1] = mT[:, 1 - net.at.c].reshape(N * r, R)

        def finish(j, v):
            dow[:, columns(j, w)] = v

        def between(half):
            k = 2 * i + half

            @pl.when(k < net.K)
            def _():
                net.begin(k, own, go[:, columns(k, w)])

            net.step(k, finish)

    (cacc, dacc, hacc, pad, dpad, colb, rowb, mask, scores, acc, dtp, dscores, dlog, csum,
     bcs) = refs[:15]
    between(0)
    T, DI, C, H, HD, ST, KW = (dims[k] for k in ("T", "DI", "C", "H", "HD", "ST", "KW"))
    HP = LANES // HD
    tiles = DI // LANES

    @pl.when(pl.program_id(0) == 0)
    def _():
        cacc[...] = jnp.zeros_like(cacc)
        dacc[...] = jnp.zeros_like(dacc)
        hacc[...] = jnp.zeros_like(hacc)

    pad[:, 0:FRONT, :] = jnp.zeros((pad.shape[0], FRONT, LANES), f32)
    dpad[:, T:, :] = jnp.zeros((dpad.shape[0], FRONT, LANES), f32)
    v, e, step, ld, ld2 = step_stage(dims, proj, hpar, dtp)
    row, col = iotas(T, T)
    mask[...] = jnp.where(row <= col, BIG, -BIG)
    rowb[...] = ld.T
    for h in range(H):
        colb[h] = jnp.broadcast_to(ld2[:, h : h + 1], (T, LANES))
    for a in range(2):
        conv = conv_tile(dims, proj, cpar, pad.at[a], DI + a * ST)
        bcs[a] = (conv * sigmoid(conv)).astype(bf16)
    scores[...] = lax.dot_general(
        bcs[0], bcs[1], (((1,), (1,)), ((), ())), preferred_element_type=f32
    )
    acc[...] = jnp.zeros_like(acc)
    dscores[...] = jnp.zeros_like(dscores)
    dlog[...] = jnp.zeros_like(dlog)
    csum[...] = jnp.zeros_like(csum)
    rb = rstd[...]

    def first(j, _):
        lanes = pl.ds(pl.multiple_of(j * LANES, LANES), LANES)
        gate = proj[:, lanes].astype(f32)
        p = dmixed[:, lanes] * (ssd[:, lanes] * (gate * sigmoid(gate)))
        acc[...] += p * dpar[1:2, lanes]
        dacc[8:16, lanes] += sum8(p * rb)
        return 0

    lax.fori_loop(0, tiles, first, 0)
    mean = jnp.sum(acc[...], axis=1, keepdims=True) * (1.0 / DI)
    mb = jnp.broadcast_to(mean, (T, LANES)) * rb * rb * rb
    acc[...] = mb

    def conv_back(c0, dact, conv, sig, u):
        lanes = pl.ds(c0, LANES)
        dconv = dact * (sig * (1.0 + conv * (1.0 - sig)))
        dpad[u, 0:T, :] = dconv
        dcin = dconv * cpar[KW - 1 : KW, lanes]
        for k in range(KW - 1):
            dcin = dcin + dpad[u, KW - 1 - k : KW - 1 - k + T, :] * cpar[k : k + 1, lanes]
        dproj[:, pl.ds(DI + c0, LANES)] = dcin.astype(bf16)
        for k in range(KW):
            start = FRONT - KW + 1 + k
            cacc[8 * k : 8 * k + 8, lanes] += sum8(dconv * pad[u, start : start + T, :])
        cacc[8 * KW : 8 * KW + 8, lanes] += sum8(dconv)

    def tile(j, u):
        c0 = pl.multiple_of(j * LANES, LANES)
        lanes = pl.ds(c0, LANES)
        conv = conv_tile(dims, proj, cpar, pad.at[u], c0)
        sig = sigmoid(conv)
        x = (conv * sig).astype(bf16)
        xf = x.astype(f32)
        gate = proj[:, lanes].astype(f32)
        gs = sigmoid(gate)
        act = gate * gs
        out = ssd[:, lanes]
        r = rstd[...]
        dgated = r * (dmixed[:, lanes] * dpar[1:2, lanes]) - (out * act) * acc[...]
        dssd = dgated * act
        dproj[:, lanes] = (dgated * out * (gs * (1.0 + gate * (1.0 - gs)))).astype(bf16)
        low = dssd.astype(bf16)
        dacc[0:8, lanes] += sum8(dssd * xf)
        lows = stack_heads(dims, low)
        dmix = lax.dot_general(
            x, lows, (((1,), (1,)), ((), ())), preferred_element_type=f32
        )
        mix = []
        part = None
        for a in range(HP):
            h = j * HP + a
            decay = jnp.exp2(jnp.minimum(rowb[pl.ds(h, 1), :] - colb[h], mask[...]))
            mix.append((decay * scores[...]).astype(bf16))
            term = dmix[:, a * T : (a + 1) * T] * decay
            part = term if part is None else part + term
        core = jnp.dot(jnp.concatenate(mix, axis=1), lows, preferred_element_type=f32)
        skip = dpar[0:1, lanes]
        from_cols = xf * core
        diff = low.astype(f32) * (out - skip * xf) - from_cols
        prow, pcol = iotas(LANES, LANES)
        place = (pcol == j * HP + prow // HD).astype(bf16)
        place = jnp.concatenate([place, place], axis=0)

        def by_head(w):
            hi = w.astype(bf16)
            lo = (w - hi.astype(f32)).astype(bf16)
            return jnp.dot(
                jnp.concatenate([hi, lo], axis=1), place, preferred_element_type=f32
            )

        conv_back(c0, core + skip * dssd, conv, sig, u)
        return part, by_head(diff), by_head(from_cols)

    def body(j, _):
        sums = tile(j * UNROLL_B, 0)
        for u in range(1, UNROLL_B):
            sums = tuple(p + q for p, q in zip(sums, tile(j * UNROLL_B + u, u)))
        dscores[...] += sums[0]
        dlog[...] += sums[1]
        csum[...] += sums[2]
        return 0

    trips = tiles // UNROLL_B
    lax.fori_loop(0, trips // 2, body, 0)
    between(1)
    lax.fori_loop(trips // 2, trips, body, 0)
    ds = dscores[...].astype(bf16)
    dst = dscores[...].T.astype(bf16)
    dact = (
        jnp.dot(ds, bcs[1], preferred_element_type=f32),
        jnp.dot(dst, bcs[0], preferred_element_type=f32),
    )
    for a in range(2):
        conv = conv_tile(dims, proj, cpar, pad.at[a], DI + a * ST)
        conv_back(DI + a * ST, dact[a], conv, sigmoid(conv), a)
    dsteps = jnp.dot(
        (row <= col).astype(f32), dlog[...], precision=lax.Precision.HIGHEST,
        preferred_element_type=f32,
    )
    sg = jnp.where(v >= 0.0, 1.0, e) / (1.0 + e)
    ratio = jnp.where(step > 1e-30, sg / jnp.maximum(step, 1e-30), 1.0)
    ddt = csum[...] * ratio + dsteps * hpar[1:2, :] * sg
    tail = dproj.shape[1] - DI - C
    if tail > H:
        dproj[:, DI + C :] = jnp.concatenate(
            [ddt[:, 0:H].astype(bf16), jnp.zeros((T, tail - H), bf16)], axis=1
        )
    else:
        dproj[:, DI + C :] = ddt[:, 0:H].astype(bf16)
    hacc[0:8, :] += sum8(ddt)
    hacc[8:16, :] += sum8(dsteps * step)

    if net_of is not None:

        @pl.when(i == steps - 1)
        def _():
            net.drain()

    @pl.when(pl.program_id(0) == steps - 1)
    def _():
        small[...] = jnp.zeros_like(small)
        for k in range(KW + 1):
            small[k : k + 1, :] = jnp.sum(cacc[8 * k : 8 * k + 8, :], axis=0, keepdims=True)
        for k in range(2):
            small[KW + 1 + k : KW + 2 + k, 0:DI] = jnp.sum(
                dacc[8 * k : 8 * k + 8, :], axis=0, keepdims=True
            )
            small[KW + 3 : KW + 4, k * LANES : (k + 1) * LANES] = jnp.sum(
                hacc[8 * k : 8 * k + 8, :], axis=0, keepdims=True
            )


def run_forward(dims, axis, geom, proj, cpar, hpar, dpar, ow):
    T, DI, C, H, KW = dims["T"], dims["DI"], dims["C"], dims["H"], dims["KW"]
    R, E = proj.shape
    steps = R // T
    rows = lambda w: pl.BlockSpec((T, w), lambda i: (i, 0))
    whole = lambda a: pl.BlockSpec(a.shape, lambda i: (0, 0))
    args, net_of, outs, shapes, sems, extra = [], None, [], [], [], {}
    if geom is not None:
        A0, A = geom
        r, D = ow.shape
        w = D // (2 * steps - 4)
        K = D // w

        def net_of(wl, wfull, sems):
            return Gather(
                Place(axis, A0, A), K, lambda j: wl.at[:, columns(j, w)],
                lambda j, a, p, c: wfull.at[a, p, c, :, columns(j, w)], *sems,
            )

        args = [ow]
        outs = [pl.BlockSpec(memory_space=pl.ANY)]
        shapes = [jax.ShapeDtypeStruct((A0, A * A, 2, r, D), bf16)]
        sems = Gather.scratch(K, A0, A)
        extra = dict(collective_id=3, has_side_effects=True)
    return pl.pallas_call(
        functools.partial(mix_forward, dims, net_of),
        grid=(steps,),
        in_specs=[rows(E), whole(cpar), whole(hpar), whole(dpar)] + [whole(a) for a in args],
        out_specs=[pl.BlockSpec((DI, T), lambda i: (0, i)), rows(DI), rows(LANES)] + outs,
        out_shape=[
            jax.ShapeDtypeStruct((DI, R), bf16),
            jax.ShapeDtypeStruct((R, DI), f32),
            jax.ShapeDtypeStruct((R, LANES), f32),
        ]
        + shapes,
        scratch_shapes=[
            pltpu.VMEM((max(2, UNROLL_F), FRONT + T, LANES), f32),
            pltpu.VMEM((T, DI), f32),
            pltpu.VMEM((H, T, LANES), f32),
            pltpu.VMEM((LANES, T), f32),
            pltpu.VMEM((T, T), f32),
            pltpu.VMEM((T, T), f32),
            pltpu.VMEM((T, LANES), f32),
            pltpu.VMEM((T, LANES), f32),
        ]
        + sems,
        compiler_params=pltpu.CompilerParams(vmem_limit_bytes=48 << 20, **extra),
        cost_estimate=pl.CostEstimate(
            flops=4 * R * DI * T, bytes_accessed=R * (2 * E + 6 * DI), transcendentals=R * H * T
        ),
        name="mix_forward",
    )(proj, cpar, hpar, dpar, *args)


def run_backward(dims, axis, geom, EP, proj, dmixed, ssd, rstd, cpar, hpar, dpar, mixed, go):
    T, DI, C, H, KW, ST = (dims[k] for k in ("T", "DI", "C", "H", "KW", "ST"))
    R, E = proj.shape
    steps = R // T
    rows = lambda w: pl.BlockSpec((T, w), lambda i: (i, 0))
    whole = lambda s: pl.BlockSpec(s, lambda i: (0,) * len(s))
    once = lambda s: pl.BlockSpec(s, lambda i: (0,) * len(s), pipeline_mode=pl.Buffered(1))
    assert KW + 4 <= 8
    sums = [(8 * (KW + 1), C), (16, DI), (16, LANES)]
    args, net_of, ins, outs, shapes, scratch, extra = [], None, [], [], [], [], {}
    if geom is not None:
        A0, A = geom
        N = A0 * A * A
        r, D = DI // (2 * N), go.shape[1]
        w = 2 * LANES
        K = D // w
        assert K + 4 <= 2 * steps

        def net_of(refs):
            return Reduce(Place(axis, A0, A), K, refs[1:15]), refs[0]

        args = [mixed.reshape(N, 2, r, R), go]
        ins = [once((N, 2, r, R)), once((R, D))]
        outs = [once((r, D))]
        shapes = [jax.ShapeDtypeStruct((r, D), f32)]
        scratch = [pltpu.VMEM((2, N * r, R), bf16)] + Reduce.scratch(K, A0, A, r, w)
        extra = dict(collective_id=4, has_side_effects=True)
    return pl.pallas_call(
        functools.partial(mix_backward, dims, steps, net_of),
        grid=(steps,),
        in_specs=[rows(E), rows(DI), rows(DI), rows(LANES)]
        + [whole(a.shape) for a in (cpar, hpar, dpar)] + ins,
        out_specs=[rows(EP), whole((8, C))] + outs,
        out_shape=[
            jax.ShapeDtypeStruct((R, EP), bf16),
            jax.ShapeDtypeStruct((8, C), f32),
        ]
        + shapes,
        scratch_shapes=[pltpu.VMEM(s, f32) for s in sums]
        + [
            pltpu.VMEM((max(2, UNROLL_B), FRONT + T, LANES), f32),
            pltpu.VMEM((max(2, UNROLL_B), FRONT + T, LANES), f32),
            pltpu.VMEM((H, T, LANES), f32),
            pltpu.VMEM((LANES, T), f32),
            pltpu.VMEM((T, T), f32),
            pltpu.VMEM((T, T), f32),
            pltpu.VMEM((T, LANES), f32),
            pltpu.VMEM((T, LANES), f32),
            pltpu.VMEM((T, T), f32),
            pltpu.VMEM((T, LANES), f32),
            pltpu.VMEM((T, LANES), f32),
            pltpu.VMEM((2, T, ST), bf16),
        ]
        + scratch,
        compiler_params=pltpu.CompilerParams(vmem_limit_bytes=VMEM, **extra),
        cost_estimate=pl.CostEstimate(
            flops=8 * R * DI * T, bytes_accessed=R * (4 * E + 8 * DI), transcendentals=R * H * T
        ),
        name="mix_backward",
    )(proj, dmixed, ssd, rstd, cpar, hpar, dpar, *args)


def gather_project(axis, geom, K, tok, wl, proj, wfull, uT, scale, buf, uh, *sems):
    A0, A = geom
    at = Place(axis, A0, A)
    i = pl.program_id(0)
    R, D = tok.shape
    w = wl.shape[2]

    @pl.when(i == 0)
    def _():
        at.barrier()

    net = Gather(at, K, lambda j: wl.at[j], lambda j, a, p, c: buf.at[j, a, p, c], *sems)
    net.step(i)

    @pl.when(i == 4)
    def _():
        last = buf[0].reshape(D, w)[:, w - LANES :].astype(f32).T
        scale[...] = jnp.broadcast_to(last[LANES - 1 :, :], scale.shape)

        def norm(k, _):
            rows = pl.ds(pl.multiple_of(k * LANES, LANES), LANES)
            u = tok[rows, :].astype(f32)
            r = lax.rsqrt(jnp.mean(u * u, axis=-1, keepdims=True) + epsilon)
            v = u * r * scale[0:1, :]
            uh[rows, :] = v.astype(bf16)
            uT[:, rows] = v.T.astype(bf16)
            return 0

        lax.fori_loop(0, R // LANES, norm, 0)

    @pl.when(i >= 4)
    def _():
        wfull[...] = buf[i - 4].reshape(D, w)
        M = 256

        def rows(k, _):
            at_ = pl.ds(pl.multiple_of(k * M, M), M)
            proj[at_, :] = jnp.dot(
                uh[at_, :], wfull[...], preferred_element_type=f32
            ).astype(bf16)
            return 0

        lax.fori_loop(0, R // M, rows, 0)

    @pl.when(i == K + 3)
    def _():
        net.drain()


def run_gather(axis, geom, tok, wl, E):
    A0, A = geom
    R, D = tok.shape
    K, r, w = wl.shape
    late = lambda i: (0, lax.rem(jnp.maximum(i - 4, 0) + K - 1, K))
    once = dict(pipeline_mode=pl.Buffered(1))
    return pl.pallas_call(
        functools.partial(gather_project, axis, geom, K),
        grid=(K + 4,),
        in_specs=[
            pl.BlockSpec((R, D), lambda i: (0, 0), **once),
            pl.BlockSpec((K, r, w), lambda i: (0, 0, 0), **once),
        ],
        out_specs=[
            pl.BlockSpec((R, w), late),
            pl.BlockSpec((D, w), late),
            pl.BlockSpec((D, R), lambda i: (0, 0), **once),
            pl.BlockSpec((8, D), lambda i: (0, 0), **once),
        ],
        out_shape=[
            jax.ShapeDtypeStruct((R, E), bf16),
            jax.ShapeDtypeStruct((D, K * w), bf16),
            jax.ShapeDtypeStruct((D, R), bf16),
            jax.ShapeDtypeStruct((8, D), f32),
        ],
        scratch_shapes=[
            pltpu.VMEM((K, A0, A * A, 2, r, w), bf16),
            pltpu.VMEM((R, D), bf16),
        ]
        + Gather.scratch(K, A0, A),
        compiler_params=pltpu.CompilerParams(
            collective_id=1, has_side_effects=True, vmem_limit_bytes=VMEM
        ),
        cost_estimate=pl.CostEstimate(
            flops=2 * R * D * E, bytes_accessed=2 * D * E * 40, transcendentals=0
        ),
        name="gather_project",
    )(tok, wl)


def reduce_in(axis, geom, K, E, uT, dproj, wfull, wl, scale, tok, go, small,
              dw, dns, dtok, sums, own, *refs):
    A0, A = geom
    at = Place(axis, A0, A)
    i = pl.program_id(0)
    R, D = tok.shape
    N, _, r, _ = uT.shape
    w = dproj.shape[1]
    net = Reduce(at, K, refs[:14])
    total = SumAll(at, refs[14:18])

    @pl.when(i == 0)
    def _():
        at.barrier()
        total.start(0, small[...])
        own[0] = uT[:, at.c].reshape(N * r, R)
        own[1] = uT[:, 1 - at.c].reshape(N * r, R)
        dns[...] = jnp.zeros_like(dns)

    for stage in range(1, 4):

        @pl.when(i == stage)
        def _(stage=stage):
            total.start(stage, total.finish(stage - 1))

    @pl.when(i == 4)
    def _():
        sums[...] = total.finish(3)

    @pl.when(i < K)
    def _():
        net.begin(i, own, dproj[...])
        M = 256

        def rows(k, _):
            at_ = pl.ds(pl.multiple_of(k * M, M), M)
            part = lax.dot_general(
                dproj[at_, :], wfull[...], (((1,), (1,)), ((), ())), preferred_element_type=f32
            )

            @pl.when(i == 0)
            def _():
                dtok[at_, :] = part

            @pl.when(i > 0)
            def _():
                dtok[at_, :] += part

            return 0

        lax.fori_loop(0, R // M, rows, 0)

    def finish(j, v):
        dw[...] = v
        _, col = iotas(r, w)
        p = jnp.where(col < E - j * w, v * wl[:, pl.ds(0, w)].astype(f32), 0.0)
        part = p[:, 0:LANES]
        for k in range(1, w // LANES):
            part = part + p[:, k * LANES : (k + 1) * LANES]
        dns[...] += part

    net.step(i, finish)

    @pl.when((i >= K) & (i < K + 4))
    def _():
        M = R // 4

        def tail(k, _):
            at_ = pl.ds(pl.multiple_of((i - K) * M + k * 64, 64), 64)
            u = tok[at_, :].astype(f32)
            rs = lax.rsqrt(jnp.mean(u * u, axis=-1, keepdims=True) + epsilon)
            u = u * rs
            d = dtok[at_, :] * scale[0:1, :]
            m = jnp.mean(d * u, axis=-1, keepdims=True)
            dtok[at_, :] = go[at_, :].astype(f32) + rs * (d - u * m)
            return 0

        lax.fori_loop(0, M // 64, tail, 0)

    @pl.when(i == K + 3)
    def _():
        net.drain()


def run_reduce_in(axis, geom, uT, dproj, wfull, wl, scale, tok, go, small):
    A0, A = geom
    R, D = tok.shape
    r, E = wl.shape
    w = CHUNK
    K = dproj.shape[1] // w
    N = A0 * A * A
    once = dict(pipeline_mode=pl.Buffered(1))
    late = lambda i: (0, jnp.clip(i - 4, 0, K - 1))
    early = lambda i: (0, jnp.minimum(i, K - 1))
    whole = lambda i: (0, 0)
    return pl.pallas_call(
        functools.partial(reduce_in, axis, geom, K, E),
        grid=(K + 4,),
        in_specs=[
            pl.BlockSpec((N, 2, r, R), lambda i: (0, 0, 0, 0), **once),
            pl.BlockSpec((R, w), early),
            pl.BlockSpec((D, w), early),
            pl.BlockSpec((r, w), late),
            pl.BlockSpec((8, D), whole, **once),
            pl.BlockSpec((R, D), whole, **once),
            pl.BlockSpec((R, D), whole, **once),
            pl.BlockSpec(small.shape, whole, **once),
        ],
        out_specs=[
            pl.BlockSpec((r, w), late),
            pl.BlockSpec((r, LANES), whole, **once),
            pl.BlockSpec((R, D), whole, **once),
            pl.BlockSpec(small.shape, whole, **once),
        ],
        out_shape=[
            jax.ShapeDtypeStruct((r, E), f32),
            jax.ShapeDtypeStruct((r, LANES), f32),
            jax.ShapeDtypeStruct((R, D), f32),
            jax.ShapeDtypeStruct(small.shape, f32),
        ],
        scratch_shapes=[pltpu.VMEM((2, N * r, R), bf16)]
        + Reduce.scratch(K, A0, A, r, w)
        + SumAll.scratch(A0, A, small.shape),
        compiler_params=pltpu.CompilerParams(
            collective_id=2, has_side_effects=True, vmem_limit_bytes=VMEM
        ),
        cost_estimate=pl.CostEstimate(
            flops=4 * R * D * E, bytes_accessed=2 * D * E * 40, transcendentals=0
        ),
        name="reduce_in",
    )(uT.reshape(N, 2, r, R), dproj, wfull, wl, scale, tok, go, small)


def local(axis, n, tokens, in_weight, conv_weight, conv_bias, dt_bias, a_log, skip_d,
          norm_scale, gate_scale, out_weight, grad_out):
    MB, S, T, D = tokens.shape
    R = MB * S * T
    r, E = in_weight.shape
    H = a_log.shape[0]
    DI = out_weight.shape[0] * n
    Cn, KW = conv_weight.shape
    C = Cn * n
    HD = DI // H
    ST = (C - DI) // 2
    dims = dict(T=T, DI=DI, C=C, H=H, HD=HD, ST=ST, KW=KW)
    assert LANES % HD == 0 and ST == LANES and DI % (LANES * 2) == 0 and T % 16 == 0
    geom = geometry(n)
    w = CHUNK
    K = -(-E // w)
    EP = K * w
    Gn = DI // n
    own = (
        geom is not None and r % 16 == 0 and EP - LANES >= E and max(Cn, Gn) < LANES
        and KW + 2 <= r
    )
    me = lax.axis_index(axis)

    ns = norm_scale.astype(f32)
    tok = tokens.reshape(R, D)
    go = grad_out.reshape(R, D)
    if own:
        rows = [conv_weight.T, conv_bias[None], gate_scale[None]]
        pads = jnp.concatenate(
            [jnp.pad(v, ((0, 0), (0, LANES - 1 - v.shape[1]))) for v in rows]
            + [jnp.zeros((r - KW - 2, LANES - 1), bf16)],
            axis=0,
        )
        wl = jnp.concatenate(
            [in_weight, jnp.zeros((r, EP - LANES - E), bf16), pads, norm_scale[:, None]], axis=1
        )
        wl = jnp.roll(wl.reshape(r, K, w).transpose(1, 0, 2), 1, axis=0)
        proj, wfull, uT, scale = run_gather(axis, geom, tok, wl, E)
        got = wfull.reshape(n, r, EP)[:, : KW + 2, EP - LANES :]
        conv, gate = got[:, : KW + 1, :Cn], got[:, KW + 1, :Gn]
    else:
        EP = E
        out_full = lax.all_gather(out_weight, axis, axis=0, tiled=True)
        wfull = lax.all_gather(in_weight, axis, axis=0, tiled=True)
        conv = lax.all_gather(jnp.concatenate([conv_weight.T, conv_bias[None]]), axis, axis=0)
        gate = lax.all_gather(gate_scale, axis, axis=0)
        scale = lax.all_gather(norm_scale, axis, axis=0).reshape(1, D).astype(f32)
        u = tok.astype(f32)
        rs = lax.rsqrt(jnp.mean(u * u, axis=-1, keepdims=True) + epsilon)
        uh = (u * rs * scale).astype(bf16)
        proj = jnp.dot(uh, wfull, preferred_element_type=f32).astype(bf16)
    conv = conv.transpose(1, 0, 2).reshape(KW + 1, C).astype(f32)

    rate = -jnp.exp(a_log)
    cpar = jnp.concatenate([conv, jnp.zeros((8 - KW - 1, C), f32)], axis=0)
    hpar = jnp.zeros((8, LANES), f32).at[0, :H].set(dt_bias).at[1, :H].set(rate)
    dpar = jnp.concatenate(
        [jnp.repeat(skip_d, HD)[None], gate.reshape(1, DI).astype(f32), jnp.zeros((6, DI), f32)]
    )
    net = geom if own else None
    mixed, ssd, rstd, *got = run_forward(dims, axis, net, proj, cpar, hpar, dpar, out_weight)
    if own:
        out_full = got[0].reshape(DI, D)
    d_mixed = lax.dot_general(go, out_full, (((1,), (1,)), ((), ())), preferred_element_type=f32)
    dproj, small, *got = run_backward(
        dims, axis, net, EP, proj, d_mixed, ssd, rstd, cpar, hpar, dpar, mixed, go
    )
    output = lax.dot_general(
        mixed, out_full, (((0,), (0,)), ((), ())), preferred_element_type=f32
    )
    output = (tok.astype(f32) + output).astype(bf16)
    if own:
        dow = got[0]
        dw, dns, dtok, sums = run_reduce_in(
            axis, geom, uT, dproj, wfull, in_weight, scale, tok, go, small
        )
    else:
        g_out = jnp.dot(mixed, go, preferred_element_type=f32).astype(bf16)
        dow = lax.psum_scatter(g_out, axis, scatter_dimension=0, tiled=True).astype(f32)
        g_in = lax.dot_general(
            uh, dproj, (((0,), (0,)), ((), ())), preferred_element_type=f32
        ).astype(bf16)
        dw = lax.psum_scatter(g_in, axis, scatter_dimension=0, tiled=True).astype(f32)
        dns = dw * in_weight.astype(f32)
        d = lax.dot_general(dproj, wfull, (((1,), (1,)), ((), ())), preferred_element_type=f32)
        u, d = u * rs, d * scale
        dtok = go.astype(f32) + rs * (d - u * jnp.mean(d * u, axis=-1, keepdims=True))
        sums = lax.psum(small, axis)
    dconv = lax.dynamic_slice(sums, (0, me * Cn), (KW + 1, Cn))
    heads = sums[KW + 3]
    return (
        output.reshape(tokens.shape),
        dtok.reshape(tokens.shape),
        dw,
        dconv[:KW].T,
        dconv[KW],
        heads[:H],
        heads[LANES : LANES + H] * rate,
        sums[KW + 1, :DI].reshape(H, HD).sum(axis=1),
        dns.sum(axis=1) / ns,
        lax.dynamic_slice(sums[KW + 2], (me * Gn,), (Gn,)),
        dow,
    )


def solution(mesh):
    axis = mesh.axis_names[0]
    n = mesh.shape[axis]
    rows, flat, batch = P(axis, None), P(axis), P(None, axis, None, None)
    return jax.shard_map(
        functools.partial(local, axis, n),
        mesh=mesh,
        in_specs=(batch, rows, rows, flat, P(), P(), P(), flat, flat, rows, batch),
        out_specs=(batch, batch, rows, rows, flat, P(), P(), P(), flat, flat, rows),
        check_vma=False,
    )
```

```python
import functools
import math

import jax
import jax.numpy as jnp
from jax import lax
from jax.experimental import pallas as pl
from jax.experimental.pallas import tpu as pltpu
from jax.sharding import PartitionSpec as P

epsilon = 1e-05
LOG2E = 1.4426950408889634
BIG = 3.0e38
LANES = 128
FRONT = 8
f32 = jnp.float32
bf16 = jnp.bfloat16
UNROLL_F = 2
UNROLL_B = 2


def sigmoid(v):
    return 0.5 * jnp.tanh(0.5 * v) + 0.5


def sum8(v):
    rows, lanes = v.shape
    return jnp.sum(v.reshape(rows // 8, 8, lanes), axis=0)


def iotas(rows, lanes):
    return (
        lax.broadcasted_iota(jnp.int32, (rows, lanes), 0),
        lax.broadcasted_iota(jnp.int32, (rows, lanes), 1),
    )


def step_stage(dims, proj, hpar, dtp):
    DI, C, H = dims["DI"], dims["C"], dims["H"]
    dtp[...] = jnp.zeros_like(dtp)
    dtp[:, 0:H] = proj[:, DI + C : DI + C + H].astype(f32)
    return steps_of(dims, dtp[...], hpar)


def steps_of(dims, dt, hpar):
    T, H = dims["T"], dims["H"]
    _, lane = iotas(T, LANES)
    v = jnp.where(lane < H, dt + hpar[0:1, :], 0.0)
    e = jnp.exp(-jnp.abs(v))
    step = jnp.maximum(v, 0.0) + jnp.log1p(e)
    row, col = iotas(T, T)
    tri = (row >= col).astype(f32)
    ld = jnp.dot(
        tri, step * (hpar[1:2, :] * LOG2E), precision=lax.Precision.HIGHEST,
        preferred_element_type=f32,
    )
    return v, e, step, ld, ld - jnp.log2(step)


def conv_of(dims, cin, cpar, pad, c0):
    T, KW = dims["T"], dims["KW"]
    lanes = pl.ds(c0, LANES)
    cin = cin.astype(f32)
    pad[FRONT : FRONT + T, :] = cin
    out = cpar[KW : KW + 1, lanes] + cin * cpar[KW - 1 : KW, lanes]
    for k in range(KW - 1):
        out = out + pad[FRONT - KW + 1 + k : FRONT - KW + 1 + k + T, :] * cpar[k : k + 1, lanes]
    return out


def conv_tile(dims, proj, cpar, pad, c0):
    return conv_of(dims, proj[:, pl.ds(dims["DI"] + c0, LANES)], cpar, pad, c0)


def stack_heads(dims, v):
    T, HD = dims["T"], dims["HD"]
    _, lane = iotas(T, LANES)
    zero = jnp.zeros_like(v)
    return jnp.concatenate(
        [jnp.where(lane // HD == a, v, zero) for a in range(LANES // HD)], axis=0
    )


MESH = pl.DeviceIdType.MESH
CHUNK = 512
VMEM = 67043328


def geometry(n):
    chips = n // 2
    A0 = 4 if chips % 4 == 0 else 1
    A = math.isqrt(chips // A0)
    return (A0, A) if n % 2 == 0 and A > 1 and A0 * A * A == chips else None


class Place:
    def __init__(self, axis, A0, A):
        me = lax.axis_index(axis)
        self.A0, self.A = A0, A
        self.c = lax.rem(me, 2)
        chip = lax.div(me, 2)
        self.a2 = lax.rem(chip, A)
        self.a1 = lax.rem(lax.div(chip, A), A)
        self.a0 = lax.div(chip, A * A)
        c = self.c
        self.f = self.a1 + c * (self.a2 - self.a1)
        self.s = self.a2 + c * (self.a1 - self.a2)
        self.sf = A + c * (1 - A)
        self.ss = 1 + c * (A - 1)

    def pos(self, f, s):
        return f * self.sf + s * self.ss

    def device(self, a0, f, s, c):
        return ((a0 * self.A * self.A + self.pos(f, s)) * 2 + c,)

    def line(self, q):
        return lax.rem(self.a0 + q + self.A0, self.A0)

    def first(self, q):
        return lax.rem(self.f + q + self.A, self.A)

    def second(self, q):
        return lax.rem(self.s + q + self.A, self.A)

    def partner(self):
        return self.device(self.a0, self.f, self.s, 1 - self.c)

    def peers(self):
        out = [self.partner()]
        out += [self.device(self.line(q), self.f, self.s, self.c) for q in range(1, self.A0)]
        out += [self.device(self.a0, self.first(q), self.s, self.c) for q in range(1, self.A)]
        out += [self.device(self.a0, self.f, self.second(q), self.c) for q in range(1, self.A)]
        return out

    def barrier(self):
        sem = pltpu.get_barrier_semaphore()
        peers = self.peers()
        for peer in peers:
            pl.semaphore_signal(sem, inc=1, device_id=peer, device_id_type=MESH)
        pl.semaphore_wait(sem, len(peers))


def columns(j, w):
    return pl.ds(pl.multiple_of(j * w, w), w)


def send(src, dst, ssem, rsem, device):
    return pltpu.make_async_remote_copy(
        src_ref=src, dst_ref=dst, send_sem=ssem, recv_sem=rsem,
        device_id=device, device_id_type=MESH,
    )


class Gather:
    def __init__(self, at, K, mine, whole, ssem, rsem, lsem):
        self.at, self.K, self.mine, self.whole = at, K, mine, whole
        self.ssem, self.rsem, self.lsem = ssem, rsem, lsem

    @staticmethod
    def scratch(K, A0, A):
        NS = (A0 - 1) + (A - 1) + (A - 1) * A + 1
        return [
            pltpu.SemaphoreType.DMA((2, NS)),
            pltpu.SemaphoreType.DMA((K, NS)),
            pltpu.SemaphoreType.DMA((2,)),
        ]

    def local(self, j):
        at = self.at
        return pltpu.make_async_copy(
            self.mine(j), self.whole(j, at.a0, at.pos(at.f, at.s), at.c),
            self.lsem.at[lax.rem(j, 2)],
        )

    def copies(self, stage, j, sending):
        at, whole = self.at, self.whole
        A0, A = at.A0, at.A
        par = lax.rem(j, 2)
        every = slice(None)
        out = []

        def add(k, src, dst, device):
            out.append(send(src, dst, self.ssem.at[par, k], self.rsem.at[j, k], device))

        if stage == 0:
            for q in range(1, A0):
                a = at.a0 if sending else at.line(-q)
                add(q - 1, self.mine(j), whole(j, a, at.pos(at.f, at.s), at.c),
                    at.device(at.line(q), at.f, at.s, at.c))
        elif stage == 1:
            for q in range(1, A):
                f = at.f if sending else at.first(-q)
                ref = whole(j, every, at.pos(f, at.s), at.c)
                add(A0 - 1 + q - 1, ref, ref, at.device(at.a0, at.first(q), at.s, at.c))
        elif stage == 2:
            for q in range(1, A):
                s = at.s if sending else at.second(-q)
                for o in range(A):
                    ref = whole(j, every, at.pos(o, s), at.c)
                    add(A0 - 1 + A - 1 + (q - 1) * A + o, ref, ref,
                        at.device(at.a0, at.f, at.second(q), at.c))
        else:
            ref = whole(j, every, every, at.c if sending else 1 - at.c)
            add(A0 - 1 + (A - 1) * (A + 1), ref, ref, at.partner())
        return out

    def step(self, i):
        for stage in range(5):
            j = i - stage

            @pl.when((j >= 0) & (j < self.K))
            def _(stage=stage, j=j):
                if stage > 0:
                    for cp in self.copies(stage - 1, j, False):
                        cp.wait_recv()
                if stage < 4:

                    @pl.when(j >= 2)
                    def _():
                        for cp in self.copies(stage, j - 2, True):
                            cp.wait_send()

                    if stage == 1:
                        self.local(j).wait()
                    for cp in self.copies(stage, j, True):
                        cp.start()
                    if stage == 0:
                        self.local(j).start()

    def drain(self):
        for j in range(max(0, self.K - 2), self.K):
            for stage in range(4):
                for cp in self.copies(stage, jnp.int32(j), True):
                    cp.wait_send()


class Reduce:
    SLOTS = 3

    def __init__(self, at, K, refs):
        self.at, self.K = at, K
        (self.own0, self.own1, self.own2, self.own3, self.s0, self.s1, self.s2, self.s3,
         self.r0, self.r1, self.r2, self.r3, self.ssem, self.rsem, self.credit) = refs

    @staticmethod
    def scratch(K, A0, A, r, w):
        N = A0 * A * A
        NS = 1 + (A - 1) + (A - 1) + (A0 - 1)
        L = Reduce.SLOTS
        return [
            pltpu.VMEM((2, N, r, w), f32),
            pltpu.VMEM((2, A0 * A, r, w), f32),
            pltpu.VMEM((2, A0, r, w), f32),
            pltpu.VMEM((2, r, w), f32),
            pltpu.VMEM((2, N, r, w), bf16),
            pltpu.VMEM((2, A - 1, A0 * A, r, w), bf16),
            pltpu.VMEM((2, A - 1, A0, r, w), bf16),
            pltpu.VMEM((2, A0 - 1, r, w), bf16),
            pltpu.VMEM((L, N, r, w), bf16),
            pltpu.VMEM((L, A - 1, A0 * A, r, w), bf16),
            pltpu.VMEM((L, A - 1, A0, r, w), bf16),
            pltpu.VMEM((L, A0 - 1, r, w), bf16),
            pltpu.SemaphoreType.DMA((2, NS)),
            pltpu.SemaphoreType.DMA((L, NS)),
            pltpu.SemaphoreType.REGULAR((NS,)),
        ]

    def routes(self, stage):
        at = self.at
        A0, A = at.A0, at.A
        if stage == 0:
            return [(0, at.partner(), at.partner())]
        if stage == 1:
            to = lambda q: at.device(at.a0, at.f, at.second(q), at.c)
            return [(q, to(q), to(-q)) for q in range(1, A)]
        if stage == 2:
            to = lambda q: at.device(at.a0, at.first(q), at.s, at.c)
            return [(A - 1 + q, to(q), to(-q)) for q in range(1, A)]
        to = lambda q: at.device(at.line(q), at.f, at.s, at.c)
        return [(2 * (A - 1) + q, to(q), to(-q)) for q in range(1, A0)]

    def copies(self, stage, j):
        par, slot = lax.rem(j, 2), lax.rem(j, self.SLOTS)
        src, dst = ((self.s0, self.r0), (self.s1, self.r1), (self.s2, self.r2),
                    (self.s3, self.r3))[stage]
        out = []
        for q, (k, to, _) in enumerate(self.routes(stage)):
            a = src.at[par] if stage == 0 else src.at[par, q]
            b = dst.at[slot] if stage == 0 else dst.at[slot, q]
            out.append(send(a, b, self.ssem.at[par, k], self.rsem.at[slot, k], to))
        return out

    def free(self, stage, j):
        @pl.when(j >= 2)
        def _():
            for cp in self.copies(stage, j - 2):
                cp.wait_send()

    def start(self, stage, j):
        @pl.when(j >= self.SLOTS)
        def _():
            for k, _, _ in self.routes(stage):
                pl.semaphore_wait(self.credit.at[k], 1)

        for cp in self.copies(stage, j):
            cp.start()

    def arrive(self, stage, j):
        for cp in self.copies(stage, j):
            cp.wait_recv()

    def done(self, stage, j):
        @pl.when(j + self.SLOTS < self.K)
        def _():
            for k, _, source in self.routes(stage):
                pl.semaphore_signal(
                    self.credit.at[k], inc=1, device_id=source, device_id_type=MESH
                )

    def begin(self, j, own, right):
        N, r, w = self.own0.shape[1:]
        par = lax.rem(j, 2)
        rows = lambda k: own[k].reshape(N * r, own.shape[3])
        self.free(0, j)
        self.s0[par] = (
            jnp.dot(rows(1), right, preferred_element_type=f32).astype(bf16).reshape(N, r, w)
        )
        self.start(0, j)
        self.own0[par] = jnp.dot(rows(0), right, preferred_element_type=f32).reshape(N, r, w)

    def step(self, i, finish):
        at = self.at
        A0, A = at.A0, at.A

        def stage1(j, par, slot):
            def line(a, _):
                for o in range(A):
                    for q in range(A):
                        b = a * A * A + at.pos(o, at.second(q))
                        v = self.own0[par, b] + self.r0[slot, b].astype(f32)
                        if q == 0:
                            self.own1[par, a * A + o] = v
                        else:
                            self.s1[par, q - 1, a * A + o] = v.astype(bf16)
                return 0

            lax.fori_loop(0, A0, line, 0)

        def stage2(j, par, slot):
            def line(a, _):
                for q in range(A):
                    b = a * A + at.first(q)
                    v = self.own1[par, b]
                    for p in range(A - 1):
                        v = v + self.r1[slot, p, b].astype(f32)
                    if q == 0:
                        self.own2[par, a] = v
                    else:
                        self.s2[par, q - 1, a] = v.astype(bf16)
                return 0

            lax.fori_loop(0, A0, line, 0)

        def stage3(j, par, slot):
            for q in range(A0):
                a = at.line(q)
                v = self.own2[par, a]
                for p in range(A - 1):
                    v = v + self.r2[slot, p, a].astype(f32)
                if q == 0:
                    self.own3[par] = v
                else:
                    self.s3[par, q - 1] = v.astype(bf16)

        def stage4(j, par, slot):
            v = self.own3[par]
            for p in range(A0 - 1):
                v = v + self.r3[slot, p].astype(f32)
            finish(j, v)

        for k, stage in ((1, stage1), (2, stage2), (3, stage3), (4, stage4)):
            j = i - k

            @pl.when((j >= 0) & (j < self.K))
            def _(j=j, k=k, stage=stage):
                self.arrive(k - 1, j)
                if k < 4:
                    self.free(k, j)
                stage(j, lax.rem(j, 2), lax.rem(j, self.SLOTS))
                self.done(k - 1, j)
                if k < 4:
                    self.start(k, j)

    def drain(self):
        for j in range(max(0, self.K - 2), self.K):
            for stage in range(4):
                for cp in self.copies(stage, jnp.int32(j)):
                    cp.wait_send()


class SumAll:
    def __init__(self, at, refs):
        self.at = at
        self.hold, self.land, self.ssem, self.rsem = refs

    @staticmethod
    def scratch(A0, A, shape):
        slots = 2 + A + A + A0
        return [
            pltpu.VMEM((4,) + shape, f32),
            pltpu.VMEM((slots,) + shape, f32),
            pltpu.SemaphoreType.DMA((slots,)),
            pltpu.SemaphoreType.DMA((slots,)),
        ]

    def group(self, stage):
        at = self.at
        A0, A = at.A0, at.A
        chip = at.a0 * A * A + at.a1 * A + at.a2
        if stage == 0:
            return 0, 2, at.c, 1, chip * 2
        if stage == 1:
            return 2, A, at.a2, 2, (chip - at.a2) * 2 + at.c
        if stage == 2:
            return 2 + A, A, at.a1, 2 * A, (chip - at.a1 * A) * 2 + at.c
        return 2 + 2 * A, A0, at.a0, 2 * A * A, (chip - at.a0 * A * A) * 2 + at.c

    def copies(self, stage, sending):
        base, size, mine, stride, origin = self.group(stage)
        out = []
        for q in range(1, size):
            to = lax.rem(mine + q, size)
            slot = mine if sending else lax.rem(mine - q + size, size)
            out.append(
                send(self.hold.at[stage], self.land.at[base + slot], self.ssem.at[base + q],
                     self.rsem.at[base + q], (origin + to * stride,))
            )
        return out

    def start(self, stage, value):
        base, _, mine, _, _ = self.group(stage)
        self.hold[stage] = value
        self.land[base + mine] = value
        for cp in self.copies(stage, True):
            cp.start()

    def finish(self, stage):
        base, size, _, _, _ = self.group(stage)
        for cp in self.copies(stage, False):
            cp.wait_recv()
        for cp in self.copies(stage, True):
            cp.wait_send()
        total = self.land[base]
        for k in range(1, size):
            total = total + self.land[base + k]
        return total


def mix_forward(dims, proj, cpar, hpar, dpar, mixed, ssd, rstd,
                pad, gated, colb, rowb, mask, scores, acc, dtp):
    T, DI, H, HD, ST = dims["T"], dims["DI"], dims["H"], dims["HD"], dims["ST"]
    HP = LANES // HD
    tiles = DI // LANES
    pad[:, 0:FRONT, :] = jnp.zeros((pad.shape[0], FRONT, LANES), f32)
    _, _, _, ld, ld2 = step_stage(dims, proj, hpar, dtp)
    row, col = iotas(T, T)
    mask[...] = jnp.where(col <= row, BIG, -BIG)
    rowb[...] = ld2.T
    for h in range(H):
        colb[h] = jnp.broadcast_to(ld[:, h : h + 1], (T, LANES))
    bc = []
    for a in range(2):
        conv = conv_tile(dims, proj, cpar, pad.at[a], DI + a * ST)
        bc.append((conv * sigmoid(conv)).astype(bf16))
    scores[...] = lax.dot_general(
        bc[1], bc[0], (((1,), (1,)), ((), ())), preferred_element_type=f32
    )
    acc[...] = jnp.zeros_like(acc)

    def tile(j, u):
        c0 = pl.multiple_of(j * LANES, LANES)
        lanes = pl.ds(c0, LANES)
        conv = conv_tile(dims, proj, cpar, pad.at[u], c0)
        x = (conv * sigmoid(conv)).astype(bf16)
        mix = []
        for a in range(HP):
            h = j * HP + a
            expo = jnp.minimum(colb[h] - rowb[pl.ds(h, 1), :], mask[...])
            mix.append((jnp.exp2(expo) * scores[...]).astype(bf16))
        core = jnp.dot(
            jnp.concatenate(mix, axis=1), stack_heads(dims, x), preferred_element_type=f32
        )
        out = core + dpar[0:1, lanes] * x.astype(f32)
        ssd[:, lanes] = out
        gate = proj[:, lanes].astype(f32)
        g = out * (gate * sigmoid(gate))
        gated[:, lanes] = g
        return g * g

    def body(j, _):
        total = tile(j * UNROLL_F, 0)
        for u in range(1, UNROLL_F):
            total = total + tile(j * UNROLL_F + u, u)
        acc[...] += total
        return 0

    lax.fori_loop(0, tiles // UNROLL_F, body, 0)
    r = lax.rsqrt(jnp.sum(acc[...], axis=1, keepdims=True) * (1.0 / DI) + epsilon)
    rb = jnp.broadcast_to(r, (T, LANES))
    rstd[...] = rb

    def finish(j, _):
        lanes = pl.ds(pl.multiple_of(j * LANES, LANES), LANES)
        mixed[:, lanes] = (gated[:, lanes] * rb * dpar[1:2, lanes]).astype(bf16)
        return 0

    lax.fori_loop(0, tiles, finish, 0)


def mix_backward(dims, steps, proj, dmixed, ssd, rstd, cpar, hpar, dpar, dproj, small,
                 cacc, dacc, hacc, pad, dpad, colb, rowb, mask, scores, acc, dtp, dscores, dlog,
                 csum, bcs):
    T, DI, C, H, HD, ST, KW = (dims[k] for k in ("T", "DI", "C", "H", "HD", "ST", "KW"))
    HP = LANES // HD
    tiles = DI // LANES

    @pl.when(pl.program_id(0) == 0)
    def _():
        cacc[...] = jnp.zeros_like(cacc)
        dacc[...] = jnp.zeros_like(dacc)
        hacc[...] = jnp.zeros_like(hacc)

    pad[:, 0:FRONT, :] = jnp.zeros((pad.shape[0], FRONT, LANES), f32)
    dpad[:, T:, :] = jnp.zeros((dpad.shape[0], FRONT, LANES), f32)
    v, e, step, ld, ld2 = step_stage(dims, proj, hpar, dtp)
    row, col = iotas(T, T)
    mask[...] = jnp.where(row <= col, BIG, -BIG)
    rowb[...] = ld.T
    for h in range(H):
        colb[h] = jnp.broadcast_to(ld2[:, h : h + 1], (T, LANES))
    for a in range(2):
        conv = conv_tile(dims, proj, cpar, pad.at[a], DI + a * ST)
        bcs[a] = (conv * sigmoid(conv)).astype(bf16)
    scores[...] = lax.dot_general(
        bcs[0], bcs[1], (((1,), (1,)), ((), ())), preferred_element_type=f32
    )
    acc[...] = jnp.zeros_like(acc)
    dscores[...] = jnp.zeros_like(dscores)
    dlog[...] = jnp.zeros_like(dlog)
    csum[...] = jnp.zeros_like(csum)
    rb = rstd[...]

    def first(j, _):
        lanes = pl.ds(pl.multiple_of(j * LANES, LANES), LANES)
        gate = proj[:, lanes].astype(f32)
        p = dmixed[:, lanes] * (ssd[:, lanes] * (gate * sigmoid(gate)))
        acc[...] += p * dpar[1:2, lanes]
        dacc[8:16, lanes] += sum8(p * rb)
        return 0

    lax.fori_loop(0, tiles, first, 0)
    mean = jnp.sum(acc[...], axis=1, keepdims=True) * (1.0 / DI)
    mb = jnp.broadcast_to(mean, (T, LANES)) * rb * rb * rb
    acc[...] = mb

    def conv_back(c0, dact, conv, sig, u):
        lanes = pl.ds(c0, LANES)
        dconv = dact * (sig * (1.0 + conv * (1.0 - sig)))
        dpad[u, 0:T, :] = dconv
        dcin = dconv * cpar[KW - 1 : KW, lanes]
        for k in range(KW - 1):
            dcin = dcin + dpad[u, KW - 1 - k : KW - 1 - k + T, :] * cpar[k : k + 1, lanes]
        dproj[:, pl.ds(DI + c0, LANES)] = dcin.astype(bf16)
        for k in range(KW):
            start = FRONT - KW + 1 + k
            cacc[8 * k : 8 * k + 8, lanes] += sum8(dconv * pad[u, start : start + T, :])
        cacc[8 * KW : 8 * KW + 8, lanes] += sum8(dconv)

    def tile(j, u):
        c0 = pl.multiple_of(j * LANES, LANES)
        lanes = pl.ds(c0, LANES)
        conv = conv_tile(dims, proj, cpar, pad.at[u], c0)
        sig = sigmoid(conv)
        x = (conv * sig).astype(bf16)
        xf = x.astype(f32)
        gate = proj[:, lanes].astype(f32)
        gs = sigmoid(gate)
        act = gate * gs
        out = ssd[:, lanes]
        r = rstd[...]
        dgated = r * (dmixed[:, lanes] * dpar[1:2, lanes]) - (out * act) * acc[...]
        dssd = dgated * act
        dproj[:, lanes] = (dgated * out * (gs * (1.0 + gate * (1.0 - gs)))).astype(bf16)
        low = dssd.astype(bf16)
        dacc[0:8, lanes] += sum8(dssd * xf)
        lows = stack_heads(dims, low)
        dmix = lax.dot_general(
            x, lows, (((1,), (1,)), ((), ())), preferred_element_type=f32
        )
        mix = []
        part = None
        for a in range(HP):
            h = j * HP + a
            decay = jnp.exp2(jnp.minimum(rowb[pl.ds(h, 1), :] - colb[h], mask[...]))
            mix.append((decay * scores[...]).astype(bf16))
            term = dmix[:, a * T : (a + 1) * T] * decay
            part = term if part is None else part + term
        core = jnp.dot(jnp.concatenate(mix, axis=1), lows, preferred_element_type=f32)
        skip = dpar[0:1, lanes]
        from_cols = xf * core
        diff = low.astype(f32) * (out - skip * xf) - from_cols
        prow, pcol = iotas(LANES, LANES)
        place = (pcol == j * HP + prow // HD).astype(bf16)
        place = jnp.concatenate([place, place], axis=0)

        def by_head(w):
            hi = w.astype(bf16)
            lo = (w - hi.astype(f32)).astype(bf16)
            return jnp.dot(
                jnp.concatenate([hi, lo], axis=1), place, preferred_element_type=f32
            )

        conv_back(c0, core + skip * dssd, conv, sig, u)
        return part, by_head(diff), by_head(from_cols)

    def body(j, _):
        sums = tile(j * UNROLL_B, 0)
        for u in range(1, UNROLL_B):
            sums = tuple(p + q for p, q in zip(sums, tile(j * UNROLL_B + u, u)))
        dscores[...] += sums[0]
        dlog[...] += sums[1]
        csum[...] += sums[2]
        return 0

    lax.fori_loop(0, tiles // UNROLL_B, body, 0)
    ds = dscores[...].astype(bf16)
    dst = dscores[...].T.astype(bf16)
    dact = (
        jnp.dot(ds, bcs[1], preferred_element_type=f32),
        jnp.dot(dst, bcs[0], preferred_element_type=f32),
    )
    for a in range(2):
        conv = conv_tile(dims, proj, cpar, pad.at[a], DI + a * ST)
        conv_back(DI + a * ST, dact[a], conv, sigmoid(conv), a)
    dsteps = jnp.dot(
        (row <= col).astype(f32), dlog[...], precision=lax.Precision.HIGHEST,
        preferred_element_type=f32,
    )
    sg = jnp.where(v >= 0.0, 1.0, e) / (1.0 + e)
    ratio = jnp.where(step > 1e-30, sg / jnp.maximum(step, 1e-30), 1.0)
    ddt = csum[...] * ratio + dsteps * hpar[1:2, :] * sg
    tail = dproj.shape[1] - DI - C
    if tail > H:
        dproj[:, DI + C :] = jnp.concatenate(
            [ddt[:, 0:H].astype(bf16), jnp.zeros((T, tail - H), bf16)], axis=1
        )
    else:
        dproj[:, DI + C :] = ddt[:, 0:H].astype(bf16)
    hacc[0:8, :] += sum8(ddt)
    hacc[8:16, :] += sum8(dsteps * step)

    @pl.when(pl.program_id(0) == steps - 1)
    def _():
        small[...] = jnp.zeros_like(small)
        for k in range(KW + 1):
            small[k : k + 1, :] = jnp.sum(cacc[8 * k : 8 * k + 8, :], axis=0, keepdims=True)
        for k in range(2):
            small[KW + 1 + k : KW + 2 + k, 0:DI] = jnp.sum(
                dacc[8 * k : 8 * k + 8, :], axis=0, keepdims=True
            )
            small[KW + 3 : KW + 4, k * LANES : (k + 1) * LANES] = jnp.sum(
                hacc[8 * k : 8 * k + 8, :], axis=0, keepdims=True
            )


def run_forward(dims, proj, cpar, hpar, dpar):
    T, DI, C, H, KW = dims["T"], dims["DI"], dims["C"], dims["H"], dims["KW"]
    R, E = proj.shape
    rows = lambda w: pl.BlockSpec((T, w), lambda i: (i, 0))
    whole = lambda a: pl.BlockSpec(a.shape, lambda i: (0, 0))
    return pl.pallas_call(
        functools.partial(mix_forward, dims),
        grid=(R // T,),
        in_specs=[rows(E), whole(cpar), whole(hpar), whole(dpar)],
        out_specs=[rows(DI), rows(DI), rows(LANES)],
        out_shape=[
            jax.ShapeDtypeStruct((R, DI), bf16),
            jax.ShapeDtypeStruct((R, DI), f32),
            jax.ShapeDtypeStruct((R, LANES), f32),
        ],
        scratch_shapes=[
            pltpu.VMEM((max(2, UNROLL_F), FRONT + T, LANES), f32),
            pltpu.VMEM((T, DI), f32),
            pltpu.VMEM((H, T, LANES), f32),
            pltpu.VMEM((LANES, T), f32),
            pltpu.VMEM((T, T), f32),
            pltpu.VMEM((T, T), f32),
            pltpu.VMEM((T, LANES), f32),
            pltpu.VMEM((T, LANES), f32),
        ],
        compiler_params=pltpu.CompilerParams(vmem_limit_bytes=48 << 20),
        name="mix_forward",
    )(proj, cpar, hpar, dpar)


def run_backward(dims, proj, dmixed, ssd, rstd, cpar, hpar, dpar):
    T, DI, C, H, KW, ST = (dims[k] for k in ("T", "DI", "C", "H", "KW", "ST"))
    R, E = proj.shape
    rows = lambda w: pl.BlockSpec((T, w), lambda i: (i, 0))
    whole = lambda s: pl.BlockSpec(s, lambda i: (0, 0))
    sums = [(8 * (KW + 1), C), (16, DI), (16, LANES)]
    return pl.pallas_call(
        functools.partial(mix_backward, dims, R // T),
        grid=(R // T,),
        in_specs=[rows(E), rows(DI), rows(DI), rows(LANES)]
        + [whole(a.shape) for a in (cpar, hpar, dpar)],
        out_specs=[rows(E), whole((8, C))],
        out_shape=[jax.ShapeDtypeStruct((R, E), bf16), jax.ShapeDtypeStruct((8, C), f32)],
        scratch_shapes=[pltpu.VMEM(s, f32) for s in sums]
        + [
            pltpu.VMEM((max(2, UNROLL_B), FRONT + T, LANES), f32),
            pltpu.VMEM((max(2, UNROLL_B), FRONT + T, LANES), f32),
            pltpu.VMEM((H, T, LANES), f32),
            pltpu.VMEM((LANES, T), f32),
            pltpu.VMEM((T, T), f32),
            pltpu.VMEM((T, T), f32),
            pltpu.VMEM((T, LANES), f32),
            pltpu.VMEM((T, LANES), f32),
            pltpu.VMEM((T, T), f32),
            pltpu.VMEM((T, LANES), f32),
            pltpu.VMEM((T, LANES), f32),
            pltpu.VMEM((2, T, ST), bf16),
        ],
        compiler_params=pltpu.CompilerParams(vmem_limit_bytes=56 << 20),
        name="mix_backward",
    )(proj, dmixed, ssd, rstd, cpar, hpar, dpar)


def assemble(parts, size, tiles):
    _, lane = iotas(8, LANES)
    out = []
    for t in range(tiles):
        total = None
        for d in range(t * LANES // size, min(len(parts), -(-(t + 1) * LANES // size))):
            shift = d * size - t * LANES
            v = parts[d] if shift % LANES == 0 else pltpu.roll(parts[d], shift % LANES, 1)
            keep = (lane >= max(shift, 0)) & (lane < min(shift + size, LANES))
            v = jnp.where(keep, v, 0.0)
            total = v if total is None else total + v
        out.append(total)
    return out


def forward(dims, axis, geom, K, KO, tok, wl, ow, hpar, skip, tokc, goc,
            proj, ssd, uT, mT, out, tabs, pars, scale, wfull, ofull,
            uh, wv, wo, pj, gated, mixed, pad, ldtab, rowtab, scores, mask, acc, dtp, wsem, osem,
            *sems):
    T, DI, C, H, HD, ST, KW = (dims[k] for k in ("T", "DI", "C", "H", "HD", "ST", "KW"))
    A0, A = geom
    at = Place(axis, A0, A)
    i = pl.program_id(0)
    R, D = tok.shape
    w = wl.shape[2]
    half = w // 2
    S = R // T
    HP = LANES // HD
    TC = half // LANES
    wo_cols = wo.shape[5]
    net = Gather(at, K, lambda j: wl.at[j], lambda j, a, p, c: wfull.at[j, a, p, c], *sems[:3])
    neto = Gather(
        at, KO, lambda j: ow.at[:, columns(j, wo_cols)],
        lambda j, a, p, c: ofull.at[a, p, c, :, columns(j, wo_cols)], *sems[3:],
    )

    @pl.when(i == 0)
    def _():
        at.barrier()

    net.step(i)
    neto.step(i - K)

    def fetch_w(j):
        slot = lax.rem(j, 2)
        return pltpu.make_async_copy(wfull.at[j], wv.at[slot], wsem.at[slot])

    def fetch_o(k):
        slot = lax.rem(k, 2)
        return pltpu.make_async_copy(
            ofull.at[:, :, :, :, columns(k, wo_cols)], wo.at[slot], osem.at[slot]
        )

    @pl.when((i >= 4) & (i < K + 4))
    def _():
        fetch_w(i - 4).start()

    @pl.when((i >= K + 4) & (i < K + KO + 4))
    def _():
        fetch_o(i - K - 4).start()

    @pl.when(i == 5)
    def _():
        row, col = iotas(T, T)
        mask[...] = jnp.where(col <= row, BIG, -BIG)
        pad[:, 0:FRONT, :] = jnp.zeros((pad.shape[0], FRONT, LANES), f32)
        acc[...] = jnp.zeros_like(acc)

        def seq(s, _):
            rows = pl.ds(pl.multiple_of(s * T, T), T)
            bc = []
            for a in range(2):
                conv = conv_of(dims, pj[0, rows, a * LANES : (a + 1) * LANES], pars, pad.at[a],
                               DI + a * ST)
                bc.append((conv * sigmoid(conv)).astype(bf16))
            scores[s] = lax.dot_general(
                bc[1], bc[0], (((1,), (1,)), ((), ())), preferred_element_type=f32
            )
            _, _, _, ld, ld2 = steps_of(
                dims, pj[0, rows, 2 * LANES : 3 * LANES].astype(f32), hpar
            )
            ldtab[s] = ld
            rowtab[s] = ld2.T
            return 0

        lax.fori_loop(0, S, seq, 0)

    @pl.when((i >= 6) & (i < K + 5))
    def _():
        j = i - 5
        slot = lax.rem(j, 2)
        h0 = (j - 1) * TC * HP

        def seq(s, _):
            rows = pl.ds(pl.multiple_of(s * T, T), T)
            turned = pltpu.roll(ldtab[s], LANES - h0, 1)
            total = None
            for u in range(TC):
                c0 = pl.multiple_of((j - 1) * half + u * LANES, LANES)
                conv = conv_of(
                    dims, pj[slot, rows, half + u * LANES : half + (u + 1) * LANES], pars,
                    pad.at[u], c0,
                )
                x = (conv * sigmoid(conv)).astype(bf16)
                mix = []
                for a in range(HP):
                    k = u * HP + a
                    left = jnp.broadcast_to(turned[:, k : k + 1], (T, T))
                    expo = jnp.minimum(left - rowtab[s, pl.ds(h0 + k, 1), :], mask[...])
                    mix.append((jnp.exp2(expo) * scores[s]).astype(bf16))
                core = jnp.dot(
                    jnp.concatenate(mix, axis=1), stack_heads(dims, x),
                    preferred_element_type=f32,
                )
                o = core + skip[0:1, pl.ds(c0, LANES)] * x.astype(f32)
                ssd[rows, u * LANES : (u + 1) * LANES] = o
                gate = pj[slot, rows, u * LANES : (u + 1) * LANES].astype(f32)
                g = o * (gate * sigmoid(gate))
                gated[rows, pl.ds(c0, LANES)] = g
                total = g * g if total is None else total + g * g
            acc[rows, :] += total
            return 0

        lax.fori_loop(0, S, seq, 0)

    @pl.when((i >= 4) & (i < K + 4))
    def _():
        fetch_w(i - 4).wait()

    @pl.when(i == 4)
    def _():
        N = A0 * A * A * 2
        r = D // N
        Cn, Gn = C // N, DI // N
        last = wv[0].reshape(D, w)[:, w - LANES :].astype(f32)
        turned = last.T
        scale[...] = jnp.broadcast_to(turned[LANES - 1 :, :], scale.shape)
        parts = [last[d * r : d * r + 8, :] for d in range(N)]
        for t, v in enumerate(assemble(parts, Cn, C // LANES)):
            pars[0:8, t * LANES : (t + 1) * LANES] = v
        for t, v in enumerate(assemble(parts, Gn, DI // LANES)):
            pars[8:16, t * LANES : (t + 1) * LANES] = v

        def norm(k, _):
            rows = pl.ds(pl.multiple_of(k * LANES, LANES), LANES)
            u = tok[rows, :].astype(f32)
            rs = lax.rsqrt(jnp.mean(u * u, axis=-1, keepdims=True) + epsilon)
            v = u * rs * scale[0:1, :]
            uh[rows, :] = v.astype(bf16)
            uT[:, rows] = v.T.astype(bf16)
            return 0

        lax.fori_loop(0, R // LANES, norm, 0)

    @pl.when((i >= 4) & (i < K + 4))
    def _():
        slot = lax.rem(i, 2)
        M = 256

        def rows(k, _):
            at_ = pl.ds(pl.multiple_of(k * M, M), M)
            v = jnp.dot(
                uh[at_, :], wv[slot].reshape(D, w), preferred_element_type=f32
            ).astype(bf16)
            pj[slot, at_, :] = v
            proj[0, at_, :] = v
            return 0

        lax.fori_loop(0, R // M, rows, 0)

    @pl.when(i == K + 5)
    def _():
        def seq(s, _):
            rows = pl.ds(pl.multiple_of(s * T, T), T)
            rs = lax.rsqrt(jnp.sum(acc[rows, :], axis=1, keepdims=True) * (1.0 / DI) + epsilon)
            rb = jnp.broadcast_to(rs, (T, LANES))
            tabs[0, rows, :] = rb

            def tile(k, _):
                for u in range(4):
                    lanes = pl.ds(pl.multiple_of((k * 4 + u) * LANES, LANES), LANES)
                    v = gated[rows, lanes] * rb * pars[8 + KW + 1 : 8 + KW + 2, lanes]
                    mixed[rows, lanes] = v.astype(bf16)
                    mT[lanes, rows] = v.T.astype(bf16)
                return 0

            lax.fori_loop(0, DI // LANES // 4, tile, 0)
            return 0

        lax.fori_loop(0, S, seq, 0)
        acc[...] = jnp.zeros_like(acc)

    @pl.when(i >= K + 5)
    def _():
        k = i - K - 5
        slot = lax.rem(k, 2)
        fetch_o(k).wait()
        M = 256

        def rows(m, _):
            at_ = pl.ds(pl.multiple_of(m * M, M), M)
            branch = jnp.dot(
                mixed[at_, :], wo[slot].reshape(DI, wo_cols), preferred_element_type=f32
            )
            out[at_, :] = (tokc[at_, :].astype(f32) + branch).astype(bf16)
            p = branch * goc[at_, :].astype(f32)
            part = p[:, 0:LANES]
            for q in range(1, wo_cols // LANES):
                part = part + p[:, q * LANES : (q + 1) * LANES]
            acc[at_, :] += part
            return 0

        lax.fori_loop(0, R // M, rows, 0)

    @pl.when(i == K + KO + 4)
    def _():
        net.drain()
        neto.drain()
        mu = jnp.sum(acc[...], axis=1, keepdims=True) * (1.0 / DI)
        rb = tabs[0]
        tabs[1] = jnp.broadcast_to(mu, rb.shape) * rb * rb


def run_forward_net(dims, axis, geom, tok, go, wl, ow, hpar, skip):
    T, DI, C, H = (dims[k] for k in ("T", "DI", "C", "H"))
    A0, A = geom
    R, D = tok.shape
    K, r, w = wl.shape
    ro = ow.shape[0]
    half = w // 2
    wc = r * w // ro
    KO = D // wc
    S = R // T
    steps = K + KO + 5
    whole = lambda s: pl.BlockSpec(s, lambda i: (0,) * len(s), pipeline_mode=pl.Buffered(1))
    late = lambda i: (0, jnp.clip(i - K - 5, 0, KO - 1))
    hbm = pl.BlockSpec(memory_space=pl.ANY)
    return pl.pallas_call(
        functools.partial(forward, dims, axis, geom, K, KO),
        grid=(steps,),
        in_specs=[whole((R, D)), whole((K, r, w)), whole((ro, D)), whole((8, LANES)),
                  whole((8, DI)), pl.BlockSpec((R, wc), late), pl.BlockSpec((R, wc), late)],
        out_specs=[
            pl.BlockSpec((1, R, w), lambda i: (jnp.clip(i - 4, 0, K - 1), 0, 0)),
            pl.BlockSpec((R, half), lambda i: (0, jnp.clip(i - 6, 0, K - 2))),
            whole((D, R)), whole((DI, R)),
            pl.BlockSpec((R, wc), late),
            whole((2, R, LANES)), whole((16, C)), whole((8, D)), hbm, hbm,
        ],
        out_shape=[
            jax.ShapeDtypeStruct((K, R, w), bf16),
            jax.ShapeDtypeStruct((R, DI), f32),
            jax.ShapeDtypeStruct((D, R), bf16),
            jax.ShapeDtypeStruct((DI, R), bf16),
            jax.ShapeDtypeStruct((R, D), bf16),
            jax.ShapeDtypeStruct((2, R, LANES), f32),
            jax.ShapeDtypeStruct((16, C), f32),
            jax.ShapeDtypeStruct((8, D), f32),
            jax.ShapeDtypeStruct((K, A0, A * A, 2, r, w), bf16),
            jax.ShapeDtypeStruct((A0, A * A, 2, ro, D), bf16),
        ],
        scratch_shapes=[
            pltpu.VMEM((R, D), bf16),
            pltpu.VMEM((2, A0, A * A, 2, r, w), bf16),
            pltpu.VMEM((2, A0, A * A, 2, ro, wc), bf16),
            pltpu.VMEM((2, R, w), bf16),
            pltpu.VMEM((R, DI), f32),
            pltpu.VMEM((R, DI), bf16),
            pltpu.VMEM((half // LANES, FRONT + T, LANES), f32),
            pltpu.VMEM((S, T, LANES), f32),
            pltpu.VMEM((S, LANES, T), f32),
            pltpu.VMEM((S, T, T), f32),
            pltpu.VMEM((T, T), f32),
            pltpu.VMEM((R, LANES), f32),
            pltpu.VMEM((T, LANES), f32),
            pltpu.SemaphoreType.DMA((2,)),
            pltpu.SemaphoreType.DMA((2,)),
        ]
        + Gather.scratch(K, A0, A) + Gather.scratch(KO, A0, A),
        compiler_params=pltpu.CompilerParams(
            collective_id=1, has_side_effects=True, vmem_limit_bytes=VMEM
        ),
        cost_estimate=pl.CostEstimate(
            flops=2 * R * D * K * w, bytes_accessed=D * K * w * 60, transcendentals=0
        ),
        name="forward",
    )(tok, wl, ow, hpar, skip, tok, go)


def backward(dims, axis, geom, K, KO, E, proj, proj0, ssd, wo, wf, uT, mT, go, wl, tabs, pars,
             skip, hpar, dn, outc, dns, sums,
             uo, mo, dmx, dpj, pad, dpad, ldtab, rowtab, scores, dscores, dlog, csum, bcs, mask,
             cacc, dacc, hacc, small, csem, *refs):
    T, DI, C, H, HD, ST, KW = (dims[k] for k in ("T", "DI", "C", "H", "HD", "ST", "KW"))
    A0, A = geom
    at = Place(axis, A0, A)
    i = pl.program_id(0)
    R = ssd.shape[0]
    _, r, w = wl.shape
    N = A0 * A * A
    half = w // 2
    S = R // T
    HP = LANES // HD
    TC = half // LANES
    D = go.shape[1]
    HF = mo.shape[0]
    slots = dpj.shape[0]
    net = Reduce(at, K + KO, refs[:15])
    total = SumAll(at, refs[15:])

    def fetches():
        out = [(uT.at[:, at.c], uo.at[0]), (uT.at[:, 1 - at.c], uo.at[1])]
        for h in range(HF):
            out += [(mT.at[:, at.c, h], mo.at[h, 0]), (mT.at[:, 1 - at.c, h], mo.at[h, 1])]
        return [pltpu.make_async_copy(s, d, csem.at[k]) for k, (s, d) in enumerate(out)]

    @pl.when(i == 0)
    def _():
        for cp in fetches():
            cp.start()
        at.barrier()
        for ref in (cacc, dacc, hacc, dlog, csum, dscores, dns):
            ref[...] = jnp.zeros_like(ref)
        row, col = iotas(T, T)
        mask[...] = jnp.where(row <= col, BIG, -BIG)
        pad[:, 0:FRONT, :] = jnp.zeros((pad.shape[0], FRONT, LANES), f32)
        dpad[:, T:, :] = jnp.zeros((dpad.shape[0], FRONT, LANES), f32)

        def seq(s, _):
            rows = pl.ds(pl.multiple_of(s * T, T), T)
            for a in range(2):
                conv = conv_of(dims, proj0[0, rows, a * LANES : (a + 1) * LANES], pars, pad.at[a],
                               DI + a * ST)
                bcs[a, rows, :] = (conv * sigmoid(conv)).astype(bf16)
            scores[s] = lax.dot_general(
                bcs[0, rows, :], bcs[1, rows, :], (((1,), (1,)), ((), ())),
                preferred_element_type=f32,
            )
            _, _, _, ld, ld2 = steps_of(
                dims, proj0[0, rows, 2 * LANES : 3 * LANES].astype(f32), hpar
            )
            ldtab[s] = ld2
            rowtab[s] = ld.T
            return 0

        lax.fori_loop(0, S, seq, 0)
        for cp in fetches():
            cp.wait()

    def finish(p, v):
        inner = (p >= 2 * KO) | (lax.rem(p, 2) == 1)

        @pl.when(inner)
        def _():
            g = jnp.where(p >= 2 * KO, p - KO, lax.div(p, 2))
            outc[g] = v
            q = v * wl[lax.rem(g + 1, K)].astype(f32)
            part = q[:, 0:LANES]
            for k in range(1, w // LANES):
                part = part + q[:, k * LANES : (k + 1) * LANES]
            dns[...] += part

        @pl.when(jnp.logical_not(inner))
        def _():
            outc[K + lax.div(p, 2)] = v

    @pl.when(i < KO)
    def _():
        h = lax.div(i, KO // HF)
        net.begin(2 * i, mo.at[h], go[:, columns(lax.rem(i, KO // HF), w)])
        net.step(2 * i, finish)

    def conv_back(slot, rows, lane0, c0, dact, conv, sig, u):
        lanes = pl.ds(c0, LANES)
        dconv = dact * (sig * (1.0 + conv * (1.0 - sig)))
        dpad[u, 0:T, :] = dconv
        dcin = dconv * pars[KW - 1 : KW, lanes]
        for k in range(KW - 1):
            dcin = dcin + dpad[u, KW - 1 - k : KW - 1 - k + T, :] * pars[k : k + 1, lanes]
        dpj[slot, rows, lane0 : lane0 + LANES] = dcin.astype(bf16)
        for k in range(KW):
            start = FRONT - KW + 1 + k
            cacc[8 * k : 8 * k + 8, lanes] += sum8(dconv * pad[u, start : start + T, :])
        cacc[8 * KW : 8 * KW + 8, lanes] += sum8(dconv)

    @pl.when(i < K - 1)
    def _():
        slot = lax.rem(i, slots)
        h0 = i * TC * HP
        M = 256

        def rows_of(m, _):
            at_ = pl.ds(pl.multiple_of(m * M, M), M)
            dmx[at_, :] = lax.dot_general(
                go[at_, :], wo[...], (((1,), (1,)), ((), ())), preferred_element_type=f32
            )
            return 0

        lax.fori_loop(0, R // M, rows_of, 0)

        def seq(s, _):
            rows = pl.ds(pl.multiple_of(s * T, T), T)
            turned = pltpu.roll(ldtab[s], LANES - h0, 1)
            rb, mb = tabs[0, rows, :], tabs[1, rows, :]
            parts = None
            for u in range(TC):
                c0 = pl.multiple_of(i * half + u * LANES, LANES)
                lanes = pl.ds(c0, LANES)
                here = slice(u * LANES, (u + 1) * LANES)
                there = slice(half + u * LANES, half + (u + 1) * LANES)
                conv = conv_of(dims, proj[0, rows, there], pars, pad.at[u], c0)
                sig = sigmoid(conv)
                x = (conv * sig).astype(bf16)
                xf = x.astype(f32)
                gate = proj[0, rows, here].astype(f32)
                gs = sigmoid(gate)
                act = gate * gs
                o = ssd[rows, here]
                dm = dmx[rows, here]
                gated = o * act
                dgated = rb * (dm * pars[8 + KW + 1 : 8 + KW + 2, lanes]) - gated * mb
                dacc[8:16, lanes] += sum8(dm * (gated * rb))
                dssd = dgated * act
                dpj[slot, rows, here] = (
                    dgated * o * (gs * (1.0 + gate * (1.0 - gs)))
                ).astype(bf16)
                low = dssd.astype(bf16)
                dacc[0:8, lanes] += sum8(dssd * xf)
                lows = stack_heads(dims, low)
                dmix = lax.dot_general(
                    x, lows, (((1,), (1,)), ((), ())), preferred_element_type=f32
                )
                mix = []
                part = None
                for a in range(HP):
                    k = u * HP + a
                    right = jnp.broadcast_to(turned[:, k : k + 1], (T, T))
                    decay = jnp.exp2(
                        jnp.minimum(rowtab[s, pl.ds(h0 + k, 1), :] - right, mask[...])
                    )
                    mix.append((decay * scores[s]).astype(bf16))
                    term = dmix[:, a * T : (a + 1) * T] * decay
                    part = term if part is None else part + term
                core = jnp.dot(
                    jnp.concatenate(mix, axis=1), lows, preferred_element_type=f32
                )
                sk = skip[0:1, lanes]
                from_cols = xf * core
                diff = low.astype(f32) * (o - sk * xf) - from_cols
                prow, pcol = iotas(LANES, LANES)
                place = (pcol == h0 + u * HP + prow // HD).astype(bf16)
                both = jnp.concatenate([diff, from_cols], axis=0)
                hi = both.astype(bf16)
                lo = (both - hi.astype(f32)).astype(bf16)
                by_head = jnp.dot(
                    jnp.concatenate([hi, lo], axis=1),
                    jnp.concatenate([place, place], axis=0), preferred_element_type=f32,
                )
                conv_back(slot, rows, half + u * LANES, c0, core + sk * dssd, conv, sig, u)
                new = (part, by_head)
                parts = new if parts is None else tuple(p + q for p, q in zip(parts, new))
            dscores[s] += parts[0]
            dlog[rows, :] += parts[1][0:T]
            csum[rows, :] += parts[1][T:]
            return 0

        lax.fori_loop(0, S, seq, 0)

    @pl.when(i == K - 1)
    def _():
        slot = lax.rem(i, slots)
        row, col = iotas(T, T)
        upper = (row <= col).astype(f32)

        def seq(s, _):
            rows = pl.ds(pl.multiple_of(s * T, T), T)
            ds = dscores[s]
            dact = (
                jnp.dot(ds.astype(bf16), bcs[1, rows, :], preferred_element_type=f32),
                jnp.dot(ds.T.astype(bf16), bcs[0, rows, :], preferred_element_type=f32),
            )
            for a in range(2):
                conv = conv_of(dims, proj0[0, rows, a * LANES : (a + 1) * LANES], pars, pad.at[a],
                               DI + a * ST)
                conv_back(slot, rows, a * LANES, DI + a * ST, dact[a], conv, sigmoid(conv), a)
            v, e, step, _, _ = steps_of(
                dims, proj0[0, rows, 2 * LANES : 3 * LANES].astype(f32), hpar
            )
            dsteps = jnp.dot(
                upper, dlog[rows, :], precision=lax.Precision.HIGHEST,
                preferred_element_type=f32,
            )
            sg = jnp.where(v >= 0.0, 1.0, e) / (1.0 + e)
            ratio = jnp.where(step > 1e-30, sg / jnp.maximum(step, 1e-30), 1.0)
            ddt = csum[rows, :] * ratio + dsteps * hpar[1:2, :] * sg
            _, lane = iotas(T, LANES)
            ddt = jnp.where(lane < H, ddt, 0.0)
            dpj[slot, rows, 2 * LANES : 3 * LANES] = ddt.astype(bf16)
            dpj[slot, rows, 3 * LANES :] = jnp.zeros((T, w - 3 * LANES), bf16)
            hacc[0:8, :] += sum8(ddt)
            hacc[8:16, :] += sum8(dsteps * step)
            return 0

        lax.fori_loop(0, S, seq, 0)
        small[...] = jnp.zeros_like(small)
        for k in range(KW + 1):
            small[k : k + 1, :] = jnp.sum(cacc[8 * k : 8 * k + 8, :], axis=0, keepdims=True)
        for k in range(2):
            small[KW + 1 + k : KW + 2 + k, 0:DI] = jnp.sum(
                dacc[8 * k : 8 * k + 8, :], axis=0, keepdims=True
            )
            small[KW + 3 : KW + 4, k * LANES : (k + 1) * LANES] = jnp.sum(
                hacc[8 * k : 8 * k + 8, :], axis=0, keepdims=True
            )
        total.start(0, small[...])

    for stage in range(1, 4):

        @pl.when(i == K - 1 + stage)
        def _(stage=stage):
            total.start(stage, total.finish(stage - 1))

    @pl.when(i == K + 3)
    def _():
        sums[...] = total.finish(3)

    p = jnp.where(i < KO, 2 * i + 1, i + KO)

    @pl.when(i < K)
    def _():
        net.begin(p, uo, dpj[lax.rem(i, slots)])

    net.step(p, finish)

    lag = slots - 1

    @pl.when(i >= lag)
    def _():
        slot = lax.rem(i - lag, slots)
        M = 256

        def rows_of(m, _):
            at_ = pl.ds(pl.multiple_of(m * M, M), M)
            part = lax.dot_general(
                dpj[slot, at_, :], wf[0], (((1,), (1,)), ((), ())), preferred_element_type=f32
            )

            @pl.when(i == lag)
            def _():
                dn[at_, :] = part

            @pl.when(i > lag)
            def _():
                dn[at_, :] += part

            return 0

        lax.fori_loop(0, R // M, rows_of, 0)

    @pl.when(i == K + 3)
    def _():
        net.drain()


def run_backward_net(dims, axis, geom, E, proj, ssd, ofull, wfull, uT, mT, go, wl, tabs, pars,
                     skip, hpar):
    T, DI, C, H, KW, ST = (dims[k] for k in ("T", "DI", "C", "H", "KW", "ST"))
    A0, A = geom
    N = A0 * A * A
    K, R, w = proj.shape
    r = wl.shape[1]
    D = go.shape[1]
    ro = DI // (2 * N)
    HF = ro // r
    half = w // 2
    S = R // T
    KO = HF * (D // w)
    assert KO <= K - 1 and HF * r == ro and D % w == 0
    slots = 5
    whole = lambda s: pl.BlockSpec(s, lambda i: (0,) * len(s), pipeline_mode=pl.Buffered(1))
    tile = lambda i: jnp.clip(i, 0, K - 2)
    hbm = pl.BlockSpec(memory_space=pl.ANY)
    lagged = lambda i: (lax.rem(jnp.clip(i - slots + 1, 0, K - 1) + 1, K), 0, 0)
    return pl.pallas_call(
        functools.partial(backward, dims, axis, geom, K, KO, E),
        grid=(K + 4,),
        in_specs=[
            pl.BlockSpec((1, R, w), lambda i: (tile(i) + 1, 0, 0)),
            whole((1, R, w)),
            pl.BlockSpec((R, half), lambda i: (0, tile(i))),
            pl.BlockSpec((half, D), lambda i: (tile(i), 0)),
            pl.BlockSpec((1, D, w), lagged),
            hbm, hbm, whole((R, D)), whole((K, r, w)), whole((2, R, LANES)), whole((16, C)),
            whole((8, DI)), whole((8, LANES)),
        ],
        out_specs=[whole((R, D)), whole((K + KO, r, w)), whole((r, LANES)), whole((8, C))],
        out_shape=[
            jax.ShapeDtypeStruct((R, D), f32),
            jax.ShapeDtypeStruct((K + KO, r, w), f32),
            jax.ShapeDtypeStruct((r, LANES), f32),
            jax.ShapeDtypeStruct((8, C), f32),
        ],
        scratch_shapes=[
            pltpu.VMEM((2, N, r, R), bf16),
            pltpu.VMEM((HF, 2, N, r, R), bf16),
            pltpu.VMEM((R, half), f32),
            pltpu.VMEM((slots, R, w), bf16),
            pltpu.VMEM((2, FRONT + T, LANES), f32),
            pltpu.VMEM((2, FRONT + T, LANES), f32),
            pltpu.VMEM((S, T, LANES), f32),
            pltpu.VMEM((S, LANES, T), f32),
            pltpu.VMEM((S, T, T), f32),
            pltpu.VMEM((S, T, T), f32),
            pltpu.VMEM((R, LANES), f32),
            pltpu.VMEM((R, LANES), f32),
            pltpu.VMEM((2, R, ST), bf16),
            pltpu.VMEM((T, T), f32),
            pltpu.VMEM((8 * (KW + 1), C), f32),
            pltpu.VMEM((16, DI), f32),
            pltpu.VMEM((16, LANES), f32),
            pltpu.VMEM((8, C), f32),
            pltpu.SemaphoreType.DMA((2 + 2 * HF,)),
        ]
        + Reduce.scratch(K + KO, A0, A, r, w)
        + SumAll.scratch(A0, A, (8, C)),
        compiler_params=pltpu.CompilerParams(
            collective_id=2, has_side_effects=True, vmem_limit_bytes=VMEM
        ),
        cost_estimate=pl.CostEstimate(
            flops=6 * R * D * K * w, bytes_accessed=D * K * w * 90, transcendentals=0
        ),
        name="backward",
    )(proj, proj, ssd, ofull.reshape(DI, D), wfull.reshape(K, D, w), uT.reshape(N, 2, r, R),
      mT.reshape(N, 2, HF, r, R), go, wl, tabs, pars, skip, hpar)


def local(axis, n, tokens, in_weight, conv_weight, conv_bias, dt_bias, a_log, skip_d,
          norm_scale, gate_scale, out_weight, grad_out):
    MB, S, T, D = tokens.shape
    R = MB * S * T
    r, E = in_weight.shape
    H = a_log.shape[0]
    DI = out_weight.shape[0] * n
    Cn, KW = conv_weight.shape
    C = Cn * n
    HD = DI // H
    ST = (C - DI) // 2
    dims = dict(T=T, DI=DI, C=C, H=H, HD=HD, ST=ST, KW=KW)
    assert LANES % HD == 0 and ST == LANES and DI % (LANES * 2) == 0 and T % 16 == 0
    geom = geometry(n)
    w = CHUNK
    Gn, ro = DI // n, out_weight.shape[0]
    own = (
        geom is not None and r % 16 == 0 and ro % r == 0 and D % w == 0 and DI % (w // 2) == 0
        and w == 2 * ST + 2 * LANES and E == 2 * DI + 2 * ST + H and H <= LANES
        and max(Cn, Gn) < LANES and 6 <= KW + 2 <= 8 and ro // r * (D // w) < DI * 2 // w
    )
    me = lax.axis_index(axis)
    tok = tokens.reshape(R, D)
    go = grad_out.reshape(R, D)
    rate = -jnp.exp(a_log)
    hpar = jnp.pad(jnp.stack([dt_bias, rate]), ((0, 6), (0, LANES - H)))
    skip = jnp.broadcast_to(jnp.repeat(skip_d, HD)[None], (8, DI))
    ns = norm_scale.astype(f32)
    if own:
        rows = [conv_weight.T, conv_bias[None], gate_scale[None]]
        pads = jnp.concatenate(
            [jnp.pad(v, ((0, 0), (0, LANES - 1 - v.shape[1]))) for v in rows]
            + [jnp.zeros((r - KW - 2, LANES - 1), bf16)],
            axis=0,
        )
        first = jnp.concatenate(
            [in_weight[:, 2 * DI :], jnp.zeros((r, LANES - H), bf16), pads, norm_scale[:, None]],
            axis=1,
        )
        K = DI * 2 // w + 1
        rest = in_weight[:, : 2 * DI].reshape(r, 2, K - 1, w // 2).transpose(2, 0, 1, 3)
        wl = jnp.concatenate([first[None], rest.reshape(K - 1, r, w)], axis=0)
        proj, ssd, uT, mT, output, tabs, pars, scale, wfull, ofull = run_forward_net(
            dims, axis, geom, tok, go, wl, out_weight, hpar, skip
        )
        dn, outc, dns, sums = run_backward_net(
            dims, axis, geom, E, proj, ssd, ofull, wfull, uT, mT, go, wl, tabs, pars, skip, hpar
        )
        scale = scale[0:1]
        rest = outc[: K - 1].reshape(K - 1, r, 2, w // 2).transpose(1, 2, 0, 3)
        dw = jnp.concatenate([rest.reshape(r, 2 * DI), outc[K - 1][:, : E - 2 * DI]], axis=1)
        dow = outc[K:].reshape(ro // r, D // w, r, w).transpose(0, 2, 1, 3).reshape(ro, D)
    else:
        out_full = lax.all_gather(out_weight, axis, axis=0, tiled=True)
        wfull = lax.all_gather(in_weight, axis, axis=0, tiled=True)
        conv = lax.all_gather(jnp.concatenate([conv_weight.T, conv_bias[None]]), axis, axis=0)
        conv = conv.transpose(1, 0, 2).reshape(KW + 1, C).astype(f32)
        gate = lax.all_gather(gate_scale, axis, axis=0).reshape(1, DI).astype(f32)
        scale = lax.all_gather(norm_scale, axis, axis=0).reshape(1, D).astype(f32)
        u = tok.astype(f32)
        u = u * lax.rsqrt(jnp.mean(u * u, axis=-1, keepdims=True) + epsilon)
        uh = (u * scale).astype(bf16)
        proj = jnp.dot(uh, wfull, preferred_element_type=f32).astype(bf16)
        cpar = jnp.pad(conv, ((0, 8 - KW - 1), (0, 0)))
        dpar = jnp.concatenate([skip[:1], gate, skip[2:]], axis=0)
        mixed, ssd, rstd = run_forward(dims, proj, cpar, hpar, dpar)
        output = jnp.dot(mixed, out_full, preferred_element_type=f32)
        output = (tok.astype(f32) + output).astype(bf16)
        d_mixed = lax.dot_general(
            go, out_full, (((1,), (1,)), ((), ())), preferred_element_type=f32
        )
        dproj, small = run_backward(dims, proj, d_mixed, ssd, rstd, cpar, hpar, dpar)
        left = (((0,), (0,)), ((), ()))
        g_out = lax.dot_general(mixed, go, left, preferred_element_type=f32).astype(bf16)
        dow = lax.psum_scatter(g_out, axis, scatter_dimension=0, tiled=True).astype(f32)
        g_in = lax.dot_general(uh, dproj, left, preferred_element_type=f32).astype(bf16)
        dw = lax.psum_scatter(g_in, axis, scatter_dimension=0, tiled=True).astype(f32)
        dns = dw * in_weight.astype(f32)
        dn = lax.dot_general(dproj, wfull, (((1,), (1,)), ((), ())), preferred_element_type=f32)
        sums = lax.psum(small, axis)
    u = tok.astype(f32)
    rs = lax.rsqrt(jnp.mean(u * u, axis=-1, keepdims=True) + epsilon)
    u, d = u * rs, dn * scale
    dtok = go.astype(f32) + rs * (d - u * jnp.mean(d * u, axis=-1, keepdims=True))
    dconv = lax.dynamic_slice(sums, (0, me * Cn), (KW + 1, Cn))
    heads = sums[KW + 3]
    return (
        output.reshape(tokens.shape),
        dtok.reshape(tokens.shape),
        dw,
        dconv[:KW].T,
        dconv[KW],
        heads[:H],
        heads[LANES : LANES + H] * rate,
        sums[KW + 1, :DI].reshape(H, HD).sum(axis=1),
        dns.sum(axis=1) / ns,
        lax.dynamic_slice(sums[KW + 2], (me * Gn,), (Gn,)),
        dow,
    )


def solution(mesh):
    axis = mesh.axis_names[0]
    n = mesh.shape[axis]
    rows, flat, batch = P(axis, None), P(axis), P(None, axis, None, None)
    return jax.shard_map(
        functools.partial(local, axis, n),
        mesh=mesh,
        in_specs=(batch, rows, rows, flat, P(), P(), P(), flat, flat, rows, batch),
        out_specs=(batch, batch, rows, rows, flat, P(), P(), P(), flat, flat, rows),
        check_vma=False,
    )
```

```python
import functools
import math

import jax
import jax.numpy as jnp
from jax import lax
from jax.experimental import pallas as pl
from jax.experimental.pallas import tpu as pltpu
from jax.sharding import PartitionSpec as P

epsilon = 1e-05
LOG2E = 1.4426950408889634
BIG = 3.0e38
LANES = 128
FRONT = 8
f32 = jnp.float32
bf16 = jnp.bfloat16
UNROLL_F = 2
UNROLL_B = 2


def sigmoid(v):
    return 0.5 * jnp.tanh(0.5 * v) + 0.5


def sum8(v):
    rows, lanes = v.shape
    return jnp.sum(v.reshape(rows // 8, 8, lanes), axis=0)


def iotas(rows, lanes):
    return (
        lax.broadcasted_iota(jnp.int32, (rows, lanes), 0),
        lax.broadcasted_iota(jnp.int32, (rows, lanes), 1),
    )


def step_stage(dims, proj, hpar, dtp):
    DI, C, H = dims["DI"], dims["C"], dims["H"]
    dtp[...] = jnp.zeros_like(dtp)
    dtp[:, 0:H] = proj[:, DI + C : DI + C + H].astype(f32)
    return steps_of(dims, dtp[...], hpar)


def steps_of(dims, dt, hpar):
    T, H = dims["T"], dims["H"]
    _, lane = iotas(T, LANES)
    v = jnp.where(lane < H, dt + hpar[0:1, :], 0.0)
    e = jnp.exp(-jnp.abs(v))
    step = jnp.maximum(v, 0.0) + jnp.log1p(e)
    row, col = iotas(T, T)
    tri = (row >= col).astype(f32)
    ld = jnp.dot(
        tri, step * (hpar[1:2, :] * LOG2E), precision=lax.Precision.HIGHEST,
        preferred_element_type=f32,
    )
    return v, e, step, ld, ld - jnp.log2(step)


def conv_of(dims, cin, cpar, pad, c0):
    T, KW = dims["T"], dims["KW"]
    lanes = pl.ds(c0, LANES)
    cin = cin.astype(f32)
    pad[FRONT : FRONT + T, :] = cin
    out = cpar[KW : KW + 1, lanes] + cin * cpar[KW - 1 : KW, lanes]
    for k in range(KW - 1):
        out = out + pad[FRONT - KW + 1 + k : FRONT - KW + 1 + k + T, :] * cpar[k : k + 1, lanes]
    return out


def conv_tile(dims, proj, cpar, pad, c0):
    return conv_of(dims, proj[:, pl.ds(dims["DI"] + c0, LANES)], cpar, pad, c0)


def stack_heads(dims, v):
    T, HD = dims["T"], dims["HD"]
    _, lane = iotas(T, LANES)
    zero = jnp.zeros_like(v)
    return jnp.concatenate(
        [jnp.where(lane // HD == a, v, zero) for a in range(LANES // HD)], axis=0
    )


MESH = pl.DeviceIdType.MESH
CHUNK = 512
VMEM = 67043328
ROWS = 512


def geometry(n):
    chips = n // 2
    A0 = 4 if chips % 4 == 0 else 1
    A = math.isqrt(chips // A0)
    return (A0, A) if n % 2 == 0 and A > 1 and A0 * A * A == chips else None


class Place:
    def __init__(self, axis, A0, A):
        me = lax.axis_index(axis)
        self.A0, self.A = A0, A
        self.c = lax.rem(me, 2)
        chip = lax.div(me, 2)
        self.a2 = lax.rem(chip, A)
        self.a1 = lax.rem(lax.div(chip, A), A)
        self.a0 = lax.div(chip, A * A)
        c = self.c
        self.f = self.a1 + c * (self.a2 - self.a1)
        self.s = self.a2 + c * (self.a1 - self.a2)
        self.sf = A + c * (1 - A)
        self.ss = 1 + c * (A - 1)

    def pos(self, f, s):
        return f * self.sf + s * self.ss

    def device(self, a0, f, s, c):
        return ((a0 * self.A * self.A + self.pos(f, s)) * 2 + c,)

    def line(self, q):
        return lax.rem(self.a0 + q + self.A0, self.A0)

    def first(self, q):
        return lax.rem(self.f + q + self.A, self.A)

    def second(self, q):
        return lax.rem(self.s + q + self.A, self.A)

    def partner(self):
        return self.device(self.a0, self.f, self.s, 1 - self.c)

    def peers(self):
        out = [self.partner()]
        out += [self.device(self.line(q), self.f, self.s, self.c) for q in range(1, self.A0)]
        out += [self.device(self.a0, self.first(q), self.s, self.c) for q in range(1, self.A)]
        out += [self.device(self.a0, self.f, self.second(q), self.c) for q in range(1, self.A)]
        return out

    def barrier(self):
        sem = pltpu.get_barrier_semaphore()
        peers = self.peers()
        for peer in peers:
            pl.semaphore_signal(sem, inc=1, device_id=peer, device_id_type=MESH)
        pl.semaphore_wait(sem, len(peers))


def columns(j, w):
    return pl.ds(pl.multiple_of(j * w, w), w)


def send(src, dst, ssem, rsem, device):
    return pltpu.make_async_remote_copy(
        src_ref=src, dst_ref=dst, send_sem=ssem, recv_sem=rsem,
        device_id=device, device_id_type=MESH,
    )


class Gather:
    LAG = 2
    DEEP = 4
    ORDER = (0, 4, 3, 2, 1)
    WARM = 2

    def __init__(self, at, K, mine, whole, ssem, rsem, lsem, warm=0):
        self.at, self.K, self.mine, self.whole, self.warm = at, K, mine, whole, warm
        self.ssem, self.rsem, self.lsem = ssem, rsem, lsem

    @staticmethod
    def scratch(K, A0, A):
        NS = (A0 - 1) * A + (A - 1) + (A - 1) * A + 1
        return [
            pltpu.SemaphoreType.DMA((Gather.DEEP, NS)),
            pltpu.SemaphoreType.DMA((K, NS)),
            pltpu.SemaphoreType.DMA((Gather.DEEP,)),
        ]

    def local(self, j):
        at = self.at
        return pltpu.make_async_copy(
            self.mine(j), self.whole(j, at.a0, at.pos(at.f, at.s), at.c),
            self.lsem.at[lax.rem(j, self.DEEP)],
        )

    def copies(self, stage, j, sending, late):
        at, whole = self.at, self.whole
        A0, A = at.A0, at.A
        par = lax.rem(j, self.DEEP)
        line0, first0 = 0, (A0 - 1) * A
        second0 = first0 + A - 1
        every = slice(None)
        out = []

        def add(k, src, dst, device):
            out.append(send(src, dst, self.ssem.at[par, k], self.rsem.at[j, k], device))

        if stage == 0 and not late:
            for q in range(1, A0):
                a = at.a0 if sending else at.line(-q)
                add(line0 + q - 1, self.mine(j), whole(j, a, at.pos(at.f, at.s), at.c),
                    at.device(at.line(q), at.f, at.s, at.c))
        elif stage == 1 and late:
            for q in range(1, A0):
                a = at.a0 if sending else at.line(-q)
                for o in range(A):
                    ref = whole(j, a, at.pos(o, at.s), at.c)
                    add(line0 + (q - 1) * A + o, ref, ref,
                        at.device(at.line(q), at.f, at.s, at.c))
        elif stage < 2:
            for q in range(1, A):
                f = at.f if sending else at.first(-q)
                ref = whole(j, at.a0 if late else every, at.pos(f, at.s), at.c)
                add(first0 + q - 1, self.mine(j) if late else ref, ref,
                    at.device(at.a0, at.first(q), at.s, at.c))
        elif stage == 2:
            for q in range(1, A):
                s = at.s if sending else at.second(-q)
                for o in range(A):
                    ref = whole(j, every, at.pos(o, s), at.c)
                    add(second0 + (q - 1) * A + o, ref, ref,
                        at.device(at.a0, at.f, at.second(q), at.c))
        else:
            ref = whole(j, every, every, at.c if sending else 1 - at.c)
            add(second0 + (A - 1) * A, ref, ref, at.partner())
        return out

    def each(self, stage, j, sending, act):
        def run(late):
            for cp in self.copies(stage, j, sending, late):
                act(cp)

        if stage >= 2:
            run(False)
            return
        late = lax.rem(j, 3) == 2
        pl.when(late)(lambda: run(True))
        pl.when(jnp.logical_not(late))(lambda: run(False))

    def step(self, i):
        for stage in self.ORDER:
            j = i - stage
            early = (j >= 0) & (j < self.warm)
            j = jnp.where(early, j, i - stage * self.LAG)

            @pl.when(early | ((j >= self.warm) & (j < self.K)))
            def _(stage=stage, j=j):
                if stage > 0:
                    self.each(stage - 1, j, False, lambda cp: cp.wait_recv())
                if stage < 4:

                    @pl.when(j >= self.DEEP)
                    def _():
                        self.each(stage, j - self.DEEP, True, lambda cp: cp.wait_send())

                    if stage == 1:
                        self.local(j).wait()
                    self.each(stage, j, True, lambda cp: cp.start())
                    if stage == 0:
                        self.local(j).start()

    def drain(self):
        for j in range(max(0, self.K - self.DEEP), self.K):
            for stage in range(4):
                for cp in self.copies(stage, jnp.int32(j), True, j % 3 == 2):
                    cp.wait_send()


class Reduce:
    SLOTS = 3
    LAG = 2

    def __init__(self, at, K, refs):
        self.at, self.K = at, K
        (self.own0, self.own1, self.own2, self.own3, self.s0, self.s1, self.s2, self.s3,
         self.r0, self.r1, self.r2, self.r3, self.ssem, self.rsem, self.credit) = refs

    @staticmethod
    def scratch(K, A0, A, r, w):
        N = A0 * A * A
        NS = 1 + (A - 1) + (A - 1) + (A0 - 1)
        L = Reduce.SLOTS
        return [
            pltpu.VMEM((2, N, r, w), f32),
            pltpu.VMEM((2, A0 * A, r, w), f32),
            pltpu.VMEM((2, A0, r, w), f32),
            pltpu.VMEM((2, r, w), f32),
            pltpu.VMEM((2, N, r, w), bf16),
            pltpu.VMEM((2, A - 1, A0 * A, r, w), bf16),
            pltpu.VMEM((2, A - 1, A0, r, w), bf16),
            pltpu.VMEM((2, A0 - 1, r, w), bf16),
            pltpu.VMEM((L, N, r, w), bf16),
            pltpu.VMEM((L, A - 1, A0 * A, r, w), bf16),
            pltpu.VMEM((L, A - 1, A0, r, w), bf16),
            pltpu.VMEM((L, A0 - 1, r, w), bf16),
            pltpu.SemaphoreType.DMA((2, NS)),
            pltpu.SemaphoreType.DMA((L, NS)),
            pltpu.SemaphoreType.REGULAR((NS,)),
        ]

    def routes(self, stage):
        at = self.at
        A0, A = at.A0, at.A
        if stage == 0:
            return [(0, at.partner(), at.partner())]
        if stage == 1:
            to = lambda q: at.device(at.a0, at.f, at.second(q), at.c)
            return [(q, to(q), to(-q)) for q in range(1, A)]
        if stage == 2:
            to = lambda q: at.device(at.a0, at.first(q), at.s, at.c)
            return [(A - 1 + q, to(q), to(-q)) for q in range(1, A)]
        to = lambda q: at.device(at.line(q), at.f, at.s, at.c)
        return [(2 * (A - 1) + q, to(q), to(-q)) for q in range(1, A0)]

    def copies(self, stage, j):
        par, slot = lax.rem(j, 2), lax.rem(j, self.SLOTS)
        src, dst = ((self.s0, self.r0), (self.s1, self.r1), (self.s2, self.r2),
                    (self.s3, self.r3))[stage]
        out = []
        for q, (k, to, _) in enumerate(self.routes(stage)):
            a = src.at[par] if stage == 0 else src.at[par, q]
            b = dst.at[slot] if stage == 0 else dst.at[slot, q]
            out.append(send(a, b, self.ssem.at[par, k], self.rsem.at[slot, k], to))
        return out

    def free(self, stage, j):
        @pl.when(j >= 2)
        def _():
            for cp in self.copies(stage, j - 2):
                cp.wait_send()

    def start(self, stage, j):
        @pl.when(j >= self.SLOTS)
        def _():
            for k, _, _ in self.routes(stage):
                pl.semaphore_wait(self.credit.at[k], 1)

        for cp in self.copies(stage, j):
            cp.start()

    def arrive(self, stage, j):
        for cp in self.copies(stage, j):
            cp.wait_recv()

    def done(self, stage, j):
        @pl.when(j + self.SLOTS < self.K)
        def _():
            for k, _, source in self.routes(stage):
                pl.semaphore_signal(
                    self.credit.at[k], inc=1, device_id=source, device_id_type=MESH
                )

    def begin(self, j, own, right):
        N, r, w = self.own0.shape[1:]
        par = lax.rem(j, 2)
        rows = lambda k: own[k].reshape(N * r, own.shape[3])
        self.free(0, j)
        self.s0[par] = (
            jnp.dot(rows(1), right, preferred_element_type=f32).astype(bf16).reshape(N, r, w)
        )
        self.start(0, j)
        self.own0[par] = jnp.dot(rows(0), right, preferred_element_type=f32).reshape(N, r, w)

    def step(self, i, finish):
        at = self.at
        A0, A = at.A0, at.A

        def stage1(j, par, slot):
            def line(a, _):
                for o in range(A):
                    for q in range(A):
                        b = a * A * A + at.pos(o, at.second(q))
                        v = self.own0[par, b] + self.r0[slot, b].astype(f32)
                        if q == 0:
                            self.own1[par, a * A + o] = v
                        else:
                            self.s1[par, q - 1, a * A + o] = v.astype(bf16)
                return 0

            lax.fori_loop(0, A0, line, 0)

        def stage2(j, par, slot):
            def line(a, _):
                for q in range(A):
                    b = a * A + at.first(q)
                    v = self.own1[par, b]
                    for p in range(A - 1):
                        v = v + self.r1[slot, p, b].astype(f32)
                    if q == 0:
                        self.own2[par, a] = v
                    else:
                        self.s2[par, q - 1, a] = v.astype(bf16)
                return 0

            lax.fori_loop(0, A0, line, 0)

        def stage3(j, par, slot):
            for q in range(A0):
                a = at.line(q)
                v = self.own2[par, a]
                for p in range(A - 1):
                    v = v + self.r2[slot, p, a].astype(f32)
                if q == 0:
                    self.own3[par] = v
                else:
                    self.s3[par, q - 1] = v.astype(bf16)

        def stage4(j, par, slot):
            v = self.own3[par]
            for p in range(A0 - 1):
                v = v + self.r3[slot, p].astype(f32)
            finish(j, v)

        for k, stage in ((4, stage4), (3, stage3), (2, stage2), (1, stage1)):
            j = i - k * self.LAG

            @pl.when((j >= 0) & (j < self.K))
            def _(j=j, k=k, stage=stage):
                self.arrive(k - 1, j)
                if k < 4:
                    self.free(k, j)
                stage(j, lax.rem(j, 2), lax.rem(j, self.SLOTS))
                self.done(k - 1, j)
                if k < 4:
                    self.start(k, j)

    def drain(self):
        for j in range(max(0, self.K - 2), self.K):
            for stage in range(4):
                for cp in self.copies(stage, jnp.int32(j)):
                    cp.wait_send()


class SumAll:
    def __init__(self, at, refs):
        self.at = at
        self.hold, self.land, self.ssem, self.rsem = refs

    @staticmethod
    def scratch(A0, A, shape):
        slots = 2 + A + A + A0
        return [
            pltpu.VMEM((4,) + shape, f32),
            pltpu.VMEM((slots,) + shape, f32),
            pltpu.SemaphoreType.DMA((slots,)),
            pltpu.SemaphoreType.DMA((slots,)),
        ]

    def group(self, stage):
        at = self.at
        A0, A = at.A0, at.A
        chip = at.a0 * A * A + at.a1 * A + at.a2
        if stage == 0:
            return 0, 2, at.c, 1, chip * 2
        if stage == 1:
            return 2, A, at.a2, 2, (chip - at.a2) * 2 + at.c
        if stage == 2:
            return 2 + A, A, at.a1, 2 * A, (chip - at.a1 * A) * 2 + at.c
        return 2 + 2 * A, A0, at.a0, 2 * A * A, (chip - at.a0 * A * A) * 2 + at.c

    def copies(self, stage, sending):
        base, size, mine, stride, origin = self.group(stage)
        out = []
        for q in range(1, size):
            to = lax.rem(mine + q, size)
            slot = mine if sending else lax.rem(mine - q + size, size)
            out.append(
                send(self.hold.at[stage], self.land.at[base + slot], self.ssem.at[base + q],
                     self.rsem.at[base + q], (origin + to * stride,))
            )
        return out

    def start(self, stage, value):
        base, _, mine, _, _ = self.group(stage)
        self.hold[stage] = value
        self.land[base + mine] = value
        for cp in self.copies(stage, True):
            cp.start()

    def finish(self, stage):
        base, size, _, _, _ = self.group(stage)
        for cp in self.copies(stage, False):
            cp.wait_recv()
        for cp in self.copies(stage, True):
            cp.wait_send()
        total = self.land[base]
        for k in range(1, size):
            total = total + self.land[base + k]
        return total


def mix_forward(dims, proj, cpar, hpar, dpar, mixed, ssd, rstd,
                pad, gated, colb, rowb, mask, scores, acc, dtp):
    T, DI, H, HD, ST = dims["T"], dims["DI"], dims["H"], dims["HD"], dims["ST"]
    HP = LANES // HD
    tiles = DI // LANES
    pad[:, 0:FRONT, :] = jnp.zeros((pad.shape[0], FRONT, LANES), f32)
    _, _, _, ld, ld2 = step_stage(dims, proj, hpar, dtp)
    row, col = iotas(T, T)
    mask[...] = jnp.where(col <= row, BIG, -BIG)
    rowb[...] = ld2.T
    for h in range(H):
        colb[h] = jnp.broadcast_to(ld[:, h : h + 1], (T, LANES))
    bc = []
    for a in range(2):
        conv = conv_tile(dims, proj, cpar, pad.at[a], DI + a * ST)
        bc.append((conv * sigmoid(conv)).astype(bf16))
    scores[...] = lax.dot_general(
        bc[1], bc[0], (((1,), (1,)), ((), ())), preferred_element_type=f32
    )
    acc[...] = jnp.zeros_like(acc)

    def tile(j, u):
        c0 = pl.multiple_of(j * LANES, LANES)
        lanes = pl.ds(c0, LANES)
        conv = conv_tile(dims, proj, cpar, pad.at[u], c0)
        x = (conv * sigmoid(conv)).astype(bf16)
        mix = []
        for a in range(HP):
            h = j * HP + a
            expo = jnp.minimum(colb[h] - rowb[pl.ds(h, 1), :], mask[...])
            mix.append((jnp.exp2(expo) * scores[...]).astype(bf16))
        core = jnp.dot(
            jnp.concatenate(mix, axis=1), stack_heads(dims, x), preferred_element_type=f32
        )
        out = core + dpar[0:1, lanes] * x.astype(f32)
        ssd[:, lanes] = out
        gate = proj[:, lanes].astype(f32)
        g = out * (gate * sigmoid(gate))
        gated[:, lanes] = g
        return g * g

    def body(j, _):
        total = tile(j * UNROLL_F, 0)
        for u in range(1, UNROLL_F):
            total = total + tile(j * UNROLL_F + u, u)
        acc[...] += total
        return 0

    lax.fori_loop(0, tiles // UNROLL_F, body, 0)
    r = lax.rsqrt(jnp.sum(acc[...], axis=1, keepdims=True) * (1.0 / DI) + epsilon)
    rb = jnp.broadcast_to(r, (T, LANES))
    rstd[...] = rb

    def finish(j, _):
        lanes = pl.ds(pl.multiple_of(j * LANES, LANES), LANES)
        mixed[:, lanes] = (gated[:, lanes] * rb * dpar[1:2, lanes]).astype(bf16)
        return 0

    lax.fori_loop(0, tiles, finish, 0)


def mix_backward(dims, steps, proj, dmixed, ssd, rstd, cpar, hpar, dpar, dproj, small,
                 cacc, dacc, hacc, pad, dpad, colb, rowb, mask, scores, acc, dtp, dscores, dlog,
                 csum, bcs):
    T, DI, C, H, HD, ST, KW = (dims[k] for k in ("T", "DI", "C", "H", "HD", "ST", "KW"))
    HP = LANES // HD
    tiles = DI // LANES

    @pl.when(pl.program_id(0) == 0)
    def _():
        cacc[...] = jnp.zeros_like(cacc)
        dacc[...] = jnp.zeros_like(dacc)
        hacc[...] = jnp.zeros_like(hacc)

    pad[:, 0:FRONT, :] = jnp.zeros((pad.shape[0], FRONT, LANES), f32)
    dpad[:, T:, :] = jnp.zeros((dpad.shape[0], FRONT, LANES), f32)
    v, e, step, ld, ld2 = step_stage(dims, proj, hpar, dtp)
    row, col = iotas(T, T)
    mask[...] = jnp.where(row <= col, BIG, -BIG)
    rowb[...] = ld.T
    for h in range(H):
        colb[h] = jnp.broadcast_to(ld2[:, h : h + 1], (T, LANES))
    for a in range(2):
        conv = conv_tile(dims, proj, cpar, pad.at[a], DI + a * ST)
        bcs[a] = (conv * sigmoid(conv)).astype(bf16)
    scores[...] = lax.dot_general(
        bcs[0], bcs[1], (((1,), (1,)), ((), ())), preferred_element_type=f32
    )
    acc[...] = jnp.zeros_like(acc)
    dscores[...] = jnp.zeros_like(dscores)
    dlog[...] = jnp.zeros_like(dlog)
    csum[...] = jnp.zeros_like(csum)
    rb = rstd[...]

    def first(j, _):
        lanes = pl.ds(pl.multiple_of(j * LANES, LANES), LANES)
        gate = proj[:, lanes].astype(f32)
        p = dmixed[:, lanes] * (ssd[:, lanes] * (gate * sigmoid(gate)))
        acc[...] += p * dpar[1:2, lanes]
        dacc[8:16, lanes] += sum8(p * rb)
        return 0

    lax.fori_loop(0, tiles, first, 0)
    mean = jnp.sum(acc[...], axis=1, keepdims=True) * (1.0 / DI)
    mb = jnp.broadcast_to(mean, (T, LANES)) * rb * rb * rb
    acc[...] = mb

    def conv_back(c0, dact, conv, sig, u):
        lanes = pl.ds(c0, LANES)
        dconv = dact * (sig * (1.0 + conv * (1.0 - sig)))
        dpad[u, 0:T, :] = dconv
        dcin = dconv * cpar[KW - 1 : KW, lanes]
        for k in range(KW - 1):
            dcin = dcin + dpad[u, KW - 1 - k : KW - 1 - k + T, :] * cpar[k : k + 1, lanes]
        dproj[:, pl.ds(DI + c0, LANES)] = dcin.astype(bf16)
        for k in range(KW):
            start = FRONT - KW + 1 + k
            cacc[8 * k : 8 * k + 8, lanes] += sum8(dconv * pad[u, start : start + T, :])
        cacc[8 * KW : 8 * KW + 8, lanes] += sum8(dconv)

    def tile(j, u):
        c0 = pl.multiple_of(j * LANES, LANES)
        lanes = pl.ds(c0, LANES)
        conv = conv_tile(dims, proj, cpar, pad.at[u], c0)
        sig = sigmoid(conv)
        x = (conv * sig).astype(bf16)
        xf = x.astype(f32)
        gate = proj[:, lanes].astype(f32)
        gs = sigmoid(gate)
        act = gate * gs
        out = ssd[:, lanes]
        r = rstd[...]
        dgated = r * (dmixed[:, lanes] * dpar[1:2, lanes]) - (out * act) * acc[...]
        dssd = dgated * act
        dproj[:, lanes] = (dgated * out * (gs * (1.0 + gate * (1.0 - gs)))).astype(bf16)
        low = dssd.astype(bf16)
        dacc[0:8, lanes] += sum8(dssd * xf)
        lows = stack_heads(dims, low)
        dmix = lax.dot_general(
            x, lows, (((1,), (1,)), ((), ())), preferred_element_type=f32
        )
        mix = []
        part = None
        for a in range(HP):
            h = j * HP + a
            decay = jnp.exp2(jnp.minimum(rowb[pl.ds(h, 1), :] - colb[h], mask[...]))
            mix.append((decay * scores[...]).astype(bf16))
            term = dmix[:, a * T : (a + 1) * T] * decay
            part = term if part is None else part + term
        core = jnp.dot(jnp.concatenate(mix, axis=1), lows, preferred_element_type=f32)
        skip = dpar[0:1, lanes]
        from_cols = xf * core
        diff = low.astype(f32) * (out - skip * xf) - from_cols
        prow, pcol = iotas(LANES, LANES)
        place = (pcol == j * HP + prow // HD).astype(bf16)
        place = jnp.concatenate([place, place], axis=0)

        def by_head(w):
            hi = w.astype(bf16)
            lo = (w - hi.astype(f32)).astype(bf16)
            return jnp.dot(
                jnp.concatenate([hi, lo], axis=1), place, preferred_element_type=f32
            )

        conv_back(c0, core + skip * dssd, conv, sig, u)
        return part, by_head(diff), by_head(from_cols)

    def body(j, _):
        sums = tile(j * UNROLL_B, 0)
        for u in range(1, UNROLL_B):
            sums = tuple(p + q for p, q in zip(sums, tile(j * UNROLL_B + u, u)))
        dscores[...] += sums[0]
        dlog[...] += sums[1]
        csum[...] += sums[2]
        return 0

    lax.fori_loop(0, tiles // UNROLL_B, body, 0)
    ds = dscores[...].astype(bf16)
    dst = dscores[...].T.astype(bf16)
    dact = (
        jnp.dot(ds, bcs[1], preferred_element_type=f32),
        jnp.dot(dst, bcs[0], preferred_element_type=f32),
    )
    for a in range(2):
        conv = conv_tile(dims, proj, cpar, pad.at[a], DI + a * ST)
        conv_back(DI + a * ST, dact[a], conv, sigmoid(conv), a)
    dsteps = jnp.dot(
        (row <= col).astype(f32), dlog[...], precision=lax.Precision.HIGHEST,
        preferred_element_type=f32,
    )
    sg = jnp.where(v >= 0.0, 1.0, e) / (1.0 + e)
    ratio = jnp.where(step > 1e-30, sg / jnp.maximum(step, 1e-30), 1.0)
    ddt = csum[...] * ratio + dsteps * hpar[1:2, :] * sg
    tail = dproj.shape[1] - DI - C
    if tail > H:
        dproj[:, DI + C :] = jnp.concatenate(
            [ddt[:, 0:H].astype(bf16), jnp.zeros((T, tail - H), bf16)], axis=1
        )
    else:
        dproj[:, DI + C :] = ddt[:, 0:H].astype(bf16)
    hacc[0:8, :] += sum8(ddt)
    hacc[8:16, :] += sum8(dsteps * step)

    @pl.when(pl.program_id(0) == steps - 1)
    def _():
        small[...] = jnp.zeros_like(small)
        for k in range(KW + 1):
            small[k : k + 1, :] = jnp.sum(cacc[8 * k : 8 * k + 8, :], axis=0, keepdims=True)
        for k in range(2):
            small[KW + 1 + k : KW + 2 + k, 0:DI] = jnp.sum(
                dacc[8 * k : 8 * k + 8, :], axis=0, keepdims=True
            )
            small[KW + 3 : KW + 4, k * LANES : (k + 1) * LANES] = jnp.sum(
                hacc[8 * k : 8 * k + 8, :], axis=0, keepdims=True
            )


def run_forward(dims, proj, cpar, hpar, dpar):
    T, DI, C, H, KW = dims["T"], dims["DI"], dims["C"], dims["H"], dims["KW"]
    R, E = proj.shape
    rows = lambda w: pl.BlockSpec((T, w), lambda i: (i, 0))
    whole = lambda a: pl.BlockSpec(a.shape, lambda i: (0, 0))
    return pl.pallas_call(
        functools.partial(mix_forward, dims),
        grid=(R // T,),
        in_specs=[rows(E), whole(cpar), whole(hpar), whole(dpar)],
        out_specs=[rows(DI), rows(DI), rows(LANES)],
        out_shape=[
            jax.ShapeDtypeStruct((R, DI), bf16),
            jax.ShapeDtypeStruct((R, DI), f32),
            jax.ShapeDtypeStruct((R, LANES), f32),
        ],
        scratch_shapes=[
            pltpu.VMEM((max(2, UNROLL_F), FRONT + T, LANES), f32),
            pltpu.VMEM((T, DI), f32),
            pltpu.VMEM((H, T, LANES), f32),
            pltpu.VMEM((LANES, T), f32),
            pltpu.VMEM((T, T), f32),
            pltpu.VMEM((T, T), f32),
            pltpu.VMEM((T, LANES), f32),
            pltpu.VMEM((T, LANES), f32),
        ],
        compiler_params=pltpu.CompilerParams(vmem_limit_bytes=48 << 20),
        name="mix_forward",
    )(proj, cpar, hpar, dpar)


def run_backward(dims, proj, dmixed, ssd, rstd, cpar, hpar, dpar):
    T, DI, C, H, KW, ST = (dims[k] for k in ("T", "DI", "C", "H", "KW", "ST"))
    R, E = proj.shape
    rows = lambda w: pl.BlockSpec((T, w), lambda i: (i, 0))
    whole = lambda s: pl.BlockSpec(s, lambda i: (0, 0))
    sums = [(8 * (KW + 1), C), (16, DI), (16, LANES)]
    return pl.pallas_call(
        functools.partial(mix_backward, dims, R // T),
        grid=(R // T,),
        in_specs=[rows(E), rows(DI), rows(DI), rows(LANES)]
        + [whole(a.shape) for a in (cpar, hpar, dpar)],
        out_specs=[rows(E), whole((8, C))],
        out_shape=[jax.ShapeDtypeStruct((R, E), bf16), jax.ShapeDtypeStruct((8, C), f32)],
        scratch_shapes=[pltpu.VMEM(s, f32) for s in sums]
        + [
            pltpu.VMEM((max(2, UNROLL_B), FRONT + T, LANES), f32),
            pltpu.VMEM((max(2, UNROLL_B), FRONT + T, LANES), f32),
            pltpu.VMEM((H, T, LANES), f32),
            pltpu.VMEM((LANES, T), f32),
            pltpu.VMEM((T, T), f32),
            pltpu.VMEM((T, T), f32),
            pltpu.VMEM((T, LANES), f32),
            pltpu.VMEM((T, LANES), f32),
            pltpu.VMEM((T, T), f32),
            pltpu.VMEM((T, LANES), f32),
            pltpu.VMEM((T, LANES), f32),
            pltpu.VMEM((2, T, ST), bf16),
        ],
        compiler_params=pltpu.CompilerParams(vmem_limit_bytes=56 << 20),
        name="mix_backward",
    )(proj, dmixed, ssd, rstd, cpar, hpar, dpar)


def assemble(parts, size, tiles):
    _, lane = iotas(8, LANES)
    out = []
    for t in range(tiles):
        total = None
        for d in range(t * LANES // size, min(len(parts), -(-(t + 1) * LANES // size))):
            shift = d * size - t * LANES
            v = parts[d] if shift % LANES == 0 else pltpu.roll(parts[d], shift % LANES, 1)
            keep = (lane >= max(shift, 0)) & (lane < min(shift + size, LANES))
            v = jnp.where(keep, v, 0.0)
            total = v if total is None else total + v
        out.append(total)
    return out


def forward(dims, axis, geom, K, KO, skip, tok, inw, taps, bias, gains, ns, dtb, alog, ow,
            tokc, goc, proj, ssd, uT, mT, out, tabs, pars, scale, wl, hpar, wfull, ofull,
            uh, wv, wo, pj, gated, mixed, pad, ldtab, rowtab, scores, mask, acc, dtp, wsem, osem,
            *sems):
    T, DI, C, H, HD, ST, KW = (dims[k] for k in ("T", "DI", "C", "H", "HD", "ST", "KW"))
    A0, A = geom
    at = Place(axis, A0, A)
    i = pl.program_id(0)
    R, D = tok.shape
    w = wl.shape[2]
    half = w // 2
    S = R // T
    HP = LANES // HD
    TC = half // LANES
    wo_cols = wo.shape[5]
    place = lambda j: lax.rem(j + K - 1, K)
    part = lambda j: columns(lax.rem(j, 2), half)
    net = Gather(
        at, 2 * K, lambda j: wl.at[lax.div(j, 2), :, part(j)],
        lambda j, a, p, c: wfull.at[place(lax.div(j, 2)), a, p, c, :, part(j)], *sems[:3],
        warm=Gather.WARM,
    )
    neto = Gather(
        at, 2 * KO, lambda j: ow.at[:, columns(j, wo_cols // 2)],
        lambda j, a, p, c: ofull.at[a, p, c, :, columns(j, wo_cols // 2)], *sems[3:],
    )

    @pl.when(i == 0)
    def _():
        r, E = inw.shape
        Cn, Gn = bias.shape[1], gains.shape[1]
        zero = jnp.zeros((LANES, LANES), f32)
        dtp[...] = zero
        dtp[0:1, 0:r] = ns[...].astype(f32)
        column = pltpu.roll(dtp[...].T, LANES - 1, 1)
        dtp[...] = column
        dtp[0:KW, 0:Cn] = taps[...].astype(f32)
        dtp[KW : KW + 1, 0:Cn] = bias[...].astype(f32)
        dtp[KW + 1 : KW + 2, 0:Gn] = gains[...].astype(f32)
        wl[0, :, 0 : half] = inw[:, 2 * DI : 2 * DI + half]
        wl[0, :, half : half + LANES] = jnp.concatenate(
            [inw[:, 2 * DI + half : E], jnp.zeros((r, LANES - H), bf16)], axis=1
        )
        wl[0, :, half + LANES :] = dtp[0:r, :].astype(bf16)
        for j in range(1, K):
            wl[j, :, 0:half] = inw[:, (j - 1) * half : j * half]
            wl[j, :, half:] = inw[:, DI + (j - 1) * half : DI + j * half]
        hpar[...] = jnp.zeros_like(hpar)
        hpar[0:1, 0:H] = dtb[...]
        hpar[1:2, 0:H] = -jnp.exp(alog[...])
        at.barrier()

    def travel(q):
        net.step(q)
        neto.step(q - 2 * K)

    trip = 2 * i
    i = i - 1
    travel(trip)

    def fetch_w(j):
        slot = lax.rem(j, 2)
        return pltpu.make_async_copy(wfull.at[place(j)], wv.at[slot], wsem.at[slot])

    def fetch_o(k):
        slot = lax.rem(k, 2)
        return pltpu.make_async_copy(
            ofull.at[:, :, :, :, columns(k, wo_cols)], wo.at[slot], osem.at[slot]
        )

    ready = (i == 2) | ((i >= 5) & (i < K + 4))
    chunk = jnp.maximum(i - 4, 0)

    @pl.when(ready)
    def _():
        fetch_w(chunk).start()

    @pl.when((i >= K + 4) & (i < K + KO + 4))
    def _():
        fetch_o(i - K - 4).start()

    @pl.when(i == 3)
    def _():
        row, col = iotas(T, T)
        mask[...] = jnp.where(col <= row, BIG, -BIG)
        pad[:, 0:FRONT, :] = jnp.zeros((pad.shape[0], FRONT, LANES), f32)
        acc[...] = jnp.zeros_like(acc)

        def seq(s, _):
            rows = pl.ds(pl.multiple_of(s * T, T), T)
            bc = []
            for a in range(2):
                conv = conv_of(dims, pj[0, rows, a * LANES : (a + 1) * LANES], pars, pad.at[a],
                               DI + a * ST)
                bc.append((conv * sigmoid(conv)).astype(bf16))
            scores[s] = lax.dot_general(
                bc[1], bc[0], (((1,), (1,)), ((), ())), preferred_element_type=f32
            )
            _, _, _, ld, ld2 = steps_of(
                dims, pj[0, rows, 2 * LANES : 3 * LANES].astype(f32), hpar
            )
            ldtab[s] = ld
            rowtab[s] = ld2.T
            return 0

        lax.fori_loop(0, S, seq, 0)

    @pl.when((i >= 6) & (i < K + 5))
    def _():
        j = i - 5
        slot = lax.rem(j, 2)
        h0 = (j - 1) * TC * HP

        def seq(s, _):
            rows = pl.ds(pl.multiple_of(s * T, T), T)
            turned = pltpu.roll(ldtab[s], LANES - h0, 1)
            total = None
            for u in range(TC):
                c0 = pl.multiple_of((j - 1) * half + u * LANES, LANES)
                conv = conv_of(
                    dims, pj[slot, rows, half + u * LANES : half + (u + 1) * LANES], pars,
                    pad.at[u], c0,
                )
                x = (conv * sigmoid(conv)).astype(bf16)
                mix = []
                for a in range(HP):
                    k = u * HP + a
                    left = jnp.broadcast_to(turned[:, k : k + 1], (T, T))
                    expo = jnp.minimum(left - rowtab[s, pl.ds(h0 + k, 1), :], mask[...])
                    mix.append((jnp.exp2(expo) * scores[s]).astype(bf16))
                core = jnp.dot(
                    jnp.concatenate(mix, axis=1), stack_heads(dims, x),
                    preferred_element_type=f32,
                )
                o = core + pars[8:9, pl.ds(c0, LANES)] * x.astype(f32)
                ssd[rows, u * LANES : (u + 1) * LANES] = o
                gate = pj[slot, rows, u * LANES : (u + 1) * LANES].astype(f32)
                g = o * (gate * sigmoid(gate))
                gated[rows, pl.ds(c0, LANES)] = g
                total = g * g if total is None else total + g * g
            acc[rows, :] += total
            return 0

        lax.fori_loop(0, S, seq, 0)

    @pl.when(i < K + 5)
    def _():
        travel(trip + 1)

    @pl.when(ready)
    def _():
        fetch_w(chunk).wait()

    @pl.when(i == 2)
    def _():
        N = A0 * A * A * 2
        r = D // N
        Cn, Gn = C // N, DI // N
        last = wv[0].reshape(D, w)[:, w - LANES :].astype(f32)
        turned = last.T
        scale[...] = jnp.broadcast_to(turned[LANES - 1 :, :], scale.shape)
        parts = [last[d * r : d * r + 8, :] for d in range(N)]
        for t, v in enumerate(assemble(parts, Cn, C // LANES)):
            pars[0:8, t * LANES : (t + 1) * LANES] = v
        for t, v in enumerate(assemble(parts, Gn, DI // LANES)):
            pars[8:16, t * LANES : (t + 1) * LANES] = v
        _, lane = iotas(1, LANES)
        for t in range(DI // LANES):
            v = jnp.zeros((1, LANES), f32)
            for q in range(HP):
                v = jnp.where(lane // HD == q, skip[t * HP + q], v)
            pars[8:9, t * LANES : (t + 1) * LANES] = v

        def norm(k, _):
            rows = pl.ds(pl.multiple_of(k * LANES, LANES), LANES)
            u = tok[rows, :].astype(f32)
            rs = lax.rsqrt(jnp.mean(u * u, axis=-1, keepdims=True) + epsilon)
            v = u * rs * scale[0:1, :]
            uh[rows, :] = v.astype(bf16)
            uT[:, rows] = v.T.astype(bf16)
            return 0

        lax.fori_loop(0, R // LANES, norm, 0)

    @pl.when(ready)
    def _():
        slot = lax.rem(i, 2)
        M = min(R, ROWS)

        def rows(k, _):
            at_ = pl.ds(pl.multiple_of(k * M, M), M)
            v = jnp.dot(
                uh[at_, :], wv[slot].reshape(D, w), preferred_element_type=f32
            ).astype(bf16)
            pj[slot, at_, :] = v
            proj[0, at_, :] = v
            return 0

        lax.fori_loop(0, R // M, rows, 0)

    @pl.when(i == K + 5)
    def _():
        def seq(s, _):
            rows = pl.ds(pl.multiple_of(s * T, T), T)
            rs = lax.rsqrt(jnp.sum(acc[rows, :], axis=1, keepdims=True) * (1.0 / DI) + epsilon)
            rb = jnp.broadcast_to(rs, (T, LANES))
            tabs[0, rows, :] = rb

            def tile(k, _):
                for u in range(4):
                    lanes = pl.ds(pl.multiple_of((k * 4 + u) * LANES, LANES), LANES)
                    v = gated[rows, lanes] * rb * pars[8 + KW + 1 : 8 + KW + 2, lanes]
                    mixed[rows, lanes] = v.astype(bf16)
                return 0

            lax.fori_loop(0, DI // LANES // 4, tile, 0)
            return 0

        lax.fori_loop(0, S, seq, 0)
        acc[...] = jnp.zeros_like(acc)

    @pl.when(i >= K + 5)
    def _():
        travel(trip + 1)

    @pl.when(i >= K + 5)
    def _():
        k = i - K - 5
        slot = lax.rem(k, 2)
        fetch_o(k).wait()
        M = 256

        def rows(m, _):
            at_ = pl.ds(pl.multiple_of(m * M, M), M)
            branch = jnp.dot(
                mixed[at_, :], wo[slot].reshape(DI, wo_cols), preferred_element_type=f32
            )
            out[at_, :] = (tokc[at_, :].astype(f32) + branch).astype(bf16)
            p = branch * goc[at_, :].astype(f32)
            part = p[:, 0:LANES]
            for q in range(1, wo_cols // LANES):
                part = part + p[:, q * LANES : (q + 1) * LANES]
            acc[at_, :] += part
            return 0

        lax.fori_loop(0, R // M, rows, 0)

        share = DI // LANES // KO

        def turn(m, _):
            for u in range(share):
                lanes = pl.ds(pl.multiple_of((k * share + u) * LANES, LANES), LANES)
                rows = pl.ds(pl.multiple_of(m * LANES, LANES), LANES)
                mT[lanes, rows] = mixed[rows, lanes].T
            return 0

        lax.fori_loop(0, R // LANES, turn, 0)

    @pl.when(i == K + KO + 4)
    def _():
        net.drain()
        neto.drain()
        mu = jnp.sum(acc[...], axis=1, keepdims=True) * (1.0 / DI)
        rb = tabs[0]
        tabs[1] = jnp.broadcast_to(mu, rb.shape) * rb * rb


def run_forward_net(dims, axis, geom, K, w, skip, tok, go, inw, smalls, ow):
    T, DI, C = (dims[k] for k in ("T", "DI", "C"))
    A0, A = geom
    R, D = tok.shape
    r = inw.shape[0]
    ro = ow.shape[0]
    half = w // 2
    wc = r * w // ro
    KO = D // wc
    S = R // T
    assert DI // LANES % KO == 0
    steps = K + KO + 6
    whole = lambda s: pl.BlockSpec(s, lambda i: (0,) * len(s), pipeline_mode=pl.Buffered(1))
    late = lambda i: (0, jnp.clip(i - K - 6, 0, KO - 1))
    hbm = pl.BlockSpec(memory_space=pl.ANY)
    return pl.pallas_call(
        functools.partial(forward, dims, axis, geom, K, KO),
        grid=(steps,),
        in_specs=[pl.BlockSpec(memory_space=pltpu.SMEM), whole((R, D)), whole(inw.shape)]
        + [whole(a.shape) for a in smalls]
        + [whole((ro, D)), pl.BlockSpec((R, wc), late), pl.BlockSpec((R, wc), late)],
        out_specs=[
            pl.BlockSpec((1, R, w), lambda i: (jnp.clip(i - 5, 0, K - 1), 0, 0)),
            pl.BlockSpec((R, half), lambda i: (0, jnp.clip(i - 7, 0, K - 2))),
            whole((D, R)), whole((DI, R)),
            pl.BlockSpec((R, wc), late),
            whole((2, R, LANES)), whole((16, C)), whole((8, D)), whole((K, r, w)),
            whole((8, LANES)), hbm, hbm,
        ],
        out_shape=[
            jax.ShapeDtypeStruct((K, R, w), bf16),
            jax.ShapeDtypeStruct((R, DI), f32),
            jax.ShapeDtypeStruct((D, R), bf16),
            jax.ShapeDtypeStruct((DI, R), bf16),
            jax.ShapeDtypeStruct((R, D), bf16),
            jax.ShapeDtypeStruct((2, R, LANES), f32),
            jax.ShapeDtypeStruct((16, C), f32),
            jax.ShapeDtypeStruct((8, D), f32),
            jax.ShapeDtypeStruct((K, r, w), bf16),
            jax.ShapeDtypeStruct((8, LANES), f32),
            jax.ShapeDtypeStruct((K, A0, A * A, 2, r, w), bf16),
            jax.ShapeDtypeStruct((A0, A * A, 2, ro, D), bf16),
        ],
        scratch_shapes=[
            pltpu.VMEM((R, D), bf16),
            pltpu.VMEM((2, A0, A * A, 2, r, w), bf16),
            pltpu.VMEM((2, A0, A * A, 2, ro, wc), bf16),
            pltpu.VMEM((2, R, w), bf16),
            pltpu.VMEM((R, DI), f32),
            pltpu.VMEM((R, DI), bf16),
            pltpu.VMEM((half // LANES, FRONT + T, LANES), f32),
            pltpu.VMEM((S, T, LANES), f32),
            pltpu.VMEM((S, LANES, T), f32),
            pltpu.VMEM((S, T, T), f32),
            pltpu.VMEM((T, T), f32),
            pltpu.VMEM((R, LANES), f32),
            pltpu.VMEM((T, LANES), f32),
            pltpu.SemaphoreType.DMA((2,)),
            pltpu.SemaphoreType.DMA((2,)),
        ]
        + Gather.scratch(2 * K, A0, A) + Gather.scratch(2 * KO, A0, A),
        compiler_params=pltpu.CompilerParams(
            collective_id=1, has_side_effects=True, vmem_limit_bytes=VMEM
        ),
        cost_estimate=pl.CostEstimate(
            flops=2 * R * D * K * w, bytes_accessed=D * K * w * 60, transcendentals=0
        ),
        name="forward",
    )(skip, tok, inw, *smalls, ow, tok, go)


def backward(dims, axis, geom, K, KO, E, proj, proj0, ssd, wo, wf, uT, mT, go, wl, tabs, pars,
             hpar, dn, outc, dns, sums,
             uo, mo, dmx, dpj, pad, dpad, ldtab, rowtab, scores, dscores, dlog, csum, bcs, mask,
             cacc, dacc, hacc, small, wv, csem, wsem, *refs):
    T, DI, C, H, HD, ST, KW = (dims[k] for k in ("T", "DI", "C", "H", "HD", "ST", "KW"))
    A0, A = geom
    at = Place(axis, A0, A)
    i = pl.program_id(0)
    R = ssd.shape[0]
    _, r, w = wl.shape
    N = A0 * A * A
    half = w // 2
    S = R // T
    HP = LANES // HD
    TC = half // LANES
    D = go.shape[1]
    HF = mT.shape[2]
    each = KO // HF
    pairs = (K + 1) // 2
    net = Reduce(at, K + KO, refs[:15])
    total = SumAll(at, refs[15:])

    def fetches():
        out = [(uT.at[:, at.c], uo.at[0]), (uT.at[:, 1 - at.c], uo.at[1])]
        return [pltpu.make_async_copy(s, d, csem.at[k]) for k, (s, d) in enumerate(out)]

    def fetch_half(h):
        out = [(mT.at[:, at.c, h], mo.at[0]), (mT.at[:, 1 - at.c, h], mo.at[1])]
        return [pltpu.make_async_copy(s, d, csem.at[2 + k]) for k, (s, d) in enumerate(out)]

    @pl.when(i == 0)
    def _():
        for cp in fetches() + fetch_half(0):
            cp.start()
        at.barrier()
        for ref in (cacc, dacc, hacc, dlog, csum, dscores, dns):
            ref[...] = jnp.zeros_like(ref)
        row, col = iotas(T, T)
        mask[...] = jnp.where(row <= col, BIG, -BIG)
        pad[:, 0:FRONT, :] = jnp.zeros((pad.shape[0], FRONT, LANES), f32)
        dpad[:, T:, :] = jnp.zeros((dpad.shape[0], FRONT, LANES), f32)

        def seq(s, _):
            rows = pl.ds(pl.multiple_of(s * T, T), T)
            for a in range(2):
                conv = conv_of(dims, proj0[0, rows, a * LANES : (a + 1) * LANES], pars, pad.at[a],
                               DI + a * ST)
                bcs[a, rows, :] = (conv * sigmoid(conv)).astype(bf16)
            scores[s] = lax.dot_general(
                bcs[0, rows, :], bcs[1, rows, :], (((1,), (1,)), ((), ())),
                preferred_element_type=f32,
            )
            _, _, _, ld, ld2 = steps_of(
                dims, proj0[0, rows, 2 * LANES : 3 * LANES].astype(f32), hpar
            )
            ldtab[s] = ld2
            rowtab[s] = ld.T
            return 0

        lax.fori_loop(0, S, seq, 0)
        for cp in fetches() + fetch_half(0):
            cp.wait()

    for h in range(1, HF):

        @pl.when(i == 2 * h * each - 1)
        def _(h=h):
            for cp in fetch_half(h):
                cp.start()

        @pl.when(i == 2 * h * each)
        def _(h=h):
            for cp in fetch_half(h):
                cp.wait()

    def finish(p, v):
        inner = (p >= 3 * KO) | (lax.rem(p, 3) > 0)

        @pl.when(inner)
        def _():
            g = jnp.where(p >= 3 * KO, p - KO, p - 1 - lax.div(p, 3))
            outc[g] = v
            q = v * wl[lax.rem(g + 1, K)].astype(f32)
            part = q[:, 0:LANES]
            for k in range(1, w // LANES):
                part = part + q[:, k * LANES : (k + 1) * LANES]
            dns[...] += part

        @pl.when(jnp.logical_not(inner))
        def _():
            outc[K + lax.div(p, 3)] = v

    def send_out():
        k = lax.div(i, 2)

        @pl.when((lax.rem(i, 2) == 0) & (k < KO))
        def _():
            net.step(3 * k, finish)
            net.begin(3 * k, mo, go[:, columns(lax.rem(k, each), w)])

    def fetch(t, q):
        return pltpu.make_async_copy(
            wf.at[2 * t + q], wv.at[:, q * w : (q + 1) * w], wsem.at[q]
        )

    def fetch_pair(t, act):
        act(fetch(t, 0))

        @pl.when(2 * t + 1 < K)
        def _():
            act(fetch(t, 1))

    @pl.when(i == 0)
    def _():
        fetch_pair(0, lambda cp: cp.start())

    slot = lax.rem(lax.div(i, 2), dpj.shape[0])
    off = lax.rem(i, 2) * w
    here_of = lambda lane: pl.ds(pl.multiple_of(off + lane, LANES), LANES)

    def conv_back(rows, lane0, c0, dact, conv, sig, u):
        lanes = pl.ds(c0, LANES)
        dconv = dact * (sig * (1.0 + conv * (1.0 - sig)))
        dpad[u, 0:T, :] = dconv
        dcin = dconv * pars[KW - 1 : KW, lanes]
        for k in range(KW - 1):
            dcin = dcin + dpad[u, KW - 1 - k : KW - 1 - k + T, :] * pars[k : k + 1, lanes]
        dpj[slot, rows, here_of(lane0)] = dcin.astype(bf16)
        for k in range(KW):
            start = FRONT - KW + 1 + k
            cacc[8 * k : 8 * k + 8, lanes] += sum8(dconv * pad[u, start : start + T, :])
        cacc[8 * KW : 8 * KW + 8, lanes] += sum8(dconv)

    @pl.when(i < K - 1)
    def _():
        h0 = i * TC * HP
        dmx[...] = lax.dot_general(
            go[...], wo[...], (((1,), (1,)), ((), ())), preferred_element_type=f32
        )

        def seq(s, _):
            rows = pl.ds(pl.multiple_of(s * T, T), T)
            turned = pltpu.roll(ldtab[s], LANES - h0, 1)
            rb, mb = tabs[0, rows, :], tabs[1, rows, :]
            parts = None
            for u in range(TC):
                c0 = pl.multiple_of(i * half + u * LANES, LANES)
                lanes = pl.ds(c0, LANES)
                here = slice(u * LANES, (u + 1) * LANES)
                there = slice(half + u * LANES, half + (u + 1) * LANES)
                conv = conv_of(dims, proj[0, rows, there], pars, pad.at[u], c0)
                sig = sigmoid(conv)
                x = (conv * sig).astype(bf16)
                xf = x.astype(f32)
                gate = proj[0, rows, here].astype(f32)
                gs = sigmoid(gate)
                act = gate * gs
                o = ssd[rows, here]
                dm = dmx[rows, here]
                gated = o * act
                dgated = rb * (dm * pars[8 + KW + 1 : 8 + KW + 2, lanes]) - gated * mb
                dacc[8:16, lanes] += sum8(dm * (gated * rb))
                dssd = dgated * act
                dpj[slot, rows, here_of(u * LANES)] = (
                    dgated * o * (gs * (1.0 + gate * (1.0 - gs)))
                ).astype(bf16)
                low = dssd.astype(bf16)
                dacc[0:8, lanes] += sum8(dssd * xf)
                lows = stack_heads(dims, low)
                dmix = lax.dot_general(
                    x, lows, (((1,), (1,)), ((), ())), preferred_element_type=f32
                )
                mix = []
                part = None
                for a in range(HP):
                    k = u * HP + a
                    right = jnp.broadcast_to(turned[:, k : k + 1], (T, T))
                    decay = jnp.exp2(
                        jnp.minimum(rowtab[s, pl.ds(h0 + k, 1), :] - right, mask[...])
                    )
                    mix.append((decay * scores[s]).astype(bf16))
                    term = dmix[:, a * T : (a + 1) * T] * decay
                    part = term if part is None else part + term
                core = jnp.dot(
                    jnp.concatenate(mix, axis=1), lows, preferred_element_type=f32
                )
                sk = pars[8:9, lanes]
                from_cols = xf * core
                diff = low.astype(f32) * (o - sk * xf) - from_cols
                prow, pcol = iotas(LANES, LANES)
                place = (pcol == h0 + u * HP + prow // HD).astype(bf16)
                both = jnp.concatenate([diff, from_cols], axis=0)
                hi = both.astype(bf16)
                lo = (both - hi.astype(f32)).astype(bf16)
                by_head = jnp.dot(
                    jnp.concatenate([hi, lo], axis=1),
                    jnp.concatenate([place, place], axis=0), preferred_element_type=f32,
                )
                conv_back(rows, half + u * LANES, c0, core + sk * dssd, conv, sig, u)
                new = (part, by_head)
                parts = new if parts is None else tuple(p + q for p, q in zip(parts, new))
            dscores[s] += parts[0]
            dlog[rows, :] += parts[1][0:T]
            csum[rows, :] += parts[1][T:]
            return 0

        lax.fori_loop(0, S // 2, seq, 0)
        send_out()
        lax.fori_loop(S // 2, S, seq, 0)

    @pl.when(i == K - 1)
    def _():
        row, col = iotas(T, T)
        upper = (row <= col).astype(f32)

        def seq(s, _):
            rows = pl.ds(pl.multiple_of(s * T, T), T)
            ds = dscores[s]
            dact = (
                jnp.dot(ds.astype(bf16), bcs[1, rows, :], preferred_element_type=f32),
                jnp.dot(ds.T.astype(bf16), bcs[0, rows, :], preferred_element_type=f32),
            )
            for a in range(2):
                conv = conv_of(dims, proj0[0, rows, a * LANES : (a + 1) * LANES], pars, pad.at[a],
                               DI + a * ST)
                conv_back(rows, a * LANES, DI + a * ST, dact[a], conv, sigmoid(conv), a)
            v, e, step, _, _ = steps_of(
                dims, proj0[0, rows, 2 * LANES : 3 * LANES].astype(f32), hpar
            )
            dsteps = jnp.dot(
                upper, dlog[rows, :], precision=lax.Precision.HIGHEST,
                preferred_element_type=f32,
            )
            sg = jnp.where(v >= 0.0, 1.0, e) / (1.0 + e)
            ratio = jnp.where(step > 1e-30, sg / jnp.maximum(step, 1e-30), 1.0)
            ddt = csum[rows, :] * ratio + dsteps * hpar[1:2, :] * sg
            _, lane = iotas(T, LANES)
            ddt = jnp.where(lane < H, ddt, 0.0)
            dpj[slot, rows, here_of(2 * LANES)] = ddt.astype(bf16)
            dpj[slot, rows, here_of(3 * LANES)] = jnp.zeros((T, LANES), bf16)
            hacc[0:8, :] += sum8(ddt)
            hacc[8:16, :] += sum8(dsteps * step)
            return 0

        lax.fori_loop(0, S, seq, 0)
        small[...] = jnp.zeros_like(small)
        for k in range(KW + 1):
            small[k : k + 1, :] = jnp.sum(cacc[8 * k : 8 * k + 8, :], axis=0, keepdims=True)
        for k in range(2):
            small[KW + 1 + k : KW + 2 + k, 0:DI] = jnp.sum(
                dacc[8 * k : 8 * k + 8, :], axis=0, keepdims=True
            )
            small[KW + 3 : KW + 4, k * LANES : (k + 1) * LANES] = jnp.sum(
                hacc[8 * k : 8 * k + 8, :], axis=0, keepdims=True
            )
        total.start(0, small[...])

    for stage in range(1, 4):

        @pl.when(i == K - 1 + stage)
        def _(stage=stage):
            total.start(stage, total.finish(stage - 1))

    @pl.when(i == K + 3)
    def _():
        sums[...] = total.finish(3)

    p = jnp.where(i < K, i + jnp.minimum(lax.div(i, 2) + 1, KO), 2 * i - K + KO)
    net.step(p, finish)

    @pl.when(i < K)
    def _():
        net.begin(p, uo, dpj[slot, :, pl.ds(pl.multiple_of(off, w), w)])

    @pl.when(i >= K)
    def _():
        net.step(p + 1, finish)

    tail = pairs - dpj.shape[0] + i - K
    t = jnp.where(i < K, lax.div(i - 7, 2), tail)
    turn = jnp.where(
        i < K, (i >= 7) & (lax.rem(i, 2) == 1) & (t < pairs - dpj.shape[0]), t >= 0
    )

    @pl.when(turn)
    def _():
        fetch_pair(t, lambda cp: cp.wait())
        mine = lax.rem(t, dpj.shape[0])

        def add(part):
            @pl.when(t == 0)
            def _():
                dn[...] = part()

            @pl.when(t > 0)
            def _():
                dn[...] += part()

        @pl.when(2 * t + 1 < K)
        def _():
            add(lambda: lax.dot_general(
                dpj[mine], wv[...], (((1,), (1,)), ((), ())), preferred_element_type=f32
            ))

        @pl.when(2 * t + 1 >= K)
        def _():
            add(lambda: lax.dot_general(
                dpj[mine, :, 0:w], wv[:, 0:w], (((1,), (1,)), ((), ())),
                preferred_element_type=f32,
            ))

        @pl.when(t + 1 < pairs)
        def _():
            fetch_pair(t + 1, lambda cp: cp.start())

    @pl.when(i == K + 3)
    def _():
        net.drain()


def run_backward_net(dims, axis, geom, E, proj, ssd, ofull, wfull, uT, mT, go, wl, tabs, pars,
                     hpar):
    T, DI, C, H, KW, ST = (dims[k] for k in ("T", "DI", "C", "H", "KW", "ST"))
    A0, A = geom
    N = A0 * A * A
    K, R, w = proj.shape
    r = wl.shape[1]
    D = go.shape[1]
    ro = DI // (2 * N)
    HF = ro // r
    half = w // 2
    S = R // T
    KO = HF * (D // w)
    assert 2 * KO <= K + 1 and HF * r == ro and D % w == 0
    whole = lambda s: pl.BlockSpec(s, lambda i: (0,) * len(s), pipeline_mode=pl.Buffered(1))
    tile = lambda i: jnp.clip(i, 0, K - 2)
    hbm = pl.BlockSpec(memory_space=pl.ANY)
    return pl.pallas_call(
        functools.partial(backward, dims, axis, geom, K, KO, E),
        grid=(K + 4,),
        in_specs=[
            pl.BlockSpec((1, R, w), lambda i: (tile(i) + 1, 0, 0)),
            whole((1, R, w)),
            pl.BlockSpec((R, half), lambda i: (0, tile(i))),
            pl.BlockSpec((half, D), lambda i: (tile(i), 0)),
            hbm, hbm, hbm, whole((R, D)), whole((K, r, w)), whole((2, R, LANES)), whole((16, C)),
            whole((8, LANES)),
        ],
        out_specs=[whole((R, D)), whole((K + KO, r, w)), whole((r, LANES)), whole((8, C))],
        out_shape=[
            jax.ShapeDtypeStruct((R, D), f32),
            jax.ShapeDtypeStruct((K + KO, r, w), f32),
            jax.ShapeDtypeStruct((r, LANES), f32),
            jax.ShapeDtypeStruct((8, C), f32),
        ],
        scratch_shapes=[
            pltpu.VMEM((2, N, r, R), bf16),
            pltpu.VMEM((2, N, r, R), bf16),
            pltpu.VMEM((R, half), f32),
            pltpu.VMEM((4, R, 2 * w), bf16),
            pltpu.VMEM((2, FRONT + T, LANES), f32),
            pltpu.VMEM((2, FRONT + T, LANES), f32),
            pltpu.VMEM((S, T, LANES), f32),
            pltpu.VMEM((S, LANES, T), f32),
            pltpu.VMEM((S, T, T), f32),
            pltpu.VMEM((S, T, T), f32),
            pltpu.VMEM((R, LANES), f32),
            pltpu.VMEM((R, LANES), f32),
            pltpu.VMEM((2, R, ST), bf16),
            pltpu.VMEM((T, T), f32),
            pltpu.VMEM((8 * (KW + 1), C), f32),
            pltpu.VMEM((16, DI), f32),
            pltpu.VMEM((16, LANES), f32),
            pltpu.VMEM((8, C), f32),
            pltpu.VMEM((D, 2 * w), bf16),
            pltpu.SemaphoreType.DMA((4,)),
            pltpu.SemaphoreType.DMA((2,)),
        ]
        + Reduce.scratch(K + KO, A0, A, r, w)
        + SumAll.scratch(A0, A, (8, C)),
        compiler_params=pltpu.CompilerParams(
            collective_id=2, has_side_effects=True, vmem_limit_bytes=VMEM
        ),
        cost_estimate=pl.CostEstimate(
            flops=6 * R * D * K * w, bytes_accessed=D * K * w * 90, transcendentals=0
        ),
        name="backward",
    )(proj, proj, ssd, ofull.reshape(DI, D), wfull.reshape(K, D, w), uT.reshape(N, 2, r, R),
      mT.reshape(N, 2, HF, r, R), go, wl, tabs, pars, hpar)


def conclude(dims, axis, K, E, dn, tok, go, out, scale, outc, dns, sums, ns, hpar,
             dtok, outs, dw, dow, dtaps, dbias, ddtb, dalog, dskip, dnorm, dgain, tmp):
    T, DI, C, H, HD, KW = (dims[k] for k in ("T", "DI", "C", "H", "HD", "KW"))
    outs[...] = out[...]
    u = tok[...].astype(f32)
    rs = lax.rsqrt(jnp.mean(u * u, axis=-1, keepdims=True) + epsilon)
    u = u * rs
    d = dn[...] * scale[0:1, :]
    m = jnp.mean(d * u, axis=-1, keepdims=True)
    dtok[...] = go[...].astype(f32) + rs * (d - u * m)

    @pl.when(pl.program_id(0) == 0)
    def _():
        me = lax.axis_index(axis)
        r, w = outc.shape[1:]
        half = w // 2
        for g in range(K - 1):
            dw[:, g * half : (g + 1) * half] = outc[g, :, 0:half]
            dw[:, DI + g * half : DI + (g + 1) * half] = outc[g, :, half:]
        dw[:, 2 * DI :] = outc[K - 1, :, 0 : E - 2 * DI]
        cols = dow.shape[1] // w
        for k in range(outc.shape[0] - K):
            h, c = k // cols, k % cols
            dow[h * r : (h + 1) * r, c * w : (c + 1) * w] = outc[K + k]

        def window(size):
            start = me * size
            base = jnp.minimum(lax.div(start, LANES), C // LANES - 2) * LANES
            v = sums[:, pl.ds(pl.multiple_of(base, LANES), 2 * LANES)]
            return pltpu.roll(v, lax.rem(2 * LANES - (start - base), 2 * LANES), 1)

        Cn, Gn = dbias.shape[0], dgain.shape[0]
        v = window(Cn)[:, 0:LANES]
        tmp[...] = jnp.zeros_like(tmp)
        tmp[0:8, :] = v
        dtaps[...] = tmp[...].T[0:Cn, 0:KW]
        dbias[...] = v[KW, 0:Cn]
        dgain[...] = window(Gn)[KW + 2, 0:Gn]
        ddtb[...] = sums[KW + 3, 0:H]
        dalog[...] = sums[KW + 3 : KW + 4, LANES : 2 * LANES][0, 0:H] * hpar[1, 0:H]
        tmp[0:r, :] = dns[...]
        tmp[r:, :] = jnp.zeros((LANES - r, LANES), f32)
        dnorm[...] = jnp.sum(tmp[...].T, axis=0)[0:r] / ns[0, :].astype(f32)
        tiles = DI // LANES
        tmp[...] = jnp.zeros_like(tmp)
        for t in range(tiles):
            tmp[t : t + 1, :] = sums[KW + 1 : KW + 2, t * LANES : (t + 1) * LANES]
        row, col = iotas(LANES, LANES)
        HP = LANES // HD
        fold = (row // HD == lax.rem(col, HP)).astype(f32)
        v = jnp.dot(tmp[...], fold, precision=lax.Precision.HIGHEST, preferred_element_type=f32)
        dskip[...] = jnp.sum(jnp.where(col // HP == row, v, 0.0), axis=0)[0:H]


def run_conclude(dims, axis, K, E, dn, tok, go, out, scale, outc, dns, sums, ns, hpar, ro):
    T, DI, C, H, KW = (dims[k] for k in ("T", "DI", "C", "H", "KW"))
    R, D = tok.shape
    r = outc.shape[1]
    n = D // r
    rows = pl.BlockSpec((T, D), lambda i: (i, 0))
    whole = lambda s: pl.BlockSpec(s, lambda i: (0,) * len(s))
    shapes = [(r, E), (ro, D), (C // n, KW), (C // n,), (H,), (H,), (H,), (r,), (DI // n,)]
    return pl.pallas_call(
        functools.partial(conclude, dims, axis, K, E),
        grid=(R // T,),
        in_specs=[rows, rows, rows, rows]
        + [whole(a.shape) for a in (scale, outc, dns, sums, ns, hpar)],
        out_specs=[rows, rows] + [whole(x) for x in shapes],
        out_shape=[jax.ShapeDtypeStruct((R, D), f32), jax.ShapeDtypeStruct((R, D), bf16)]
        + [jax.ShapeDtypeStruct(x, f32) for x in shapes],
        scratch_shapes=[pltpu.VMEM((LANES, LANES), f32)],
        name="conclude",
    )(dn, tok, go, out, scale, outc, dns, sums, ns, hpar)


def local(axis, n, tokens, in_weight, conv_weight, conv_bias, dt_bias, a_log, skip_d,
          norm_scale, gate_scale, out_weight, grad_out):
    MB, S, T, D = tokens.shape
    R = MB * S * T
    r, E = in_weight.shape
    H = a_log.shape[0]
    DI = out_weight.shape[0] * n
    Cn, KW = conv_weight.shape
    C = Cn * n
    HD = DI // H
    ST = (C - DI) // 2
    dims = dict(T=T, DI=DI, C=C, H=H, HD=HD, ST=ST, KW=KW)
    assert LANES % HD == 0 and ST == LANES and DI % (LANES * 2) == 0 and T % 16 == 0
    geom = geometry(n)
    w = CHUNK
    Gn, ro = DI // n, out_weight.shape[0]
    own = (
        geom is not None and r % 16 == 0 and ro % r == 0 and D % w == 0 and DI % (w // 2) == 0
        and w == 2 * ST + 2 * LANES and E == 2 * DI + 2 * ST + H and H <= LANES
        and max(Cn, Gn) < LANES and 6 <= KW + 2 <= 8 and 2 * (ro // r) * (D // w) <= DI * 2 // w + 2
    )
    me = lax.axis_index(axis)
    tok = tokens.reshape(R, D)
    go = grad_out.reshape(R, D)
    if own:
        row = lambda v: v.reshape(1, -1)
        K = DI * 2 // w + 1
        smalls = [conv_weight.T] + [
            row(v) for v in (conv_bias, gate_scale, norm_scale, dt_bias, a_log)
        ]
        proj, ssd, uT, mT, output, tabs, pars, scale, wl, hpar, wfull, ofull = run_forward_net(
            dims, axis, geom, K, w, skip_d, tok, go, in_weight, smalls, out_weight
        )
        dn, outc, dns, sums = run_backward_net(
            dims, axis, geom, E, proj, ssd, ofull, wfull, uT, mT, go, wl, tabs, pars, hpar
        )
        dtok, output, dw, dow, dtaps, dbias, ddtb, dalog, dskip, dnorm, dgain = run_conclude(
            dims, axis, K, E, dn, tok, go, output, scale, outc, dns, sums, row(norm_scale), hpar,
            ro,
        )
        return (
            output.reshape(tokens.shape), dtok.reshape(tokens.shape), dw, dtaps, dbias, ddtb,
            dalog, dskip, dnorm, dgain, dow,
        )
    rate = -jnp.exp(a_log)
    hpar = jnp.pad(jnp.stack([dt_bias, rate]), ((0, 6), (0, LANES - H)))
    skip = jnp.broadcast_to(jnp.repeat(skip_d, HD)[None], (8, DI))
    ns = norm_scale.astype(f32)
    out_full = lax.all_gather(out_weight, axis, axis=0, tiled=True)
    wfull = lax.all_gather(in_weight, axis, axis=0, tiled=True)
    conv = lax.all_gather(jnp.concatenate([conv_weight.T, conv_bias[None]]), axis, axis=0)
    conv = conv.transpose(1, 0, 2).reshape(KW + 1, C).astype(f32)
    gate = lax.all_gather(gate_scale, axis, axis=0).reshape(1, DI).astype(f32)
    scale = lax.all_gather(norm_scale, axis, axis=0).reshape(1, D).astype(f32)
    u = tok.astype(f32)
    u = u * lax.rsqrt(jnp.mean(u * u, axis=-1, keepdims=True) + epsilon)
    uh = (u * scale).astype(bf16)
    proj = jnp.dot(uh, wfull, preferred_element_type=f32).astype(bf16)
    cpar = jnp.pad(conv, ((0, 8 - KW - 1), (0, 0)))
    dpar = jnp.concatenate([skip[:1], gate, skip[2:]], axis=0)
    mixed, ssd, rstd = run_forward(dims, proj, cpar, hpar, dpar)
    output = jnp.dot(mixed, out_full, preferred_element_type=f32)
    output = (tok.astype(f32) + output).astype(bf16)
    d_mixed = lax.dot_general(
        go, out_full, (((1,), (1,)), ((), ())), preferred_element_type=f32
    )
    dproj, small = run_backward(dims, proj, d_mixed, ssd, rstd, cpar, hpar, dpar)
    left = (((0,), (0,)), ((), ()))
    g_out = lax.dot_general(mixed, go, left, preferred_element_type=f32).astype(bf16)
    dow = lax.psum_scatter(g_out, axis, scatter_dimension=0, tiled=True).astype(f32)
    g_in = lax.dot_general(uh, dproj, left, preferred_element_type=f32).astype(bf16)
    dw = lax.psum_scatter(g_in, axis, scatter_dimension=0, tiled=True).astype(f32)
    dns = dw * in_weight.astype(f32)
    dn = lax.dot_general(dproj, wfull, (((1,), (1,)), ((), ())), preferred_element_type=f32)
    sums = lax.psum(small, axis)
    u = tok.astype(f32)
    rs = lax.rsqrt(jnp.mean(u * u, axis=-1, keepdims=True) + epsilon)
    u, d = u * rs, dn * scale
    dtok = go.astype(f32) + rs * (d - u * jnp.mean(d * u, axis=-1, keepdims=True))
    dconv = lax.dynamic_slice(sums, (0, me * Cn), (KW + 1, Cn))
    heads = sums[KW + 3]
    return (
        output.reshape(tokens.shape),
        dtok.reshape(tokens.shape),
        dw,
        dconv[:KW].T,
        dconv[KW],
        heads[:H],
        heads[LANES : LANES + H] * rate,
        sums[KW + 1, :DI].reshape(H, HD).sum(axis=1),
        dns.sum(axis=1) / ns,
        lax.dynamic_slice(sums[KW + 2], (me * Gn,), (Gn,)),
        dow,
    )


def solution(mesh):
    axis = mesh.axis_names[0]
    n = mesh.shape[axis]
    rows, flat, batch = P(axis, None), P(axis), P(None, axis, None, None)
    return jax.shard_map(
        functools.partial(local, axis, n),
        mesh=mesh,
        in_specs=(batch, rows, rows, flat, P(), P(), P(), flat, flat, rows, batch),
        out_specs=(batch, batch, rows, rows, flat, P(), P(), P(), flat, flat, rows),
        check_vma=False,
    )
```

```python
import functools
import math

import jax
import jax.numpy as jnp
from jax import lax
from jax.experimental import pallas as pl
from jax.experimental.pallas import tpu as pltpu
from jax.sharding import PartitionSpec as P

epsilon = 1e-05
LOG2E = 1.4426950408889634
BIG = 3.0e38
LANES = 128
FRONT = 8
f32 = jnp.float32
bf16 = jnp.bfloat16
UNROLL_F = 2
UNROLL_B = 2


def sigmoid(v):
    return 0.5 * jnp.tanh(0.5 * v) + 0.5


def sum8(v):
    rows, lanes = v.shape
    return jnp.sum(v.reshape(rows // 8, 8, lanes), axis=0)


def iotas(rows, lanes):
    return (
        lax.broadcasted_iota(jnp.int32, (rows, lanes), 0),
        lax.broadcasted_iota(jnp.int32, (rows, lanes), 1),
    )


def step_stage(dims, proj, hpar, dtp):
    DI, C, H = dims["DI"], dims["C"], dims["H"]
    dtp[...] = jnp.zeros_like(dtp)
    dtp[:, 0:H] = proj[:, DI + C : DI + C + H].astype(f32)
    return steps_of(dims, dtp[...], hpar)


def steps_of(dims, dt, hpar):
    T, H = dims["T"], dims["H"]
    _, lane = iotas(T, LANES)
    v = jnp.where(lane < H, dt + hpar[0:1, :], 0.0)
    e = jnp.exp(-jnp.abs(v))
    step = jnp.maximum(v, 0.0) + jnp.log1p(e)
    row, col = iotas(T, T)
    tri = (row >= col).astype(f32)
    ld = jnp.dot(
        tri, step * (hpar[1:2, :] * LOG2E), precision=lax.Precision.HIGHEST,
        preferred_element_type=f32,
    )
    return v, e, step, ld, ld - jnp.log2(step)


def conv_of(dims, cin, cpar, pad, c0):
    T, KW = dims["T"], dims["KW"]
    lanes = pl.ds(c0, LANES)
    cin = cin.astype(f32)
    pad[FRONT : FRONT + T, :] = cin
    out = cpar[KW : KW + 1, lanes] + cin * cpar[KW - 1 : KW, lanes]
    for k in range(KW - 1):
        out = out + pad[FRONT - KW + 1 + k : FRONT - KW + 1 + k + T, :] * cpar[k : k + 1, lanes]
    return out


def conv_tile(dims, proj, cpar, pad, c0):
    return conv_of(dims, proj[:, pl.ds(dims["DI"] + c0, LANES)], cpar, pad, c0)


def stack_heads(dims, v):
    T, HD = dims["T"], dims["HD"]
    _, lane = iotas(T, LANES)
    zero = jnp.zeros_like(v)
    return jnp.concatenate(
        [jnp.where(lane // HD == a, v, zero) for a in range(LANES // HD)], axis=0
    )


MESH = pl.DeviceIdType.MESH
CHUNK = 512
VMEM = 67043328
ROWS = 512
SEQ_F = 2
SEQ_B = 2


def geometry(n):
    chips = n // 2
    A0 = 4 if chips % 4 == 0 else 1
    A = math.isqrt(chips // A0)
    return (A0, A) if n % 2 == 0 and A > 1 and A0 * A * A == chips else None


class Place:
    def __init__(self, axis, A0, A):
        me = lax.axis_index(axis)
        self.A0, self.A = A0, A
        self.c = lax.rem(me, 2)
        chip = lax.div(me, 2)
        self.a2 = lax.rem(chip, A)
        self.a1 = lax.rem(lax.div(chip, A), A)
        self.a0 = lax.div(chip, A * A)
        c = self.c
        self.f = self.a1 + c * (self.a2 - self.a1)
        self.s = self.a2 + c * (self.a1 - self.a2)
        self.sf = A + c * (1 - A)
        self.ss = 1 + c * (A - 1)

    def pos(self, f, s):
        return f * self.sf + s * self.ss

    def device(self, a0, f, s, c):
        return ((a0 * self.A * self.A + self.pos(f, s)) * 2 + c,)

    def line(self, q):
        return lax.rem(self.a0 + q + self.A0, self.A0)

    def first(self, q):
        return lax.rem(self.f + q + self.A, self.A)

    def second(self, q):
        return lax.rem(self.s + q + self.A, self.A)

    def partner(self):
        return self.device(self.a0, self.f, self.s, 1 - self.c)

    def peers(self):
        out = [self.partner()]
        out += [self.device(self.line(q), self.f, self.s, self.c) for q in range(1, self.A0)]
        out += [self.device(self.a0, self.first(q), self.s, self.c) for q in range(1, self.A)]
        out += [self.device(self.a0, self.f, self.second(q), self.c) for q in range(1, self.A)]
        return out

    def greet(self):
        for peer in self.peers():
            pl.semaphore_signal(
                pltpu.get_barrier_semaphore(), inc=1, device_id=peer, device_id_type=MESH
            )

    def meet(self):
        pl.semaphore_wait(pltpu.get_barrier_semaphore(), len(self.peers()))


def columns(j, w):
    return pl.ds(pl.multiple_of(j * w, w), w)


def send(src, dst, ssem, rsem, device):
    return pltpu.make_async_remote_copy(
        src_ref=src, dst_ref=dst, send_sem=ssem, recv_sem=rsem,
        device_id=device, device_id_type=MESH,
    )


class Gather:
    AFTER = (0, 2, 4, 6, 7)
    DEEP = 5
    ORDER = (0, 4, 3, 2, 1)
    TURN = 0

    def __init__(self, at, K, mine, whole, ssem, rsem, lsem):
        self.at, self.K, self.mine, self.whole = at, K, mine, whole
        self.ssem, self.rsem, self.lsem = ssem, rsem, lsem

    @staticmethod
    def scratch(K, A0, A):
        NS = (A0 - 1) * A + (A - 1) + (A - 1) * A + 1
        return [
            pltpu.SemaphoreType.DMA((Gather.DEEP, NS)),
            pltpu.SemaphoreType.DMA((K, NS)),
            pltpu.SemaphoreType.DMA((Gather.DEEP,)),
        ]

    def local(self, j):
        at = self.at
        return pltpu.make_async_copy(
            self.mine(j), self.whole(j, at.a0, at.pos(at.f, at.s), at.c),
            self.lsem.at[lax.rem(j, self.DEEP)],
        )

    def copies(self, stage, j, sending, late):
        at, whole = self.at, self.whole
        A0, A = at.A0, at.A
        par = lax.rem(j, self.DEEP)
        line0, first0 = 0, (A0 - 1) * A
        second0 = first0 + A - 1
        every = slice(None)
        out = []

        def add(k, src, dst, device):
            out.append(send(src, dst, self.ssem.at[par, k], self.rsem.at[j, k], device))

        if stage == 0 and not late:
            for q in range(1, A0):
                a = at.a0 if sending else at.line(-q)
                add(line0 + q - 1, self.mine(j), whole(j, a, at.pos(at.f, at.s), at.c),
                    at.device(at.line(q), at.f, at.s, at.c))
        elif stage == 1 and late:
            for q in range(1, A0):
                a = at.a0 if sending else at.line(-q)
                for o in range(A):
                    ref = whole(j, a, at.pos(o, at.s), at.c)
                    add(line0 + (q - 1) * A + o, ref, ref,
                        at.device(at.line(q), at.f, at.s, at.c))
        elif stage < 2:
            for q in range(1, A):
                f = at.f if sending else at.first(-q)
                ref = whole(j, at.a0 if late else every, at.pos(f, at.s), at.c)
                add(first0 + q - 1, self.mine(j) if late else ref, ref,
                    at.device(at.a0, at.first(q), at.s, at.c))
        elif stage == 2:
            for q in range(1, A):
                s = at.s if sending else at.second(-q)
                for o in range(A):
                    ref = whole(j, every, at.pos(o, s), at.c)
                    add(second0 + (q - 1) * A + o, ref, ref,
                        at.device(at.a0, at.f, at.second(q), at.c))
        else:
            ref = whole(j, every, every, at.c if sending else 1 - at.c)
            add(second0 + (A - 1) * A, ref, ref, at.partner())
        return out

    def each(self, stage, j, sending, act):
        def run(late):
            for cp in self.copies(stage, j, sending, late):
                act(cp)

        if stage >= 2:
            run(False)
            return
        late = lax.rem(j, 3) == self.TURN
        pl.when(late)(lambda: run(True))
        pl.when(jnp.logical_not(late))(lambda: run(False))

    def step(self, i):
        for stage in self.ORDER:
            j = i - self.AFTER[stage]

            @pl.when((j >= 0) & (j < self.K))
            def _(stage=stage, j=j):
                if stage > 0:
                    self.each(stage - 1, j, False, lambda cp: cp.wait_recv())
                if stage < 4:

                    @pl.when(j >= self.DEEP)
                    def _():
                        self.each(stage, j - self.DEEP, True, lambda cp: cp.wait_send())

                    if stage == 1:
                        self.local(j).wait()
                    self.each(stage, j, True, lambda cp: cp.start())
                    if stage == 0:
                        self.local(j).start()

    def drain(self):
        for j in range(max(0, self.K - self.DEEP), self.K):
            for stage in range(4):
                for cp in self.copies(stage, jnp.int32(j), True, j % 3 == self.TURN):
                    cp.wait_send()


class Reduce:
    SLOTS = 3
    LAG = 2

    def __init__(self, at, K, begun, refs):
        self.at, self.K, self.begun = at, K, begun
        (self.own0, self.own1, self.own2, self.own3, self.s0, self.s1, self.s2, self.s3,
         self.r0, self.r1, self.r2, self.r3, self.ssem, self.rsem, self.credit) = refs

    @staticmethod
    def scratch(K, A0, A, r, w):
        N = A0 * A * A
        NS = 1 + (A - 1) + (A - 1) + (A0 - 1)
        L = Reduce.SLOTS
        return [
            pltpu.VMEM((2, N, r, w), f32),
            pltpu.VMEM((2, A0 * A, r, w), f32),
            pltpu.VMEM((2, A0, r, w), f32),
            pltpu.VMEM((2, r, w), f32),
            pltpu.VMEM((2, N, r, w), bf16),
            pltpu.VMEM((2, A - 1, A0 * A, r, w), bf16),
            pltpu.VMEM((2, A - 1, A0, r, w), bf16),
            pltpu.VMEM((2, A0 - 1, r, w), bf16),
            pltpu.VMEM((L, N, r, w), bf16),
            pltpu.VMEM((L, A - 1, A0 * A, r, w), bf16),
            pltpu.VMEM((L, A - 1, A0, r, w), bf16),
            pltpu.VMEM((L, A0 - 1, r, w), bf16),
            pltpu.SemaphoreType.DMA((2, NS)),
            pltpu.SemaphoreType.DMA((L, NS)),
            pltpu.SemaphoreType.REGULAR((NS,)),
        ]

    def routes(self, stage):
        at = self.at
        A0, A = at.A0, at.A
        if stage == 0:
            return [(0, at.partner(), at.partner())]
        if stage == 1:
            to = lambda q: at.device(at.a0, at.f, at.second(q), at.c)
            return [(q, to(q), to(-q)) for q in range(1, A)]
        if stage == 2:
            to = lambda q: at.device(at.a0, at.first(q), at.s, at.c)
            return [(A - 1 + q, to(q), to(-q)) for q in range(1, A)]
        to = lambda q: at.device(at.line(q), at.f, at.s, at.c)
        return [(2 * (A - 1) + q, to(q), to(-q)) for q in range(1, A0)]

    def copies(self, stage, j):
        par, slot = lax.rem(j, 2), lax.rem(j, self.SLOTS)
        src, dst = ((self.s0, self.r0), (self.s1, self.r1), (self.s2, self.r2),
                    (self.s3, self.r3))[stage]
        out = []
        for q, (k, to, _) in enumerate(self.routes(stage)):
            a = src.at[par] if stage == 0 else src.at[par, q]
            b = dst.at[slot] if stage == 0 else dst.at[slot, q]
            out.append(send(a, b, self.ssem.at[par, k], self.rsem.at[slot, k], to))
        return out

    def free(self, stage, j):
        @pl.when(j >= 2)
        def _():
            for cp in self.copies(stage, j - 2):
                cp.wait_send()

    def start(self, stage, j):
        @pl.when(j >= self.SLOTS)
        def _():
            for k, _, _ in self.routes(stage):
                pl.semaphore_wait(self.credit.at[k], 1)

        for cp in self.copies(stage, j):
            cp.start()

    def arrive(self, stage, j):
        for cp in self.copies(stage, j):
            cp.wait_recv()

    def done(self, stage, j):
        @pl.when(j + self.SLOTS < self.K)
        def _():
            for k, _, source in self.routes(stage):
                pl.semaphore_signal(
                    self.credit.at[k], inc=1, device_id=source, device_id_type=MESH
                )

    def begin(self, j, own, right):
        N, r, w = self.own0.shape[1:]
        par = lax.rem(j, 2)
        rows = lambda k: own[k].reshape(N * r, own.shape[3])
        self.free(0, j)
        self.s0[par] = (
            jnp.dot(rows(1), right, preferred_element_type=f32).astype(bf16).reshape(N, r, w)
        )
        self.start(0, j)
        self.own0[par] = jnp.dot(rows(0), right, preferred_element_type=f32).reshape(N, r, w)

    def step(self, i, finish):
        at = self.at
        A0, A = at.A0, at.A

        def stage1(j, par, slot):
            def line(a, _):
                for o in range(A):
                    for q in range(A):
                        b = a * A * A + at.pos(o, at.second(q))
                        v = self.own0[par, b] + self.r0[slot, b].astype(f32)
                        if q == 0:
                            self.own1[par, a * A + o] = v
                        else:
                            self.s1[par, q - 1, a * A + o] = v.astype(bf16)
                return 0

            lax.fori_loop(0, A0, line, 0)

        def stage2(j, par, slot):
            def line(a, _):
                for q in range(A):
                    b = a * A + at.first(q)
                    v = self.own1[par, b]
                    for p in range(A - 1):
                        v = v + self.r1[slot, p, b].astype(f32)
                    if q == 0:
                        self.own2[par, a] = v
                    else:
                        self.s2[par, q - 1, a] = v.astype(bf16)
                return 0

            lax.fori_loop(0, A0, line, 0)

        def stage3(j, par, slot):
            for q in range(A0):
                a = at.line(q)
                v = self.own2[par, a]
                for p in range(A - 1):
                    v = v + self.r2[slot, p, a].astype(f32)
                if q == 0:
                    self.own3[par] = v
                else:
                    self.s3[par, q - 1] = v.astype(bf16)

        def stage4(j, par, slot):
            v = self.own3[par]
            for p in range(A0 - 1):
                v = v + self.r3[slot, p].astype(f32)
            finish(j, v)

        for k, stage in ((4, stage4), (3, stage3), (2, stage2), (1, stage1)):
            valid, j = self.begun(i - k * self.LAG)

            @pl.when(valid)
            def _(j=j, k=k, stage=stage):
                self.arrive(k - 1, j)
                if k < 4:
                    self.free(k, j)
                stage(j, lax.rem(j, 2), lax.rem(j, self.SLOTS))
                self.done(k - 1, j)
                if k < 4:
                    self.start(k, j)

    def drain(self):
        for j in range(max(0, self.K - 2), self.K):
            for stage in range(4):
                for cp in self.copies(stage, jnp.int32(j)):
                    cp.wait_send()


class SumAll:
    def __init__(self, at, refs):
        self.at = at
        self.hold, self.land, self.ssem, self.rsem = refs

    @staticmethod
    def scratch(A0, A, shape):
        slots = 2 + A + A + A0
        return [
            pltpu.VMEM((4,) + shape, f32),
            pltpu.VMEM((slots,) + shape, f32),
            pltpu.SemaphoreType.DMA((slots,)),
            pltpu.SemaphoreType.DMA((slots,)),
        ]

    def group(self, stage):
        at = self.at
        A0, A = at.A0, at.A
        chip = at.a0 * A * A + at.a1 * A + at.a2
        if stage == 0:
            return 0, 2, at.c, 1, chip * 2
        if stage == 1:
            return 2, A, at.a2, 2, (chip - at.a2) * 2 + at.c
        if stage == 2:
            return 2 + A, A, at.a1, 2 * A, (chip - at.a1 * A) * 2 + at.c
        return 2 + 2 * A, A0, at.a0, 2 * A * A, (chip - at.a0 * A * A) * 2 + at.c

    def copies(self, stage, sending):
        base, size, mine, stride, origin = self.group(stage)
        out = []
        for q in range(1, size):
            to = lax.rem(mine + q, size)
            slot = mine if sending else lax.rem(mine - q + size, size)
            out.append(
                send(self.hold.at[stage], self.land.at[base + slot], self.ssem.at[base + q],
                     self.rsem.at[base + q], (origin + to * stride,))
            )
        return out

    def start(self, stage, value):
        base, _, mine, _, _ = self.group(stage)
        self.hold[stage] = value
        self.land[base + mine] = value
        for cp in self.copies(stage, True):
            cp.start()

    def finish(self, stage):
        base, size, _, _, _ = self.group(stage)
        for cp in self.copies(stage, False):
            cp.wait_recv()
        for cp in self.copies(stage, True):
            cp.wait_send()
        total = self.land[base]
        for k in range(1, size):
            total = total + self.land[base + k]
        return total


def mix_forward(dims, proj, cpar, hpar, dpar, mixed, ssd, rstd,
                pad, gated, colb, rowb, mask, scores, acc, dtp):
    T, DI, H, HD, ST = dims["T"], dims["DI"], dims["H"], dims["HD"], dims["ST"]
    HP = LANES // HD
    tiles = DI // LANES
    pad[:, 0:FRONT, :] = jnp.zeros((pad.shape[0], FRONT, LANES), f32)
    _, _, _, ld, ld2 = step_stage(dims, proj, hpar, dtp)
    row, col = iotas(T, T)
    mask[...] = jnp.where(col <= row, BIG, -BIG)
    rowb[...] = ld2.T
    for h in range(H):
        colb[h] = jnp.broadcast_to(ld[:, h : h + 1], (T, LANES))
    bc = []
    for a in range(2):
        conv = conv_tile(dims, proj, cpar, pad.at[a], DI + a * ST)
        bc.append((conv * sigmoid(conv)).astype(bf16))
    scores[...] = lax.dot_general(
        bc[1], bc[0], (((1,), (1,)), ((), ())), preferred_element_type=f32
    )
    acc[...] = jnp.zeros_like(acc)

    def tile(j, u):
        c0 = pl.multiple_of(j * LANES, LANES)
        lanes = pl.ds(c0, LANES)
        conv = conv_tile(dims, proj, cpar, pad.at[u], c0)
        x = (conv * sigmoid(conv)).astype(bf16)
        mix = []
        for a in range(HP):
            h = j * HP + a
            expo = jnp.minimum(colb[h] - rowb[pl.ds(h, 1), :], mask[...])
            mix.append((jnp.exp2(expo) * scores[...]).astype(bf16))
        core = jnp.dot(
            jnp.concatenate(mix, axis=1), stack_heads(dims, x), preferred_element_type=f32
        )
        out = core + dpar[0:1, lanes] * x.astype(f32)
        ssd[:, lanes] = out
        gate = proj[:, lanes].astype(f32)
        g = out * (gate * sigmoid(gate))
        gated[:, lanes] = g
        return g * g

    def body(j, _):
        total = tile(j * UNROLL_F, 0)
        for u in range(1, UNROLL_F):
            total = total + tile(j * UNROLL_F + u, u)
        acc[...] += total
        return 0

    lax.fori_loop(0, tiles // UNROLL_F, body, 0)
    r = lax.rsqrt(jnp.sum(acc[...], axis=1, keepdims=True) * (1.0 / DI) + epsilon)
    rb = jnp.broadcast_to(r, (T, LANES))
    rstd[...] = rb

    def finish(j, _):
        lanes = pl.ds(pl.multiple_of(j * LANES, LANES), LANES)
        mixed[:, lanes] = (gated[:, lanes] * rb * dpar[1:2, lanes]).astype(bf16)
        return 0

    lax.fori_loop(0, tiles, finish, 0)


def mix_backward(dims, steps, proj, dmixed, ssd, rstd, cpar, hpar, dpar, dproj, small,
                 cacc, dacc, hacc, pad, dpad, colb, rowb, mask, scores, acc, dtp, dscores, dlog,
                 csum, bcs):
    T, DI, C, H, HD, ST, KW = (dims[k] for k in ("T", "DI", "C", "H", "HD", "ST", "KW"))
    HP = LANES // HD
    tiles = DI // LANES

    @pl.when(pl.program_id(0) == 0)
    def _():
        cacc[...] = jnp.zeros_like(cacc)
        dacc[...] = jnp.zeros_like(dacc)
        hacc[...] = jnp.zeros_like(hacc)

    pad[:, 0:FRONT, :] = jnp.zeros((pad.shape[0], FRONT, LANES), f32)
    dpad[:, T:, :] = jnp.zeros((dpad.shape[0], FRONT, LANES), f32)
    v, e, step, ld, ld2 = step_stage(dims, proj, hpar, dtp)
    row, col = iotas(T, T)
    mask[...] = jnp.where(row <= col, BIG, -BIG)
    rowb[...] = ld.T
    for h in range(H):
        colb[h] = jnp.broadcast_to(ld2[:, h : h + 1], (T, LANES))
    for a in range(2):
        conv = conv_tile(dims, proj, cpar, pad.at[a], DI + a * ST)
        bcs[a] = (conv * sigmoid(conv)).astype(bf16)
    scores[...] = lax.dot_general(
        bcs[0], bcs[1], (((1,), (1,)), ((), ())), preferred_element_type=f32
    )
    acc[...] = jnp.zeros_like(acc)
    dscores[...] = jnp.zeros_like(dscores)
    dlog[...] = jnp.zeros_like(dlog)
    csum[...] = jnp.zeros_like(csum)
    rb = rstd[...]

    def first(j, _):
        lanes = pl.ds(pl.multiple_of(j * LANES, LANES), LANES)
        gate = proj[:, lanes].astype(f32)
        p = dmixed[:, lanes] * (ssd[:, lanes] * (gate * sigmoid(gate)))
        acc[...] += p * dpar[1:2, lanes]
        dacc[8:16, lanes] += sum8(p * rb)
        return 0

    lax.fori_loop(0, tiles, first, 0)
    mean = jnp.sum(acc[...], axis=1, keepdims=True) * (1.0 / DI)
    mb = jnp.broadcast_to(mean, (T, LANES)) * rb * rb * rb
    acc[...] = mb

    def conv_back(c0, dact, conv, sig, u):
        lanes = pl.ds(c0, LANES)
        dconv = dact * (sig * (1.0 + conv * (1.0 - sig)))
        dpad[u, 0:T, :] = dconv
        dcin = dconv * cpar[KW - 1 : KW, lanes]
        for k in range(KW - 1):
            dcin = dcin + dpad[u, KW - 1 - k : KW - 1 - k + T, :] * cpar[k : k + 1, lanes]
        dproj[:, pl.ds(DI + c0, LANES)] = dcin.astype(bf16)
        for k in range(KW):
            start = FRONT - KW + 1 + k
            cacc[8 * k : 8 * k + 8, lanes] += sum8(dconv * pad[u, start : start + T, :])
        cacc[8 * KW : 8 * KW + 8, lanes] += sum8(dconv)

    def tile(j, u):
        c0 = pl.multiple_of(j * LANES, LANES)
        lanes = pl.ds(c0, LANES)
        conv = conv_tile(dims, proj, cpar, pad.at[u], c0)
        sig = sigmoid(conv)
        x = (conv * sig).astype(bf16)
        xf = x.astype(f32)
        gate = proj[:, lanes].astype(f32)
        gs = sigmoid(gate)
        act = gate * gs
        out = ssd[:, lanes]
        r = rstd[...]
        dgated = r * (dmixed[:, lanes] * dpar[1:2, lanes]) - (out * act) * acc[...]
        dssd = dgated * act
        dproj[:, lanes] = (dgated * out * (gs * (1.0 + gate * (1.0 - gs)))).astype(bf16)
        low = dssd.astype(bf16)
        dacc[0:8, lanes] += sum8(dssd * xf)
        lows = stack_heads(dims, low)
        dmix = lax.dot_general(
            x, lows, (((1,), (1,)), ((), ())), preferred_element_type=f32
        )
        mix = []
        part = None
        for a in range(HP):
            h = j * HP + a
            decay = jnp.exp2(jnp.minimum(rowb[pl.ds(h, 1), :] - colb[h], mask[...]))
            mix.append((decay * scores[...]).astype(bf16))
            term = dmix[:, a * T : (a + 1) * T] * decay
            part = term if part is None else part + term
        core = jnp.dot(jnp.concatenate(mix, axis=1), lows, preferred_element_type=f32)
        skip = dpar[0:1, lanes]
        from_cols = xf * core
        diff = low.astype(f32) * (out - skip * xf) - from_cols
        prow, pcol = iotas(LANES, LANES)
        place = (pcol == j * HP + prow // HD).astype(bf16)
        place = jnp.concatenate([place, place], axis=0)

        def by_head(w):
            hi = w.astype(bf16)
            lo = (w - hi.astype(f32)).astype(bf16)
            return jnp.dot(
                jnp.concatenate([hi, lo], axis=1), place, preferred_element_type=f32
            )

        conv_back(c0, core + skip * dssd, conv, sig, u)
        return part, by_head(diff), by_head(from_cols)

    def body(j, _):
        sums = tile(j * UNROLL_B, 0)
        for u in range(1, UNROLL_B):
            sums = tuple(p + q for p, q in zip(sums, tile(j * UNROLL_B + u, u)))
        dscores[...] += sums[0]
        dlog[...] += sums[1]
        csum[...] += sums[2]
        return 0

    lax.fori_loop(0, tiles // UNROLL_B, body, 0)
    ds = dscores[...].astype(bf16)
    dst = dscores[...].T.astype(bf16)
    dact = (
        jnp.dot(ds, bcs[1], preferred_element_type=f32),
        jnp.dot(dst, bcs[0], preferred_element_type=f32),
    )
    for a in range(2):
        conv = conv_tile(dims, proj, cpar, pad.at[a], DI + a * ST)
        conv_back(DI + a * ST, dact[a], conv, sigmoid(conv), a)
    dsteps = jnp.dot(
        (row <= col).astype(f32), dlog[...], precision=lax.Precision.HIGHEST,
        preferred_element_type=f32,
    )
    sg = jnp.where(v >= 0.0, 1.0, e) / (1.0 + e)
    ratio = jnp.where(step > 1e-30, sg / jnp.maximum(step, 1e-30), 1.0)
    ddt = csum[...] * ratio + dsteps * hpar[1:2, :] * sg
    tail = dproj.shape[1] - DI - C
    if tail > H:
        dproj[:, DI + C :] = jnp.concatenate(
            [ddt[:, 0:H].astype(bf16), jnp.zeros((T, tail - H), bf16)], axis=1
        )
    else:
        dproj[:, DI + C :] = ddt[:, 0:H].astype(bf16)
    hacc[0:8, :] += sum8(ddt)
    hacc[8:16, :] += sum8(dsteps * step)

    @pl.when(pl.program_id(0) == steps - 1)
    def _():
        small[...] = jnp.zeros_like(small)
        for k in range(KW + 1):
            small[k : k + 1, :] = jnp.sum(cacc[8 * k : 8 * k + 8, :], axis=0, keepdims=True)
        for k in range(2):
            small[KW + 1 + k : KW + 2 + k, 0:DI] = jnp.sum(
                dacc[8 * k : 8 * k + 8, :], axis=0, keepdims=True
            )
            small[KW + 3 : KW + 4, k * LANES : (k + 1) * LANES] = jnp.sum(
                hacc[8 * k : 8 * k + 8, :], axis=0, keepdims=True
            )


def run_forward(dims, proj, cpar, hpar, dpar):
    T, DI, C, H, KW = dims["T"], dims["DI"], dims["C"], dims["H"], dims["KW"]
    R, E = proj.shape
    rows = lambda w: pl.BlockSpec((T, w), lambda i: (i, 0))
    whole = lambda a: pl.BlockSpec(a.shape, lambda i: (0, 0))
    return pl.pallas_call(
        functools.partial(mix_forward, dims),
        grid=(R // T,),
        in_specs=[rows(E), whole(cpar), whole(hpar), whole(dpar)],
        out_specs=[rows(DI), rows(DI), rows(LANES)],
        out_shape=[
            jax.ShapeDtypeStruct((R, DI), bf16),
            jax.ShapeDtypeStruct((R, DI), f32),
            jax.ShapeDtypeStruct((R, LANES), f32),
        ],
        scratch_shapes=[
            pltpu.VMEM((max(2, UNROLL_F), FRONT + T, LANES), f32),
            pltpu.VMEM((T, DI), f32),
            pltpu.VMEM((H, T, LANES), f32),
            pltpu.VMEM((LANES, T), f32),
            pltpu.VMEM((T, T), f32),
            pltpu.VMEM((T, T), f32),
            pltpu.VMEM((T, LANES), f32),
            pltpu.VMEM((T, LANES), f32),
        ],
        compiler_params=pltpu.CompilerParams(vmem_limit_bytes=48 << 20),
        name="mix_forward",
    )(proj, cpar, hpar, dpar)


def run_backward(dims, proj, dmixed, ssd, rstd, cpar, hpar, dpar):
    T, DI, C, H, KW, ST = (dims[k] for k in ("T", "DI", "C", "H", "KW", "ST"))
    R, E = proj.shape
    rows = lambda w: pl.BlockSpec((T, w), lambda i: (i, 0))
    whole = lambda s: pl.BlockSpec(s, lambda i: (0, 0))
    sums = [(8 * (KW + 1), C), (16, DI), (16, LANES)]
    return pl.pallas_call(
        functools.partial(mix_backward, dims, R // T),
        grid=(R // T,),
        in_specs=[rows(E), rows(DI), rows(DI), rows(LANES)]
        + [whole(a.shape) for a in (cpar, hpar, dpar)],
        out_specs=[rows(E), whole((8, C))],
        out_shape=[jax.ShapeDtypeStruct((R, E), bf16), jax.ShapeDtypeStruct((8, C), f32)],
        scratch_shapes=[pltpu.VMEM(s, f32) for s in sums]
        + [
            pltpu.VMEM((max(2, UNROLL_B), FRONT + T, LANES), f32),
            pltpu.VMEM((max(2, UNROLL_B), FRONT + T, LANES), f32),
            pltpu.VMEM((H, T, LANES), f32),
            pltpu.VMEM((LANES, T), f32),
            pltpu.VMEM((T, T), f32),
            pltpu.VMEM((T, T), f32),
            pltpu.VMEM((T, LANES), f32),
            pltpu.VMEM((T, LANES), f32),
            pltpu.VMEM((T, T), f32),
            pltpu.VMEM((T, LANES), f32),
            pltpu.VMEM((T, LANES), f32),
            pltpu.VMEM((2, T, ST), bf16),
        ],
        compiler_params=pltpu.CompilerParams(vmem_limit_bytes=56 << 20),
        name="mix_backward",
    )(proj, dmixed, ssd, rstd, cpar, hpar, dpar)


def several(count, width, body):
    width = math.gcd(width, count)

    def trip(m, _):
        for q in range(width):
            body(m * width + q, q)
        return 0

    lax.fori_loop(0, count // width, trip, 0)


def assemble(parts, size, tiles):
    _, lane = iotas(8, LANES)
    out = []
    for t in range(tiles):
        total = None
        for d in range(t * LANES // size, min(len(parts), -(-(t + 1) * LANES // size))):
            shift = d * size - t * LANES
            v = parts[d] if shift % LANES == 0 else pltpu.roll(parts[d], shift % LANES, 1)
            keep = (lane >= max(shift, 0)) & (lane < min(shift + size, LANES))
            v = jnp.where(keep, v, 0.0)
            total = v if total is None else total + v
        out.append(total)
    return out


def forward(dims, axis, geom, K, KO, skip, tok, inw, taps, bias, gains, ns, dtb, alog, ow,
            tokc, goc, proj, ssd, uT, mT, out, tabs, pars, scale, wl, hpar, wfull, ofull,
            uh, wv, wo, pj, gated, mixed, pad, ldtab, rowtab, scores, mask, acc, dtp, wsem, osem,
            *sems):
    T, DI, C, H, HD, ST, KW = (dims[k] for k in ("T", "DI", "C", "H", "HD", "ST", "KW"))
    A0, A = geom
    at = Place(axis, A0, A)
    i = pl.program_id(0)
    R, D = tok.shape
    w = wl.shape[2]
    half = w // 2
    S = R // T
    HP = LANES // HD
    TC = half // LANES
    wo_cols = wo.shape[5]
    place = lambda j: lax.rem(j + K - 1, K)
    part = lambda j: columns(lax.rem(j, 2), half)
    net = Gather(
        at, 2 * K, lambda j: wl.at[lax.div(j, 2), :, part(j)],
        lambda j, a, p, c: wfull.at[place(lax.div(j, 2)), a, p, c, :, part(j)], *sems[:3],
    )
    neto = Gather(
        at, 2 * KO, lambda j: ow.at[:, columns(j, wo_cols // 2)],
        lambda j, a, p, c: ofull.at[a, p, c, :, columns(j, wo_cols // 2)], *sems[3:],
    )

    @pl.when(i == 0)
    def _():
        at.greet()
        r, E = inw.shape
        Cn, Gn = bias.shape[1], gains.shape[1]
        zero = jnp.zeros((LANES, LANES), f32)
        dtp[...] = zero
        dtp[0:1, 0:r] = ns[...].astype(f32)
        column = pltpu.roll(dtp[...].T, LANES - 1, 1)
        dtp[...] = column
        dtp[0:KW, 0:Cn] = taps[...].astype(f32)
        dtp[KW : KW + 1, 0:Cn] = bias[...].astype(f32)
        dtp[KW + 1 : KW + 2, 0:Gn] = gains[...].astype(f32)
        wl[0, :, 0 : half] = inw[:, 2 * DI : 2 * DI + half]
        wl[0, :, half : half + LANES] = jnp.concatenate(
            [inw[:, 2 * DI + half : E], jnp.zeros((r, LANES - H), bf16)], axis=1
        )
        wl[0, :, half + LANES :] = dtp[0:r, :].astype(bf16)
        for j in range(1, K):
            wl[j, :, 0:half] = inw[:, (j - 1) * half : j * half]
            wl[j, :, half:] = inw[:, DI + (j - 1) * half : DI + j * half]
        hpar[...] = jnp.zeros_like(hpar)
        hpar[0:1, 0:H] = dtb[...]
        hpar[1:2, 0:H] = -jnp.exp(alog[...])
        at.meet()

    def travel(q):
        net.step(q)
        neto.step(q - 2 * K)

    trip = 2 * i
    i = i - ((Gather.AFTER[4] + 2) // 2 - 4)
    travel(trip)

    def fetch_w(j):
        slot = lax.rem(j, 2)
        return pltpu.make_async_copy(wfull.at[place(j)], wv.at[slot], wsem.at[slot])

    def fetch_o(k):
        slot = lax.rem(k, 2)
        return pltpu.make_async_copy(
            ofull.at[:, :, :, :, columns(k, wo_cols)], wo.at[slot], osem.at[slot]
        )

    ready = (i >= 4) & (i < K + 4)
    chunk = jnp.maximum(i - 4, 0)

    @pl.when(ready)
    def _():
        fetch_w(chunk).start()

    @pl.when((i >= K + 4) & (i < K + KO + 4))
    def _():
        fetch_o(i - K - 4).start()

    @pl.when(i == 5)
    def _():
        row, col = iotas(T, T)
        mask[...] = jnp.where(col <= row, BIG, -BIG)
        pad[:, 0:FRONT, :] = jnp.zeros((pad.shape[0], FRONT, LANES), f32)
        acc[...] = jnp.zeros_like(acc)

        def seq(s, _):
            rows = pl.ds(pl.multiple_of(s * T, T), T)
            bc = []
            for a in range(2):
                conv = conv_of(dims, pj[0, rows, a * LANES : (a + 1) * LANES], pars, pad.at[a],
                               DI + a * ST)
                bc.append((conv * sigmoid(conv)).astype(bf16))
            scores[s] = lax.dot_general(
                bc[1], bc[0], (((1,), (1,)), ((), ())), preferred_element_type=f32
            )
            _, _, _, ld, ld2 = steps_of(
                dims, pj[0, rows, 2 * LANES : 3 * LANES].astype(f32), hpar
            )
            ldtab[s] = ld
            rowtab[s] = ld2.T
            return 0

        lax.fori_loop(0, S, seq, 0)

    @pl.when((i >= 6) & (i < K + 5))
    def _():
        j = i - 5
        slot = lax.rem(j, 2)
        h0 = (j - 1) * TC * HP

        def seq(s, q):
            rows = pl.ds(pl.multiple_of(s * T, T), T)
            turned = pltpu.roll(ldtab[s], LANES - h0, 1)
            total = None
            for u in range(TC):
                c0 = pl.multiple_of((j - 1) * half + u * LANES, LANES)
                conv = conv_of(
                    dims, pj[slot, rows, half + u * LANES : half + (u + 1) * LANES], pars,
                    pad.at[q * TC + u], c0,
                )
                x = (conv * sigmoid(conv)).astype(bf16)
                mix = []
                for a in range(HP):
                    k = u * HP + a
                    left = jnp.broadcast_to(turned[:, k : k + 1], (T, T))
                    expo = jnp.minimum(left - rowtab[s, pl.ds(h0 + k, 1), :], mask[...])
                    mix.append((jnp.exp2(expo) * scores[s]).astype(bf16))
                core = jnp.dot(
                    jnp.concatenate(mix, axis=1), stack_heads(dims, x),
                    preferred_element_type=f32,
                )
                o = core + pars[8:9, pl.ds(c0, LANES)] * x.astype(f32)
                ssd[rows, u * LANES : (u + 1) * LANES] = o
                gate = pj[slot, rows, u * LANES : (u + 1) * LANES].astype(f32)
                g = o * (gate * sigmoid(gate))
                gated[rows, pl.ds(c0, LANES)] = g
                total = g * g if total is None else total + g * g
            acc[rows, :] += total

        several(S, SEQ_F, seq)

    @pl.when(i < K + 5)
    def _():
        travel(trip + 1)

    @pl.when(ready)
    def _():
        fetch_w(chunk).wait()

    @pl.when(i == 4)
    def _():
        N = A0 * A * A * 2
        r = D // N
        Cn, Gn = C // N, DI // N
        last = wv[0].reshape(D, w)[:, w - LANES :].astype(f32)
        turned = last.T
        scale[...] = jnp.broadcast_to(turned[LANES - 1 :, :], scale.shape)
        parts = [last[d * r : d * r + 8, :] for d in range(N)]
        for t, v in enumerate(assemble(parts, Cn, C // LANES)):
            pars[0:8, t * LANES : (t + 1) * LANES] = v
        for t, v in enumerate(assemble(parts, Gn, DI // LANES)):
            pars[8:16, t * LANES : (t + 1) * LANES] = v
        _, lane = iotas(1, LANES)
        for t in range(DI // LANES):
            v = jnp.zeros((1, LANES), f32)
            for q in range(HP):
                v = jnp.where(lane // HD == q, skip[t * HP + q], v)
            pars[8:9, t * LANES : (t + 1) * LANES] = v

        def norm(k, _):
            rows = pl.ds(pl.multiple_of(k * LANES, LANES), LANES)
            u = tok[rows, :].astype(f32)
            rs = lax.rsqrt(jnp.mean(u * u, axis=-1, keepdims=True) + epsilon)
            v = u * rs * scale[0:1, :]
            uh[rows, :] = v.astype(bf16)
            uT[:, rows] = v.T.astype(bf16)
            return 0

        lax.fori_loop(0, R // LANES, norm, 0)

    @pl.when(ready)
    def _():
        slot = lax.rem(i, 2)
        M = min(R, ROWS)

        def rows(k, _):
            at_ = pl.ds(pl.multiple_of(k * M, M), M)
            v = jnp.dot(
                uh[at_, :], wv[slot].reshape(D, w), preferred_element_type=f32
            ).astype(bf16)
            pj[slot, at_, :] = v
            proj[0, at_, :] = v
            return 0

        lax.fori_loop(0, R // M, rows, 0)

    @pl.when(i == K + 5)
    def _():
        def seq(s, _):
            rows = pl.ds(pl.multiple_of(s * T, T), T)
            rs = lax.rsqrt(jnp.sum(acc[rows, :], axis=1, keepdims=True) * (1.0 / DI) + epsilon)
            rb = jnp.broadcast_to(rs, (T, LANES))
            tabs[0, rows, :] = rb

            def tile(k, _):
                for u in range(4):
                    lanes = pl.ds(pl.multiple_of((k * 4 + u) * LANES, LANES), LANES)
                    v = gated[rows, lanes] * rb * pars[8 + KW + 1 : 8 + KW + 2, lanes]
                    mixed[rows, lanes] = v.astype(bf16)
                return 0

            lax.fori_loop(0, DI // LANES // 4, tile, 0)
            return 0

        lax.fori_loop(0, S, seq, 0)
        acc[...] = jnp.zeros_like(acc)

    @pl.when(i >= K + 5)
    def _():
        travel(trip + 1)

    @pl.when(i >= K + 5)
    def _():
        k = i - K - 5
        slot = lax.rem(k, 2)
        fetch_o(k).wait()
        M = 256

        def rows(m, _):
            at_ = pl.ds(pl.multiple_of(m * M, M), M)
            branch = jnp.dot(
                mixed[at_, :], wo[slot].reshape(DI, wo_cols), preferred_element_type=f32
            )
            out[at_, :] = (tokc[at_, :].astype(f32) + branch).astype(bf16)
            p = branch * goc[at_, :].astype(f32)
            part = p[:, 0:LANES]
            for q in range(1, wo_cols // LANES):
                part = part + p[:, q * LANES : (q + 1) * LANES]
            acc[at_, :] += part
            return 0

        lax.fori_loop(0, R // M, rows, 0)

        share = DI // LANES // KO

        def turn(m, _):
            for u in range(share):
                lanes = pl.ds(pl.multiple_of((k * share + u) * LANES, LANES), LANES)
                rows = pl.ds(pl.multiple_of(m * LANES, LANES), LANES)
                mT[lanes, rows] = mixed[rows, lanes].T
            return 0

        lax.fori_loop(0, R // LANES, turn, 0)

    @pl.when(i == K + KO + 4)
    def _():
        net.drain()
        neto.drain()
        mu = jnp.sum(acc[...], axis=1, keepdims=True) * (1.0 / DI)
        rb = tabs[0]
        tabs[1] = jnp.broadcast_to(mu, rb.shape) * rb * rb


def run_forward_net(dims, axis, geom, K, w, skip, tok, go, inw, smalls, ow):
    T, DI, C = (dims[k] for k in ("T", "DI", "C"))
    A0, A = geom
    R, D = tok.shape
    r = inw.shape[0]
    ro = ow.shape[0]
    half = w // 2
    wc = r * w // ro
    KO = D // wc
    S = R // T
    assert DI // LANES % KO == 0
    shift = (Gather.AFTER[4] + 2) // 2 - 4
    steps = K + KO + 5 + shift
    whole = lambda s: pl.BlockSpec(s, lambda i: (0,) * len(s), pipeline_mode=pl.Buffered(1))
    late = lambda i: (0, jnp.clip(i - K - 5 - shift, 0, KO - 1))
    hbm = pl.BlockSpec(memory_space=pl.ANY)
    return pl.pallas_call(
        functools.partial(forward, dims, axis, geom, K, KO),
        grid=(steps,),
        in_specs=[pl.BlockSpec(memory_space=pltpu.SMEM), whole((R, D)), whole(inw.shape)]
        + [whole(a.shape) for a in smalls]
        + [whole((ro, D)), pl.BlockSpec((R, wc), late), pl.BlockSpec((R, wc), late)],
        out_specs=[
            pl.BlockSpec((1, R, w), lambda i: (jnp.clip(i - 4 - shift, 0, K - 1), 0, 0)),
            pl.BlockSpec((R, half), lambda i: (0, jnp.clip(i - 6 - shift, 0, K - 2))),
            whole((D, R)), whole((DI, R)),
            pl.BlockSpec((R, wc), late),
            whole((2, R, LANES)), whole((16, C)), whole((8, D)), whole((K, r, w)),
            whole((8, LANES)), hbm, hbm,
        ],
        out_shape=[
            jax.ShapeDtypeStruct((K, R, w), bf16),
            jax.ShapeDtypeStruct((R, DI), f32),
            jax.ShapeDtypeStruct((D, R), bf16),
            jax.ShapeDtypeStruct((DI, R), bf16),
            jax.ShapeDtypeStruct((R, D), bf16),
            jax.ShapeDtypeStruct((2, R, LANES), f32),
            jax.ShapeDtypeStruct((16, C), f32),
            jax.ShapeDtypeStruct((8, D), f32),
            jax.ShapeDtypeStruct((K, r, w), bf16),
            jax.ShapeDtypeStruct((8, LANES), f32),
            jax.ShapeDtypeStruct((K, A0, A * A, 2, r, w), bf16),
            jax.ShapeDtypeStruct((A0, A * A, 2, ro, D), bf16),
        ],
        scratch_shapes=[
            pltpu.VMEM((R, D), bf16),
            pltpu.VMEM((2, A0, A * A, 2, r, w), bf16),
            pltpu.VMEM((2, A0, A * A, 2, ro, wc), bf16),
            pltpu.VMEM((2, R, w), bf16),
            pltpu.VMEM((R, DI), f32),
            pltpu.VMEM((R, DI), bf16),
            pltpu.VMEM((SEQ_F * half // LANES, FRONT + T, LANES), f32),
            pltpu.VMEM((S, T, LANES), f32),
            pltpu.VMEM((S, LANES, T), f32),
            pltpu.VMEM((S, T, T), f32),
            pltpu.VMEM((T, T), f32),
            pltpu.VMEM((R, LANES), f32),
            pltpu.VMEM((T, LANES), f32),
            pltpu.SemaphoreType.DMA((2,)),
            pltpu.SemaphoreType.DMA((2,)),
        ]
        + Gather.scratch(2 * K, A0, A) + Gather.scratch(2 * KO, A0, A),
        compiler_params=pltpu.CompilerParams(
            collective_id=1, has_side_effects=True, vmem_limit_bytes=VMEM
        ),
        cost_estimate=pl.CostEstimate(
            flops=2 * R * D * K * w, bytes_accessed=D * K * w * 60, transcendentals=0
        ),
        name="forward",
    )(skip, tok, inw, *smalls, ow, tok, go)


def backward(dims, axis, geom, K, KO, E, proj, proj0, ssd, wo, wf, uT, mT, go, wl, tabs, pars,
             hpar, dn, outc, dns, sums,
             uo, mo, dmx, dpj, pad, dpad, ldtab, rowtab, scores, dscores, dlog, csum, bcs, mask,
             cacc, dacc, hacc, small, wv, csem, wsem, *refs):
    T, DI, C, H, HD, ST, KW = (dims[k] for k in ("T", "DI", "C", "H", "HD", "ST", "KW"))
    A0, A = geom
    at = Place(axis, A0, A)
    i = pl.program_id(0)
    R = ssd.shape[0]
    _, r, w = wl.shape
    N = A0 * A * A
    half = w // 2
    S = R // T
    HP = LANES // HD
    TC = half // LANES
    D = go.shape[1]
    HF = mT.shape[2]
    each = KO // HF
    pairs = (K + 1) // 2

    def begun(t):
        step = lax.div(t, 2)
        ends = lax.rem(t, 2) == 1
        outer = (lax.rem(step, 2) == 0) & (step < 2 * KO)
        valid = (t >= 0) & ((ends & (step < K)) | (jnp.logical_not(ends) & outer))
        done = jnp.minimum(lax.div(step + 1, 2), KO)
        return valid, step + done + (ends & outer).astype(jnp.int32)

    net = Reduce(at, K + KO, begun, refs[:15])
    total = SumAll(at, refs[15:])

    def fetches():
        out = [(uT.at[:, at.c], uo.at[0]), (uT.at[:, 1 - at.c], uo.at[1])]
        return [pltpu.make_async_copy(s, d, csem.at[k]) for k, (s, d) in enumerate(out)]

    def fetch_half(h):
        out = [(mT.at[:, at.c, h], mo.at[0]), (mT.at[:, 1 - at.c, h], mo.at[1])]
        return [pltpu.make_async_copy(s, d, csem.at[2 + k]) for k, (s, d) in enumerate(out)]

    @pl.when(i == 0)
    def _():
        at.greet()
        for cp in fetches() + fetch_half(0):
            cp.start()
        for ref in (cacc, dacc, hacc, dlog, csum, dscores, dns):
            ref[...] = jnp.zeros_like(ref)
        row, col = iotas(T, T)
        mask[...] = jnp.where(row <= col, BIG, -BIG)
        pad[:, 0:FRONT, :] = jnp.zeros((pad.shape[0], FRONT, LANES), f32)
        dpad[:, T:, :] = jnp.zeros((dpad.shape[0], FRONT, LANES), f32)

        def seq(s, _):
            rows = pl.ds(pl.multiple_of(s * T, T), T)
            for a in range(2):
                conv = conv_of(dims, proj0[0, rows, a * LANES : (a + 1) * LANES], pars, pad.at[a],
                               DI + a * ST)
                bcs[a, rows, :] = (conv * sigmoid(conv)).astype(bf16)
            scores[s] = lax.dot_general(
                bcs[0, rows, :], bcs[1, rows, :], (((1,), (1,)), ((), ())),
                preferred_element_type=f32,
            )
            _, _, _, ld, ld2 = steps_of(
                dims, proj0[0, rows, 2 * LANES : 3 * LANES].astype(f32), hpar
            )
            ldtab[s] = ld2
            rowtab[s] = ld.T
            return 0

        lax.fori_loop(0, S, seq, 0)
        for cp in fetches() + fetch_half(0):
            cp.wait()
        at.meet()

    for h in range(1, HF):

        @pl.when(i == 2 * h * each - 1)
        def _(h=h):
            for cp in fetch_half(h):
                cp.start()

        @pl.when(i == 2 * h * each)
        def _(h=h):
            for cp in fetch_half(h):
                cp.wait()

    def finish(p, v):
        inner = (p >= 3 * KO) | (lax.rem(p, 3) > 0)

        @pl.when(inner)
        def _():
            g = jnp.where(p >= 3 * KO, p - KO, p - 1 - lax.div(p, 3))
            outc[g] = v
            q = v * wl[lax.rem(g + 1, K)].astype(f32)
            part = q[:, 0:LANES]
            for k in range(1, w // LANES):
                part = part + q[:, k * LANES : (k + 1) * LANES]
            dns[...] += part

        @pl.when(jnp.logical_not(inner))
        def _():
            outc[K + lax.div(p, 3)] = v

    def send_out():
        k = lax.div(i, 2)
        net.step(2 * i, finish)

        @pl.when((lax.rem(i, 2) == 0) & (k < KO))
        def _():
            net.begin(3 * k, mo, go[:, columns(lax.rem(k, each), w)])

    def fetch(t, q):
        return pltpu.make_async_copy(
            wf.at[2 * t + q], wv.at[:, q * w : (q + 1) * w], wsem.at[q]
        )

    def fetch_pair(t, act):
        act(fetch(t, 0))

        @pl.when(2 * t + 1 < K)
        def _():
            act(fetch(t, 1))

    @pl.when(i == 0)
    def _():
        fetch_pair(0, lambda cp: cp.start())

    slot = lax.rem(lax.div(i, 2), dpj.shape[0])
    off = lax.rem(i, 2) * w
    here_of = lambda lane: pl.ds(pl.multiple_of(off + lane, LANES), LANES)

    def conv_back(rows, lane0, c0, dact, conv, sig, u):
        lanes = pl.ds(c0, LANES)
        dconv = dact * (sig * (1.0 + conv * (1.0 - sig)))
        dpad[u, 0:T, :] = dconv
        dcin = dconv * pars[KW - 1 : KW, lanes]
        for k in range(KW - 1):
            dcin = dcin + dpad[u, KW - 1 - k : KW - 1 - k + T, :] * pars[k : k + 1, lanes]
        dpj[slot, rows, here_of(lane0)] = dcin.astype(bf16)
        for k in range(KW):
            start = FRONT - KW + 1 + k
            cacc[8 * k : 8 * k + 8, lanes] += sum8(dconv * pad[u, start : start + T, :])
        cacc[8 * KW : 8 * KW + 8, lanes] += sum8(dconv)

    @pl.when(i < K - 1)
    def _():
        h0 = i * TC * HP
        dmx[...] = lax.dot_general(
            go[...], wo[...], (((1,), (1,)), ((), ())), preferred_element_type=f32
        )

        def seq(s, q):
            rows = pl.ds(pl.multiple_of(s * T, T), T)
            turned = pltpu.roll(ldtab[s], LANES - h0, 1)
            rb, mb = tabs[0, rows, :], tabs[1, rows, :]
            parts = None
            for u in range(TC):
                c0 = pl.multiple_of(i * half + u * LANES, LANES)
                lanes = pl.ds(c0, LANES)
                here = slice(u * LANES, (u + 1) * LANES)
                there = slice(half + u * LANES, half + (u + 1) * LANES)
                conv = conv_of(dims, proj[0, rows, there], pars, pad.at[q * TC + u], c0)
                sig = sigmoid(conv)
                x = (conv * sig).astype(bf16)
                xf = x.astype(f32)
                gate = proj[0, rows, here].astype(f32)
                gs = sigmoid(gate)
                act = gate * gs
                o = ssd[rows, here]
                dm = dmx[rows, here]
                gated = o * act
                dgated = rb * (dm * pars[8 + KW + 1 : 8 + KW + 2, lanes]) - gated * mb
                dacc[8:16, lanes] += sum8(dm * (gated * rb))
                dssd = dgated * act
                dpj[slot, rows, here_of(u * LANES)] = (
                    dgated * o * (gs * (1.0 + gate * (1.0 - gs)))
                ).astype(bf16)
                low = dssd.astype(bf16)
                dacc[0:8, lanes] += sum8(dssd * xf)
                lows = stack_heads(dims, low)
                dmix = lax.dot_general(
                    x, lows, (((1,), (1,)), ((), ())), preferred_element_type=f32
                )
                mix = []
                part = None
                for a in range(HP):
                    k = u * HP + a
                    right = jnp.broadcast_to(turned[:, k : k + 1], (T, T))
                    decay = jnp.exp2(
                        jnp.minimum(rowtab[s, pl.ds(h0 + k, 1), :] - right, mask[...])
                    )
                    mix.append((decay * scores[s]).astype(bf16))
                    term = dmix[:, a * T : (a + 1) * T] * decay
                    part = term if part is None else part + term
                core = jnp.dot(
                    jnp.concatenate(mix, axis=1), lows, preferred_element_type=f32
                )
                sk = pars[8:9, lanes]
                from_cols = xf * core
                diff = low.astype(f32) * (o - sk * xf) - from_cols
                prow, pcol = iotas(LANES, LANES)
                place = (pcol == h0 + u * HP + prow // HD).astype(bf16)
                both = jnp.concatenate([diff, from_cols], axis=0)
                hi = both.astype(bf16)
                lo = (both - hi.astype(f32)).astype(bf16)
                by_head = jnp.dot(
                    jnp.concatenate([hi, lo], axis=1),
                    jnp.concatenate([place, place], axis=0), preferred_element_type=f32,
                )
                conv_back(rows, half + u * LANES, c0, core + sk * dssd, conv, sig,
                          q * TC + u)
                new = (part, by_head)
                parts = new if parts is None else tuple(p + q for p, q in zip(parts, new))
            dscores[s] += parts[0]
            dlog[rows, :] += parts[1][0:T]
            csum[rows, :] += parts[1][T:]

        several(S // 2, SEQ_B, seq)
        send_out()
        several(S // 2, SEQ_B, lambda s, q: seq(S // 2 + s, q))

    @pl.when(i == K - 1)
    def _():
        row, col = iotas(T, T)
        upper = (row <= col).astype(f32)

        def seq(s, _):
            rows = pl.ds(pl.multiple_of(s * T, T), T)
            ds = dscores[s]
            dact = (
                jnp.dot(ds.astype(bf16), bcs[1, rows, :], preferred_element_type=f32),
                jnp.dot(ds.T.astype(bf16), bcs[0, rows, :], preferred_element_type=f32),
            )
            for a in range(2):
                conv = conv_of(dims, proj0[0, rows, a * LANES : (a + 1) * LANES], pars, pad.at[a],
                               DI + a * ST)
                conv_back(rows, a * LANES, DI + a * ST, dact[a], conv, sigmoid(conv), a)
            v, e, step, _, _ = steps_of(
                dims, proj0[0, rows, 2 * LANES : 3 * LANES].astype(f32), hpar
            )
            dsteps = jnp.dot(
                upper, dlog[rows, :], precision=lax.Precision.HIGHEST,
                preferred_element_type=f32,
            )
            sg = jnp.where(v >= 0.0, 1.0, e) / (1.0 + e)
            ratio = jnp.where(step > 1e-30, sg / jnp.maximum(step, 1e-30), 1.0)
            ddt = csum[rows, :] * ratio + dsteps * hpar[1:2, :] * sg
            _, lane = iotas(T, LANES)
            ddt = jnp.where(lane < H, ddt, 0.0)
            dpj[slot, rows, here_of(2 * LANES)] = ddt.astype(bf16)
            dpj[slot, rows, here_of(3 * LANES)] = jnp.zeros((T, LANES), bf16)
            hacc[0:8, :] += sum8(ddt)
            hacc[8:16, :] += sum8(dsteps * step)
            return 0

        lax.fori_loop(0, S, seq, 0)
        small[...] = jnp.zeros_like(small)
        for k in range(KW + 1):
            small[k : k + 1, :] = jnp.sum(cacc[8 * k : 8 * k + 8, :], axis=0, keepdims=True)
        for k in range(2):
            small[KW + 1 + k : KW + 2 + k, 0:DI] = jnp.sum(
                dacc[8 * k : 8 * k + 8, :], axis=0, keepdims=True
            )
            small[KW + 3 : KW + 4, k * LANES : (k + 1) * LANES] = jnp.sum(
                hacc[8 * k : 8 * k + 8, :], axis=0, keepdims=True
            )
        total.start(0, small[...])

    tail = pairs - dpj.shape[0] + i - K
    t = jnp.where(i < K, lax.div(i - 7, 2), tail)
    turn = jnp.where(
        i < K, (i >= 7) & (lax.rem(i, 2) == 1) & (t < pairs - dpj.shape[0]), t >= 0
    )

    @pl.when(turn)
    def _():
        fetch_pair(t, lambda cp: cp.wait())
        mine = lax.rem(t, dpj.shape[0])

        def add(part):
            @pl.when(t == 0)
            def _():
                dn[...] = part()

            @pl.when(t > 0)
            def _():
                dn[...] += part()

        @pl.when(2 * t + 1 < K)
        def _():
            add(lambda: lax.dot_general(
                dpj[mine], wv[...], (((1,), (1,)), ((), ())), preferred_element_type=f32
            ))

        @pl.when(2 * t + 1 >= K)
        def _():
            add(lambda: lax.dot_general(
                dpj[mine, :, 0:w], wv[:, 0:w], (((1,), (1,)), ((), ())),
                preferred_element_type=f32,
            ))

        @pl.when(t + 1 < pairs)
        def _():
            fetch_pair(t + 1, lambda cp: cp.start())

    @pl.when(i >= K - 1)
    def _():
        net.step(2 * i, finish)

    net.step(2 * i + 1, finish)

    @pl.when(i < K)
    def _():
        net.begin(begun(2 * i + 1)[1], uo, dpj[slot, :, pl.ds(pl.multiple_of(off, w), w)])

    for stage in range(1, 4):

        @pl.when(i == K - 1 + stage)
        def _(stage=stage):
            total.start(stage, total.finish(stage - 1))

    @pl.when(i == K + 3)
    def _():
        sums[...] = total.finish(3)

    @pl.when(i == K + 3)
    def _():
        net.drain()


def run_backward_net(dims, axis, geom, E, proj, ssd, ofull, wfull, uT, mT, go, wl, tabs, pars,
                     hpar):
    T, DI, C, H, KW, ST = (dims[k] for k in ("T", "DI", "C", "H", "KW", "ST"))
    A0, A = geom
    N = A0 * A * A
    K, R, w = proj.shape
    r = wl.shape[1]
    D = go.shape[1]
    ro = DI // (2 * N)
    HF = ro // r
    half = w // 2
    S = R // T
    KO = HF * (D // w)
    assert 2 * KO <= K + 1 and HF * r == ro and D % w == 0
    whole = lambda s: pl.BlockSpec(s, lambda i: (0,) * len(s), pipeline_mode=pl.Buffered(1))
    tile = lambda i: jnp.clip(i, 0, K - 2)
    hbm = pl.BlockSpec(memory_space=pl.ANY)
    return pl.pallas_call(
        functools.partial(backward, dims, axis, geom, K, KO, E),
        grid=(K + 4,),
        in_specs=[
            pl.BlockSpec((1, R, w), lambda i: (tile(i) + 1, 0, 0)),
            whole((1, R, w)),
            pl.BlockSpec((R, half), lambda i: (0, tile(i))),
            pl.BlockSpec((half, D), lambda i: (tile(i), 0)),
            hbm, hbm, hbm, whole((R, D)), whole((K, r, w)), whole((2, R, LANES)), whole((16, C)),
            whole((8, LANES)),
        ],
        out_specs=[whole((R, D)), whole((K + KO, r, w)), whole((r, LANES)), whole((8, C))],
        out_shape=[
            jax.ShapeDtypeStruct((R, D), f32),
            jax.ShapeDtypeStruct((K + KO, r, w), f32),
            jax.ShapeDtypeStruct((r, LANES), f32),
            jax.ShapeDtypeStruct((8, C), f32),
        ],
        scratch_shapes=[
            pltpu.VMEM((2, N, r, R), bf16),
            pltpu.VMEM((2, N, r, R), bf16),
            pltpu.VMEM((R, half), f32),
            pltpu.VMEM((4, R, 2 * w), bf16),
            pltpu.VMEM((2 * SEQ_B, FRONT + T, LANES), f32),
            pltpu.VMEM((2 * SEQ_B, FRONT + T, LANES), f32),
            pltpu.VMEM((S, T, LANES), f32),
            pltpu.VMEM((S, LANES, T), f32),
            pltpu.VMEM((S, T, T), f32),
            pltpu.VMEM((S, T, T), f32),
            pltpu.VMEM((R, LANES), f32),
            pltpu.VMEM((R, LANES), f32),
            pltpu.VMEM((2, R, ST), bf16),
            pltpu.VMEM((T, T), f32),
            pltpu.VMEM((8 * (KW + 1), C), f32),
            pltpu.VMEM((16, DI), f32),
            pltpu.VMEM((16, LANES), f32),
            pltpu.VMEM((8, C), f32),
            pltpu.VMEM((D, 2 * w), bf16),
            pltpu.SemaphoreType.DMA((4,)),
            pltpu.SemaphoreType.DMA((2,)),
        ]
        + Reduce.scratch(K + KO, A0, A, r, w)
        + SumAll.scratch(A0, A, (8, C)),
        compiler_params=pltpu.CompilerParams(
            collective_id=2, has_side_effects=True, vmem_limit_bytes=VMEM
        ),
        cost_estimate=pl.CostEstimate(
            flops=6 * R * D * K * w, bytes_accessed=D * K * w * 90, transcendentals=0
        ),
        name="backward",
    )(proj, proj, ssd, ofull.reshape(DI, D), wfull.reshape(K, D, w), uT.reshape(N, 2, r, R),
      mT.reshape(N, 2, HF, r, R), go, wl, tabs, pars, hpar)


def conclude(dims, axis, K, E, dn, tok, go, out, scale, outc, dns, sums, ns, hpar,
             dtok, outs, dw, dow, dtaps, dbias, ddtb, dalog, dskip, dnorm, dgain, tmp):
    T, DI, C, H, HD, KW = (dims[k] for k in ("T", "DI", "C", "H", "HD", "KW"))
    outs[...] = out[...]
    u = tok[...].astype(f32)
    rs = lax.rsqrt(jnp.mean(u * u, axis=-1, keepdims=True) + epsilon)
    u = u * rs
    d = dn[...] * scale[0:1, :]
    m = jnp.mean(d * u, axis=-1, keepdims=True)
    dtok[...] = go[...].astype(f32) + rs * (d - u * m)

    @pl.when(pl.program_id(0) == 0)
    def _():
        me = lax.axis_index(axis)
        r, w = outc.shape[1:]
        half = w // 2
        for g in range(K - 1):
            dw[:, g * half : (g + 1) * half] = outc[g, :, 0:half]
            dw[:, DI + g * half : DI + (g + 1) * half] = outc[g, :, half:]
        dw[:, 2 * DI :] = outc[K - 1, :, 0 : E - 2 * DI]
        cols = dow.shape[1] // w
        for k in range(outc.shape[0] - K):
            h, c = k // cols, k % cols
            dow[h * r : (h + 1) * r, c * w : (c + 1) * w] = outc[K + k]

        def window(size):
            start = me * size
            base = jnp.minimum(lax.div(start, LANES), C // LANES - 2) * LANES
            v = sums[:, pl.ds(pl.multiple_of(base, LANES), 2 * LANES)]
            return pltpu.roll(v, lax.rem(2 * LANES - (start - base), 2 * LANES), 1)

        Cn, Gn = dbias.shape[0], dgain.shape[0]
        v = window(Cn)[:, 0:LANES]
        tmp[...] = jnp.zeros_like(tmp)
        tmp[0:8, :] = v
        dtaps[...] = tmp[...].T[0:Cn, 0:KW]
        dbias[...] = v[KW, 0:Cn]
        dgain[...] = window(Gn)[KW + 2, 0:Gn]
        ddtb[...] = sums[KW + 3, 0:H]
        dalog[...] = sums[KW + 3 : KW + 4, LANES : 2 * LANES][0, 0:H] * hpar[1, 0:H]
        tmp[0:r, :] = dns[...]
        tmp[r:, :] = jnp.zeros((LANES - r, LANES), f32)
        dnorm[...] = jnp.sum(tmp[...].T, axis=0)[0:r] / ns[0, :].astype(f32)
        tiles = DI // LANES
        tmp[...] = jnp.zeros_like(tmp)
        for t in range(tiles):
            tmp[t : t + 1, :] = sums[KW + 1 : KW + 2, t * LANES : (t + 1) * LANES]
        row, col = iotas(LANES, LANES)
        HP = LANES // HD
        fold = (row // HD == lax.rem(col, HP)).astype(f32)
        v = jnp.dot(tmp[...], fold, precision=lax.Precision.HIGHEST, preferred_element_type=f32)
        dskip[...] = jnp.sum(jnp.where(col // HP == row, v, 0.0), axis=0)[0:H]


def run_conclude(dims, axis, K, E, dn, tok, go, out, scale, outc, dns, sums, ns, hpar, ro):
    T, DI, C, H, KW = (dims[k] for k in ("T", "DI", "C", "H", "KW"))
    R, D = tok.shape
    r = outc.shape[1]
    n = D // r
    rows = pl.BlockSpec((T, D), lambda i: (i, 0))
    whole = lambda s: pl.BlockSpec(s, lambda i: (0,) * len(s))
    shapes = [(r, E), (ro, D), (C // n, KW), (C // n,), (H,), (H,), (H,), (r,), (DI // n,)]
    return pl.pallas_call(
        functools.partial(conclude, dims, axis, K, E),
        grid=(R // T,),
        in_specs=[rows, rows, rows, rows]
        + [whole(a.shape) for a in (scale, outc, dns, sums, ns, hpar)],
        out_specs=[rows, rows] + [whole(x) for x in shapes],
        out_shape=[jax.ShapeDtypeStruct((R, D), f32), jax.ShapeDtypeStruct((R, D), bf16)]
        + [jax.ShapeDtypeStruct(x, f32) for x in shapes],
        scratch_shapes=[pltpu.VMEM((LANES, LANES), f32)],
        name="conclude",
    )(dn, tok, go, out, scale, outc, dns, sums, ns, hpar)


def local(axis, n, tokens, in_weight, conv_weight, conv_bias, dt_bias, a_log, skip_d,
          norm_scale, gate_scale, out_weight, grad_out):
    MB, S, T, D = tokens.shape
    R = MB * S * T
    r, E = in_weight.shape
    H = a_log.shape[0]
    DI = out_weight.shape[0] * n
    Cn, KW = conv_weight.shape
    C = Cn * n
    HD = DI // H
    ST = (C - DI) // 2
    dims = dict(T=T, DI=DI, C=C, H=H, HD=HD, ST=ST, KW=KW)
    assert LANES % HD == 0 and ST == LANES and DI % (LANES * 2) == 0 and T % 16 == 0
    geom = geometry(n)
    w = CHUNK
    Gn, ro = DI // n, out_weight.shape[0]
    own = (
        geom is not None and r % 16 == 0 and ro % r == 0 and D % w == 0 and DI % (w // 2) == 0
        and w == 2 * ST + 2 * LANES and E == 2 * DI + 2 * ST + H and H <= LANES
        and max(Cn, Gn) < LANES and 6 <= KW + 2 <= 8 and 2 * (ro // r) * (D // w) <= DI * 2 // w + 2
    )
    me = lax.axis_index(axis)
    tok = tokens.reshape(R, D)
    go = grad_out.reshape(R, D)
    if own:
        row = lambda v: v.reshape(1, -1)
        K = DI * 2 // w + 1
        smalls = [conv_weight.T] + [
            row(v) for v in (conv_bias, gate_scale, norm_scale, dt_bias, a_log)
        ]
        proj, ssd, uT, mT, output, tabs, pars, scale, wl, hpar, wfull, ofull = run_forward_net(
            dims, axis, geom, K, w, skip_d, tok, go, in_weight, smalls, out_weight
        )
        dn, outc, dns, sums = run_backward_net(
            dims, axis, geom, E, proj, ssd, ofull, wfull, uT, mT, go, wl, tabs, pars, hpar
        )
        dtok, output, dw, dow, dtaps, dbias, ddtb, dalog, dskip, dnorm, dgain = run_conclude(
            dims, axis, K, E, dn, tok, go, output, scale, outc, dns, sums, row(norm_scale), hpar,
            ro,
        )
        return (
            output.reshape(tokens.shape), dtok.reshape(tokens.shape), dw, dtaps, dbias, ddtb,
            dalog, dskip, dnorm, dgain, dow,
        )
    rate = -jnp.exp(a_log)
    hpar = jnp.pad(jnp.stack([dt_bias, rate]), ((0, 6), (0, LANES - H)))
    skip = jnp.broadcast_to(jnp.repeat(skip_d, HD)[None], (8, DI))
    ns = norm_scale.astype(f32)
    out_full = lax.all_gather(out_weight, axis, axis=0, tiled=True)
    wfull = lax.all_gather(in_weight, axis, axis=0, tiled=True)
    conv = lax.all_gather(jnp.concatenate([conv_weight.T, conv_bias[None]]), axis, axis=0)
    conv = conv.transpose(1, 0, 2).reshape(KW + 1, C).astype(f32)
    gate = lax.all_gather(gate_scale, axis, axis=0).reshape(1, DI).astype(f32)
    scale = lax.all_gather(norm_scale, axis, axis=0).reshape(1, D).astype(f32)
    u = tok.astype(f32)
    u = u * lax.rsqrt(jnp.mean(u * u, axis=-1, keepdims=True) + epsilon)
    uh = (u * scale).astype(bf16)
    proj = jnp.dot(uh, wfull, preferred_element_type=f32).astype(bf16)
    cpar = jnp.pad(conv, ((0, 8 - KW - 1), (0, 0)))
    dpar = jnp.concatenate([skip[:1], gate, skip[2:]], axis=0)
    mixed, ssd, rstd = run_forward(dims, proj, cpar, hpar, dpar)
    output = jnp.dot(mixed, out_full, preferred_element_type=f32)
    output = (tok.astype(f32) + output).astype(bf16)
    d_mixed = lax.dot_general(
        go, out_full, (((1,), (1,)), ((), ())), preferred_element_type=f32
    )
    dproj, small = run_backward(dims, proj, d_mixed, ssd, rstd, cpar, hpar, dpar)
    left = (((0,), (0,)), ((), ()))
    g_out = lax.dot_general(mixed, go, left, preferred_element_type=f32).astype(bf16)
    dow = lax.psum_scatter(g_out, axis, scatter_dimension=0, tiled=True).astype(f32)
    g_in = lax.dot_general(uh, dproj, left, preferred_element_type=f32).astype(bf16)
    dw = lax.psum_scatter(g_in, axis, scatter_dimension=0, tiled=True).astype(f32)
    dns = dw * in_weight.astype(f32)
    dn = lax.dot_general(dproj, wfull, (((1,), (1,)), ((), ())), preferred_element_type=f32)
    sums = lax.psum(small, axis)
    u = tok.astype(f32)
    rs = lax.rsqrt(jnp.mean(u * u, axis=-1, keepdims=True) + epsilon)
    u, d = u * rs, dn * scale
    dtok = go.astype(f32) + rs * (d - u * jnp.mean(d * u, axis=-1, keepdims=True))
    dconv = lax.dynamic_slice(sums, (0, me * Cn), (KW + 1, Cn))
    heads = sums[KW + 3]
    return (
        output.reshape(tokens.shape),
        dtok.reshape(tokens.shape),
        dw,
        dconv[:KW].T,
        dconv[KW],
        heads[:H],
        heads[LANES : LANES + H] * rate,
        sums[KW + 1, :DI].reshape(H, HD).sum(axis=1),
        dns.sum(axis=1) / ns,
        lax.dynamic_slice(sums[KW + 2], (me * Gn,), (Gn,)),
        dow,
    )


def solution(mesh):
    axis = mesh.axis_names[0]
    n = mesh.shape[axis]
    rows, flat, batch = P(axis, None), P(axis), P(None, axis, None, None)
    return jax.shard_map(
        functools.partial(local, axis, n),
        mesh=mesh,
        in_specs=(batch, rows, rows, flat, P(), P(), P(), flat, flat, rows, batch),
        out_specs=(batch, batch, rows, rows, flat, P(), P(), P(), flat, flat, rows),
        check_vma=False,
    )
```

```python
import functools
import math

import jax
import jax.numpy as jnp
from jax import lax
from jax.experimental import pallas as pl
from jax.experimental.pallas import tpu as pltpu
from jax.sharding import PartitionSpec as P

epsilon = 1e-05
LOG2E = 1.4426950408889634
BIG = 3.0e38
LANES = 128
FRONT = 8
f32 = jnp.float32
bf16 = jnp.bfloat16
UNROLL_F = 2
UNROLL_B = 2


def sigmoid(v):
    return 0.5 * jnp.tanh(0.5 * v) + 0.5


def sum8(v):
    rows, lanes = v.shape
    return jnp.sum(v.reshape(rows // 8, 8, lanes), axis=0)


def iotas(rows, lanes):
    return (
        lax.broadcasted_iota(jnp.int32, (rows, lanes), 0),
        lax.broadcasted_iota(jnp.int32, (rows, lanes), 1),
    )


def step_stage(dims, proj, hpar, dtp):
    DI, C, H = dims["DI"], dims["C"], dims["H"]
    dtp[...] = jnp.zeros_like(dtp)
    dtp[:, 0:H] = proj[:, DI + C : DI + C + H].astype(f32)
    return steps_of(dims, dtp[...], hpar)


def steps_of(dims, dt, hpar):
    T, H = dims["T"], dims["H"]
    _, lane = iotas(T, LANES)
    v = jnp.where(lane < H, dt + hpar[0:1, :], 0.0)
    e = jnp.exp(-jnp.abs(v))
    step = jnp.maximum(v, 0.0) + jnp.log1p(e)
    row, col = iotas(T, T)
    tri = (row >= col).astype(f32)
    ld = jnp.dot(
        tri, step * (hpar[1:2, :] * LOG2E), precision=lax.Precision.HIGHEST,
        preferred_element_type=f32,
    )
    return v, e, step, ld, ld - jnp.log2(step)


def conv_of(dims, cin, cpar, pad, c0):
    T, KW = dims["T"], dims["KW"]
    lanes = pl.ds(c0, LANES)
    cin = cin.astype(f32)
    pad[FRONT : FRONT + T, :] = cin
    out = cpar[KW : KW + 1, lanes] + cin * cpar[KW - 1 : KW, lanes]
    for k in range(KW - 1):
        out = out + pad[FRONT - KW + 1 + k : FRONT - KW + 1 + k + T, :] * cpar[k : k + 1, lanes]
    return out


def conv_tile(dims, proj, cpar, pad, c0):
    return conv_of(dims, proj[:, pl.ds(dims["DI"] + c0, LANES)], cpar, pad, c0)


def stack_heads(dims, v):
    T, HD = dims["T"], dims["HD"]
    _, lane = iotas(T, LANES)
    zero = jnp.zeros_like(v)
    return jnp.concatenate(
        [jnp.where(lane // HD == a, v, zero) for a in range(LANES // HD)], axis=0
    )


MESH = pl.DeviceIdType.MESH
CHUNK = 512
VMEM = 67043328
ROWS = 1024
SEQ_F = 2
BLOCK = 256
SEQ_B = 2


def geometry(n):
    chips = n // 2
    A0 = 4 if chips % 4 == 0 else 1
    A = math.isqrt(chips // A0)
    return (A0, A) if n % 2 == 0 and A > 1 and A0 * A * A == chips else None


class Place:
    def __init__(self, axis, A0, A):
        me = lax.axis_index(axis)
        self.A0, self.A = A0, A
        self.c = lax.rem(me, 2)
        chip = lax.div(me, 2)
        self.a2 = lax.rem(chip, A)
        self.a1 = lax.rem(lax.div(chip, A), A)
        self.a0 = lax.div(chip, A * A)
        c = self.c
        self.f = self.a1 + c * (self.a2 - self.a1)
        self.s = self.a2 + c * (self.a1 - self.a2)
        self.sf = A + c * (1 - A)
        self.ss = 1 + c * (A - 1)

    def pos(self, f, s):
        return f * self.sf + s * self.ss

    def device(self, a0, f, s, c):
        return ((a0 * self.A * self.A + self.pos(f, s)) * 2 + c,)

    def line(self, q):
        return lax.rem(self.a0 + q + self.A0, self.A0)

    def first(self, q):
        return lax.rem(self.f + q + self.A, self.A)

    def second(self, q):
        return lax.rem(self.s + q + self.A, self.A)

    def partner(self):
        return self.device(self.a0, self.f, self.s, 1 - self.c)

    def peers(self):
        out = [self.partner()]
        out += [self.device(self.line(q), self.f, self.s, self.c) for q in range(1, self.A0)]
        out += [self.device(self.a0, self.first(q), self.s, self.c) for q in range(1, self.A)]
        out += [self.device(self.a0, self.f, self.second(q), self.c) for q in range(1, self.A)]
        return out

    def greet(self):
        for peer in self.peers():
            pl.semaphore_signal(
                pltpu.get_barrier_semaphore(), inc=1, device_id=peer, device_id_type=MESH
            )

    def meet(self):
        pl.semaphore_wait(pltpu.get_barrier_semaphore(), len(self.peers()))


def columns(j, w):
    return pl.ds(pl.multiple_of(j * w, w), w)


def send(src, dst, ssem, rsem, device):
    return pltpu.make_async_remote_copy(
        src_ref=src, dst_ref=dst, send_sem=ssem, recv_sem=rsem,
        device_id=device, device_id_type=MESH,
    )


class Gather:
    AFTER = (0, 3, 6, 9, 12)
    DEEP = 5
    ORDER = (0, 4, 3, 2, 1)
    TURN = 0

    def __init__(self, at, K, mine, whole, ssem, rsem, lsem):
        self.at, self.K, self.mine, self.whole = at, K, mine, whole
        self.ssem, self.rsem, self.lsem = ssem, rsem, lsem

    @staticmethod
    def scratch(K, A0, A):
        NS = (A0 - 1) * A + (A - 1) + (A - 1) * A + 1
        return [
            pltpu.SemaphoreType.DMA((Gather.DEEP, NS)),
            pltpu.SemaphoreType.DMA((K, NS)),
            pltpu.SemaphoreType.DMA((Gather.DEEP,)),
        ]

    def local(self, j):
        at = self.at
        return pltpu.make_async_copy(
            self.mine(j), self.whole(j, at.a0, at.pos(at.f, at.s), at.c),
            self.lsem.at[lax.rem(j, self.DEEP)],
        )

    def copies(self, stage, j, sending, late):
        at, whole = self.at, self.whole
        A0, A = at.A0, at.A
        par = lax.rem(j, self.DEEP)
        line0, first0 = 0, (A0 - 1) * A
        second0 = first0 + A - 1
        every = slice(None)
        out = []

        def add(k, src, dst, device):
            out.append(send(src, dst, self.ssem.at[par, k], self.rsem.at[j, k], device))

        if stage == 0 and not late:
            for q in range(1, A0):
                a = at.a0 if sending else at.line(-q)
                add(line0 + q - 1, self.mine(j), whole(j, a, at.pos(at.f, at.s), at.c),
                    at.device(at.line(q), at.f, at.s, at.c))
        elif stage == 1 and late:
            for q in range(1, A0):
                a = at.a0 if sending else at.line(-q)
                for o in range(A):
                    ref = whole(j, a, at.pos(o, at.s), at.c)
                    add(line0 + (q - 1) * A + o, ref, ref,
                        at.device(at.line(q), at.f, at.s, at.c))
        elif stage < 2:
            for q in range(1, A):
                f = at.f if sending else at.first(-q)
                ref = whole(j, at.a0 if late else every, at.pos(f, at.s), at.c)
                add(first0 + q - 1, self.mine(j) if late else ref, ref,
                    at.device(at.a0, at.first(q), at.s, at.c))
        elif stage == 2:
            for q in range(1, A):
                s = at.s if sending else at.second(-q)
                for o in range(A):
                    ref = whole(j, every, at.pos(o, s), at.c)
                    add(second0 + (q - 1) * A + o, ref, ref,
                        at.device(at.a0, at.f, at.second(q), at.c))
        else:
            ref = whole(j, every, every, at.c if sending else 1 - at.c)
            add(second0 + (A - 1) * A, ref, ref, at.partner())
        return out

    def each(self, stage, j, sending, act):
        def run(late):
            for cp in self.copies(stage, j, sending, late):
                act(cp)

        if stage >= 2:
            run(False)
            return
        late = lax.rem(j, 3) == self.TURN
        pl.when(late)(lambda: run(True))
        pl.when(jnp.logical_not(late))(lambda: run(False))

    def step(self, i):
        for stage in self.ORDER:
            j = i - self.AFTER[stage]

            @pl.when((j >= 0) & (j < self.K))
            def _(stage=stage, j=j):
                if stage > 0:
                    self.each(stage - 1, j, False, lambda cp: cp.wait_recv())
                if stage < 4:

                    @pl.when(j >= self.DEEP)
                    def _():
                        self.each(stage, j - self.DEEP, True, lambda cp: cp.wait_send())

                    if stage == 1:
                        self.local(j).wait()
                    self.each(stage, j, True, lambda cp: cp.start())
                    if stage == 0:
                        self.local(j).start()

    def drain(self):
        for j in range(max(0, self.K - self.DEEP), self.K):
            for stage in range(4):
                for cp in self.copies(stage, jnp.int32(j), True, j % 3 == self.TURN):
                    cp.wait_send()


class Reduce:
    SLOTS = 3
    LAG = 2

    def __init__(self, at, K, begun, refs):
        self.at, self.K, self.begun = at, K, begun
        (self.own0, self.own1, self.own2, self.own3, self.s0, self.s1, self.s2, self.s3,
         self.r0, self.r1, self.r2, self.r3, self.ssem, self.rsem, self.credit) = refs

    @staticmethod
    def scratch(K, A0, A, r, w):
        N = A0 * A * A
        NS = 1 + (A - 1) + (A - 1) + (A0 - 1)
        L = Reduce.SLOTS
        return [
            pltpu.VMEM((2, N, r, w), f32),
            pltpu.VMEM((2, A0 * A, r, w), f32),
            pltpu.VMEM((2, A0, r, w), f32),
            pltpu.VMEM((2, r, w), f32),
            pltpu.VMEM((2, N, r, w), bf16),
            pltpu.VMEM((2, A - 1, A0 * A, r, w), bf16),
            pltpu.VMEM((2, A - 1, A0, r, w), bf16),
            pltpu.VMEM((2, A0 - 1, r, w), bf16),
            pltpu.VMEM((L, N, r, w), bf16),
            pltpu.VMEM((L, A - 1, A0 * A, r, w), bf16),
            pltpu.VMEM((L, A - 1, A0, r, w), bf16),
            pltpu.VMEM((L, A0 - 1, r, w), bf16),
            pltpu.SemaphoreType.DMA((2, NS)),
            pltpu.SemaphoreType.DMA((L, NS)),
            pltpu.SemaphoreType.REGULAR((NS,)),
        ]

    def routes(self, stage):
        at = self.at
        A0, A = at.A0, at.A
        if stage == 0:
            return [(0, at.partner(), at.partner())]
        if stage == 1:
            to = lambda q: at.device(at.a0, at.f, at.second(q), at.c)
            return [(q, to(q), to(-q)) for q in range(1, A)]
        if stage == 2:
            to = lambda q: at.device(at.a0, at.first(q), at.s, at.c)
            return [(A - 1 + q, to(q), to(-q)) for q in range(1, A)]
        to = lambda q: at.device(at.line(q), at.f, at.s, at.c)
        return [(2 * (A - 1) + q, to(q), to(-q)) for q in range(1, A0)]

    def copies(self, stage, j):
        par, slot = lax.rem(j, 2), lax.rem(j, self.SLOTS)
        src, dst = ((self.s0, self.r0), (self.s1, self.r1), (self.s2, self.r2),
                    (self.s3, self.r3))[stage]
        out = []
        for q, (k, to, _) in enumerate(self.routes(stage)):
            a = src.at[par] if stage == 0 else src.at[par, q]
            b = dst.at[slot] if stage == 0 else dst.at[slot, q]
            out.append(send(a, b, self.ssem.at[par, k], self.rsem.at[slot, k], to))
        return out

    def free(self, stage, j):
        @pl.when(j >= 2)
        def _():
            for cp in self.copies(stage, j - 2):
                cp.wait_send()

    def start(self, stage, j):
        @pl.when(j >= self.SLOTS)
        def _():
            for k, _, _ in self.routes(stage):
                pl.semaphore_wait(self.credit.at[k], 1)

        for cp in self.copies(stage, j):
            cp.start()

    def arrive(self, stage, j):
        for cp in self.copies(stage, j):
            cp.wait_recv()

    def done(self, stage, j):
        @pl.when(j + self.SLOTS < self.K)
        def _():
            for k, _, source in self.routes(stage):
                pl.semaphore_signal(
                    self.credit.at[k], inc=1, device_id=source, device_id_type=MESH
                )

    def begin(self, j, own, right):
        N, r, w = self.own0.shape[1:]
        par = lax.rem(j, 2)
        rows = lambda k: own[k].reshape(N * r, own.shape[3])
        self.free(0, j)
        self.s0[par] = (
            jnp.dot(rows(1), right, preferred_element_type=f32).astype(bf16).reshape(N, r, w)
        )
        self.start(0, j)
        self.own0[par] = jnp.dot(rows(0), right, preferred_element_type=f32).reshape(N, r, w)

    def step(self, i, finish):
        at = self.at
        A0, A = at.A0, at.A

        def stage1(j, par, slot):
            def line(a, _):
                for o in range(A):
                    for q in range(A):
                        b = a * A * A + at.pos(o, at.second(q))
                        v = self.own0[par, b] + self.r0[slot, b].astype(f32)
                        if q == 0:
                            self.own1[par, a * A + o] = v
                        else:
                            self.s1[par, q - 1, a * A + o] = v.astype(bf16)
                return 0

            lax.fori_loop(0, A0, line, 0)

        def stage2(j, par, slot):
            def line(a, _):
                for q in range(A):
                    b = a * A + at.first(q)
                    v = self.own1[par, b]
                    for p in range(A - 1):
                        v = v + self.r1[slot, p, b].astype(f32)
                    if q == 0:
                        self.own2[par, a] = v
                    else:
                        self.s2[par, q - 1, a] = v.astype(bf16)
                return 0

            lax.fori_loop(0, A0, line, 0)

        def stage3(j, par, slot):
            for q in range(A0):
                a = at.line(q)
                v = self.own2[par, a]
                for p in range(A - 1):
                    v = v + self.r2[slot, p, a].astype(f32)
                if q == 0:
                    self.own3[par] = v
                else:
                    self.s3[par, q - 1] = v.astype(bf16)

        def stage4(j, par, slot):
            v = self.own3[par]
            for p in range(A0 - 1):
                v = v + self.r3[slot, p].astype(f32)
            finish(j, v)

        for k, stage in ((4, stage4), (3, stage3), (2, stage2), (1, stage1)):
            valid, j = self.begun(i - k * self.LAG)

            @pl.when(valid)
            def _(j=j, k=k, stage=stage):
                self.arrive(k - 1, j)
                if k < 4:
                    self.free(k, j)
                stage(j, lax.rem(j, 2), lax.rem(j, self.SLOTS))
                self.done(k - 1, j)
                if k < 4:
                    self.start(k, j)

    def drain(self):
        for j in range(max(0, self.K - 2), self.K):
            for stage in range(4):
                for cp in self.copies(stage, jnp.int32(j)):
                    cp.wait_send()


class SumAll:
    def __init__(self, at, refs):
        self.at = at
        self.hold, self.land, self.ssem, self.rsem = refs

    @staticmethod
    def scratch(A0, A, shape):
        slots = 2 + A + A + A0
        return [
            pltpu.VMEM((4,) + shape, f32),
            pltpu.VMEM((slots,) + shape, f32),
            pltpu.SemaphoreType.DMA((slots,)),
            pltpu.SemaphoreType.DMA((slots,)),
        ]

    def group(self, stage):
        at = self.at
        A0, A = at.A0, at.A
        chip = at.a0 * A * A + at.a1 * A + at.a2
        if stage == 0:
            return 0, 2, at.c, 1, chip * 2
        if stage == 1:
            return 2, A, at.a2, 2, (chip - at.a2) * 2 + at.c
        if stage == 2:
            return 2 + A, A, at.a1, 2 * A, (chip - at.a1 * A) * 2 + at.c
        return 2 + 2 * A, A0, at.a0, 2 * A * A, (chip - at.a0 * A * A) * 2 + at.c

    def copies(self, stage, sending):
        base, size, mine, stride, origin = self.group(stage)
        out = []
        for q in range(1, size):
            to = lax.rem(mine + q, size)
            slot = mine if sending else lax.rem(mine - q + size, size)
            out.append(
                send(self.hold.at[stage], self.land.at[base + slot], self.ssem.at[base + q],
                     self.rsem.at[base + q], (origin + to * stride,))
            )
        return out

    def start(self, stage, value):
        base, _, mine, _, _ = self.group(stage)
        self.hold[stage] = value
        self.land[base + mine] = value
        for cp in self.copies(stage, True):
            cp.start()

    def finish(self, stage):
        base, size, _, _, _ = self.group(stage)
        for cp in self.copies(stage, False):
            cp.wait_recv()
        for cp in self.copies(stage, True):
            cp.wait_send()
        total = self.land[base]
        for k in range(1, size):
            total = total + self.land[base + k]
        return total


def mix_forward(dims, proj, cpar, hpar, dpar, mixed, ssd, rstd,
                pad, gated, colb, rowb, mask, scores, acc, dtp):
    T, DI, H, HD, ST = dims["T"], dims["DI"], dims["H"], dims["HD"], dims["ST"]
    HP = LANES // HD
    tiles = DI // LANES
    pad[:, 0:FRONT, :] = jnp.zeros((pad.shape[0], FRONT, LANES), f32)
    _, _, _, ld, ld2 = step_stage(dims, proj, hpar, dtp)
    row, col = iotas(T, T)
    mask[...] = jnp.where(col <= row, BIG, -BIG)
    rowb[...] = ld2.T
    for h in range(H):
        colb[h] = jnp.broadcast_to(ld[:, h : h + 1], (T, LANES))
    bc = []
    for a in range(2):
        conv = conv_tile(dims, proj, cpar, pad.at[a], DI + a * ST)
        bc.append((conv * sigmoid(conv)).astype(bf16))
    scores[...] = lax.dot_general(
        bc[1], bc[0], (((1,), (1,)), ((), ())), preferred_element_type=f32
    )
    acc[...] = jnp.zeros_like(acc)

    def tile(j, u):
        c0 = pl.multiple_of(j * LANES, LANES)
        lanes = pl.ds(c0, LANES)
        conv = conv_tile(dims, proj, cpar, pad.at[u], c0)
        x = (conv * sigmoid(conv)).astype(bf16)
        mix = []
        for a in range(HP):
            h = j * HP + a
            expo = jnp.minimum(colb[h] - rowb[pl.ds(h, 1), :], mask[...])
            mix.append((jnp.exp2(expo) * scores[...]).astype(bf16))
        core = jnp.dot(
            jnp.concatenate(mix, axis=1), stack_heads(dims, x), preferred_element_type=f32
        )
        out = core + dpar[0:1, lanes] * x.astype(f32)
        ssd[:, lanes] = out
        gate = proj[:, lanes].astype(f32)
        g = out * (gate * sigmoid(gate))
        gated[:, lanes] = g
        return g * g

    def body(j, _):
        total = tile(j * UNROLL_F, 0)
        for u in range(1, UNROLL_F):
            total = total + tile(j * UNROLL_F + u, u)
        acc[...] += total
        return 0

    lax.fori_loop(0, tiles // UNROLL_F, body, 0)
    r = lax.rsqrt(jnp.sum(acc[...], axis=1, keepdims=True) * (1.0 / DI) + epsilon)
    rb = jnp.broadcast_to(r, (T, LANES))
    rstd[...] = rb

    def finish(j, _):
        lanes = pl.ds(pl.multiple_of(j * LANES, LANES), LANES)
        mixed[:, lanes] = (gated[:, lanes] * rb * dpar[1:2, lanes]).astype(bf16)
        return 0

    lax.fori_loop(0, tiles, finish, 0)


def mix_backward(dims, steps, proj, dmixed, ssd, rstd, cpar, hpar, dpar, dproj, small,
                 cacc, dacc, hacc, pad, dpad, colb, rowb, mask, scores, acc, dtp, dscores, dlog,
                 csum, bcs):
    T, DI, C, H, HD, ST, KW = (dims[k] for k in ("T", "DI", "C", "H", "HD", "ST", "KW"))
    HP = LANES // HD
    tiles = DI // LANES

    @pl.when(pl.program_id(0) == 0)
    def _():
        cacc[...] = jnp.zeros_like(cacc)
        dacc[...] = jnp.zeros_like(dacc)
        hacc[...] = jnp.zeros_like(hacc)

    pad[:, 0:FRONT, :] = jnp.zeros((pad.shape[0], FRONT, LANES), f32)
    dpad[:, T:, :] = jnp.zeros((dpad.shape[0], FRONT, LANES), f32)
    v, e, step, ld, ld2 = step_stage(dims, proj, hpar, dtp)
    row, col = iotas(T, T)
    mask[...] = jnp.where(row <= col, BIG, -BIG)
    rowb[...] = ld.T
    for h in range(H):
        colb[h] = jnp.broadcast_to(ld2[:, h : h + 1], (T, LANES))
    for a in range(2):
        conv = conv_tile(dims, proj, cpar, pad.at[a], DI + a * ST)
        bcs[a] = (conv * sigmoid(conv)).astype(bf16)
    scores[...] = lax.dot_general(
        bcs[0], bcs[1], (((1,), (1,)), ((), ())), preferred_element_type=f32
    )
    acc[...] = jnp.zeros_like(acc)
    dscores[...] = jnp.zeros_like(dscores)
    dlog[...] = jnp.zeros_like(dlog)
    csum[...] = jnp.zeros_like(csum)
    rb = rstd[...]

    def first(j, _):
        lanes = pl.ds(pl.multiple_of(j * LANES, LANES), LANES)
        gate = proj[:, lanes].astype(f32)
        p = dmixed[:, lanes] * (ssd[:, lanes] * (gate * sigmoid(gate)))
        acc[...] += p * dpar[1:2, lanes]
        dacc[8:16, lanes] += sum8(p * rb)
        return 0

    lax.fori_loop(0, tiles, first, 0)
    mean = jnp.sum(acc[...], axis=1, keepdims=True) * (1.0 / DI)
    mb = jnp.broadcast_to(mean, (T, LANES)) * rb * rb * rb
    acc[...] = mb

    def conv_back(c0, dact, conv, sig, u):
        lanes = pl.ds(c0, LANES)
        dconv = dact * (sig * (1.0 + conv * (1.0 - sig)))
        dpad[u, 0:T, :] = dconv
        dcin = dconv * cpar[KW - 1 : KW, lanes]
        for k in range(KW - 1):
            dcin = dcin + dpad[u, KW - 1 - k : KW - 1 - k + T, :] * cpar[k : k + 1, lanes]
        dproj[:, pl.ds(DI + c0, LANES)] = dcin.astype(bf16)
        for k in range(KW):
            start = FRONT - KW + 1 + k
            cacc[8 * k : 8 * k + 8, lanes] += sum8(dconv * pad[u, start : start + T, :])
        cacc[8 * KW : 8 * KW + 8, lanes] += sum8(dconv)

    def tile(j, u):
        c0 = pl.multiple_of(j * LANES, LANES)
        lanes = pl.ds(c0, LANES)
        conv = conv_tile(dims, proj, cpar, pad.at[u], c0)
        sig = sigmoid(conv)
        x = (conv * sig).astype(bf16)
        xf = x.astype(f32)
        gate = proj[:, lanes].astype(f32)
        gs = sigmoid(gate)
        act = gate * gs
        out = ssd[:, lanes]
        r = rstd[...]
        dgated = r * (dmixed[:, lanes] * dpar[1:2, lanes]) - (out * act) * acc[...]
        dssd = dgated * act
        dproj[:, lanes] = (dgated * out * (gs * (1.0 + gate * (1.0 - gs)))).astype(bf16)
        low = dssd.astype(bf16)
        dacc[0:8, lanes] += sum8(dssd * xf)
        lows = stack_heads(dims, low)
        dmix = lax.dot_general(
            x, lows, (((1,), (1,)), ((), ())), preferred_element_type=f32
        )
        mix = []
        part = None
        for a in range(HP):
            h = j * HP + a
            decay = jnp.exp2(jnp.minimum(rowb[pl.ds(h, 1), :] - colb[h], mask[...]))
            mix.append((decay * scores[...]).astype(bf16))
            term = dmix[:, a * T : (a + 1) * T] * decay
            part = term if part is None else part + term
        core = jnp.dot(jnp.concatenate(mix, axis=1), lows, preferred_element_type=f32)
        skip = dpar[0:1, lanes]
        from_cols = xf * core
        diff = low.astype(f32) * (out - skip * xf) - from_cols
        prow, pcol = iotas(LANES, LANES)
        place = (pcol == j * HP + prow // HD).astype(bf16)
        place = jnp.concatenate([place, place], axis=0)

        def by_head(w):
            hi = w.astype(bf16)
            lo = (w - hi.astype(f32)).astype(bf16)
            return jnp.dot(
                jnp.concatenate([hi, lo], axis=1), place, preferred_element_type=f32
            )

        conv_back(c0, core + skip * dssd, conv, sig, u)
        return part, by_head(diff), by_head(from_cols)

    def body(j, _):
        sums = tile(j * UNROLL_B, 0)
        for u in range(1, UNROLL_B):
            sums = tuple(p + q for p, q in zip(sums, tile(j * UNROLL_B + u, u)))
        dscores[...] += sums[0]
        dlog[...] += sums[1]
        csum[...] += sums[2]
        return 0

    lax.fori_loop(0, tiles // UNROLL_B, body, 0)
    ds = dscores[...].astype(bf16)
    dst = dscores[...].T.astype(bf16)
    dact = (
        jnp.dot(ds, bcs[1], preferred_element_type=f32),
        jnp.dot(dst, bcs[0], preferred_element_type=f32),
    )
    for a in range(2):
        conv = conv_tile(dims, proj, cpar, pad.at[a], DI + a * ST)
        conv_back(DI + a * ST, dact[a], conv, sigmoid(conv), a)
    dsteps = jnp.dot(
        (row <= col).astype(f32), dlog[...], precision=lax.Precision.HIGHEST,
        preferred_element_type=f32,
    )
    sg = jnp.where(v >= 0.0, 1.0, e) / (1.0 + e)
    ratio = jnp.where(step > 1e-30, sg / jnp.maximum(step, 1e-30), 1.0)
    ddt = csum[...] * ratio + dsteps * hpar[1:2, :] * sg
    tail = dproj.shape[1] - DI - C
    if tail > H:
        dproj[:, DI + C :] = jnp.concatenate(
            [ddt[:, 0:H].astype(bf16), jnp.zeros((T, tail - H), bf16)], axis=1
        )
    else:
        dproj[:, DI + C :] = ddt[:, 0:H].astype(bf16)
    hacc[0:8, :] += sum8(ddt)
    hacc[8:16, :] += sum8(dsteps * step)

    @pl.when(pl.program_id(0) == steps - 1)
    def _():
        small[...] = jnp.zeros_like(small)
        for k in range(KW + 1):
            small[k : k + 1, :] = jnp.sum(cacc[8 * k : 8 * k + 8, :], axis=0, keepdims=True)
        for k in range(2):
            small[KW + 1 + k : KW + 2 + k, 0:DI] = jnp.sum(
                dacc[8 * k : 8 * k + 8, :], axis=0, keepdims=True
            )
            small[KW + 3 : KW + 4, k * LANES : (k + 1) * LANES] = jnp.sum(
                hacc[8 * k : 8 * k + 8, :], axis=0, keepdims=True
            )


def run_forward(dims, proj, cpar, hpar, dpar):
    T, DI, C, H, KW = dims["T"], dims["DI"], dims["C"], dims["H"], dims["KW"]
    R, E = proj.shape
    rows = lambda w: pl.BlockSpec((T, w), lambda i: (i, 0))
    whole = lambda a: pl.BlockSpec(a.shape, lambda i: (0, 0))
    return pl.pallas_call(
        functools.partial(mix_forward, dims),
        grid=(R // T,),
        in_specs=[rows(E), whole(cpar), whole(hpar), whole(dpar)],
        out_specs=[rows(DI), rows(DI), rows(LANES)],
        out_shape=[
            jax.ShapeDtypeStruct((R, DI), bf16),
            jax.ShapeDtypeStruct((R, DI), f32),
            jax.ShapeDtypeStruct((R, LANES), f32),
        ],
        scratch_shapes=[
            pltpu.VMEM((max(2, UNROLL_F), FRONT + T, LANES), f32),
            pltpu.VMEM((T, DI), f32),
            pltpu.VMEM((H, T, LANES), f32),
            pltpu.VMEM((LANES, T), f32),
            pltpu.VMEM((T, T), f32),
            pltpu.VMEM((T, T), f32),
            pltpu.VMEM((T, LANES), f32),
            pltpu.VMEM((T, LANES), f32),
        ],
        compiler_params=pltpu.CompilerParams(vmem_limit_bytes=48 << 20),
        name="mix_forward",
    )(proj, cpar, hpar, dpar)


def run_backward(dims, proj, dmixed, ssd, rstd, cpar, hpar, dpar):
    T, DI, C, H, KW, ST = (dims[k] for k in ("T", "DI", "C", "H", "KW", "ST"))
    R, E = proj.shape
    rows = lambda w: pl.BlockSpec((T, w), lambda i: (i, 0))
    whole = lambda s: pl.BlockSpec(s, lambda i: (0, 0))
    sums = [(8 * (KW + 1), C), (16, DI), (16, LANES)]
    return pl.pallas_call(
        functools.partial(mix_backward, dims, R // T),
        grid=(R // T,),
        in_specs=[rows(E), rows(DI), rows(DI), rows(LANES)]
        + [whole(a.shape) for a in (cpar, hpar, dpar)],
        out_specs=[rows(E), whole((8, C))],
        out_shape=[jax.ShapeDtypeStruct((R, E), bf16), jax.ShapeDtypeStruct((8, C), f32)],
        scratch_shapes=[pltpu.VMEM(s, f32) for s in sums]
        + [
            pltpu.VMEM((max(2, UNROLL_B), FRONT + T, LANES), f32),
            pltpu.VMEM((max(2, UNROLL_B), FRONT + T, LANES), f32),
            pltpu.VMEM((H, T, LANES), f32),
            pltpu.VMEM((LANES, T), f32),
            pltpu.VMEM((T, T), f32),
            pltpu.VMEM((T, T), f32),
            pltpu.VMEM((T, LANES), f32),
            pltpu.VMEM((T, LANES), f32),
            pltpu.VMEM((T, T), f32),
            pltpu.VMEM((T, LANES), f32),
            pltpu.VMEM((T, LANES), f32),
            pltpu.VMEM((2, T, ST), bf16),
        ],
        compiler_params=pltpu.CompilerParams(vmem_limit_bytes=56 << 20),
        name="mix_backward",
    )(proj, dmixed, ssd, rstd, cpar, hpar, dpar)


def several(count, width, body):
    width = math.gcd(width, count)

    def trip(m, _):
        for q in range(width):
            body(m * width + q, q)
        return 0

    lax.fori_loop(0, count // width, trip, 0)


def assemble(parts, size, tiles):
    _, lane = iotas(8, LANES)
    out = []
    for t in range(tiles):
        total = None
        for d in range(t * LANES // size, min(len(parts), -(-(t + 1) * LANES // size))):
            shift = d * size - t * LANES
            v = parts[d] if shift % LANES == 0 else pltpu.roll(parts[d], shift % LANES, 1)
            keep = (lane >= max(shift, 0)) & (lane < min(shift + size, LANES))
            v = jnp.where(keep, v, 0.0)
            total = v if total is None else total + v
        out.append(total)
    return out


def forward(dims, axis, geom, K, KO, skip, tok, inw, taps, bias, gains, ns, dtb, alog, ow,
            tokc, goc, proj, ssd, uT, mT, out, tabs, pars, scale, wl, hpar, wfull, ofull,
            uh, wv, wo, pj, gated, mixed, pad, ldtab, rowtab, scores, mask, acc, dtp, wsem, osem,
            *sems):
    T, DI, C, H, HD, ST, KW = (dims[k] for k in ("T", "DI", "C", "H", "HD", "ST", "KW"))
    A0, A = geom
    at = Place(axis, A0, A)
    i = pl.program_id(0)
    R, D = tok.shape
    w = wl.shape[2]
    half = w // 2
    S = R // T
    HP = LANES // HD
    TC = half // LANES
    wo_cols = wo.shape[5]
    place = lambda j: lax.rem(j + K - 1, K)
    part = lambda j: columns(lax.rem(j, 2), half)
    net = Gather(
        at, 2 * K, lambda j: wl.at[lax.div(j, 2), :, part(j)],
        lambda j, a, p, c: wfull.at[place(lax.div(j, 2)), a, p, c, :, part(j)], *sems[:3],
    )
    neto = Gather(
        at, 2 * KO, lambda j: ow.at[:, columns(j, wo_cols // 2)],
        lambda j, a, p, c: ofull.at[a, p, c, :, columns(j, wo_cols // 2)], *sems[3:],
    )

    @pl.when(i == 0)
    def _():
        at.greet()
        r, E = inw.shape
        Cn, Gn = bias.shape[1], gains.shape[1]
        zero = jnp.zeros((LANES, LANES), f32)
        dtp[...] = zero
        dtp[0:1, 0:r] = ns[...].astype(f32)
        column = pltpu.roll(dtp[...].T, LANES - 1, 1)
        dtp[...] = column
        dtp[0:KW, 0:Cn] = taps[...].astype(f32)
        dtp[KW : KW + 1, 0:Cn] = bias[...].astype(f32)
        dtp[KW + 1 : KW + 2, 0:Gn] = gains[...].astype(f32)
        wl[0, :, 0 : half] = inw[:, 2 * DI : 2 * DI + half]
        wl[0, :, half : half + LANES] = jnp.concatenate(
            [inw[:, 2 * DI + half : E], jnp.zeros((r, LANES - H), bf16)], axis=1
        )
        wl[0, :, half + LANES :] = dtp[0:r, :].astype(bf16)
        for j in range(1, K):
            wl[j, :, 0:half] = inw[:, (j - 1) * half : j * half]
            wl[j, :, half:] = inw[:, DI + (j - 1) * half : DI + j * half]
        hpar[...] = jnp.zeros_like(hpar)
        hpar[0:1, 0:H] = dtb[...]
        hpar[1:2, 0:H] = -jnp.exp(alog[...])
        at.meet()

    def travel(q):
        net.step(q)
        neto.step(q - 2 * K)

    trip = 2 * i
    i = i - ((Gather.AFTER[4] + 2) // 2 - 4)
    travel(trip)

    def fetch_w(j):
        slot = lax.rem(j, 2)
        return pltpu.make_async_copy(wfull.at[place(j)], wv.at[slot], wsem.at[slot])

    def fetch_o(k):
        slot = lax.rem(k, 2)
        return pltpu.make_async_copy(
            ofull.at[:, :, :, :, columns(k, wo_cols)], wo.at[slot], osem.at[slot]
        )

    ready = (i >= 4) & (i < K + 4)
    chunk = jnp.maximum(i - 4, 0)

    @pl.when(ready)
    def _():
        fetch_w(chunk).start()

    @pl.when((i >= K + 4) & (i < K + KO + 4))
    def _():
        fetch_o(i - K - 4).start()

    @pl.when(i == 5)
    def _():
        row, col = iotas(T, T)
        mask[...] = jnp.where(col <= row, BIG, -BIG)
        pad[:, 0:FRONT, :] = jnp.zeros((pad.shape[0], FRONT, LANES), f32)
        acc[...] = jnp.zeros_like(acc)

        def seq(s, _):
            rows = pl.ds(pl.multiple_of(s * T, T), T)
            bc = []
            for a in range(2):
                conv = conv_of(dims, pj[0, rows, a * LANES : (a + 1) * LANES], pars, pad.at[a],
                               DI + a * ST)
                bc.append((conv * sigmoid(conv)).astype(bf16))
            scores[s] = lax.dot_general(
                bc[1], bc[0], (((1,), (1,)), ((), ())), preferred_element_type=f32
            )
            _, _, _, ld, ld2 = steps_of(
                dims, pj[0, rows, 2 * LANES : 3 * LANES].astype(f32), hpar
            )
            ldtab[s] = ld
            rowtab[s] = ld2.T
            return 0

        lax.fori_loop(0, S, seq, 0)

    @pl.when((i >= 6) & (i < K + 5))
    def _():
        j = i - 5
        slot = lax.rem(j, 2)
        h0 = (j - 1) * TC * HP

        def seq(s, q):
            rows = pl.ds(pl.multiple_of(s * T, T), T)
            turned = pltpu.roll(ldtab[s], LANES - h0, 1)
            total = None
            for u in range(TC):
                c0 = pl.multiple_of((j - 1) * half + u * LANES, LANES)
                conv = conv_of(
                    dims, pj[slot, rows, half + u * LANES : half + (u + 1) * LANES], pars,
                    pad.at[q * TC + u], c0,
                )
                x = (conv * sigmoid(conv)).astype(bf16)
                mix = []
                for a in range(HP):
                    k = u * HP + a
                    left = jnp.broadcast_to(turned[:, k : k + 1], (T, T))
                    expo = jnp.minimum(left - rowtab[s, pl.ds(h0 + k, 1), :], mask[...])
                    mix.append((jnp.exp2(expo) * scores[s]).astype(bf16))
                core = jnp.dot(
                    jnp.concatenate(mix, axis=1), stack_heads(dims, x),
                    preferred_element_type=f32,
                )
                o = core + pars[8:9, pl.ds(c0, LANES)] * x.astype(f32)
                ssd[rows, u * LANES : (u + 1) * LANES] = o
                gate = pj[slot, rows, u * LANES : (u + 1) * LANES].astype(f32)
                g = o * (gate * sigmoid(gate))
                gated[rows, pl.ds(c0, LANES)] = g
                total = g * g if total is None else total + g * g
            acc[rows, :] += total

        several(S, SEQ_F, seq)

    @pl.when(i < K + 5)
    def _():
        travel(trip + 1)

    @pl.when(ready)
    def _():
        fetch_w(chunk).wait()

    @pl.when(i == 4)
    def _():
        N = A0 * A * A * 2
        r = D // N
        Cn, Gn = C // N, DI // N
        last = wv[0].reshape(D, w)[:, w - LANES :].astype(f32)
        turned = last.T
        scale[...] = jnp.broadcast_to(turned[LANES - 1 :, :], scale.shape)
        parts = [last[d * r : d * r + 8, :] for d in range(N)]
        for t, v in enumerate(assemble(parts, Cn, C // LANES)):
            pars[0:8, t * LANES : (t + 1) * LANES] = v
        for t, v in enumerate(assemble(parts, Gn, DI // LANES)):
            pars[8:16, t * LANES : (t + 1) * LANES] = v
        _, lane = iotas(1, LANES)
        for t in range(DI // LANES):
            v = jnp.zeros((1, LANES), f32)
            for q in range(HP):
                v = jnp.where(lane // HD == q, skip[t * HP + q], v)
            pars[8:9, t * LANES : (t + 1) * LANES] = v

        def norm(k, _):
            rows = pl.ds(pl.multiple_of(k * LANES, LANES), LANES)
            u = tok[rows, :].astype(f32)
            rs = lax.rsqrt(jnp.mean(u * u, axis=-1, keepdims=True) + epsilon)
            v = u * rs * scale[0:1, :]
            uh[rows, :] = v.astype(bf16)
            uT[:, rows] = v.T.astype(bf16)
            return 0

        lax.fori_loop(0, R // LANES, norm, 0)

    @pl.when(ready)
    def _():
        slot = lax.rem(i, 2)
        M = min(R, ROWS)

        def rows(k, _):
            at_ = pl.ds(pl.multiple_of(k * M, M), M)
            v = jnp.dot(
                uh[at_, :], wv[slot].reshape(D, w), preferred_element_type=f32
            ).astype(bf16)
            pj[slot, at_, :] = v
            proj[0, at_, :] = v
            return 0

        lax.fori_loop(0, R // M, rows, 0)

    @pl.when(i == K + 5)
    def _():
        def seq(s, _):
            rows = pl.ds(pl.multiple_of(s * T, T), T)
            rs = lax.rsqrt(jnp.sum(acc[rows, :], axis=1, keepdims=True) * (1.0 / DI) + epsilon)
            rb = jnp.broadcast_to(rs, (T, LANES))
            tabs[0, rows, :] = rb

            def tile(k, _):
                for u in range(4):
                    lanes = pl.ds(pl.multiple_of((k * 4 + u) * LANES, LANES), LANES)
                    v = gated[rows, lanes] * rb * pars[8 + KW + 1 : 8 + KW + 2, lanes]
                    mixed[rows, lanes] = v.astype(bf16)
                return 0

            lax.fori_loop(0, DI // LANES // 4, tile, 0)
            return 0

        lax.fori_loop(0, S, seq, 0)
        acc[...] = jnp.zeros_like(acc)

    @pl.when(i >= K + 5)
    def _():
        travel(trip + 1)

    @pl.when(i >= K + 5)
    def _():
        k = i - K - 5
        slot = lax.rem(k, 2)
        fetch_o(k).wait()
        M = min(R, ROWS)

        def rows(m, _):
            at_ = pl.ds(pl.multiple_of(m * M, M), M)
            branch = jnp.dot(
                mixed[at_, :], wo[slot].reshape(DI, wo_cols), preferred_element_type=f32
            )
            out[at_, :] = (tokc[at_, :].astype(f32) + branch).astype(bf16)
            p = branch * goc[at_, :].astype(f32)
            part = p[:, 0:LANES]
            for q in range(1, wo_cols // LANES):
                part = part + p[:, q * LANES : (q + 1) * LANES]
            acc[at_, :] += part
            return 0

        lax.fori_loop(0, R // M, rows, 0)

        share = DI // LANES // KO

        def turn(m, _):
            for u in range(share):
                lanes = pl.ds(pl.multiple_of((k * share + u) * LANES, LANES), LANES)
                rows = pl.ds(pl.multiple_of(m * LANES, LANES), LANES)
                mT[lanes, rows] = mixed[rows, lanes].T
            return 0

        lax.fori_loop(0, R // LANES, turn, 0)

    @pl.when(i == K + KO + 4)
    def _():
        net.drain()
        neto.drain()
        mu = jnp.sum(acc[...], axis=1, keepdims=True) * (1.0 / DI)
        rb = tabs[0]
        tabs[1] = jnp.broadcast_to(mu, rb.shape) * rb * rb


def run_forward_net(dims, axis, geom, K, w, skip, tok, go, inw, smalls, ow):
    T, DI, C = (dims[k] for k in ("T", "DI", "C"))
    A0, A = geom
    R, D = tok.shape
    r = inw.shape[0]
    ro = ow.shape[0]
    half = w // 2
    wc = r * w // ro
    KO = D // wc
    S = R // T
    assert DI // LANES % KO == 0
    shift = (Gather.AFTER[4] + 2) // 2 - 4
    steps = K + KO + 5 + shift
    whole = lambda s: pl.BlockSpec(s, lambda i: (0,) * len(s), pipeline_mode=pl.Buffered(1))
    late = lambda i: (0, jnp.clip(i - K - 5 - shift, 0, KO - 1))
    hbm = pl.BlockSpec(memory_space=pl.ANY)
    return pl.pallas_call(
        functools.partial(forward, dims, axis, geom, K, KO),
        grid=(steps,),
        in_specs=[pl.BlockSpec(memory_space=pltpu.SMEM), whole((R, D)), whole(inw.shape)]
        + [whole(a.shape) for a in smalls]
        + [whole((ro, D)), pl.BlockSpec((R, wc), late), pl.BlockSpec((R, wc), late)],
        out_specs=[
            pl.BlockSpec((1, R, w), lambda i: (jnp.clip(i - 4 - shift, 0, K - 1), 0, 0)),
            pl.BlockSpec((R, half), lambda i: (0, jnp.clip(i - 6 - shift, 0, K - 2))),
            whole((D, R)), whole((DI, R)),
            pl.BlockSpec((R, wc), late),
            whole((2, R, LANES)), whole((16, C)), whole((8, D)), whole((K, r, w)),
            whole((8, LANES)), hbm, hbm,
        ],
        out_shape=[
            jax.ShapeDtypeStruct((K, R, w), bf16),
            jax.ShapeDtypeStruct((R, DI), f32),
            jax.ShapeDtypeStruct((D, R), bf16),
            jax.ShapeDtypeStruct((DI, R), bf16),
            jax.ShapeDtypeStruct((R, D), bf16),
            jax.ShapeDtypeStruct((2, R, LANES), f32),
            jax.ShapeDtypeStruct((16, C), f32),
            jax.ShapeDtypeStruct((8, D), f32),
            jax.ShapeDtypeStruct((K, r, w), bf16),
            jax.ShapeDtypeStruct((8, LANES), f32),
            jax.ShapeDtypeStruct((K, A0, A * A, 2, r, w), bf16),
            jax.ShapeDtypeStruct((A0, A * A, 2, ro, D), bf16),
        ],
        scratch_shapes=[
            pltpu.VMEM((R, D), bf16),
            pltpu.VMEM((2, A0, A * A, 2, r, w), bf16),
            pltpu.VMEM((2, A0, A * A, 2, ro, wc), bf16),
            pltpu.VMEM((2, R, w), bf16),
            pltpu.VMEM((R, DI), f32),
            pltpu.VMEM((R, DI), bf16),
            pltpu.VMEM((SEQ_F * half // LANES, FRONT + T, LANES), f32),
            pltpu.VMEM((S, T, LANES), f32),
            pltpu.VMEM((S, LANES, T), f32),
            pltpu.VMEM((S, T, T), f32),
            pltpu.VMEM((T, T), f32),
            pltpu.VMEM((R, LANES), f32),
            pltpu.VMEM((T, LANES), f32),
            pltpu.SemaphoreType.DMA((2,)),
            pltpu.SemaphoreType.DMA((2,)),
        ]
        + Gather.scratch(2 * K, A0, A) + Gather.scratch(2 * KO, A0, A),
        compiler_params=pltpu.CompilerParams(
            collective_id=1, has_side_effects=True, vmem_limit_bytes=VMEM
        ),
        cost_estimate=pl.CostEstimate(
            flops=2 * R * D * K * w, bytes_accessed=D * K * w * 60, transcendentals=0
        ),
        name="forward",
    )(skip, tok, inw, *smalls, ow, tok, go)


def backward(dims, axis, geom, K, KO, E, proj, proj0, ssd, wo, wf, uT, mT, go, wl, tabs, pars,
             hpar, dn, outc, dns, sums,
             uo, mo, dmx, dpj, pad, dpad, ldtab, rowtab, scores, dscores, dlog, csum, bcs, mask,
             cacc, dacc, hacc, small, wv, csem, wsem, *refs):
    T, DI, C, H, HD, ST, KW = (dims[k] for k in ("T", "DI", "C", "H", "HD", "ST", "KW"))
    A0, A = geom
    at = Place(axis, A0, A)
    i = pl.program_id(0)
    R = ssd.shape[0]
    _, r, w = wl.shape
    N = A0 * A * A
    half = w // 2
    S = R // T
    HP = LANES // HD
    TC = half // LANES
    D = go.shape[1]
    HF = mT.shape[2]
    each = KO // HF
    pairs = (K + 1) // 2

    def begun(t):
        step = lax.div(t, 2)
        ends = lax.rem(t, 2) == 1
        outer = (lax.rem(step, 2) == 0) & (step < 2 * KO)
        valid = (t >= 0) & ((ends & (step < K)) | (jnp.logical_not(ends) & outer))
        done = jnp.minimum(lax.div(step + 1, 2), KO)
        return valid, step + done + (ends & outer).astype(jnp.int32)

    net = Reduce(at, K + KO, begun, refs[:15])
    total = SumAll(at, refs[15:])

    def fetches():
        out = [(uT.at[:, at.c], uo.at[0]), (uT.at[:, 1 - at.c], uo.at[1])]
        return [pltpu.make_async_copy(s, d, csem.at[k]) for k, (s, d) in enumerate(out)]

    def fetch_half(h):
        out = [(mT.at[:, at.c, h], mo.at[0]), (mT.at[:, 1 - at.c, h], mo.at[1])]
        return [pltpu.make_async_copy(s, d, csem.at[2 + k]) for k, (s, d) in enumerate(out)]

    @pl.when(i == 0)
    def _():
        at.greet()
        for cp in fetches() + fetch_half(0):
            cp.start()
        for ref in (cacc, dacc, hacc, dlog, csum, dscores, dns):
            ref[...] = jnp.zeros_like(ref)
        row, col = iotas(T, T)
        mask[...] = jnp.where(row <= col, BIG, -BIG)
        pad[:, 0:FRONT, :] = jnp.zeros((pad.shape[0], FRONT, LANES), f32)
        dpad[:, T:, :] = jnp.zeros((dpad.shape[0], FRONT, LANES), f32)

        def seq(s, _):
            rows = pl.ds(pl.multiple_of(s * T, T), T)
            for a in range(2):
                conv = conv_of(dims, proj0[0, rows, a * LANES : (a + 1) * LANES], pars, pad.at[a],
                               DI + a * ST)
                bcs[a, rows, :] = (conv * sigmoid(conv)).astype(bf16)
            scores[s] = lax.dot_general(
                bcs[0, rows, :], bcs[1, rows, :], (((1,), (1,)), ((), ())),
                preferred_element_type=f32,
            )
            _, _, _, ld, ld2 = steps_of(
                dims, proj0[0, rows, 2 * LANES : 3 * LANES].astype(f32), hpar
            )
            ldtab[s] = ld2
            rowtab[s] = ld.T
            return 0

        lax.fori_loop(0, S, seq, 0)
        for cp in fetches() + fetch_half(0):
            cp.wait()
        at.meet()

    for h in range(1, HF):

        @pl.when(i == 2 * h * each - 1)
        def _(h=h):
            for cp in fetch_half(h):
                cp.start()

        @pl.when(i == 2 * h * each)
        def _(h=h):
            for cp in fetch_half(h):
                cp.wait()

    def finish(p, v):
        inner = (p >= 3 * KO) | (lax.rem(p, 3) > 0)

        @pl.when(inner)
        def _():
            g = jnp.where(p >= 3 * KO, p - KO, p - 1 - lax.div(p, 3))
            outc[g] = v
            q = v * wl[lax.rem(g + 1, K)].astype(f32)
            part = q[:, 0:LANES]
            for k in range(1, w // LANES):
                part = part + q[:, k * LANES : (k + 1) * LANES]
            dns[...] += part

        @pl.when(jnp.logical_not(inner))
        def _():
            outc[K + lax.div(p, 3)] = v

    def send_out():
        k = lax.div(i, 2)
        net.step(2 * i, finish)

        @pl.when((lax.rem(i, 2) == 0) & (k < KO))
        def _():
            net.begin(3 * k, mo, go[:, columns(lax.rem(k, each), w)])

    def fetch(t, q):
        return pltpu.make_async_copy(
            wf.at[2 * t + q], wv.at[:, q * w : (q + 1) * w], wsem.at[q]
        )

    def fetch_pair(t, act):
        act(fetch(t, 0))

        @pl.when(2 * t + 1 < K)
        def _():
            act(fetch(t, 1))

    @pl.when(i == 0)
    def _():
        fetch_pair(0, lambda cp: cp.start())

    slot = lax.rem(lax.div(i, 2), dpj.shape[0])
    off = lax.rem(i, 2) * w
    here_of = lambda lane: pl.ds(pl.multiple_of(off + lane, LANES), LANES)

    def conv_back(rows, lane0, c0, dact, conv, sig, u):
        lanes = pl.ds(c0, LANES)
        dconv = dact * (sig * (1.0 + conv * (1.0 - sig)))
        dpad[u, 0:T, :] = dconv
        dcin = dconv * pars[KW - 1 : KW, lanes]
        for k in range(KW - 1):
            dcin = dcin + dpad[u, KW - 1 - k : KW - 1 - k + T, :] * pars[k : k + 1, lanes]
        dpj[slot, rows, here_of(lane0)] = dcin.astype(bf16)
        for k in range(KW):
            start = FRONT - KW + 1 + k
            cacc[8 * k : 8 * k + 8, lanes] += sum8(dconv * pad[u, start : start + T, :])
        cacc[8 * KW : 8 * KW + 8, lanes] += sum8(dconv)

    @pl.when(i < K - 1)
    def _():
        h0 = i * TC * HP
        dmx[...] = lax.dot_general(
            go[...], wo[...], (((1,), (1,)), ((), ())), preferred_element_type=f32
        )

        def seq(s, q):
            rows = pl.ds(pl.multiple_of(s * T, T), T)
            turned = pltpu.roll(ldtab[s], LANES - h0, 1)
            rb, mb = tabs[0, rows, :], tabs[1, rows, :]
            parts = None
            for u in range(TC):
                c0 = pl.multiple_of(i * half + u * LANES, LANES)
                lanes = pl.ds(c0, LANES)
                here = slice(u * LANES, (u + 1) * LANES)
                there = slice(half + u * LANES, half + (u + 1) * LANES)
                conv = conv_of(dims, proj[0, rows, there], pars, pad.at[q * TC + u], c0)
                sig = sigmoid(conv)
                x = (conv * sig).astype(bf16)
                xf = x.astype(f32)
                gate = proj[0, rows, here].astype(f32)
                gs = sigmoid(gate)
                act = gate * gs
                o = ssd[rows, here]
                dm = dmx[rows, here]
                gated = o * act
                dgated = rb * (dm * pars[8 + KW + 1 : 8 + KW + 2, lanes]) - gated * mb
                dacc[8:16, lanes] += sum8(dm * (gated * rb))
                dssd = dgated * act
                dpj[slot, rows, here_of(u * LANES)] = (
                    dgated * o * (gs * (1.0 + gate * (1.0 - gs)))
                ).astype(bf16)
                low = dssd.astype(bf16)
                dacc[0:8, lanes] += sum8(dssd * xf)
                lows = stack_heads(dims, low)
                dmix = lax.dot_general(
                    x, lows, (((1,), (1,)), ((), ())), preferred_element_type=f32
                )
                mix = []
                part = None
                for a in range(HP):
                    k = u * HP + a
                    right = jnp.broadcast_to(turned[:, k : k + 1], (T, T))
                    decay = jnp.exp2(
                        jnp.minimum(rowtab[s, pl.ds(h0 + k, 1), :] - right, mask[...])
                    )
                    mix.append((decay * scores[s]).astype(bf16))
                    term = dmix[:, a * T : (a + 1) * T] * decay
                    part = term if part is None else part + term
                core = jnp.dot(
                    jnp.concatenate(mix, axis=1), lows, preferred_element_type=f32
                )
                sk = pars[8:9, lanes]
                from_cols = xf * core
                diff = low.astype(f32) * (o - sk * xf) - from_cols
                prow, pcol = iotas(LANES, LANES)
                place = (pcol == h0 + u * HP + prow // HD).astype(bf16)
                both = jnp.concatenate([diff, from_cols], axis=0)
                hi = both.astype(bf16)
                lo = (both - hi.astype(f32)).astype(bf16)
                by_head = jnp.dot(
                    jnp.concatenate([hi, lo], axis=1),
                    jnp.concatenate([place, place], axis=0), preferred_element_type=f32,
                )
                conv_back(rows, half + u * LANES, c0, core + sk * dssd, conv, sig,
                          q * TC + u)
                new = (part, by_head)
                parts = new if parts is None else tuple(p + q for p, q in zip(parts, new))
            dscores[s] += parts[0]
            dlog[rows, :] += parts[1][0:T]
            csum[rows, :] += parts[1][T:]

        several(S // 2, SEQ_B, seq)
        send_out()
        several(S // 2, SEQ_B, lambda s, q: seq(S // 2 + s, q))

    @pl.when(i == K - 1)
    def _():
        row, col = iotas(T, T)
        upper = (row <= col).astype(f32)

        def seq(s, _):
            rows = pl.ds(pl.multiple_of(s * T, T), T)
            ds = dscores[s]
            dact = (
                jnp.dot(ds.astype(bf16), bcs[1, rows, :], preferred_element_type=f32),
                jnp.dot(ds.T.astype(bf16), bcs[0, rows, :], preferred_element_type=f32),
            )
            for a in range(2):
                conv = conv_of(dims, proj0[0, rows, a * LANES : (a + 1) * LANES], pars, pad.at[a],
                               DI + a * ST)
                conv_back(rows, a * LANES, DI + a * ST, dact[a], conv, sigmoid(conv), a)
            v, e, step, _, _ = steps_of(
                dims, proj0[0, rows, 2 * LANES : 3 * LANES].astype(f32), hpar
            )
            dsteps = jnp.dot(
                upper, dlog[rows, :], precision=lax.Precision.HIGHEST,
                preferred_element_type=f32,
            )
            sg = jnp.where(v >= 0.0, 1.0, e) / (1.0 + e)
            ratio = jnp.where(step > 1e-30, sg / jnp.maximum(step, 1e-30), 1.0)
            ddt = csum[rows, :] * ratio + dsteps * hpar[1:2, :] * sg
            _, lane = iotas(T, LANES)
            ddt = jnp.where(lane < H, ddt, 0.0)
            dpj[slot, rows, here_of(2 * LANES)] = ddt.astype(bf16)
            dpj[slot, rows, here_of(3 * LANES)] = jnp.zeros((T, LANES), bf16)
            hacc[0:8, :] += sum8(ddt)
            hacc[8:16, :] += sum8(dsteps * step)
            return 0

        lax.fori_loop(0, S, seq, 0)
        small[...] = jnp.zeros_like(small)
        for k in range(KW + 1):
            small[k : k + 1, :] = jnp.sum(cacc[8 * k : 8 * k + 8, :], axis=0, keepdims=True)
        for k in range(2):
            small[KW + 1 + k : KW + 2 + k, 0:DI] = jnp.sum(
                dacc[8 * k : 8 * k + 8, :], axis=0, keepdims=True
            )
            small[KW + 3 : KW + 4, k * LANES : (k + 1) * LANES] = jnp.sum(
                hacc[8 * k : 8 * k + 8, :], axis=0, keepdims=True
            )
        total.start(0, small[...])

    tail = pairs - dpj.shape[0] + i - K
    t = jnp.where(i < K, lax.div(i - 7, 2), tail)
    turn = jnp.where(
        i < K, (i >= 7) & (lax.rem(i, 2) == 1) & (t < pairs - dpj.shape[0]), t >= 0
    )

    @pl.when(turn)
    def _():
        fetch_pair(t, lambda cp: cp.wait())
        mine = lax.rem(t, dpj.shape[0])

        def add(part):
            @pl.when(t == 0)
            def _():
                dn[...] = part()

            @pl.when(t > 0)
            def _():
                dn[...] += part()

        @pl.when(2 * t + 1 < K)
        def _():
            add(lambda: lax.dot_general(
                dpj[mine], wv[...], (((1,), (1,)), ((), ())), preferred_element_type=f32
            ))

        @pl.when(2 * t + 1 >= K)
        def _():
            add(lambda: lax.dot_general(
                dpj[mine, :, 0:w], wv[:, 0:w], (((1,), (1,)), ((), ())),
                preferred_element_type=f32,
            ))

        @pl.when(t + 1 < pairs)
        def _():
            fetch_pair(t + 1, lambda cp: cp.start())

    @pl.when(i >= K - 1)
    def _():
        net.step(2 * i, finish)

    net.step(2 * i + 1, finish)

    @pl.when(i < K)
    def _():
        net.begin(begun(2 * i + 1)[1], uo, dpj[slot, :, pl.ds(pl.multiple_of(off, w), w)])

    for stage in range(1, 4):

        @pl.when(i == K - 1 + stage)
        def _(stage=stage):
            total.start(stage, total.finish(stage - 1))

    @pl.when(i == K + 3)
    def _():
        sums[...] = total.finish(3)

    @pl.when(i == K + 3)
    def _():
        net.drain()


def run_backward_net(dims, axis, geom, E, proj, ssd, ofull, wfull, uT, mT, go, wl, tabs, pars,
                     hpar):
    T, DI, C, H, KW, ST = (dims[k] for k in ("T", "DI", "C", "H", "KW", "ST"))
    A0, A = geom
    N = A0 * A * A
    K, R, w = proj.shape
    r = wl.shape[1]
    D = go.shape[1]
    ro = DI // (2 * N)
    HF = ro // r
    half = w // 2
    S = R // T
    KO = HF * (D // w)
    assert 2 * KO <= K + 1 and HF * r == ro and D % w == 0
    whole = lambda s: pl.BlockSpec(s, lambda i: (0,) * len(s), pipeline_mode=pl.Buffered(1))
    tile = lambda i: jnp.clip(i, 0, K - 2)
    hbm = pl.BlockSpec(memory_space=pl.ANY)
    return pl.pallas_call(
        functools.partial(backward, dims, axis, geom, K, KO, E),
        grid=(K + 4,),
        in_specs=[
            pl.BlockSpec((1, R, w), lambda i: (tile(i) + 1, 0, 0)),
            whole((1, R, w)),
            pl.BlockSpec((R, half), lambda i: (0, tile(i))),
            pl.BlockSpec((half, D), lambda i: (tile(i), 0)),
            hbm, hbm, hbm, whole((R, D)), whole((K, r, w)), whole((2, R, LANES)), whole((16, C)),
            whole((8, LANES)),
        ],
        out_specs=[whole((R, D)), whole((K + KO, r, w)), whole((r, LANES)), whole((8, C))],
        out_shape=[
            jax.ShapeDtypeStruct((R, D), f32),
            jax.ShapeDtypeStruct((K + KO, r, w), f32),
            jax.ShapeDtypeStruct((r, LANES), f32),
            jax.ShapeDtypeStruct((8, C), f32),
        ],
        scratch_shapes=[
            pltpu.VMEM((2, N, r, R), bf16),
            pltpu.VMEM((2, N, r, R), bf16),
            pltpu.VMEM((R, half), f32),
            pltpu.VMEM((4, R, 2 * w), bf16),
            pltpu.VMEM((2 * SEQ_B, FRONT + T, LANES), f32),
            pltpu.VMEM((2 * SEQ_B, FRONT + T, LANES), f32),
            pltpu.VMEM((S, T, LANES), f32),
            pltpu.VMEM((S, LANES, T), f32),
            pltpu.VMEM((S, T, T), f32),
            pltpu.VMEM((S, T, T), f32),
            pltpu.VMEM((R, LANES), f32),
            pltpu.VMEM((R, LANES), f32),
            pltpu.VMEM((2, R, ST), bf16),
            pltpu.VMEM((T, T), f32),
            pltpu.VMEM((8 * (KW + 1), C), f32),
            pltpu.VMEM((16, DI), f32),
            pltpu.VMEM((16, LANES), f32),
            pltpu.VMEM((8, C), f32),
            pltpu.VMEM((D, 2 * w), bf16),
            pltpu.SemaphoreType.DMA((4,)),
            pltpu.SemaphoreType.DMA((2,)),
        ]
        + Reduce.scratch(K + KO, A0, A, r, w)
        + SumAll.scratch(A0, A, (8, C)),
        compiler_params=pltpu.CompilerParams(
            collective_id=2, has_side_effects=True, vmem_limit_bytes=VMEM
        ),
        cost_estimate=pl.CostEstimate(
            flops=6 * R * D * K * w, bytes_accessed=D * K * w * 90, transcendentals=0
        ),
        name="backward",
    )(proj, proj, ssd, ofull.reshape(DI, D), wfull.reshape(K, D, w), uT.reshape(N, 2, r, R),
      mT.reshape(N, 2, HF, r, R), go, wl, tabs, pars, hpar)


def conclude(dims, axis, K, E, dn, tok, go, out, scale, outc, dns, sums, ns, hpar,
             dtok, outs, dw, dow, dtaps, dbias, ddtb, dalog, dskip, dnorm, dgain, tmp):
    T, DI, C, H, HD, KW = (dims[k] for k in ("T", "DI", "C", "H", "HD", "KW"))
    outs[...] = out[...]
    u = tok[...].astype(f32)
    rs = lax.rsqrt(jnp.mean(u * u, axis=-1, keepdims=True) + epsilon)
    u = u * rs
    d = dn[...] * scale[0:1, :]
    m = jnp.mean(d * u, axis=-1, keepdims=True)
    dtok[...] = go[...].astype(f32) + rs * (d - u * m)

    @pl.when(pl.program_id(0) == 0)
    def _():
        me = lax.axis_index(axis)
        r, w = outc.shape[1:]
        half = w // 2
        for g in range(K - 1):
            dw[:, g * half : (g + 1) * half] = outc[g, :, 0:half]
            dw[:, DI + g * half : DI + (g + 1) * half] = outc[g, :, half:]
        dw[:, 2 * DI :] = outc[K - 1, :, 0 : E - 2 * DI]
        cols = dow.shape[1] // w
        for k in range(outc.shape[0] - K):
            h, c = k // cols, k % cols
            dow[h * r : (h + 1) * r, c * w : (c + 1) * w] = outc[K + k]

        def window(size):
            start = me * size
            base = jnp.minimum(lax.div(start, LANES), C // LANES - 2) * LANES
            v = sums[:, pl.ds(pl.multiple_of(base, LANES), 2 * LANES)]
            return pltpu.roll(v, lax.rem(2 * LANES - (start - base), 2 * LANES), 1)

        Cn, Gn = dbias.shape[0], dgain.shape[0]
        v = window(Cn)[:, 0:LANES]
        tmp[...] = jnp.zeros_like(tmp)
        tmp[0:8, :] = v
        dtaps[...] = tmp[...].T[0:Cn, 0:KW]
        dbias[...] = v[KW, 0:Cn]
        dgain[...] = window(Gn)[KW + 2, 0:Gn]
        ddtb[...] = sums[KW + 3, 0:H]
        dalog[...] = sums[KW + 3 : KW + 4, LANES : 2 * LANES][0, 0:H] * hpar[1, 0:H]
        tmp[0:r, :] = dns[...]
        tmp[r:, :] = jnp.zeros((LANES - r, LANES), f32)
        dnorm[...] = jnp.sum(tmp[...].T, axis=0)[0:r] / ns[0, :].astype(f32)
        tiles = DI // LANES
        tmp[...] = jnp.zeros_like(tmp)
        for t in range(tiles):
            tmp[t : t + 1, :] = sums[KW + 1 : KW + 2, t * LANES : (t + 1) * LANES]
        row, col = iotas(LANES, LANES)
        HP = LANES // HD
        fold = (row // HD == lax.rem(col, HP)).astype(f32)
        v = jnp.dot(tmp[...], fold, precision=lax.Precision.HIGHEST, preferred_element_type=f32)
        dskip[...] = jnp.sum(jnp.where(col // HP == row, v, 0.0), axis=0)[0:H]


def run_conclude(dims, axis, K, E, dn, tok, go, out, scale, outc, dns, sums, ns, hpar, ro):
    T, DI, C, H, KW = (dims[k] for k in ("T", "DI", "C", "H", "KW"))
    R, D = tok.shape
    r = outc.shape[1]
    n = D // r
    T = math.gcd(R, BLOCK)
    rows = pl.BlockSpec((T, D), lambda i: (i, 0))
    whole = lambda s: pl.BlockSpec(s, lambda i: (0,) * len(s))
    shapes = [(r, E), (ro, D), (C // n, KW), (C // n,), (H,), (H,), (H,), (r,), (DI // n,)]
    return pl.pallas_call(
        functools.partial(conclude, dims, axis, K, E),
        grid=(R // T,),
        in_specs=[rows, rows, rows, rows]
        + [whole(a.shape) for a in (scale, outc, dns, sums, ns, hpar)],
        out_specs=[rows, rows] + [whole(x) for x in shapes],
        out_shape=[jax.ShapeDtypeStruct((R, D), f32), jax.ShapeDtypeStruct((R, D), bf16)]
        + [jax.ShapeDtypeStruct(x, f32) for x in shapes],
        scratch_shapes=[pltpu.VMEM((LANES, LANES), f32)],
        name="conclude",
    )(dn, tok, go, out, scale, outc, dns, sums, ns, hpar)


def local(axis, n, tokens, in_weight, conv_weight, conv_bias, dt_bias, a_log, skip_d,
          norm_scale, gate_scale, out_weight, grad_out):
    MB, S, T, D = tokens.shape
    R = MB * S * T
    r, E = in_weight.shape
    H = a_log.shape[0]
    DI = out_weight.shape[0] * n
    Cn, KW = conv_weight.shape
    C = Cn * n
    HD = DI // H
    ST = (C - DI) // 2
    dims = dict(T=T, DI=DI, C=C, H=H, HD=HD, ST=ST, KW=KW)
    assert LANES % HD == 0 and ST == LANES and DI % (LANES * 2) == 0 and T % 16 == 0
    geom = geometry(n)
    w = CHUNK
    Gn, ro = DI // n, out_weight.shape[0]
    own = (
        geom is not None and r % 16 == 0 and ro % r == 0 and D % w == 0 and DI % (w // 2) == 0
        and w == 2 * ST + 2 * LANES and E == 2 * DI + 2 * ST + H and H <= LANES
        and max(Cn, Gn) < LANES and 6 <= KW + 2 <= 8 and 2 * (ro // r) * (D // w) <= DI * 2 // w + 2
    )
    me = lax.axis_index(axis)
    tok = tokens.reshape(R, D)
    go = grad_out.reshape(R, D)
    if own:
        row = lambda v: v.reshape(1, -1)
        K = DI * 2 // w + 1
        smalls = [conv_weight.T] + [
            row(v) for v in (conv_bias, gate_scale, norm_scale, dt_bias, a_log)
        ]
        proj, ssd, uT, mT, output, tabs, pars, scale, wl, hpar, wfull, ofull = run_forward_net(
            dims, axis, geom, K, w, skip_d, tok, go, in_weight, smalls, out_weight
        )
        dn, outc, dns, sums = run_backward_net(
            dims, axis, geom, E, proj, ssd, ofull, wfull, uT, mT, go, wl, tabs, pars, hpar
        )
        dtok, output, dw, dow, dtaps, dbias, ddtb, dalog, dskip, dnorm, dgain = run_conclude(
            dims, axis, K, E, dn, tok, go, output, scale, outc, dns, sums, row(norm_scale), hpar,
            ro,
        )
        return (
            output.reshape(tokens.shape), dtok.reshape(tokens.shape), dw, dtaps, dbias, ddtb,
            dalog, dskip, dnorm, dgain, dow,
        )
    rate = -jnp.exp(a_log)
    hpar = jnp.pad(jnp.stack([dt_bias, rate]), ((0, 6), (0, LANES - H)))
    skip = jnp.broadcast_to(jnp.repeat(skip_d, HD)[None], (8, DI))
    ns = norm_scale.astype(f32)
    out_full = lax.all_gather(out_weight, axis, axis=0, tiled=True)
    wfull = lax.all_gather(in_weight, axis, axis=0, tiled=True)
    conv = lax.all_gather(jnp.concatenate([conv_weight.T, conv_bias[None]]), axis, axis=0)
    conv = conv.transpose(1, 0, 2).reshape(KW + 1, C).astype(f32)
    gate = lax.all_gather(gate_scale, axis, axis=0).reshape(1, DI).astype(f32)
    scale = lax.all_gather(norm_scale, axis, axis=0).reshape(1, D).astype(f32)
    u = tok.astype(f32)
    u = u * lax.rsqrt(jnp.mean(u * u, axis=-1, keepdims=True) + epsilon)
    uh = (u * scale).astype(bf16)
    proj = jnp.dot(uh, wfull, preferred_element_type=f32).astype(bf16)
    cpar = jnp.pad(conv, ((0, 8 - KW - 1), (0, 0)))
    dpar = jnp.concatenate([skip[:1], gate, skip[2:]], axis=0)
    mixed, ssd, rstd = run_forward(dims, proj, cpar, hpar, dpar)
    output = jnp.dot(mixed, out_full, preferred_element_type=f32)
    output = (tok.astype(f32) + output).astype(bf16)
    d_mixed = lax.dot_general(
        go, out_full, (((1,), (1,)), ((), ())), preferred_element_type=f32
    )
    dproj, small = run_backward(dims, proj, d_mixed, ssd, rstd, cpar, hpar, dpar)
    left = (((0,), (0,)), ((), ()))
    g_out = lax.dot_general(mixed, go, left, preferred_element_type=f32).astype(bf16)
    dow = lax.psum_scatter(g_out, axis, scatter_dimension=0, tiled=True).astype(f32)
    g_in = lax.dot_general(uh, dproj, left, preferred_element_type=f32).astype(bf16)
    dw = lax.psum_scatter(g_in, axis, scatter_dimension=0, tiled=True).astype(f32)
    dns = dw * in_weight.astype(f32)
    dn = lax.dot_general(dproj, wfull, (((1,), (1,)), ((), ())), preferred_element_type=f32)
    sums = lax.psum(small, axis)
    u = tok.astype(f32)
    rs = lax.rsqrt(jnp.mean(u * u, axis=-1, keepdims=True) + epsilon)
    u, d = u * rs, dn * scale
    dtok = go.astype(f32) + rs * (d - u * jnp.mean(d * u, axis=-1, keepdims=True))
    dconv = lax.dynamic_slice(sums, (0, me * Cn), (KW + 1, Cn))
    heads = sums[KW + 3]
    return (
        output.reshape(tokens.shape),
        dtok.reshape(tokens.shape),
        dw,
        dconv[:KW].T,
        dconv[KW],
        heads[:H],
        heads[LANES : LANES + H] * rate,
        sums[KW + 1, :DI].reshape(H, HD).sum(axis=1),
        dns.sum(axis=1) / ns,
        lax.dynamic_slice(sums[KW + 2], (me * Gn,), (Gn,)),
        dow,
    )


def solution(mesh):
    axis = mesh.axis_names[0]
    n = mesh.shape[axis]
    rows, flat, batch = P(axis, None), P(axis), P(None, axis, None, None)
    return jax.shard_map(
        functools.partial(local, axis, n),
        mesh=mesh,
        in_specs=(batch, rows, rows, flat, P(), P(), P(), flat, flat, rows, batch),
        out_specs=(batch, batch, rows, rows, flat, P(), P(), P(), flat, flat, rows),
        check_vma=False,
    )
```

```python
import functools
import math

import jax
import jax.numpy as jnp
from jax import lax
from jax.experimental import pallas as pl
from jax.experimental.pallas import tpu as pltpu
from jax.sharding import PartitionSpec as P

epsilon = 1e-05
LOG2E = 1.4426950408889634
BIG = 3.0e38
LANES = 128
FRONT = 8
f32 = jnp.float32
bf16 = jnp.bfloat16
UNROLL_F = 2
UNROLL_B = 2


def sigmoid(v):
    return 0.5 * jnp.tanh(0.5 * v) + 0.5


def sum8(v):
    rows, lanes = v.shape
    return jnp.sum(v.reshape(rows // 8, 8, lanes), axis=0)


def iotas(rows, lanes):
    return (
        lax.broadcasted_iota(jnp.int32, (rows, lanes), 0),
        lax.broadcasted_iota(jnp.int32, (rows, lanes), 1),
    )


def step_stage(dims, proj, hpar, dtp):
    DI, C, H = dims["DI"], dims["C"], dims["H"]
    dtp[...] = jnp.zeros_like(dtp)
    dtp[:, 0:H] = proj[:, DI + C : DI + C + H].astype(f32)
    return steps_of(dims, dtp[...], hpar)


def steps_of(dims, dt, hpar):
    T, H = dims["T"], dims["H"]
    _, lane = iotas(T, LANES)
    v = jnp.where(lane < H, dt + hpar[0:1, :], 0.0)
    e = jnp.exp(-jnp.abs(v))
    step = jnp.maximum(v, 0.0) + jnp.log1p(e)
    row, col = iotas(T, T)
    tri = (row >= col).astype(f32)
    ld = jnp.dot(
        tri, step * (hpar[1:2, :] * LOG2E), precision=lax.Precision.HIGHEST,
        preferred_element_type=f32,
    )
    return v, e, step, ld, ld - jnp.log2(step)


def conv_of(dims, cin, cpar, pad, c0):
    T, KW = dims["T"], dims["KW"]
    lanes = pl.ds(c0, LANES)
    cin = cin.astype(f32)
    pad[FRONT : FRONT + T, :] = cin
    out = cpar[KW : KW + 1, lanes] + cin * cpar[KW - 1 : KW, lanes]
    for k in range(KW - 1):
        out = out + pad[FRONT - KW + 1 + k : FRONT - KW + 1 + k + T, :] * cpar[k : k + 1, lanes]
    return out


def conv_tile(dims, proj, cpar, pad, c0):
    return conv_of(dims, proj[:, pl.ds(dims["DI"] + c0, LANES)], cpar, pad, c0)


def stack_heads(dims, v):
    T, HD = dims["T"], dims["HD"]
    _, lane = iotas(T, LANES)
    zero = jnp.zeros_like(v)
    return jnp.concatenate(
        [jnp.where(lane // HD == a, v, zero) for a in range(LANES // HD)], axis=0
    )


MESH = pl.DeviceIdType.MESH
CHUNK = 512
VMEM = 67043328
ROWS = 1024
SEQ_F = 2
BLOCK = 256
SEQ_B = 2


def geometry(n):
    chips = n // 2
    A0 = 4 if chips % 4 == 0 else 1
    A = math.isqrt(chips // A0)
    return (A0, A) if n % 2 == 0 and A > 1 and A0 * A * A == chips else None


class Place:
    def __init__(self, axis, A0, A):
        me = lax.axis_index(axis)
        self.A0, self.A = A0, A
        self.c = lax.rem(me, 2)
        chip = lax.div(me, 2)
        self.a2 = lax.rem(chip, A)
        self.a1 = lax.rem(lax.div(chip, A), A)
        self.a0 = lax.div(chip, A * A)
        c = self.c
        self.f = self.a1 + c * (self.a2 - self.a1)
        self.s = self.a2 + c * (self.a1 - self.a2)
        self.sf = A + c * (1 - A)
        self.ss = 1 + c * (A - 1)

    def pos(self, f, s):
        return f * self.sf + s * self.ss

    def device(self, a0, f, s, c):
        return ((a0 * self.A * self.A + self.pos(f, s)) * 2 + c,)

    def line(self, q):
        return lax.rem(self.a0 + q + self.A0, self.A0)

    def first(self, q):
        return lax.rem(self.f + q + self.A, self.A)

    def second(self, q):
        return lax.rem(self.s + q + self.A, self.A)

    def partner(self):
        return self.device(self.a0, self.f, self.s, 1 - self.c)

    def peers(self):
        out = [self.partner()]
        out += [self.device(self.line(q), self.f, self.s, self.c) for q in range(1, self.A0)]
        out += [self.device(self.a0, self.first(q), self.s, self.c) for q in range(1, self.A)]
        out += [self.device(self.a0, self.f, self.second(q), self.c) for q in range(1, self.A)]
        return out

    def greet(self):
        for peer in self.peers():
            pl.semaphore_signal(
                pltpu.get_barrier_semaphore(), inc=1, device_id=peer, device_id_type=MESH
            )

    def meet(self):
        pl.semaphore_wait(pltpu.get_barrier_semaphore(), len(self.peers()))


def columns(j, w):
    return pl.ds(pl.multiple_of(j * w, w), w)


def send(src, dst, ssem, rsem, device):
    return pltpu.make_async_remote_copy(
        src_ref=src, dst_ref=dst, send_sem=ssem, recv_sem=rsem,
        device_id=device, device_id_type=MESH,
    )


class Gather:
    AFTER = (0, 3, 6, 9, 12)
    DEEP = 5
    ORDER = (0, 4, 3, 2, 1)
    TURN = 1

    def __init__(self, at, K, mine, whole, ssem, rsem, lsem):
        self.at, self.K, self.mine, self.whole = at, K, mine, whole
        self.ssem, self.rsem, self.lsem = ssem, rsem, lsem

    @staticmethod
    def scratch(K, A0, A):
        NS = (A0 - 1) * A + (A - 1) + (A - 1) * A + 1
        return [
            pltpu.SemaphoreType.DMA((Gather.DEEP, NS)),
            pltpu.SemaphoreType.DMA((K, NS)),
            pltpu.SemaphoreType.DMA((Gather.DEEP,)),
        ]

    def local(self, j):
        at = self.at
        return pltpu.make_async_copy(
            self.mine(j), self.whole(j, at.a0, at.pos(at.f, at.s), at.c),
            self.lsem.at[lax.rem(j, self.DEEP)],
        )

    def copies(self, stage, j, sending, late):
        at, whole = self.at, self.whole
        A0, A = at.A0, at.A
        par = lax.rem(j, self.DEEP)
        line0, first0 = 0, (A0 - 1) * A
        second0 = first0 + A - 1
        every = slice(None)
        out = []

        def add(k, src, dst, device):
            out.append(send(src, dst, self.ssem.at[par, k], self.rsem.at[j, k], device))

        if stage == 0 and not late:
            for q in range(1, A0):
                a = at.a0 if sending else at.line(-q)
                add(line0 + q - 1, self.mine(j), whole(j, a, at.pos(at.f, at.s), at.c),
                    at.device(at.line(q), at.f, at.s, at.c))
        elif stage == 1 and late:
            for q in range(1, A0):
                a = at.a0 if sending else at.line(-q)
                for o in range(A):
                    ref = whole(j, a, at.pos(o, at.s), at.c)
                    add(line0 + (q - 1) * A + o, ref, ref,
                        at.device(at.line(q), at.f, at.s, at.c))
        elif stage < 2:
            for q in range(1, A):
                f = at.f if sending else at.first(-q)
                ref = whole(j, at.a0 if late else every, at.pos(f, at.s), at.c)
                add(first0 + q - 1, self.mine(j) if late else ref, ref,
                    at.device(at.a0, at.first(q), at.s, at.c))
        elif stage == 2:
            for q in range(1, A):
                s = at.s if sending else at.second(-q)
                for o in range(A):
                    ref = whole(j, every, at.pos(o, s), at.c)
                    add(second0 + (q - 1) * A + o, ref, ref,
                        at.device(at.a0, at.f, at.second(q), at.c))
        else:
            ref = whole(j, every, every, at.c if sending else 1 - at.c)
            add(second0 + (A - 1) * A, ref, ref, at.partner())
        return out

    def each(self, stage, j, sending, act):
        def run(late):
            for cp in self.copies(stage, j, sending, late):
                act(cp)

        if stage >= 2:
            run(False)
            return
        late = lax.rem(j, 3) == self.TURN
        pl.when(late)(lambda: run(True))
        pl.when(jnp.logical_not(late))(lambda: run(False))

    def step(self, i):
        for stage in self.ORDER:
            j = i - self.AFTER[stage]

            @pl.when((j >= 0) & (j < self.K))
            def _(stage=stage, j=j):
                if stage > 0:
                    self.each(stage - 1, j, False, lambda cp: cp.wait_recv())
                if stage < 4:

                    @pl.when(j >= self.DEEP)
                    def _():
                        self.each(stage, j - self.DEEP, True, lambda cp: cp.wait_send())

                    if stage == 1:
                        self.local(j).wait()
                    self.each(stage, j, True, lambda cp: cp.start())
                    if stage == 0:
                        self.local(j).start()

    def drain(self):
        for j in range(max(0, self.K - self.DEEP), self.K):
            for stage in range(4):
                for cp in self.copies(stage, jnp.int32(j), True, j % 3 == self.TURN):
                    cp.wait_send()


class Reduce:
    SLOTS = 3
    LAG = 2

    def __init__(self, at, K, begun, refs):
        self.at, self.K, self.begun = at, K, begun
        (self.own0, self.own1, self.own2, self.own3, self.s0, self.s1, self.s2, self.s3,
         self.r0, self.r1, self.r2, self.r3, self.ssem, self.rsem, self.credit) = refs

    @staticmethod
    def scratch(K, A0, A, r, w):
        N = A0 * A * A
        NS = 1 + (A - 1) + (A - 1) + (A0 - 1)
        L = Reduce.SLOTS
        return [
            pltpu.VMEM((2, N, r, w), f32),
            pltpu.VMEM((2, A0 * A, r, w), f32),
            pltpu.VMEM((2, A0, r, w), f32),
            pltpu.VMEM((2, r, w), f32),
            pltpu.VMEM((2, N, r, w), bf16),
            pltpu.VMEM((2, A - 1, A0 * A, r, w), bf16),
            pltpu.VMEM((2, A - 1, A0, r, w), bf16),
            pltpu.VMEM((2, A0 - 1, r, w), bf16),
            pltpu.VMEM((L, N, r, w), bf16),
            pltpu.VMEM((L, A - 1, A0 * A, r, w), bf16),
            pltpu.VMEM((L, A - 1, A0, r, w), bf16),
            pltpu.VMEM((L, A0 - 1, r, w), bf16),
            pltpu.SemaphoreType.DMA((2, NS)),
            pltpu.SemaphoreType.DMA((L, NS)),
            pltpu.SemaphoreType.REGULAR((NS,)),
        ]

    def routes(self, stage):
        at = self.at
        A0, A = at.A0, at.A
        if stage == 0:
            return [(0, at.partner(), at.partner())]
        if stage == 1:
            to = lambda q: at.device(at.a0, at.f, at.second(q), at.c)
            return [(q, to(q), to(-q)) for q in range(1, A)]
        if stage == 2:
            to = lambda q: at.device(at.a0, at.first(q), at.s, at.c)
            return [(A - 1 + q, to(q), to(-q)) for q in range(1, A)]
        to = lambda q: at.device(at.line(q), at.f, at.s, at.c)
        return [(2 * (A - 1) + q, to(q), to(-q)) for q in range(1, A0)]

    def copies(self, stage, j):
        par, slot = lax.rem(j, 2), lax.rem(j, self.SLOTS)
        src, dst = ((self.s0, self.r0), (self.s1, self.r1), (self.s2, self.r2),
                    (self.s3, self.r3))[stage]
        out = []
        for q, (k, to, _) in enumerate(self.routes(stage)):
            a = src.at[par] if stage == 0 else src.at[par, q]
            b = dst.at[slot] if stage == 0 else dst.at[slot, q]
            out.append(send(a, b, self.ssem.at[par, k], self.rsem.at[slot, k], to))
        return out

    def free(self, stage, j):
        @pl.when(j >= 2)
        def _():
            for cp in self.copies(stage, j - 2):
                cp.wait_send()

    def start(self, stage, j):
        @pl.when(j >= self.SLOTS)
        def _():
            for k, _, _ in self.routes(stage):
                pl.semaphore_wait(self.credit.at[k], 1)

        for cp in self.copies(stage, j):
            cp.start()

    def arrive(self, stage, j):
        for cp in self.copies(stage, j):
            cp.wait_recv()

    def done(self, stage, j):
        @pl.when(j + self.SLOTS < self.K)
        def _():
            for k, _, source in self.routes(stage):
                pl.semaphore_signal(
                    self.credit.at[k], inc=1, device_id=source, device_id_type=MESH
                )

    def begin(self, j, own, right):
        N, r, w = self.own0.shape[1:]
        par = lax.rem(j, 2)
        rows = lambda k: own[k].reshape(N * r, own.shape[3])
        self.free(0, j)
        self.s0[par] = (
            jnp.dot(rows(1), right, preferred_element_type=f32).astype(bf16).reshape(N, r, w)
        )
        self.start(0, j)
        self.own0[par] = jnp.dot(rows(0), right, preferred_element_type=f32).reshape(N, r, w)

    def step(self, i, finish):
        at = self.at
        A0, A = at.A0, at.A

        def stage1(j, par, slot):
            def line(a, _):
                for o in range(A):
                    for q in range(A):
                        b = a * A * A + at.pos(o, at.second(q))
                        v = self.own0[par, b] + self.r0[slot, b].astype(f32)
                        if q == 0:
                            self.own1[par, a * A + o] = v
                        else:
                            self.s1[par, q - 1, a * A + o] = v.astype(bf16)
                return 0

            lax.fori_loop(0, A0, line, 0)

        def stage2(j, par, slot):
            def line(a, _):
                for q in range(A):
                    b = a * A + at.first(q)
                    v = self.own1[par, b]
                    for p in range(A - 1):
                        v = v + self.r1[slot, p, b].astype(f32)
                    if q == 0:
                        self.own2[par, a] = v
                    else:
                        self.s2[par, q - 1, a] = v.astype(bf16)
                return 0

            lax.fori_loop(0, A0, line, 0)

        def stage3(j, par, slot):
            for q in range(A0):
                a = at.line(q)
                v = self.own2[par, a]
                for p in range(A - 1):
                    v = v + self.r2[slot, p, a].astype(f32)
                if q == 0:
                    self.own3[par] = v
                else:
                    self.s3[par, q - 1] = v.astype(bf16)

        def stage4(j, par, slot):
            v = self.own3[par]
            for p in range(A0 - 1):
                v = v + self.r3[slot, p].astype(f32)
            finish(j, v)

        for k, stage in ((4, stage4), (3, stage3), (2, stage2), (1, stage1)):
            valid, j = self.begun(i - k * self.LAG)

            @pl.when(valid)
            def _(j=j, k=k, stage=stage):
                self.arrive(k - 1, j)
                if k < 4:
                    self.free(k, j)
                stage(j, lax.rem(j, 2), lax.rem(j, self.SLOTS))
                self.done(k - 1, j)
                if k < 4:
                    self.start(k, j)

    def drain(self):
        for j in range(max(0, self.K - 2), self.K):
            for stage in range(4):
                for cp in self.copies(stage, jnp.int32(j)):
                    cp.wait_send()


class SumAll:
    def __init__(self, at, refs):
        self.at = at
        self.hold, self.land, self.ssem, self.rsem = refs

    @staticmethod
    def scratch(A0, A, shape):
        slots = 2 + A + A + A0
        return [
            pltpu.VMEM((4,) + shape, f32),
            pltpu.VMEM((slots,) + shape, f32),
            pltpu.SemaphoreType.DMA((slots,)),
            pltpu.SemaphoreType.DMA((slots,)),
        ]

    def group(self, stage):
        at = self.at
        A0, A = at.A0, at.A
        chip = at.a0 * A * A + at.a1 * A + at.a2
        if stage == 0:
            return 0, 2, at.c, 1, chip * 2
        if stage == 1:
            return 2, A, at.a2, 2, (chip - at.a2) * 2 + at.c
        if stage == 2:
            return 2 + A, A, at.a1, 2 * A, (chip - at.a1 * A) * 2 + at.c
        return 2 + 2 * A, A0, at.a0, 2 * A * A, (chip - at.a0 * A * A) * 2 + at.c

    def copies(self, stage, sending):
        base, size, mine, stride, origin = self.group(stage)
        out = []
        for q in range(1, size):
            to = lax.rem(mine + q, size)
            slot = mine if sending else lax.rem(mine - q + size, size)
            out.append(
                send(self.hold.at[stage], self.land.at[base + slot], self.ssem.at[base + q],
                     self.rsem.at[base + q], (origin + to * stride,))
            )
        return out

    def start(self, stage, value):
        base, _, mine, _, _ = self.group(stage)
        self.hold[stage] = value
        self.land[base + mine] = value
        for cp in self.copies(stage, True):
            cp.start()

    def finish(self, stage):
        base, size, _, _, _ = self.group(stage)
        for cp in self.copies(stage, False):
            cp.wait_recv()
        for cp in self.copies(stage, True):
            cp.wait_send()
        total = self.land[base]
        for k in range(1, size):
            total = total + self.land[base + k]
        return total


def mix_forward(dims, proj, cpar, hpar, dpar, mixed, ssd, rstd,
                pad, gated, colb, rowb, mask, scores, acc, dtp):
    T, DI, H, HD, ST = dims["T"], dims["DI"], dims["H"], dims["HD"], dims["ST"]
    HP = LANES // HD
    tiles = DI // LANES
    pad[:, 0:FRONT, :] = jnp.zeros((pad.shape[0], FRONT, LANES), f32)
    _, _, _, ld, ld2 = step_stage(dims, proj, hpar, dtp)
    row, col = iotas(T, T)
    mask[...] = jnp.where(col <= row, BIG, -BIG)
    rowb[...] = ld2.T
    for h in range(H):
        colb[h] = jnp.broadcast_to(ld[:, h : h + 1], (T, LANES))
    bc = []
    for a in range(2):
        conv = conv_tile(dims, proj, cpar, pad.at[a], DI + a * ST)
        bc.append((conv * sigmoid(conv)).astype(bf16))
    scores[...] = lax.dot_general(
        bc[1], bc[0], (((1,), (1,)), ((), ())), preferred_element_type=f32
    )
    acc[...] = jnp.zeros_like(acc)

    def tile(j, u):
        c0 = pl.multiple_of(j * LANES, LANES)
        lanes = pl.ds(c0, LANES)
        conv = conv_tile(dims, proj, cpar, pad.at[u], c0)
        x = (conv * sigmoid(conv)).astype(bf16)
        mix = []
        for a in range(HP):
            h = j * HP + a
            expo = jnp.minimum(colb[h] - rowb[pl.ds(h, 1), :], mask[...])
            mix.append((jnp.exp2(expo) * scores[...]).astype(bf16))
        core = jnp.dot(
            jnp.concatenate(mix, axis=1), stack_heads(dims, x), preferred_element_type=f32
        )
        out = core + dpar[0:1, lanes] * x.astype(f32)
        ssd[:, lanes] = out
        gate = proj[:, lanes].astype(f32)
        g = out * (gate * sigmoid(gate))
        gated[:, lanes] = g
        return g * g

    def body(j, _):
        total = tile(j * UNROLL_F, 0)
        for u in range(1, UNROLL_F):
            total = total + tile(j * UNROLL_F + u, u)
        acc[...] += total
        return 0

    lax.fori_loop(0, tiles // UNROLL_F, body, 0)
    r = lax.rsqrt(jnp.sum(acc[...], axis=1, keepdims=True) * (1.0 / DI) + epsilon)
    rb = jnp.broadcast_to(r, (T, LANES))
    rstd[...] = rb

    def finish(j, _):
        lanes = pl.ds(pl.multiple_of(j * LANES, LANES), LANES)
        mixed[:, lanes] = (gated[:, lanes] * rb * dpar[1:2, lanes]).astype(bf16)
        return 0

    lax.fori_loop(0, tiles, finish, 0)


def mix_backward(dims, steps, proj, dmixed, ssd, rstd, cpar, hpar, dpar, dproj, small,
                 cacc, dacc, hacc, pad, dpad, colb, rowb, mask, scores, acc, dtp, dscores, dlog,
                 csum, bcs):
    T, DI, C, H, HD, ST, KW = (dims[k] for k in ("T", "DI", "C", "H", "HD", "ST", "KW"))
    HP = LANES // HD
    tiles = DI // LANES

    @pl.when(pl.program_id(0) == 0)
    def _():
        cacc[...] = jnp.zeros_like(cacc)
        dacc[...] = jnp.zeros_like(dacc)
        hacc[...] = jnp.zeros_like(hacc)

    pad[:, 0:FRONT, :] = jnp.zeros((pad.shape[0], FRONT, LANES), f32)
    dpad[:, T:, :] = jnp.zeros((dpad.shape[0], FRONT, LANES), f32)
    v, e, step, ld, ld2 = step_stage(dims, proj, hpar, dtp)
    row, col = iotas(T, T)
    mask[...] = jnp.where(row <= col, BIG, -BIG)
    rowb[...] = ld.T
    for h in range(H):
        colb[h] = jnp.broadcast_to(ld2[:, h : h + 1], (T, LANES))
    for a in range(2):
        conv = conv_tile(dims, proj, cpar, pad.at[a], DI + a * ST)
        bcs[a] = (conv * sigmoid(conv)).astype(bf16)
    scores[...] = lax.dot_general(
        bcs[0], bcs[1], (((1,), (1,)), ((), ())), preferred_element_type=f32
    )
    acc[...] = jnp.zeros_like(acc)
    dscores[...] = jnp.zeros_like(dscores)
    dlog[...] = jnp.zeros_like(dlog)
    csum[...] = jnp.zeros_like(csum)
    rb = rstd[...]

    def first(j, _):
        lanes = pl.ds(pl.multiple_of(j * LANES, LANES), LANES)
        gate = proj[:, lanes].astype(f32)
        p = dmixed[:, lanes] * (ssd[:, lanes] * (gate * sigmoid(gate)))
        acc[...] += p * dpar[1:2, lanes]
        dacc[8:16, lanes] += sum8(p * rb)
        return 0

    lax.fori_loop(0, tiles, first, 0)
    mean = jnp.sum(acc[...], axis=1, keepdims=True) * (1.0 / DI)
    mb = jnp.broadcast_to(mean, (T, LANES)) * rb * rb * rb
    acc[...] = mb

    def conv_back(c0, dact, conv, sig, u):
        lanes = pl.ds(c0, LANES)
        dconv = dact * (sig * (1.0 + conv * (1.0 - sig)))
        dpad[u, 0:T, :] = dconv
        dcin = dconv * cpar[KW - 1 : KW, lanes]
        for k in range(KW - 1):
            dcin = dcin + dpad[u, KW - 1 - k : KW - 1 - k + T, :] * cpar[k : k + 1, lanes]
        dproj[:, pl.ds(DI + c0, LANES)] = dcin.astype(bf16)
        for k in range(KW):
            start = FRONT - KW + 1 + k
            cacc[8 * k : 8 * k + 8, lanes] += sum8(dconv * pad[u, start : start + T, :])
        cacc[8 * KW : 8 * KW + 8, lanes] += sum8(dconv)

    def tile(j, u):
        c0 = pl.multiple_of(j * LANES, LANES)
        lanes = pl.ds(c0, LANES)
        conv = conv_tile(dims, proj, cpar, pad.at[u], c0)
        sig = sigmoid(conv)
        x = (conv * sig).astype(bf16)
        xf = x.astype(f32)
        gate = proj[:, lanes].astype(f32)
        gs = sigmoid(gate)
        act = gate * gs
        out = ssd[:, lanes]
        r = rstd[...]
        dgated = r * (dmixed[:, lanes] * dpar[1:2, lanes]) - (out * act) * acc[...]
        dssd = dgated * act
        dproj[:, lanes] = (dgated * out * (gs * (1.0 + gate * (1.0 - gs)))).astype(bf16)
        low = dssd.astype(bf16)
        dacc[0:8, lanes] += sum8(dssd * xf)
        lows = stack_heads(dims, low)
        dmix = lax.dot_general(
            x, lows, (((1,), (1,)), ((), ())), preferred_element_type=f32
        )
        mix = []
        part = None
        for a in range(HP):
            h = j * HP + a
            decay = jnp.exp2(jnp.minimum(rowb[pl.ds(h, 1), :] - colb[h], mask[...]))
            mix.append((decay * scores[...]).astype(bf16))
            term = dmix[:, a * T : (a + 1) * T] * decay
            part = term if part is None else part + term
        core = jnp.dot(jnp.concatenate(mix, axis=1), lows, preferred_element_type=f32)
        skip = dpar[0:1, lanes]
        from_cols = xf * core
        diff = low.astype(f32) * (out - skip * xf) - from_cols
        prow, pcol = iotas(LANES, LANES)
        place = (pcol == j * HP + prow // HD).astype(bf16)
        place = jnp.concatenate([place, place], axis=0)

        def by_head(w):
            hi = w.astype(bf16)
            lo = (w - hi.astype(f32)).astype(bf16)
            return jnp.dot(
                jnp.concatenate([hi, lo], axis=1), place, preferred_element_type=f32
            )

        conv_back(c0, core + skip * dssd, conv, sig, u)
        return part, by_head(diff), by_head(from_cols)

    def body(j, _):
        sums = tile(j * UNROLL_B, 0)
        for u in range(1, UNROLL_B):
            sums = tuple(p + q for p, q in zip(sums, tile(j * UNROLL_B + u, u)))
        dscores[...] += sums[0]
        dlog[...] += sums[1]
        csum[...] += sums[2]
        return 0

    lax.fori_loop(0, tiles // UNROLL_B, body, 0)
    ds = dscores[...].astype(bf16)
    dst = dscores[...].T.astype(bf16)
    dact = (
        jnp.dot(ds, bcs[1], preferred_element_type=f32),
        jnp.dot(dst, bcs[0], preferred_element_type=f32),
    )
    for a in range(2):
        conv = conv_tile(dims, proj, cpar, pad.at[a], DI + a * ST)
        conv_back(DI + a * ST, dact[a], conv, sigmoid(conv), a)
    dsteps = jnp.dot(
        (row <= col).astype(f32), dlog[...], precision=lax.Precision.HIGHEST,
        preferred_element_type=f32,
    )
    sg = jnp.where(v >= 0.0, 1.0, e) / (1.0 + e)
    ratio = jnp.where(step > 1e-30, sg / jnp.maximum(step, 1e-30), 1.0)
    ddt = csum[...] * ratio + dsteps * hpar[1:2, :] * sg
    tail = dproj.shape[1] - DI - C
    if tail > H:
        dproj[:, DI + C :] = jnp.concatenate(
            [ddt[:, 0:H].astype(bf16), jnp.zeros((T, tail - H), bf16)], axis=1
        )
    else:
        dproj[:, DI + C :] = ddt[:, 0:H].astype(bf16)
    hacc[0:8, :] += sum8(ddt)
    hacc[8:16, :] += sum8(dsteps * step)

    @pl.when(pl.program_id(0) == steps - 1)
    def _():
        small[...] = jnp.zeros_like(small)
        for k in range(KW + 1):
            small[k : k + 1, :] = jnp.sum(cacc[8 * k : 8 * k + 8, :], axis=0, keepdims=True)
        for k in range(2):
            small[KW + 1 + k : KW + 2 + k, 0:DI] = jnp.sum(
                dacc[8 * k : 8 * k + 8, :], axis=0, keepdims=True
            )
            small[KW + 3 : KW + 4, k * LANES : (k + 1) * LANES] = jnp.sum(
                hacc[8 * k : 8 * k + 8, :], axis=0, keepdims=True
            )


def run_forward(dims, proj, cpar, hpar, dpar):
    T, DI, C, H, KW = dims["T"], dims["DI"], dims["C"], dims["H"], dims["KW"]
    R, E = proj.shape
    rows = lambda w: pl.BlockSpec((T, w), lambda i: (i, 0))
    whole = lambda a: pl.BlockSpec(a.shape, lambda i: (0, 0))
    return pl.pallas_call(
        functools.partial(mix_forward, dims),
        grid=(R // T,),
        in_specs=[rows(E), whole(cpar), whole(hpar), whole(dpar)],
        out_specs=[rows(DI), rows(DI), rows(LANES)],
        out_shape=[
            jax.ShapeDtypeStruct((R, DI), bf16),
            jax.ShapeDtypeStruct((R, DI), f32),
            jax.ShapeDtypeStruct((R, LANES), f32),
        ],
        scratch_shapes=[
            pltpu.VMEM((max(2, UNROLL_F), FRONT + T, LANES), f32),
            pltpu.VMEM((T, DI), f32),
            pltpu.VMEM((H, T, LANES), f32),
            pltpu.VMEM((LANES, T), f32),
            pltpu.VMEM((T, T), f32),
            pltpu.VMEM((T, T), f32),
            pltpu.VMEM((T, LANES), f32),
            pltpu.VMEM((T, LANES), f32),
        ],
        compiler_params=pltpu.CompilerParams(vmem_limit_bytes=48 << 20),
        name="mix_forward",
    )(proj, cpar, hpar, dpar)


def run_backward(dims, proj, dmixed, ssd, rstd, cpar, hpar, dpar):
    T, DI, C, H, KW, ST = (dims[k] for k in ("T", "DI", "C", "H", "KW", "ST"))
    R, E = proj.shape
    rows = lambda w: pl.BlockSpec((T, w), lambda i: (i, 0))
    whole = lambda s: pl.BlockSpec(s, lambda i: (0, 0))
    sums = [(8 * (KW + 1), C), (16, DI), (16, LANES)]
    return pl.pallas_call(
        functools.partial(mix_backward, dims, R // T),
        grid=(R // T,),
        in_specs=[rows(E), rows(DI), rows(DI), rows(LANES)]
        + [whole(a.shape) for a in (cpar, hpar, dpar)],
        out_specs=[rows(E), whole((8, C))],
        out_shape=[jax.ShapeDtypeStruct((R, E), bf16), jax.ShapeDtypeStruct((8, C), f32)],
        scratch_shapes=[pltpu.VMEM(s, f32) for s in sums]
        + [
            pltpu.VMEM((max(2, UNROLL_B), FRONT + T, LANES), f32),
            pltpu.VMEM((max(2, UNROLL_B), FRONT + T, LANES), f32),
            pltpu.VMEM((H, T, LANES), f32),
            pltpu.VMEM((LANES, T), f32),
            pltpu.VMEM((T, T), f32),
            pltpu.VMEM((T, T), f32),
            pltpu.VMEM((T, LANES), f32),
            pltpu.VMEM((T, LANES), f32),
            pltpu.VMEM((T, T), f32),
            pltpu.VMEM((T, LANES), f32),
            pltpu.VMEM((T, LANES), f32),
            pltpu.VMEM((2, T, ST), bf16),
        ],
        compiler_params=pltpu.CompilerParams(vmem_limit_bytes=56 << 20),
        name="mix_backward",
    )(proj, dmixed, ssd, rstd, cpar, hpar, dpar)


def several(count, width, body):
    width = math.gcd(width, count)

    def trip(m, _):
        for q in range(width):
            body(m * width + q, q)
        return 0

    lax.fori_loop(0, count // width, trip, 0)


def assemble(parts, size, tiles):
    _, lane = iotas(8, LANES)
    out = []
    for t in range(tiles):
        total = None
        for d in range(t * LANES // size, min(len(parts), -(-(t + 1) * LANES // size))):
            shift = d * size - t * LANES
            v = parts[d] if shift % LANES == 0 else pltpu.roll(parts[d], shift % LANES, 1)
            keep = (lane >= max(shift, 0)) & (lane < min(shift + size, LANES))
            v = jnp.where(keep, v, 0.0)
            total = v if total is None else total + v
        out.append(total)
    return out


def forward(dims, axis, geom, K, KO, skip, tok, inw, taps, bias, gains, ns, dtb, alog, ow,
            tokc, goc, proj, ssd, uT, mT, out, tabs, pars, scale, wl, hpar, wfull, ofull,
            uh, wv, wo, pj, gated, mixed, pad, ldtab, rowtab, scores, mask, acc, dtp, wsem, osem,
            *sems):
    T, DI, C, H, HD, ST, KW = (dims[k] for k in ("T", "DI", "C", "H", "HD", "ST", "KW"))
    A0, A = geom
    at = Place(axis, A0, A)
    i = pl.program_id(0)
    R, D = tok.shape
    w = wl.shape[2]
    half = w // 2
    S = R // T
    HP = LANES // HD
    TC = half // LANES
    wo_cols = wo.shape[5]
    place = lambda j: lax.rem(j + K - 1, K)
    part = lambda j: columns(lax.rem(j, 2), half)
    net = Gather(
        at, 2 * K, lambda j: wl.at[lax.div(j, 2), :, part(j)],
        lambda j, a, p, c: wfull.at[place(lax.div(j, 2)), a, p, c, :, part(j)], *sems[:3],
    )
    neto = Gather(
        at, 2 * KO, lambda j: ow.at[:, columns(j, wo_cols // 2)],
        lambda j, a, p, c: ofull.at[a, p, c, :, columns(j, wo_cols // 2)], *sems[3:],
    )

    @pl.when(i == 0)
    def _():
        at.greet()
        r, E = inw.shape
        Cn, Gn = bias.shape[1], gains.shape[1]
        zero = jnp.zeros((LANES, LANES), f32)
        dtp[...] = zero
        dtp[0:1, 0:r] = ns[...].astype(f32)
        column = pltpu.roll(dtp[...].T, LANES - 1, 1)
        dtp[...] = column
        dtp[0:KW, 0:Cn] = taps[...].astype(f32)
        dtp[KW : KW + 1, 0:Cn] = bias[...].astype(f32)
        dtp[KW + 1 : KW + 2, 0:Gn] = gains[...].astype(f32)
        wl[0, :, 0 : half] = inw[:, 2 * DI : 2 * DI + half]
        wl[0, :, half : half + LANES] = jnp.concatenate(
            [inw[:, 2 * DI + half : E], jnp.zeros((r, LANES - H), bf16)], axis=1
        )
        wl[0, :, half + LANES :] = dtp[0:r, :].astype(bf16)
        for j in range(1, K):
            wl[j, :, 0:half] = inw[:, (j - 1) * half : j * half]
            wl[j, :, half:] = inw[:, DI + (j - 1) * half : DI + j * half]
        hpar[...] = jnp.zeros_like(hpar)
        hpar[0:1, 0:H] = dtb[...]
        hpar[1:2, 0:H] = -jnp.exp(alog[...])
        at.meet()

    def travel(q):
        net.step(q)
        neto.step(q - 2 * K)

    trip = 2 * i
    i = i - ((Gather.AFTER[4] + 2) // 2 - 4)
    travel(trip)

    def fetch_w(j):
        slot = lax.rem(j, 2)
        return pltpu.make_async_copy(wfull.at[place(j)], wv.at[slot], wsem.at[slot])

    def fetch_o(k):
        slot = lax.rem(k, 2)
        return pltpu.make_async_copy(
            ofull.at[:, :, :, :, columns(k, wo_cols)], wo.at[slot], osem.at[slot]
        )

    ready = (i >= 4) & (i < K + 4)
    chunk = jnp.maximum(i - 4, 0)

    @pl.when(ready)
    def _():
        fetch_w(chunk).start()

    @pl.when((i >= K + 4) & (i < K + KO + 4))
    def _():
        fetch_o(i - K - 4).start()

    @pl.when(i == 5)
    def _():
        row, col = iotas(T, T)
        mask[...] = jnp.where(col <= row, BIG, -BIG)
        pad[:, 0:FRONT, :] = jnp.zeros((pad.shape[0], FRONT, LANES), f32)
        acc[...] = jnp.zeros_like(acc)

        def seq(s, _):
            rows = pl.ds(pl.multiple_of(s * T, T), T)
            bc = []
            for a in range(2):
                conv = conv_of(dims, pj[0, rows, a * LANES : (a + 1) * LANES], pars, pad.at[a],
                               DI + a * ST)
                bc.append((conv * sigmoid(conv)).astype(bf16))
            scores[s] = lax.dot_general(
                bc[1], bc[0], (((1,), (1,)), ((), ())), preferred_element_type=f32
            )
            _, _, _, ld, ld2 = steps_of(
                dims, pj[0, rows, 2 * LANES : 3 * LANES].astype(f32), hpar
            )
            ldtab[s] = ld
            rowtab[s] = ld2.T
            return 0

        lax.fori_loop(0, S, seq, 0)

    @pl.when((i >= 6) & (i < K + 5))
    def _():
        j = i - 5
        slot = lax.rem(j, 2)
        h0 = (j - 1) * TC * HP

        def seq(s, q):
            rows = pl.ds(pl.multiple_of(s * T, T), T)
            turned = pltpu.roll(ldtab[s], LANES - h0, 1)
            total = None
            for u in range(TC):
                c0 = pl.multiple_of((j - 1) * half + u * LANES, LANES)
                conv = conv_of(
                    dims, pj[slot, rows, half + u * LANES : half + (u + 1) * LANES], pars,
                    pad.at[q * TC + u], c0,
                )
                x = (conv * sigmoid(conv)).astype(bf16)
                mix = []
                for a in range(HP):
                    k = u * HP + a
                    left = jnp.broadcast_to(turned[:, k : k + 1], (T, T))
                    expo = jnp.minimum(left - rowtab[s, pl.ds(h0 + k, 1), :], mask[...])
                    mix.append((jnp.exp2(expo) * scores[s]).astype(bf16))
                core = jnp.dot(
                    jnp.concatenate(mix, axis=1), stack_heads(dims, x),
                    preferred_element_type=f32,
                )
                o = core + pars[8:9, pl.ds(c0, LANES)] * x.astype(f32)
                ssd[rows, u * LANES : (u + 1) * LANES] = o
                gate = pj[slot, rows, u * LANES : (u + 1) * LANES].astype(f32)
                g = o * (gate * sigmoid(gate))
                gated[rows, pl.ds(c0, LANES)] = g
                total = g * g if total is None else total + g * g
            acc[rows, :] += total

        several(S, SEQ_F, seq)

    @pl.when(i < K + 5)
    def _():
        travel(trip + 1)

    @pl.when(ready)
    def _():
        fetch_w(chunk).wait()

    @pl.when(i == 4)
    def _():
        N = A0 * A * A * 2
        r = D // N
        Cn, Gn = C // N, DI // N
        last = wv[0].reshape(D, w)[:, w - LANES :].astype(f32)
        turned = last.T
        scale[...] = jnp.broadcast_to(turned[LANES - 1 :, :], scale.shape)
        parts = [last[d * r : d * r + 8, :] for d in range(N)]
        for t, v in enumerate(assemble(parts, Cn, C // LANES)):
            pars[0:8, t * LANES : (t + 1) * LANES] = v
        for t, v in enumerate(assemble(parts, Gn, DI // LANES)):
            pars[8:16, t * LANES : (t + 1) * LANES] = v
        _, lane = iotas(1, LANES)
        for t in range(DI // LANES):
            v = jnp.zeros((1, LANES), f32)
            for q in range(HP):
                v = jnp.where(lane // HD == q, skip[t * HP + q], v)
            pars[8:9, t * LANES : (t + 1) * LANES] = v

        def norm(k, _):
            rows = pl.ds(pl.multiple_of(k * LANES, LANES), LANES)
            u = tok[rows, :].astype(f32)
            rs = lax.rsqrt(jnp.mean(u * u, axis=-1, keepdims=True) + epsilon)
            v = u * rs * scale[0:1, :]
            uh[rows, :] = v.astype(bf16)
            uT[:, rows] = v.T.astype(bf16)
            return 0

        lax.fori_loop(0, R // LANES, norm, 0)

    @pl.when(ready)
    def _():
        slot = lax.rem(i, 2)
        M = min(R, ROWS)

        def rows(k, _):
            at_ = pl.ds(pl.multiple_of(k * M, M), M)
            v = jnp.dot(
                uh[at_, :], wv[slot].reshape(D, w), preferred_element_type=f32
            ).astype(bf16)
            pj[slot, at_, :] = v
            proj[0, at_, :] = v
            return 0

        lax.fori_loop(0, R // M, rows, 0)

    @pl.when(i == K + 5)
    def _():
        def seq(s, _):
            rows = pl.ds(pl.multiple_of(s * T, T), T)
            rs = lax.rsqrt(jnp.sum(acc[rows, :], axis=1, keepdims=True) * (1.0 / DI) + epsilon)
            rb = jnp.broadcast_to(rs, (T, LANES))
            tabs[0, rows, :] = rb

            def tile(k, _):
                for u in range(4):
                    lanes = pl.ds(pl.multiple_of((k * 4 + u) * LANES, LANES), LANES)
                    v = gated[rows, lanes] * rb * pars[8 + KW + 1 : 8 + KW + 2, lanes]
                    mixed[rows, lanes] = v.astype(bf16)
                return 0

            lax.fori_loop(0, DI // LANES // 4, tile, 0)
            return 0

        lax.fori_loop(0, S, seq, 0)
        acc[...] = jnp.zeros_like(acc)

    @pl.when(i >= K + 5)
    def _():
        travel(trip + 1)

    @pl.when(i >= K + 5)
    def _():
        k = i - K - 5
        slot = lax.rem(k, 2)
        fetch_o(k).wait()
        M = min(R, ROWS)

        def rows(m, _):
            at_ = pl.ds(pl.multiple_of(m * M, M), M)
            branch = jnp.dot(
                mixed[at_, :], wo[slot].reshape(DI, wo_cols), preferred_element_type=f32
            )
            out[at_, :] = (tokc[at_, :].astype(f32) + branch).astype(bf16)
            p = branch * goc[at_, :].astype(f32)
            part = p[:, 0:LANES]
            for q in range(1, wo_cols // LANES):
                part = part + p[:, q * LANES : (q + 1) * LANES]
            acc[at_, :] += part
            return 0

        lax.fori_loop(0, R // M, rows, 0)

        share = DI // LANES // KO

        def turn(m, _):
            for u in range(share):
                lanes = pl.ds(pl.multiple_of((k * share + u) * LANES, LANES), LANES)
                rows = pl.ds(pl.multiple_of(m * LANES, LANES), LANES)
                mT[lanes, rows] = mixed[rows, lanes].T
            return 0

        lax.fori_loop(0, R // LANES, turn, 0)

    @pl.when(i == K + KO + 4)
    def _():
        net.drain()
        neto.drain()
        mu = jnp.sum(acc[...], axis=1, keepdims=True) * (1.0 / DI)
        rb = tabs[0]
        tabs[1] = jnp.broadcast_to(mu, rb.shape) * rb * rb


def run_forward_net(dims, axis, geom, K, w, skip, tok, go, inw, smalls, ow):
    T, DI, C = (dims[k] for k in ("T", "DI", "C"))
    A0, A = geom
    R, D = tok.shape
    r = inw.shape[0]
    ro = ow.shape[0]
    half = w // 2
    wc = r * w // ro
    KO = D // wc
    S = R // T
    assert DI // LANES % KO == 0
    shift = (Gather.AFTER[4] + 2) // 2 - 4
    steps = K + KO + 5 + shift
    whole = lambda s: pl.BlockSpec(s, lambda i: (0,) * len(s), pipeline_mode=pl.Buffered(1))
    late = lambda i: (0, jnp.clip(i - K - 5 - shift, 0, KO - 1))
    hbm = pl.BlockSpec(memory_space=pl.ANY)
    return pl.pallas_call(
        functools.partial(forward, dims, axis, geom, K, KO),
        grid=(steps,),
        in_specs=[pl.BlockSpec(memory_space=pltpu.SMEM), whole((R, D)), whole(inw.shape)]
        + [whole(a.shape) for a in smalls]
        + [whole((ro, D)), pl.BlockSpec((R, wc), late), pl.BlockSpec((R, wc), late)],
        out_specs=[
            pl.BlockSpec((1, R, w), lambda i: (jnp.clip(i - 4 - shift, 0, K - 1), 0, 0)),
            pl.BlockSpec((R, half), lambda i: (0, jnp.clip(i - 6 - shift, 0, K - 2))),
            whole((D, R)), whole((DI, R)),
            pl.BlockSpec((R, wc), late),
            whole((2, R, LANES)), whole((16, C)), whole((8, D)), whole((K, r, w)),
            whole((8, LANES)), hbm, hbm,
        ],
        out_shape=[
            jax.ShapeDtypeStruct((K, R, w), bf16),
            jax.ShapeDtypeStruct((R, DI), f32),
            jax.ShapeDtypeStruct((D, R), bf16),
            jax.ShapeDtypeStruct((DI, R), bf16),
            jax.ShapeDtypeStruct((R, D), bf16),
            jax.ShapeDtypeStruct((2, R, LANES), f32),
            jax.ShapeDtypeStruct((16, C), f32),
            jax.ShapeDtypeStruct((8, D), f32),
            jax.ShapeDtypeStruct((K, r, w), bf16),
            jax.ShapeDtypeStruct((8, LANES), f32),
            jax.ShapeDtypeStruct((K, A0, A * A, 2, r, w), bf16),
            jax.ShapeDtypeStruct((A0, A * A, 2, ro, D), bf16),
        ],
        scratch_shapes=[
            pltpu.VMEM((R, D), bf16),
            pltpu.VMEM((2, A0, A * A, 2, r, w), bf16),
            pltpu.VMEM((2, A0, A * A, 2, ro, wc), bf16),
            pltpu.VMEM((2, R, w), bf16),
            pltpu.VMEM((R, DI), f32),
            pltpu.VMEM((R, DI), bf16),
            pltpu.VMEM((SEQ_F * half // LANES, FRONT + T, LANES), f32),
            pltpu.VMEM((S, T, LANES), f32),
            pltpu.VMEM((S, LANES, T), f32),
            pltpu.VMEM((S, T, T), f32),
            pltpu.VMEM((T, T), f32),
            pltpu.VMEM((R, LANES), f32),
            pltpu.VMEM((T, LANES), f32),
            pltpu.SemaphoreType.DMA((2,)),
            pltpu.SemaphoreType.DMA((2,)),
        ]
        + Gather.scratch(2 * K, A0, A) + Gather.scratch(2 * KO, A0, A),
        compiler_params=pltpu.CompilerParams(
            collective_id=1, has_side_effects=True, vmem_limit_bytes=VMEM,
        ),
        cost_estimate=pl.CostEstimate(
            flops=2 * R * D * K * w, bytes_accessed=D * K * w * 60, transcendentals=0
        ),
        name="forward",
    )(skip, tok, inw, *smalls, ow, tok, go)


def backward(dims, axis, geom, K, KO, E, proj, proj0, ssd, wo, wf, uT, mT, go, wl, tabs, pars,
             hpar, dn, outc, dns, sums,
             uo, mo, dmx, dpj, pad, dpad, ldtab, rowtab, scores, dscores, dlog, csum, bcs, mask,
             cacc, dacc, hacc, small, wv, csem, wsem, *refs):
    T, DI, C, H, HD, ST, KW = (dims[k] for k in ("T", "DI", "C", "H", "HD", "ST", "KW"))
    A0, A = geom
    at = Place(axis, A0, A)
    i = pl.program_id(0)
    R = ssd.shape[0]
    _, r, w = wl.shape
    N = A0 * A * A
    half = w // 2
    S = R // T
    HP = LANES // HD
    TC = half // LANES
    D = go.shape[1]
    HF = mT.shape[2]
    each = KO // HF
    pairs = (K + 1) // 2

    def begun(t):
        step = lax.div(t, 2)
        ends = lax.rem(t, 2) == 1
        outer = (lax.rem(step, 2) == 0) & (step < 2 * KO)
        valid = (t >= 0) & ((ends & (step < K)) | (jnp.logical_not(ends) & outer))
        done = jnp.minimum(lax.div(step + 1, 2), KO)
        return valid, step + done + (ends & outer).astype(jnp.int32)

    net = Reduce(at, K + KO, begun, refs[:15])
    total = SumAll(at, refs[15:])

    def fetches():
        out = [(uT.at[:, at.c], uo.at[0]), (uT.at[:, 1 - at.c], uo.at[1])]
        return [pltpu.make_async_copy(s, d, csem.at[k]) for k, (s, d) in enumerate(out)]

    def fetch_half(h):
        out = [(mT.at[:, at.c, h], mo.at[0]), (mT.at[:, 1 - at.c, h], mo.at[1])]
        return [pltpu.make_async_copy(s, d, csem.at[2 + k]) for k, (s, d) in enumerate(out)]

    @pl.when(i == 0)
    def _():
        at.greet()
        for cp in fetches() + fetch_half(0):
            cp.start()
        for ref in (cacc, dacc, hacc, dlog, csum, dscores, dns):
            ref[...] = jnp.zeros_like(ref)
        row, col = iotas(T, T)
        mask[...] = jnp.where(row <= col, BIG, -BIG)
        pad[:, 0:FRONT, :] = jnp.zeros((pad.shape[0], FRONT, LANES), f32)
        dpad[:, T:, :] = jnp.zeros((dpad.shape[0], FRONT, LANES), f32)

        def seq(s, _):
            rows = pl.ds(pl.multiple_of(s * T, T), T)
            for a in range(2):
                conv = conv_of(dims, proj0[0, rows, a * LANES : (a + 1) * LANES], pars, pad.at[a],
                               DI + a * ST)
                bcs[a, rows, :] = (conv * sigmoid(conv)).astype(bf16)
            scores[s] = lax.dot_general(
                bcs[0, rows, :], bcs[1, rows, :], (((1,), (1,)), ((), ())),
                preferred_element_type=f32,
            )
            _, _, _, ld, ld2 = steps_of(
                dims, proj0[0, rows, 2 * LANES : 3 * LANES].astype(f32), hpar
            )
            ldtab[s] = ld2
            rowtab[s] = ld.T
            return 0

        lax.fori_loop(0, S, seq, 0)
        for cp in fetches() + fetch_half(0):
            cp.wait()
        at.meet()

    for h in range(1, HF):

        @pl.when(i == 2 * h * each - 1)
        def _(h=h):
            for cp in fetch_half(h):
                cp.start()

        @pl.when(i == 2 * h * each)
        def _(h=h):
            for cp in fetch_half(h):
                cp.wait()

    def finish(p, v):
        inner = (p >= 3 * KO) | (lax.rem(p, 3) > 0)

        @pl.when(inner)
        def _():
            g = jnp.where(p >= 3 * KO, p - KO, p - 1 - lax.div(p, 3))
            outc[g] = v
            q = v * wl[lax.rem(g + 1, K)].astype(f32)
            part = q[:, 0:LANES]
            for k in range(1, w // LANES):
                part = part + q[:, k * LANES : (k + 1) * LANES]
            dns[...] += part

        @pl.when(jnp.logical_not(inner))
        def _():
            outc[K + lax.div(p, 3)] = v

    def send_out():
        k = lax.div(i, 2)
        net.step(2 * i, finish)

        @pl.when((lax.rem(i, 2) == 0) & (k < KO))
        def _():
            net.begin(3 * k, mo, go[:, columns(lax.rem(k, each), w)])

    def fetch(t, q):
        return pltpu.make_async_copy(
            wf.at[2 * t + q], wv.at[:, q * w : (q + 1) * w], wsem.at[q]
        )

    def fetch_pair(t, act):
        act(fetch(t, 0))

        @pl.when(2 * t + 1 < K)
        def _():
            act(fetch(t, 1))

    @pl.when(i == 0)
    def _():
        fetch_pair(0, lambda cp: cp.start())

    slot = lax.rem(lax.div(i, 2), dpj.shape[0])
    off = lax.rem(i, 2) * w
    here_of = lambda lane: pl.ds(pl.multiple_of(off + lane, LANES), LANES)

    def conv_back(rows, lane0, c0, dact, conv, sig, u):
        lanes = pl.ds(c0, LANES)
        dconv = dact * (sig * (1.0 + conv * (1.0 - sig)))
        dpad[u, 0:T, :] = dconv
        dcin = dconv * pars[KW - 1 : KW, lanes]
        for k in range(KW - 1):
            dcin = dcin + dpad[u, KW - 1 - k : KW - 1 - k + T, :] * pars[k : k + 1, lanes]
        dpj[slot, rows, here_of(lane0)] = dcin.astype(bf16)
        for k in range(KW):
            start = FRONT - KW + 1 + k
            cacc[8 * k : 8 * k + 8, lanes] += sum8(dconv * pad[u, start : start + T, :])
        cacc[8 * KW : 8 * KW + 8, lanes] += sum8(dconv)

    @pl.when(i < K - 1)
    def _():
        h0 = i * TC * HP
        dmx[...] = lax.dot_general(
            go[...], wo[...], (((1,), (1,)), ((), ())), preferred_element_type=f32
        )

        def seq(s, q):
            rows = pl.ds(pl.multiple_of(s * T, T), T)
            turned = pltpu.roll(ldtab[s], LANES - h0, 1)
            rb, mb = tabs[0, rows, :], tabs[1, rows, :]
            parts = None
            for u in range(TC):
                c0 = pl.multiple_of(i * half + u * LANES, LANES)
                lanes = pl.ds(c0, LANES)
                here = slice(u * LANES, (u + 1) * LANES)
                there = slice(half + u * LANES, half + (u + 1) * LANES)
                conv = conv_of(dims, proj[0, rows, there], pars, pad.at[q * TC + u], c0)
                sig = sigmoid(conv)
                x = (conv * sig).astype(bf16)
                xf = x.astype(f32)
                gate = proj[0, rows, here].astype(f32)
                gs = sigmoid(gate)
                act = gate * gs
                o = ssd[rows, here]
                dm = dmx[rows, here]
                gated = o * act
                dgated = rb * (dm * pars[8 + KW + 1 : 8 + KW + 2, lanes]) - gated * mb
                dacc[8:16, lanes] += sum8(dm * (gated * rb))
                dssd = dgated * act
                dpj[slot, rows, here_of(u * LANES)] = (
                    dgated * o * (gs * (1.0 + gate * (1.0 - gs)))
                ).astype(bf16)
                low = dssd.astype(bf16)
                dacc[0:8, lanes] += sum8(dssd * xf)
                lows = stack_heads(dims, low)
                dmix = lax.dot_general(
                    x, lows, (((1,), (1,)), ((), ())), preferred_element_type=f32
                )
                mix = []
                part = None
                for a in range(HP):
                    k = u * HP + a
                    right = jnp.broadcast_to(turned[:, k : k + 1], (T, T))
                    decay = jnp.exp2(
                        jnp.minimum(rowtab[s, pl.ds(h0 + k, 1), :] - right, mask[...])
                    )
                    mix.append((decay * scores[s]).astype(bf16))
                    term = dmix[:, a * T : (a + 1) * T] * decay
                    part = term if part is None else part + term
                core = jnp.dot(
                    jnp.concatenate(mix, axis=1), lows, preferred_element_type=f32
                )
                sk = pars[8:9, lanes]
                from_cols = xf * core
                diff = low.astype(f32) * (o - sk * xf) - from_cols
                prow, pcol = iotas(LANES, LANES)
                place = (pcol == h0 + u * HP + prow // HD).astype(bf16)
                both = jnp.concatenate([diff, from_cols], axis=0)
                hi = both.astype(bf16)
                lo = (both - hi.astype(f32)).astype(bf16)
                by_head = jnp.dot(
                    jnp.concatenate([hi, lo], axis=1),
                    jnp.concatenate([place, place], axis=0), preferred_element_type=f32,
                )
                conv_back(rows, half + u * LANES, c0, core + sk * dssd, conv, sig,
                          q * TC + u)
                new = (part, by_head)
                parts = new if parts is None else tuple(p + q for p, q in zip(parts, new))
            dscores[s] += parts[0]
            dlog[rows, :] += parts[1][0:T]
            csum[rows, :] += parts[1][T:]

        several(S // 2, SEQ_B, seq)
        send_out()
        several(S // 2, SEQ_B, lambda s, q: seq(S // 2 + s, q))

    @pl.when(i == K - 1)
    def _():
        row, col = iotas(T, T)
        upper = (row <= col).astype(f32)

        def seq(s, _):
            rows = pl.ds(pl.multiple_of(s * T, T), T)
            ds = dscores[s]
            dact = (
                jnp.dot(ds.astype(bf16), bcs[1, rows, :], preferred_element_type=f32),
                jnp.dot(ds.T.astype(bf16), bcs[0, rows, :], preferred_element_type=f32),
            )
            for a in range(2):
                conv = conv_of(dims, proj0[0, rows, a * LANES : (a + 1) * LANES], pars, pad.at[a],
                               DI + a * ST)
                conv_back(rows, a * LANES, DI + a * ST, dact[a], conv, sigmoid(conv), a)
            v, e, step, _, _ = steps_of(
                dims, proj0[0, rows, 2 * LANES : 3 * LANES].astype(f32), hpar
            )
            dsteps = jnp.dot(
                upper, dlog[rows, :], precision=lax.Precision.HIGHEST,
                preferred_element_type=f32,
            )
            sg = jnp.where(v >= 0.0, 1.0, e) / (1.0 + e)
            ratio = jnp.where(step > 1e-30, sg / jnp.maximum(step, 1e-30), 1.0)
            ddt = csum[rows, :] * ratio + dsteps * hpar[1:2, :] * sg
            _, lane = iotas(T, LANES)
            ddt = jnp.where(lane < H, ddt, 0.0)
            dpj[slot, rows, here_of(2 * LANES)] = ddt.astype(bf16)
            dpj[slot, rows, here_of(3 * LANES)] = jnp.zeros((T, LANES), bf16)
            hacc[0:8, :] += sum8(ddt)
            hacc[8:16, :] += sum8(dsteps * step)
            return 0

        lax.fori_loop(0, S, seq, 0)
        small[...] = jnp.zeros_like(small)
        for k in range(KW + 1):
            small[k : k + 1, :] = jnp.sum(cacc[8 * k : 8 * k + 8, :], axis=0, keepdims=True)
        for k in range(2):
            small[KW + 1 + k : KW + 2 + k, 0:DI] = jnp.sum(
                dacc[8 * k : 8 * k + 8, :], axis=0, keepdims=True
            )
            small[KW + 3 : KW + 4, k * LANES : (k + 1) * LANES] = jnp.sum(
                hacc[8 * k : 8 * k + 8, :], axis=0, keepdims=True
            )
        total.start(0, small[...])

    tail = pairs - dpj.shape[0] + i - K
    t = jnp.where(i < K, lax.div(i - 7, 2), tail)
    turn = jnp.where(
        i < K, (i >= 7) & (lax.rem(i, 2) == 1) & (t < pairs - dpj.shape[0]), t >= 0
    )

    @pl.when(turn)
    def _():
        fetch_pair(t, lambda cp: cp.wait())
        mine = lax.rem(t, dpj.shape[0])

        def add(part):
            @pl.when(t == 0)
            def _():
                dn[...] = part()

            @pl.when(t > 0)
            def _():
                dn[...] += part()

        @pl.when(2 * t + 1 < K)
        def _():
            add(lambda: lax.dot_general(
                dpj[mine], wv[...], (((1,), (1,)), ((), ())), preferred_element_type=f32
            ))

        @pl.when(2 * t + 1 >= K)
        def _():
            add(lambda: lax.dot_general(
                dpj[mine, :, 0:w], wv[:, 0:w], (((1,), (1,)), ((), ())),
                preferred_element_type=f32,
            ))

        @pl.when(t + 1 < pairs)
        def _():
            fetch_pair(t + 1, lambda cp: cp.start())

    @pl.when(i >= K - 1)
    def _():
        net.step(2 * i, finish)

    net.step(2 * i + 1, finish)

    @pl.when(i < K)
    def _():
        net.begin(begun(2 * i + 1)[1], uo, dpj[slot, :, pl.ds(pl.multiple_of(off, w), w)])

    for stage in range(1, 4):

        @pl.when(i == K - 1 + stage)
        def _(stage=stage):
            total.start(stage, total.finish(stage - 1))

    @pl.when(i == K + 3)
    def _():
        sums[...] = total.finish(3)

    @pl.when(i == K + 3)
    def _():
        net.drain()


def run_backward_net(dims, axis, geom, E, proj, ssd, ofull, wfull, uT, mT, go, wl, tabs, pars,
                     hpar):
    T, DI, C, H, KW, ST = (dims[k] for k in ("T", "DI", "C", "H", "KW", "ST"))
    A0, A = geom
    N = A0 * A * A
    K, R, w = proj.shape
    r = wl.shape[1]
    D = go.shape[1]
    ro = DI // (2 * N)
    HF = ro // r
    half = w // 2
    S = R // T
    KO = HF * (D // w)
    assert 2 * KO <= K + 1 and HF * r == ro and D % w == 0
    whole = lambda s: pl.BlockSpec(s, lambda i: (0,) * len(s), pipeline_mode=pl.Buffered(1))
    tile = lambda i: jnp.clip(i, 0, K - 2)
    hbm = pl.BlockSpec(memory_space=pl.ANY)
    return pl.pallas_call(
        functools.partial(backward, dims, axis, geom, K, KO, E),
        grid=(K + 4,),
        in_specs=[
            pl.BlockSpec((1, R, w), lambda i: (tile(i) + 1, 0, 0)),
            whole((1, R, w)),
            pl.BlockSpec((R, half), lambda i: (0, tile(i))),
            pl.BlockSpec((half, D), lambda i: (tile(i), 0)),
            hbm, hbm, hbm, whole((R, D)), whole((K, r, w)), whole((2, R, LANES)), whole((16, C)),
            whole((8, LANES)),
        ],
        out_specs=[whole((R, D)), whole((K + KO, r, w)), whole((r, LANES)), whole((8, C))],
        out_shape=[
            jax.ShapeDtypeStruct((R, D), f32),
            jax.ShapeDtypeStruct((K + KO, r, w), f32),
            jax.ShapeDtypeStruct((r, LANES), f32),
            jax.ShapeDtypeStruct((8, C), f32),
        ],
        scratch_shapes=[
            pltpu.VMEM((2, N, r, R), bf16),
            pltpu.VMEM((2, N, r, R), bf16),
            pltpu.VMEM((R, half), f32),
            pltpu.VMEM((4, R, 2 * w), bf16),
            pltpu.VMEM((2 * SEQ_B, FRONT + T, LANES), f32),
            pltpu.VMEM((2 * SEQ_B, FRONT + T, LANES), f32),
            pltpu.VMEM((S, T, LANES), f32),
            pltpu.VMEM((S, LANES, T), f32),
            pltpu.VMEM((S, T, T), f32),
            pltpu.VMEM((S, T, T), f32),
            pltpu.VMEM((R, LANES), f32),
            pltpu.VMEM((R, LANES), f32),
            pltpu.VMEM((2, R, ST), bf16),
            pltpu.VMEM((T, T), f32),
            pltpu.VMEM((8 * (KW + 1), C), f32),
            pltpu.VMEM((16, DI), f32),
            pltpu.VMEM((16, LANES), f32),
            pltpu.VMEM((8, C), f32),
            pltpu.VMEM((D, 2 * w), bf16),
            pltpu.SemaphoreType.DMA((4,)),
            pltpu.SemaphoreType.DMA((2,)),
        ]
        + Reduce.scratch(K + KO, A0, A, r, w)
        + SumAll.scratch(A0, A, (8, C)),
        compiler_params=pltpu.CompilerParams(
            collective_id=2, has_side_effects=True, vmem_limit_bytes=VMEM,
        ),
        cost_estimate=pl.CostEstimate(
            flops=6 * R * D * K * w, bytes_accessed=D * K * w * 90, transcendentals=0
        ),
        name="backward",
    )(proj, proj, ssd, ofull.reshape(DI, D), wfull.reshape(K, D, w), uT.reshape(N, 2, r, R),
      mT.reshape(N, 2, HF, r, R), go, wl, tabs, pars, hpar)


def conclude(dims, axis, K, E, dn, tok, go, out, scale, outc, dns, sums, ns, hpar,
             dtok, outs, dw, dow, dtaps, dbias, ddtb, dalog, dskip, dnorm, dgain, tmp):
    T, DI, C, H, HD, KW = (dims[k] for k in ("T", "DI", "C", "H", "HD", "KW"))
    outs[...] = out[...]
    u = tok[...].astype(f32)
    rs = lax.rsqrt(jnp.mean(u * u, axis=-1, keepdims=True) + epsilon)
    u = u * rs
    d = dn[...] * scale[0:1, :]
    m = jnp.mean(d * u, axis=-1, keepdims=True)
    dtok[...] = go[...].astype(f32) + rs * (d - u * m)

    @pl.when(pl.program_id(0) == 0)
    def _():
        me = lax.axis_index(axis)
        r, w = outc.shape[1:]
        half = w // 2
        for g in range(K - 1):
            dw[:, g * half : (g + 1) * half] = outc[g, :, 0:half]
            dw[:, DI + g * half : DI + (g + 1) * half] = outc[g, :, half:]
        dw[:, 2 * DI :] = outc[K - 1, :, 0 : E - 2 * DI]
        cols = dow.shape[1] // w
        for k in range(outc.shape[0] - K):
            h, c = k // cols, k % cols
            dow[h * r : (h + 1) * r, c * w : (c + 1) * w] = outc[K + k]

        def window(size):
            start = me * size
            base = jnp.minimum(lax.div(start, LANES), C // LANES - 2) * LANES
            v = sums[:, pl.ds(pl.multiple_of(base, LANES), 2 * LANES)]
            return pltpu.roll(v, lax.rem(2 * LANES - (start - base), 2 * LANES), 1)

        Cn, Gn = dbias.shape[0], dgain.shape[0]
        v = window(Cn)[:, 0:LANES]
        tmp[...] = jnp.zeros_like(tmp)
        tmp[0:8, :] = v
        dtaps[...] = tmp[...].T[0:Cn, 0:KW]
        dbias[...] = v[KW, 0:Cn]
        dgain[...] = window(Gn)[KW + 2, 0:Gn]
        ddtb[...] = sums[KW + 3, 0:H]
        dalog[...] = sums[KW + 3 : KW + 4, LANES : 2 * LANES][0, 0:H] * hpar[1, 0:H]
        tmp[0:r, :] = dns[...]
        tmp[r:, :] = jnp.zeros((LANES - r, LANES), f32)
        dnorm[...] = jnp.sum(tmp[...].T, axis=0)[0:r] / ns[0, :].astype(f32)
        tiles = DI // LANES
        tmp[...] = jnp.zeros_like(tmp)
        for t in range(tiles):
            tmp[t : t + 1, :] = sums[KW + 1 : KW + 2, t * LANES : (t + 1) * LANES]
        row, col = iotas(LANES, LANES)
        HP = LANES // HD
        fold = (row // HD == lax.rem(col, HP)).astype(f32)
        v = jnp.dot(tmp[...], fold, precision=lax.Precision.HIGHEST, preferred_element_type=f32)
        dskip[...] = jnp.sum(jnp.where(col // HP == row, v, 0.0), axis=0)[0:H]


def run_conclude(dims, axis, K, E, dn, tok, go, out, scale, outc, dns, sums, ns, hpar, ro):
    T, DI, C, H, KW = (dims[k] for k in ("T", "DI", "C", "H", "KW"))
    R, D = tok.shape
    r = outc.shape[1]
    n = D // r
    T = math.gcd(R, BLOCK)
    rows = pl.BlockSpec((T, D), lambda i: (i, 0))
    whole = lambda s: pl.BlockSpec(s, lambda i: (0,) * len(s))
    shapes = [(r, E), (ro, D), (C // n, KW), (C // n,), (H,), (H,), (H,), (r,), (DI // n,)]
    return pl.pallas_call(
        functools.partial(conclude, dims, axis, K, E),
        grid=(R // T,),
        in_specs=[rows, rows, rows, rows]
        + [whole(a.shape) for a in (scale, outc, dns, sums, ns, hpar)],
        out_specs=[rows, rows] + [whole(x) for x in shapes],
        out_shape=[jax.ShapeDtypeStruct((R, D), f32), jax.ShapeDtypeStruct((R, D), bf16)]
        + [jax.ShapeDtypeStruct(x, f32) for x in shapes],
        scratch_shapes=[pltpu.VMEM((LANES, LANES), f32)],
        name="conclude",
    )(dn, tok, go, out, scale, outc, dns, sums, ns, hpar)


def local(axis, n, tokens, in_weight, conv_weight, conv_bias, dt_bias, a_log, skip_d,
          norm_scale, gate_scale, out_weight, grad_out):
    MB, S, T, D = tokens.shape
    R = MB * S * T
    r, E = in_weight.shape
    H = a_log.shape[0]
    DI = out_weight.shape[0] * n
    Cn, KW = conv_weight.shape
    C = Cn * n
    HD = DI // H
    ST = (C - DI) // 2
    dims = dict(T=T, DI=DI, C=C, H=H, HD=HD, ST=ST, KW=KW)
    assert LANES % HD == 0 and ST == LANES and DI % (LANES * 2) == 0 and T % 16 == 0
    geom = geometry(n)
    w = CHUNK
    Gn, ro = DI // n, out_weight.shape[0]
    own = (
        geom is not None and r % 16 == 0 and ro % r == 0 and D % w == 0 and DI % (w // 2) == 0
        and w == 2 * ST + 2 * LANES and E == 2 * DI + 2 * ST + H and H <= LANES
        and max(Cn, Gn) < LANES and 6 <= KW + 2 <= 8 and 2 * (ro // r) * (D // w) <= DI * 2 // w + 2
    )
    me = lax.axis_index(axis)
    tok = tokens.reshape(R, D)
    go = grad_out.reshape(R, D)
    if own:
        row = lambda v: v.reshape(1, -1)
        K = DI * 2 // w + 1
        smalls = [conv_weight.T] + [
            row(v) for v in (conv_bias, gate_scale, norm_scale, dt_bias, a_log)
        ]
        proj, ssd, uT, mT, output, tabs, pars, scale, wl, hpar, wfull, ofull = run_forward_net(
            dims, axis, geom, K, w, skip_d, tok, go, in_weight, smalls, out_weight
        )
        dn, outc, dns, sums = run_backward_net(
            dims, axis, geom, E, proj, ssd, ofull, wfull, uT, mT, go, wl, tabs, pars, hpar
        )
        dtok, output, dw, dow, dtaps, dbias, ddtb, dalog, dskip, dnorm, dgain = run_conclude(
            dims, axis, K, E, dn, tok, go, output, scale, outc, dns, sums, row(norm_scale), hpar,
            ro,
        )
        return (
            output.reshape(tokens.shape), dtok.reshape(tokens.shape), dw, dtaps, dbias, ddtb,
            dalog, dskip, dnorm, dgain, dow,
        )
    rate = -jnp.exp(a_log)
    hpar = jnp.pad(jnp.stack([dt_bias, rate]), ((0, 6), (0, LANES - H)))
    skip = jnp.broadcast_to(jnp.repeat(skip_d, HD)[None], (8, DI))
    ns = norm_scale.astype(f32)
    out_full = lax.all_gather(out_weight, axis, axis=0, tiled=True)
    wfull = lax.all_gather(in_weight, axis, axis=0, tiled=True)
    conv = lax.all_gather(jnp.concatenate([conv_weight.T, conv_bias[None]]), axis, axis=0)
    conv = conv.transpose(1, 0, 2).reshape(KW + 1, C).astype(f32)
    gate = lax.all_gather(gate_scale, axis, axis=0).reshape(1, DI).astype(f32)
    scale = lax.all_gather(norm_scale, axis, axis=0).reshape(1, D).astype(f32)
    u = tok.astype(f32)
    u = u * lax.rsqrt(jnp.mean(u * u, axis=-1, keepdims=True) + epsilon)
    uh = (u * scale).astype(bf16)
    proj = jnp.dot(uh, wfull, preferred_element_type=f32).astype(bf16)
    cpar = jnp.pad(conv, ((0, 8 - KW - 1), (0, 0)))
    dpar = jnp.concatenate([skip[:1], gate, skip[2:]], axis=0)
    mixed, ssd, rstd = run_forward(dims, proj, cpar, hpar, dpar)
    output = jnp.dot(mixed, out_full, preferred_element_type=f32)
    output = (tok.astype(f32) + output).astype(bf16)
    d_mixed = lax.dot_general(
        go, out_full, (((1,), (1,)), ((), ())), preferred_element_type=f32
    )
    dproj, small = run_backward(dims, proj, d_mixed, ssd, rstd, cpar, hpar, dpar)
    left = (((0,), (0,)), ((), ()))
    g_out = lax.dot_general(mixed, go, left, preferred_element_type=f32).astype(bf16)
    dow = lax.psum_scatter(g_out, axis, scatter_dimension=0, tiled=True).astype(f32)
    g_in = lax.dot_general(uh, dproj, left, preferred_element_type=f32).astype(bf16)
    dw = lax.psum_scatter(g_in, axis, scatter_dimension=0, tiled=True).astype(f32)
    dns = dw * in_weight.astype(f32)
    dn = lax.dot_general(dproj, wfull, (((1,), (1,)), ((), ())), preferred_element_type=f32)
    sums = lax.psum(small, axis)
    u = tok.astype(f32)
    rs = lax.rsqrt(jnp.mean(u * u, axis=-1, keepdims=True) + epsilon)
    u, d = u * rs, dn * scale
    dtok = go.astype(f32) + rs * (d - u * jnp.mean(d * u, axis=-1, keepdims=True))
    dconv = lax.dynamic_slice(sums, (0, me * Cn), (KW + 1, Cn))
    heads = sums[KW + 3]
    return (
        output.reshape(tokens.shape),
        dtok.reshape(tokens.shape),
        dw,
        dconv[:KW].T,
        dconv[KW],
        heads[:H],
        heads[LANES : LANES + H] * rate,
        sums[KW + 1, :DI].reshape(H, HD).sum(axis=1),
        dns.sum(axis=1) / ns,
        lax.dynamic_slice(sums[KW + 2], (me * Gn,), (Gn,)),
        dow,
    )


def solution(mesh):
    axis = mesh.axis_names[0]
    n = mesh.shape[axis]
    rows, flat, batch = P(axis, None), P(axis), P(None, axis, None, None)
    return jax.shard_map(
        functools.partial(local, axis, n),
        mesh=mesh,
        in_specs=(batch, rows, rows, flat, P(), P(), P(), flat, flat, rows, batch),
        out_specs=(batch, batch, rows, rows, flat, P(), P(), P(), flat, flat, rows),
        check_vma=False,
    )
```
